32 devices in a mesh: dp: 8 (over z, x), tensor: 4 (over y, core).
Axes of the slice: x: 2, y: 2, z: 4, core: 2. Of those that a mesh axis runs over, the one named last changes fastest.
Arguments:
- incoming_signals: bfloat16 [4096, 2048], P(('dp', 'tensor')), may hold values from -6 to 6
- loss_sensitivity: bfloat16 [4096, 2048], P(('dp', 'tensor')), may hold values from -6 to 6
- token_counts_per_slot: int32 [8], P('dp'), may hold values from 1 to 512, as said below
- leading_norm_multiplier: bfloat16 [2048], P('dp'), may hold values from 0.099609375 to 1.8984375
- leading_norm_offset: bfloat16 [2048], P('dp'), may hold values from -1.5 to 1.5
- question_projection: bfloat16 [2048, 2048], P('dp', 'tensor'), may hold values from -0.125 to 0.125
- lookup_projection: bfloat16 [2048, 2048], P('dp', 'tensor'), may hold values from -0.125 to 0.125
- content_projection: bfloat16 [2048, 4096], P('dp', 'tensor'), may hold values from -0.125 to 0.125
- silu_switch_projection: bfloat16 [2048, 4096], P('dp', 'tensor'), may hold values from -0.125 to 0.125
- retention_result_projection: bfloat16 [4096, 2048], P('tensor', 'dp'), may hold values from -0.09375 to 0.09375
- trailing_norm_multiplier: bfloat16 [2048], P('dp'), may hold values from 0.099609375 to 1.8984375
- trailing_norm_offset: bfloat16 [2048], P('dp'), may hold values from -1.5 to 1.5
- feedforward_switch_projection: bfloat16 [2048, 4096], P('dp', 'tensor'), may hold values from -0.125 to 0.125
- expanding_projection: bfloat16 [2048, 4096], P('dp', 'tensor'), may hold values from -0.125 to 0.125
- contracting_projection: bfloat16 [4096, 2048], P('tensor', 'dp'), may hold values from -0.09375 to 0.09375
Outputs:
- layer_output: bfloat16 [4096, 2048], P(('dp', 'tensor'))
- input_delta: float32 [4096, 2048], P(('dp', 'tensor'))
- before_scale_gradient: float32 [2048], P('dp')
- before_bias_gradient: float32 [2048], P('dp')
- query_gradient: float32 [2048, 2048], P('dp', 'tensor')
- key_gradient: float32 [2048, 2048], P('dp', 'tensor')
- value_gradient: float32 [2048, 4096], P('dp', 'tensor')
- swish_gradient: float32 [2048, 4096], P('dp', 'tensor')
- output_gradient: float32 [4096, 2048], P('tensor', 'dp')
- after_scale_gradient: float32 [2048], P('dp')
- after_bias_gradient: float32 [2048], P('dp')
- gate_gradient: float32 [2048, 4096], P('dp', 'tensor')
- up_gradient: float32 [2048, 4096], P('dp', 'tensor')
- down_gradient: float32 [4096, 2048], P('tensor', 'dp')
The draws below stay inside these ranges and needn't reach their ends.
Inputs may be any that keep to these rules, and one draw needn't show every extreme that they name: token_counts_per_slot[s] counts the valid leading rows of slot s, the slot being 512 consecutive rows; at least one sequence fills its slot.
All inputs are finite; a program needn't handle non-finite values.
Results may differ from the reference program's by a relative error of at most 0.024.
Values may be sent and summed in bfloat16 or wider, within the bound.
A program may use at most 192 MiB of HBM per device.

```python
import jax
import jax.numpy as jnp
from jax import lax

HIDDEN_SIZE = 2048
HEADS = 8
KEY_DIM = 256
VAL_DIM = 512
FF = 4096
SEQ_LEN = 512
SEQS = 8
TOKENS = 4096


def draw_token_counts_per_slot(key, part):
    first_key, second_key = jax.random.split(jax.random.fold_in(key, 17))
    drawn = jax.random.randint(first_key, (SEQS,), 1, SEQ_LEN + 1)
    chosen = jax.random.randint(second_key, (), 0, SEQS)
    return jnp.where(jnp.arange(SEQS) == chosen, SEQ_LEN, drawn).astype(jnp.int32)


def block_levels(key, dims, pieces, smallest, high):
    def one(axis_at, blocks):
        draws = jax.random.uniform(jax.random.fold_in(jax.random.fold_in(key, 6), axis_at), (blocks,), jnp.float32, smallest / len(pieces), high / len(pieces))
        return jnp.repeat(jnp.exp(draws), dims[axis_at] // blocks).reshape((-1,) + (1,) * (len(dims) - axis_at - 1))

    loudness = one(*pieces[0])
    for cut in pieces[1:]:
        loudness = loudness * one(*cut)
    return loudness


def scatter_about(key, extent, spread, bound, pieces=(), kind=jnp.bfloat16):
    gain = block_levels(key, extent, pieces, -0.22, 0.18) if pieces else 1.0
    result = jax.random.normal(key, extent, jnp.float32) * spread * gain
    return jnp.minimum(jnp.maximum(result, -bound), bound).astype(kind)


def setup_inputs(seed: int = 0) -> dict:
    key_of = jax.random.split(jax.random.key(seed), 16)
    return {
        "incoming_signals": scatter_about(key_of[0], (TOKENS, HIDDEN_SIZE), 1.0, 6.0, ((0, 32),)),
        "loss_sensitivity": scatter_about(key_of[1], (TOKENS, HIDDEN_SIZE), 1.0, 6.0, ((0, 32),)),
        "token_counts_per_slot": draw_token_counts_per_slot(jax.random.fold_in(key_of[15], 71), 0),
        "leading_norm_multiplier": jnp.clip(1.0 + 0.18 * jax.random.normal(key_of[3], (HIDDEN_SIZE,), jnp.float32), 0.099609375, 1.8984375).astype(jnp.bfloat16),
        "leading_norm_offset": scatter_about(key_of[4], (HIDDEN_SIZE,), 0.3, 1.5, ((0, 8),)),
        "question_projection": scatter_about(key_of[5], (HIDDEN_SIZE, HEADS * KEY_DIM), HIDDEN_SIZE ** -0.5, 0.125, ((0, 8), (1, 4))),
        "lookup_projection": scatter_about(key_of[6], (HIDDEN_SIZE, HEADS * KEY_DIM), HIDDEN_SIZE ** -0.5, 0.125, ((0, 8), (1, 4))),
        "content_projection": scatter_about(key_of[7], (HIDDEN_SIZE, HEADS * VAL_DIM), HIDDEN_SIZE ** -0.5, 0.125, ((0, 8), (1, 4))),
        "silu_switch_projection": scatter_about(key_of[8], (HIDDEN_SIZE, HEADS * VAL_DIM), HIDDEN_SIZE ** -0.5, 0.125, ((0, 8), (1, 4))),
        "retention_result_projection": scatter_about(key_of[9], (HEADS * VAL_DIM, HIDDEN_SIZE), (HEADS * VAL_DIM) ** -0.5, 0.09375, ((0, 4), (1, 8))),
        "trailing_norm_multiplier": jnp.clip(1.0 + 0.18 * jax.random.normal(key_of[10], (HIDDEN_SIZE,), jnp.float32), 0.099609375, 1.8984375).astype(jnp.bfloat16),
        "trailing_norm_offset": scatter_about(key_of[11], (HIDDEN_SIZE,), 0.3, 1.5, ((0, 8),)),
        "feedforward_switch_projection": scatter_about(key_of[12], (HIDDEN_SIZE, FF), HIDDEN_SIZE ** -0.5, 0.125, ((0, 8), (1, 4))),
        "expanding_projection": scatter_about(key_of[13], (HIDDEN_SIZE, FF), HIDDEN_SIZE ** -0.5, 0.125, ((0, 8), (1, 4))),
        "contracting_projection": scatter_about(key_of[14], (FF, HIDDEN_SIZE), FF ** -0.5, 0.09375, ((0, 4), (1, 8))),
    }


EPSILON = 1e-05
GROUP_EPSILON = 0.1

def normalize(values, epsilon):
    centre = values - lax.optimization_barrier(jnp.mean(values, axis=-1, keepdims=True))
    inverse = lax.rsqrt(lax.optimization_barrier(jnp.mean(centre * centre, axis=-1, keepdims=True)) + epsilon)
    return (centre * inverse, inverse)

def normalize_back(upstream, normed, inverse):
    return inverse * (upstream - lax.optimization_barrier(jnp.mean(upstream, axis=-1, keepdims=True)) - normed * lax.optimization_barrier(jnp.mean(upstream * normed, axis=-1, keepdims=True)))

def rotate_half(values):
    middle = values.shape[-1] // 2
    return jnp.concatenate([-values[..., middle:], values[..., :middle]], axis=-1)

def rotary_tables(span, columns):
    middle = columns // 2
    places = jnp.arange(span, dtype=jnp.int32).astype(jnp.float32)
    spectrum = 10000.0 ** (-jnp.arange(middle, dtype=jnp.int32).astype(jnp.float32) / middle)
    angles = places[:, None] * spectrum[None, :]
    angles = jnp.concatenate([angles, angles], axis=1)
    return (jnp.cos(angles)[None, :, None, :], jnp.sin(angles)[None, :, None, :])

def decay_table(span, head_ids):
    log_rates = jnp.log(1.0 - jnp.exp2(-5.0 - head_ids.astype(jnp.float32)))
    places = jnp.arange(span, dtype=jnp.int32)
    offsets = places[:, None] - places[None, :]
    decayed = jnp.exp(jnp.maximum(offsets, 0).astype(jnp.float32)[None] * log_rates[:, None, None])
    return jnp.where(offsets[None] >= 0, decayed, 0.0)

def gelu_tanh(values):
    return jax.nn.gelu(values, approximate=True)

def matmul(left, right):
    return jnp.dot(left, right, preferred_element_type=jnp.float32)

def layer_block(block_input, block_cot, block_lengths, parameter_bundle, cosines, sines, decays):
    leading_norm_multiplier, leading_norm_offset, question_projection, lookup_projection, content_projection, silu_switch_projection, retention_result_projection, trailing_norm_multiplier, trailing_norm_offset, feedforward_switch_projection, expanding_projection, contracting_projection = parameter_bundle
    slot_count = block_lengths.shape[0]
    total_rows = block_input.shape[0]
    places = jnp.arange(SEQ_LEN, dtype=jnp.int32)
    valid_rows = (places[None, :] < block_lengths[:, None]).reshape(total_rows, 1)
    shape_key = (slot_count, SEQ_LEN, HEADS, KEY_DIM)
    shape_value = (slot_count, SEQ_LEN, HEADS, VAL_DIM)
    input_rows = block_input.astype(jnp.float32)
    initial_demeaned, first_inverse = normalize(input_rows, EPSILON)
    initial_standardized = (initial_demeaned * leading_norm_multiplier.astype(jnp.float32) + leading_norm_offset.astype(jnp.float32)).astype(jnp.bfloat16)
    query_proj = matmul(initial_standardized, question_projection)
    key_proj = matmul(initial_standardized, lookup_projection)
    value_proj = matmul(initial_standardized, content_projection)
    swish_proj = matmul(initial_standardized, silu_switch_projection)
    query_rot = (query_proj.reshape(shape_key) * cosines + rotate_half(query_proj.reshape(shape_key)) * sines).astype(jnp.bfloat16)
    key_rot = ((key_proj.reshape(shape_key) * cosines + rotate_half(key_proj.reshape(shape_key)) * sines) * KEY_DIM ** (-0.5)).astype(jnp.bfloat16)
    value_heads = value_proj.reshape(shape_value).astype(jnp.bfloat16)
    raw_scores = jnp.einsum('snhk,smhk->shnm', query_rot.astype(jnp.float32), key_rot.astype(jnp.float32))
    scores = (raw_scores * decays[None]).astype(jnp.bfloat16)
    retained = jnp.einsum('shnm,smhv->snhv', scores.astype(jnp.float32), value_heads.astype(jnp.float32))
    group_hat, group_inverse = normalize(retained, GROUP_EPSILON)
    swish_heads = swish_proj.reshape(shape_value)
    sigmoid_gate = jax.nn.sigmoid(swish_heads)
    gated = (swish_heads * sigmoid_gate * group_hat).reshape(total_rows, HEADS * VAL_DIM).astype(jnp.bfloat16)
    middle_rows = input_rows + matmul(gated, retention_result_projection)
    second_hat, second_inverse = normalize(middle_rows, EPSILON)
    second_normed = (second_hat * trailing_norm_multiplier.astype(jnp.float32) + trailing_norm_offset.astype(jnp.float32)).astype(jnp.bfloat16)
    gate_proj = matmul(second_normed, feedforward_switch_projection)
    up_proj = matmul(second_normed, expanding_projection)
    gelu_gate, gelu_back = jax.vjp(gelu_tanh, gate_proj)
    hidden = (gelu_gate * up_proj).astype(jnp.bfloat16)
    final_rows = middle_rows + matmul(hidden, contracting_projection)
    layer_output = jnp.where(valid_rows, final_rows, 0.0).astype(jnp.bfloat16)
    out_back = jnp.where(valid_rows, block_cot.astype(jnp.float32), 0.0)
    out_low = out_back.astype(jnp.bfloat16)
    down_gradient = matmul(hidden.T, out_low)
    hidden_back = matmul(out_low, contracting_projection.T)
    gate_back = gelu_back(hidden_back * up_proj)[0].astype(jnp.bfloat16)
    up_back = (hidden_back * gelu_gate).astype(jnp.bfloat16)
    gate_gradient = matmul(second_normed.T, gate_back)
    up_gradient = matmul(second_normed.T, up_back)
    mixer_input = matmul(gate_back, feedforward_switch_projection.T) + matmul(up_back, expanding_projection.T)
    after_scale_gradient = lax.optimization_barrier(jnp.sum(mixer_input * second_hat, axis=0))
    after_bias_gradient = lax.optimization_barrier(jnp.sum(mixer_input, axis=0))
    middle_back = out_back + normalize_back(mixer_input * trailing_norm_multiplier.astype(jnp.float32), second_hat, second_inverse)
    middle_low = middle_back.astype(jnp.bfloat16)
    output_gradient = matmul(gated.T, middle_low)
    gated_back = matmul(middle_low, retention_result_projection.T).reshape(shape_value)
    swish_back = (gated_back * group_hat * sigmoid_gate * (1.0 + swish_heads * (1.0 - sigmoid_gate))).reshape(total_rows, HEADS * VAL_DIM).astype(jnp.bfloat16)
    retained_back = normalize_back(gated_back * swish_heads * sigmoid_gate, group_hat, group_inverse).astype(jnp.bfloat16)
    score_back = (jnp.einsum('snhv,smhv->shnm', retained_back.astype(jnp.float32), value_heads.astype(jnp.float32)) * decays[None]).astype(jnp.bfloat16)
    query_rot_back = jnp.einsum('shnm,smhk->snhk', score_back.astype(jnp.float32), key_rot.astype(jnp.float32))
    key_rot_back = jnp.einsum('shnm,snhk->smhk', score_back.astype(jnp.float32), query_rot.astype(jnp.float32))
    value_back = jnp.einsum('shnm,snhv->smhv', scores.astype(jnp.float32), retained_back.astype(jnp.float32))
    query_back = (query_rot_back * cosines - rotate_half(query_rot_back) * sines).reshape(total_rows, HEADS * KEY_DIM).astype(jnp.bfloat16)
    key_back = ((key_rot_back * cosines - rotate_half(key_rot_back) * sines) * KEY_DIM ** (-0.5)).reshape(total_rows, HEADS * KEY_DIM).astype(jnp.bfloat16)
    value_low = value_back.reshape(total_rows, HEADS * VAL_DIM).astype(jnp.bfloat16)
    query_gradient = matmul(initial_standardized.T, query_back)
    key_gradient = matmul(initial_standardized.T, key_back)
    value_gradient = matmul(initial_standardized.T, value_low)
    swish_gradient = matmul(initial_standardized.T, swish_back)
    first_layer_input = matmul(query_back, question_projection.T) + matmul(key_back, lookup_projection.T) + matmul(value_low, content_projection.T) + matmul(swish_back, silu_switch_projection.T)
    before_scale_gradient = lax.optimization_barrier(jnp.sum(first_layer_input * initial_demeaned, axis=0))
    before_bias_gradient = lax.optimization_barrier(jnp.sum(first_layer_input, axis=0))
    input_delta = middle_back + normalize_back(first_layer_input * leading_norm_multiplier.astype(jnp.float32), initial_demeaned, first_inverse)
    weight_gradients = (before_scale_gradient, before_bias_gradient, query_gradient, key_gradient, value_gradient, swish_gradient, output_gradient, after_scale_gradient, after_bias_gradient, gate_gradient, up_gradient, down_gradient)
    return ((layer_output, input_delta), weight_gradients)

def reference(incoming_signals, loss_sensitivity, token_counts_per_slot, leading_norm_multiplier, leading_norm_offset, question_projection, lookup_projection, content_projection, silu_switch_projection, retention_result_projection, trailing_norm_multiplier, trailing_norm_offset, feedforward_switch_projection, expanding_projection, contracting_projection):
    block_slots = 8
    block_count = SEQS // block_slots
    block_rows = block_slots * SEQ_LEN
    cosines, sines = rotary_tables(SEQ_LEN, KEY_DIM)
    decays = decay_table(SEQ_LEN, jnp.arange(HEADS, dtype=jnp.int32))
    parameter_bundle = (leading_norm_multiplier, leading_norm_offset, question_projection, lookup_projection, content_projection, silu_switch_projection, retention_result_projection, trailing_norm_multiplier, trailing_norm_offset, feedforward_switch_projection, expanding_projection, contracting_projection)

    def step_block(totals, inputs):
        block_input, block_cot, block_lengths = inputs
        results, weight_gradients = layer_block(block_input, block_cot, block_lengths, parameter_bundle, cosines, sines, decays)
        return (tuple((total + delta for total, delta in zip(totals, weight_gradients))), results)
    zeros = tuple((jnp.zeros(weight_array.shape, jnp.float32) for weight_array in parameter_bundle))
    totals, results = lax.scan(step_block, zeros, (incoming_signals.reshape(block_count, block_rows, HIDDEN_SIZE), loss_sensitivity.reshape(block_count, block_rows, HIDDEN_SIZE), token_counts_per_slot.reshape(block_count, block_slots)))
    outputs = results[0].reshape(TOKENS, HIDDEN_SIZE)
    input_deltas = results[1].reshape(TOKENS, HIDDEN_SIZE)
    return (outputs, input_deltas, totals[0], totals[1], totals[2], totals[3], totals[4], totals[5], totals[6], totals[7], totals[8], totals[9], totals[10], totals[11])
```

```python
import functools

import jax
import jax.numpy as jnp
from jax import lax
from jax.experimental import pallas as pl
from jax.experimental.pallas import tpu as pltpu
from jax.sharding import PartitionSpec as P

KEY_DIM = 256
VAL_DIM = 512
SEQ_LEN = 512

EPSILON = 1e-05
GROUP_EPSILON = 0.1

MESH = pl.DeviceIdType.MESH
F32 = jnp.float32
BF16 = jnp.bfloat16
CHUNK = 16


def normalize(values, epsilon):
    centre = values - jnp.mean(values, axis=-1, keepdims=True)
    inverse = lax.rsqrt(jnp.mean(centre * centre, axis=-1, keepdims=True) + epsilon)
    return (centre * inverse, inverse)


def normalize_back(upstream, normed, inverse):
    return inverse * (
        upstream
        - jnp.mean(upstream, axis=-1, keepdims=True)
        - normed * jnp.mean(upstream * normed, axis=-1, keepdims=True)
    )


def rotate_half(values):
    middle = values.shape[-1] // 2
    return jnp.concatenate([-values[..., middle:], values[..., :middle]], axis=-1)


def rotary_tables(span, columns):
    middle = columns // 2
    places = jnp.arange(span, dtype=jnp.int32).astype(jnp.float32)
    spectrum = 10000.0 ** (-jnp.arange(middle, dtype=jnp.int32).astype(jnp.float32) / middle)
    angles = places[:, None] * spectrum[None, :]
    angles = jnp.concatenate([angles, angles], axis=1)
    return (jnp.cos(angles)[None], jnp.sin(angles)[None])


def decay_table(span, head_id):
    log_rate = jnp.log(1.0 - jnp.exp2(-5.0 - head_id.astype(jnp.float32)))
    places = jnp.arange(span, dtype=jnp.int32)
    offsets = places[:, None] - places[None, :]
    decayed = jnp.exp(jnp.maximum(offsets, 0).astype(jnp.float32) * log_rate)
    return jnp.where(offsets >= 0, decayed, 0.0)


def gelu_tanh(values):
    return jax.nn.gelu(values, approximate=True)


def matmul(left, right):
    return jnp.dot(left, right, preferred_element_type=jnp.float32)


class Place:
    def __init__(self):
        d, t = lax.axis_index("dp"), lax.axis_index("tensor")
        self.x, self.y, self.c = lax.rem(d, 2), t // 2, lax.rem(t, 2)
        dx, ty = d + 1 - 2 * self.x, (1 - self.y) * 2 + self.c
        self.sib = (d, t + 1 - 2 * self.c)
        self.xn = (dx, t)
        self.yn = (d, ty)

    def block(self, j, other_core=0):
        x = 1 - self.x if j in (1, 3) else self.x
        y = 1 - self.y if j in (2, 3) else self.y
        c = 1 - self.c if other_core else self.c
        return x * 4 + y * 2 + c


def greet(place):
    barrier = pltpu.get_barrier_semaphore()
    for partner in (place.sib, place.xn, place.yn):
        pl.semaphore_signal(barrier, inc=1, device_id=partner, device_id_type=MESH)
    pl.semaphore_wait(barrier, 3)


def rows_of(index, rows):
    return pl.ds(pl.multiple_of(index * rows, rows), rows)


class Gather:
    @staticmethod
    def scratch():
        return [pltpu.SemaphoreType.DMA((13,)), pltpu.SemaphoreType.DMA((13,))]

    def __init__(self, place, src, out, send, recv):
        rows = src.shape[0]
        half = rows // 2
        p = place

        def remote(k, source, j, lo, n, target, core=0):
            where = pl.ds(pl.multiple_of(p.block(j, core) * rows + lo, 8), n)
            source = source.at[pl.ds(lo, n)] if source is src else source.at[where]
            return pltpu.make_async_remote_copy(
                src_ref=source,
                dst_ref=out.at[where],
                send_sem=send.at[k],
                recv_sem=recv.at[k],
                device_id=target,
                device_id_type=MESH,
            )

        self.p, self.rows, self.half = p, rows, half
        self.local = pltpu.make_async_copy(src, out.at[rows_of(p.block(0), rows)], send.at[12])
        h = half
        self.xa = remote(0, src, 0, 0, h, p.xn)
        self.xb = remote(1, src, 0, h, h, p.xn)
        self.ya = remote(2, src, 0, 0, h, p.yn)
        self.yb = remote(3, src, 0, h, h, p.yn)
        self.s0 = remote(4, src, 0, 0, rows, p.sib)
        self.da = remote(5, out, 1, 0, h, p.yn)
        self.db = remote(6, out, 2, h, h, p.xn)
        self.s1 = remote(7, out, 1, 0, rows, p.sib)
        self.s2 = remote(8, out, 2, 0, rows, p.sib)
        self.s3a = remote(9, out, 3, 0, h, p.sib)
        self.s3b = remote(10, out, 3, h, h, p.sib)

    def start(self):
        for copy in (self.xa, self.yb, self.xb, self.ya, self.s0, self.local):
            copy.start()

    def forward(self):
        self.xa.wait_recv()
        self.da.start()
        self.yb.wait_recv()
        self.db.start()
        self.xb.wait_recv()
        self.s1.start()
        self.ya.wait_recv()
        self.s2.start()

    def finish(self):
        self.da.wait_recv()
        self.s3a.start()
        self.db.wait_recv()
        self.s3b.start()
        self.local.wait()
        for copy in (self.s0, self.s1, self.s2, self.s3a, self.s3b):
            copy.wait()
        for copy in (self.xa, self.xb, self.ya, self.yb, self.da, self.db):
            copy.wait_send()


class Reduce:
    @staticmethod
    def scratch(rows, columns):
        return [
            pltpu.VMEM((4, rows, columns), BF16),
            pltpu.VMEM((4, rows, columns), BF16),
            pltpu.VMEM((2, rows, columns), BF16),
            pltpu.VMEM((2, rows // 2, columns), BF16),
            pltpu.SemaphoreType.DMA((14,)),
            pltpu.SemaphoreType.DMA((10,)),
        ]

    def __init__(self, place, part, mine, theirs, got, across, send, recv):
        p = place
        rows = mine.shape[1]
        h = rows // 2
        self.rows, self.half = rows, h
        self.mine, self.theirs, self.got, self.across = mine, theirs, got, across

        def remote(k, source, target_ref, target):
            return pltpu.make_async_remote_copy(
                src_ref=source,
                dst_ref=target_ref,
                send_sem=send.at[k],
                recv_sem=recv.at[k],
                device_id=target,
                device_id_type=MESH,
            )

        a, b = pl.ds(0, h), pl.ds(h, h)
        self.load = [
            pltpu.make_async_copy(part.at[rows_of(p.block(j), rows)], mine.at[j], send.at[10 + j])
            for j in range(4)
        ]
        self.swap = [
            remote(j, part.at[rows_of(p.block(j, 1), rows)], theirs.at[j], p.sib) for j in range(4)
        ]
        self.da = remote(4, mine.at[3, a], across.at[0], p.xn)
        self.db = remote(5, mine.at[3, b], across.at[1], p.yn)
        self.xa = remote(6, mine.at[1, a], got.at[0, a], p.xn)
        self.xb = remote(7, mine.at[1, b], got.at[0, b], p.xn)
        self.ya = remote(8, mine.at[2, a], got.at[1, a], p.yn)
        self.yb = remote(9, mine.at[2, b], got.at[1, b], p.yn)

    def add(self, j, lo, n, other, other_lo):
        def body(i, carry):
            r = pl.ds(pl.multiple_of(lo + i * CHUNK, CHUNK), CHUNK)
            q = pl.ds(pl.multiple_of(other_lo + i * CHUNK, CHUNK), CHUNK)
            self.mine[j, r] = (self.mine[j, r].astype(F32) + other[q].astype(F32)).astype(BF16)
            return carry

        lax.fori_loop(0, n // CHUNK, body, 0)

    def start(self):
        for j in (3, 1, 2, 0):
            self.swap[j].start()
            self.load[j].start()

    def run(self):
        rows, h = self.rows, self.half
        for j, copies in ((3, (self.da, self.db)), (1, (self.xa,)), (2, (self.yb,))):
            self.load[j].wait()
            self.swap[j].wait_recv()
            self.add(j, 0, rows, self.theirs.at[j], 0)
            for copy in copies:
                copy.start()
        self.db.wait_recv()
        self.add(1, h, h, self.across.at[1], 0)
        self.xb.start()
        self.da.wait_recv()
        self.add(2, 0, h, self.across.at[0], 0)
        self.ya.start()
        self.load[0].wait()
        self.swap[0].wait_recv()
        for copy in (self.xa, self.yb, self.xb, self.ya):
            copy.wait_recv()

    def total(self, r):
        pieces = (self.mine[0, r], self.theirs[0, r], self.got[0, r], self.got[1, r])
        one, two, three, four = (piece.astype(F32) for piece in pieces)
        return (one + two) + (three + four)

    def finish(self):
        for copy in (*self.swap, self.da, self.db, self.xa, self.xb, self.ya, self.yb):
            copy.wait_send()


def chunks(rows, body):
    def step(i, carry):
        body(pl.ds(pl.multiple_of(i * CHUNK, CHUNK), CHUNK))
        return carry

    lax.fori_loop(0, rows // CHUNK, step, 0)


def first_kernel(x_ref, cot_ref, gains_ref, out_x, out_cot, normed, *sems):
    place = Place()
    greet(place)
    gain, shift = gains_ref[0:1, :], gains_ref[1:2, :]

    def body(r):
        hat, _ = normalize(x_ref[r].astype(F32), EPSILON)
        normed[r] = (hat * gain + shift).astype(BF16)

    chunks(x_ref.shape[0], body)
    one = Gather(place, normed, out_x, *sems[:2])
    two = Gather(place, cot_ref, out_cot, *sems[2:])
    one.start()
    two.start()
    one.forward()
    two.forward()
    one.finish()
    two.finish()


def second_kernel(part_ref, x_ref, gains_ref, out_all, middle_ref, normed, *scratch):
    place = Place()
    greet(place)
    reduce = Reduce(place, part_ref, *scratch[:6])
    reduce.start()
    reduce.run()
    gain, shift = gains_ref[2:3, :], gains_ref[3:4, :]

    def body(r):
        middle = x_ref[r].astype(F32) + reduce.total(r)
        middle_ref[r] = middle
        hat, _ = normalize(middle, EPSILON)
        normed[r] = (hat * gain + shift).astype(BF16)

    chunks(x_ref.shape[0], body)
    gather = Gather(place, normed, out_all, *scratch[6:])
    gather.start()
    gather.forward()
    gather.finish()
    reduce.finish()


def third_kernel(
    part_ref, middle_ref, cot_ref, gains_ref, out_all, back_ref, pieces_ref, low, *scratch
):
    place = Place()
    greet(place)
    reduce = Reduce(place, part_ref, *scratch[:6])
    reduce.start()
    pieces_ref[...] = jnp.zeros_like(pieces_ref)
    reduce.run()
    gain = gains_ref[2:3, :]

    def body(r):
        upstream = reduce.total(r)
        hat, inverse = normalize(middle_ref[r], EPSILON)
        scaled = upstream * hat
        pieces_ref[0] += scaled[0:8] + scaled[8:16]
        pieces_ref[1] += upstream[0:8] + upstream[8:16]
        back = cot_ref[r].astype(F32) + normalize_back(upstream * gain, hat, inverse)
        back_ref[r] = back
        low[r] = back.astype(BF16)

    chunks(middle_ref.shape[0], body)
    gather = Gather(place, low, out_all, *scratch[6:])
    gather.start()
    gather.forward()
    gather.finish()
    reduce.finish()


def fourth_kernel(
    first_ref, mixer_ref, x_ref, middle_ref, gains_ref, delta_ref, final_ref, pieces_ref, *scratch
):
    place = Place()
    greet(place)
    one = Reduce(place, first_ref, *scratch[:6])
    two = Reduce(place, mixer_ref, *scratch[6:])
    one.start()
    two.start()
    pieces_ref[...] = jnp.zeros_like(pieces_ref)
    one.run()
    two.run()
    gain = gains_ref[0:1, :]

    def body(r):
        upstream = one.total(r)
        hat, inverse = normalize(x_ref[r].astype(F32), EPSILON)
        scaled = upstream * hat
        pieces_ref[0] += scaled[0:8] + scaled[8:16]
        pieces_ref[1] += upstream[0:8] + upstream[8:16]
        delta_ref[r] = normalize_back(upstream * gain, hat, inverse)
        final_ref[r] = middle_ref[r] + two.total(r)

    chunks(x_ref.shape[0], body)
    one.finish()
    two.finish()


ANY = pl.BlockSpec(memory_space=pl.ANY)
VM = pl.BlockSpec(memory_space=pltpu.VMEM)


def call(kernel, ident, args, specs, outs, out_specs, scratch, nbytes):
    return pl.pallas_call(
        kernel,
        out_shape=outs,
        in_specs=specs,
        out_specs=out_specs,
        scratch_shapes=scratch,
        compiler_params=pltpu.CompilerParams(
            collective_id=ident, has_side_effects=True, vmem_limit_bytes=32 << 20
        ),
        cost_estimate=pl.CostEstimate(flops=0, bytes_accessed=nbytes, transcendentals=0),
        name=kernel.__name__,
    )(*args)


def per_device(
    groups,
    swap,
    incoming_signals,
    loss_sensitivity,
    token_counts_per_slot,
    leading_norm_multiplier,
    leading_norm_offset,
    question_projection,
    lookup_projection,
    content_projection,
    silu_switch_projection,
    retention_result_projection,
    trailing_norm_multiplier,
    trailing_norm_offset,
    feedforward_switch_projection,
    expanding_projection,
    contracting_projection,
):
    local_rows, hidden_size = incoming_signals.shape
    total_rows = 8 * local_rows
    slots_here = token_counts_per_slot.shape[0]
    dp_rank, tensor_rank = lax.axis_index("dp"), lax.axis_index("tensor")
    side = lax.rem(dp_rank, 2)
    row_ids = tensor_rank * local_rows + jnp.arange(local_rows, dtype=jnp.int32)
    slot_match = (row_ids // SEQ_LEN)[:, None] == jnp.arange(slots_here, dtype=jnp.int32)[None, :]
    row_lengths = jnp.sum(jnp.where(slot_match, token_counts_per_slot[None, :], 0), axis=1)
    valid_rows = (row_ids % SEQ_LEN < row_lengths)[:, None]

    def exchange(weight, axis, join):
        half = weight.shape[axis] // 2
        keep = lax.dynamic_slice_in_dim(weight, side * half, half, axis)
        give = lax.dynamic_slice_in_dim(weight, (1 - side) * half, half, axis)
        take = lax.ppermute(give, "dp", swap)
        return jnp.where(
            side == 0,
            jnp.concatenate([keep, take], axis=join),
            jnp.concatenate([take, keep], axis=join),
        )

    def spread(block, axis):
        return lax.all_gather(block, "dp", axis=axis, tiled=True, axis_index_groups=groups)

    query_half = exchange(question_projection, 1, 0)
    key_half = exchange(lookup_projection, 1, 0)
    query_key = spread(jnp.concatenate([query_half, key_half], axis=1), 0)
    value_full = spread(exchange(content_projection, 1, 0), 0)
    swish_full = spread(exchange(silu_switch_projection, 1, 0), 0)
    output_full = spread(exchange(retention_result_projection, 0, 1), 1)
    gate_full = spread(exchange(feedforward_switch_projection, 1, 0), 0)
    up_full = spread(exchange(expanding_projection, 1, 0), 0)
    down_full = spread(exchange(contracting_projection, 0, 1), 1)

    gains = jnp.stack(
        [leading_norm_multiplier, leading_norm_offset, trailing_norm_multiplier, trailing_norm_offset]
    )
    gains = lax.all_gather(gains, "dp", axis=1, tiled=True).astype(F32)
    gains = jnp.concatenate([gains, gains], axis=0)

    all_rows = jax.ShapeDtypeStruct((total_rows, hidden_size), BF16)
    own_rows = jax.ShapeDtypeStruct((local_rows, hidden_size), F32)
    pieces = jax.ShapeDtypeStruct((2, 8, hidden_size), F32)
    row_low = pltpu.VMEM((local_rows, hidden_size), BF16)
    reduce_scratch = Reduce.scratch(local_rows, hidden_size)
    moved = total_rows * hidden_size * 2

    out_low = jnp.where(valid_rows, loss_sensitivity, 0)
    normed_all, out_all = call(
        first_kernel,
        0,
        (incoming_signals, out_low, gains),
        [VM, VM, VM],
        (all_rows, all_rows),
        (ANY, ANY),
        [row_low, *Gather.scratch(), *Gather.scratch()],
        24 * moved,
    )

    slot_count = total_rows // SEQ_LEN
    shape_key = (slot_count, SEQ_LEN, KEY_DIM)
    shape_value = (slot_count, SEQ_LEN, VAL_DIM)
    query_key_proj = matmul(normed_all, query_key)
    query_proj = query_key_proj[:, :KEY_DIM].reshape(shape_key)
    key_proj = query_key_proj[:, KEY_DIM:].reshape(shape_key)
    value_heads = matmul(normed_all, value_full).reshape(shape_value).astype(BF16)
    swish_heads = matmul(normed_all, swish_full).reshape(shape_value)
    cosines, sines = rotary_tables(SEQ_LEN, KEY_DIM)
    decays = decay_table(SEQ_LEN, tensor_rank * 2 + side)
    query_rot = (query_proj * cosines + rotate_half(query_proj) * sines).astype(BF16)
    key_rot = ((key_proj * cosines + rotate_half(key_proj) * sines) * KEY_DIM ** (-0.5)).astype(BF16)
    scores = (
        jnp.einsum("snk,smk->snm", query_rot, key_rot, preferred_element_type=F32) * decays[None]
    ).astype(BF16)
    retained = jnp.einsum("snm,smv->snv", scores, value_heads, preferred_element_type=F32)
    group_hat, group_inverse = normalize(retained, GROUP_EPSILON)
    sigmoid_gate = jax.nn.sigmoid(swish_heads)
    gated = (swish_heads * sigmoid_gate * group_hat).reshape(total_rows, VAL_DIM).astype(BF16)
    retention_part = matmul(gated, output_full).astype(BF16)

    mixer_all, middle_rows = call(
        second_kernel,
        1,
        (retention_part, incoming_signals, gains),
        [ANY, VM, VM],
        (all_rows, own_rows),
        (ANY, VM),
        [row_low, *reduce_scratch, *Gather.scratch()],
        24 * moved,
    )

    gate_proj = matmul(mixer_all, gate_full)
    up_proj = matmul(mixer_all, up_full)
    gelu_gate, gelu_back = jax.vjp(gelu_tanh, gate_proj)
    hidden = (gelu_gate * up_proj).astype(BF16)
    down_gradient = matmul(hidden.T, out_all).astype(BF16)
    hidden_back = matmul(out_all, down_full.T)
    gate_back = gelu_back(hidden_back * up_proj)[0].astype(BF16)
    up_back = (hidden_back * gelu_gate).astype(BF16)
    gate_gradient = matmul(mixer_all.T, gate_back).astype(BF16)
    up_gradient = matmul(mixer_all.T, up_back).astype(BF16)
    mixer_input_part = (matmul(gate_back, gate_full.T) + matmul(up_back, up_full.T)).astype(BF16)
    mixer_part = matmul(hidden, down_full).astype(BF16)

    middle_all, middle_back, after_pieces = call(
        third_kernel,
        2,
        (mixer_input_part, middle_rows, out_low, gains),
        [ANY, VM, VM, VM],
        (all_rows, own_rows, pieces),
        (ANY, VM, VM),
        [row_low, *reduce_scratch, *Gather.scratch()],
        24 * moved,
    )

    output_gradient = matmul(gated.T, middle_all).astype(BF16)
    gated_back = matmul(middle_all, output_full.T).reshape(shape_value)
    swish_back = (
        (gated_back * group_hat * sigmoid_gate * (1.0 + swish_heads * (1.0 - sigmoid_gate)))
        .reshape(total_rows, VAL_DIM)
        .astype(BF16)
    )
    retained_back = normalize_back(
        gated_back * swish_heads * sigmoid_gate, group_hat, group_inverse
    ).astype(BF16)
    score_back = (
        jnp.einsum("snv,smv->snm", retained_back, value_heads, preferred_element_type=F32)
        * decays[None]
    ).astype(BF16)
    query_rot_back = jnp.einsum("snm,smk->snk", score_back, key_rot, preferred_element_type=F32)
    key_rot_back = jnp.einsum("snm,snk->smk", score_back, query_rot, preferred_element_type=F32)
    value_back = jnp.einsum("snm,snv->smv", scores, retained_back, preferred_element_type=F32)
    query_back = (
        (query_rot_back * cosines - rotate_half(query_rot_back) * sines)
        .reshape(total_rows, KEY_DIM)
        .astype(BF16)
    )
    key_back = (
        ((key_rot_back * cosines - rotate_half(key_rot_back) * sines) * KEY_DIM ** (-0.5))
        .reshape(total_rows, KEY_DIM)
        .astype(BF16)
    )
    value_low = value_back.reshape(total_rows, VAL_DIM).astype(BF16)
    swish_gradient = matmul(normed_all.T, swish_back).astype(BF16)
    value_gradient = matmul(normed_all.T, value_low).astype(BF16)
    query_key_back = jnp.concatenate([query_back, key_back], axis=1)
    query_key_gradient = matmul(normed_all.T, query_key_back).astype(BF16)
    first_part = (
        matmul(query_key_back, query_key.T)
        + matmul(value_low, value_full.T)
        + matmul(swish_back, swish_full.T)
    ).astype(BF16)

    delta, final_rows, before_pieces = call(
        fourth_kernel,
        3,
        (first_part, mixer_part, incoming_signals, middle_rows, gains),
        [ANY, ANY, VM, VM, VM],
        (own_rows, own_rows, pieces),
        (VM, VM, VM),
        [*reduce_scratch, *reduce_scratch],
        24 * moved,
    )
    layer_output = jnp.where(valid_rows, final_rows, 0.0).astype(BF16)
    input_delta = middle_back + delta

    gain_pieces = jnp.concatenate(
        [jnp.sum(before_pieces, axis=1), jnp.sum(after_pieces, axis=1)], axis=0
    )
    gain_sums = lax.psum(gain_pieces, ("dp", "tensor"))
    width = leading_norm_multiplier.shape[0]
    gain_sums = lax.dynamic_slice_in_dim(gain_sums, dp_rank * width, width, 1)

    def collect(gradient, axis):
        return lax.psum_scatter(
            gradient, "dp", scatter_dimension=axis, tiled=True, axis_index_groups=groups
        )

    def restore(block, axis, join):
        half = block.shape[axis] // 2
        keep = lax.dynamic_slice_in_dim(block, side * half, half, axis)
        give = lax.dynamic_slice_in_dim(block, (1 - side) * half, half, axis)
        take = lax.ppermute(give, "dp", swap)
        return jnp.where(
            side == 0,
            jnp.concatenate([keep, take], axis=join),
            jnp.concatenate([take, keep], axis=join),
        ).astype(F32)

    down_owned = restore(collect(down_gradient, 1), 1, 0)
    gate_owned = restore(collect(gate_gradient, 0), 0, 1)
    up_owned = restore(collect(up_gradient, 0), 0, 1)
    output_owned = restore(collect(output_gradient, 1), 1, 0)
    swish_owned = restore(collect(swish_gradient, 0), 0, 1)
    value_owned = restore(collect(value_gradient, 0), 0, 1)
    query_key_owned = collect(query_key_gradient, 0)
    query_owned = restore(query_key_owned[:, :KEY_DIM], 0, 1)
    key_owned = restore(query_key_owned[:, KEY_DIM:], 0, 1)
    return (
        layer_output,
        input_delta,
        gain_sums[0],
        gain_sums[1],
        query_owned,
        key_owned,
        value_owned,
        swish_owned,
        output_owned,
        gain_sums[2],
        gain_sums[3],
        gate_owned,
        up_owned,
        down_owned,
    )


def solution(mesh):
    ranks = mesh.shape["dp"]
    groups = [[2 * k + side for k in range(ranks // 2)] for side in range(2)]
    swap = [(rank, rank + 1 - 2 * (rank % 2)) for rank in range(ranks)]
    rows, gain, column, row = P(("dp", "tensor"), None), P("dp"), P("dp", "tensor"), P("tensor", "dp")
    weights = (gain, gain, column, column, column, column, row, gain, gain, column, column, row)
    return jax.shard_map(
        functools.partial(per_device, groups, swap),
        mesh=mesh,
        in_specs=(rows, rows, P("dp"), *weights),
        out_specs=(rows, rows, *weights),
        check_vma=False,
    )
```

```python
import functools

import jax
import jax.numpy as jnp
import numpy as np
from jax import lax
from jax.experimental import pallas as pl
from jax.experimental.pallas import tpu as pltpu
from jax.sharding import PartitionSpec as P

KEY_DIM = 256
VAL_DIM = 512
SEQ_LEN = 512

EPSILON = 1e-05
GROUP_EPSILON = 0.1

MESH = pl.DeviceIdType.MESH
F32 = jnp.float32
BF16 = jnp.bfloat16
CHUNK = 16


def normalize(values, epsilon):
    centre = values - jnp.mean(values, axis=-1, keepdims=True)
    inverse = lax.rsqrt(jnp.mean(centre * centre, axis=-1, keepdims=True) + epsilon)
    return (centre * inverse, inverse)


def normalize_back(upstream, normed, inverse):
    return inverse * (
        upstream
        - jnp.mean(upstream, axis=-1, keepdims=True)
        - normed * jnp.mean(upstream * normed, axis=-1, keepdims=True)
    )


def rotate_half(values):
    middle = values.shape[-1] // 2
    return jnp.concatenate([-values[..., middle:], values[..., :middle]], axis=-1)


def rotary_tables(span, columns):
    middle = columns // 2
    places = jnp.arange(span, dtype=jnp.int32).astype(jnp.float32)
    spectrum = 10000.0 ** (-jnp.arange(middle, dtype=jnp.int32).astype(jnp.float32) / middle)
    angles = places[:, None] * spectrum[None, :]
    angles = jnp.concatenate([angles, angles], axis=1)
    return (jnp.cos(angles)[None], jnp.sin(angles)[None])


def decay_table(span, head_id):
    log_rate = jnp.log(1.0 - jnp.exp2(-5.0 - head_id.astype(jnp.float32)))
    places = jnp.arange(span, dtype=jnp.int32)
    offsets = places[:, None] - places[None, :]
    decayed = jnp.exp(jnp.maximum(offsets, 0).astype(jnp.float32) * log_rate)
    return jnp.where(offsets >= 0, decayed, 0.0)


def gelu_tanh(values):
    return jax.nn.gelu(values, approximate=True)


def matmul(left, right):
    return jnp.dot(left, right, preferred_element_type=jnp.float32)


class Place:
    def __init__(self):
        d, t = lax.axis_index("dp"), lax.axis_index("tensor")
        self.x, self.y, self.c = lax.rem(d, 2), t // 2, lax.rem(t, 2)
        dx, ty = d + 1 - 2 * self.x, (1 - self.y) * 2 + self.c
        self.sib = (d, t + 1 - 2 * self.c)
        self.xn = (dx, t)
        self.yn = (d, ty)

    def block(self, j, other_core=0):
        x = 1 - self.x if j in (1, 3) else self.x
        y = 1 - self.y if j in (2, 3) else self.y
        c = 1 - self.c if other_core else self.c
        return x * 4 + y * 2 + c


def greet(place):
    barrier = pltpu.get_barrier_semaphore()
    for partner in (place.sib, place.xn, place.yn):
        pl.semaphore_signal(barrier, inc=1, device_id=partner, device_id_type=MESH)
    pl.semaphore_wait(barrier, 3)


def rows_of(index, rows):
    return pl.ds(pl.multiple_of(index * rows, rows), rows)


class Gather:
    @staticmethod
    def scratch():
        return [pltpu.SemaphoreType.DMA((13,)), pltpu.SemaphoreType.DMA((13,))]

    def __init__(self, place, src, out, send, recv):
        rows = src.shape[0]
        half = rows // 2
        p = place

        def remote(k, source, j, lo, n, target, core=0):
            where = pl.ds(pl.multiple_of(p.block(j, core) * rows + lo, 8), n)
            source = source.at[pl.ds(lo, n)] if source is src else source.at[where]
            return pltpu.make_async_remote_copy(
                src_ref=source,
                dst_ref=out.at[where],
                send_sem=send.at[k],
                recv_sem=recv.at[k],
                device_id=target,
                device_id_type=MESH,
            )

        self.p, self.rows, self.half = p, rows, half
        self.local = pltpu.make_async_copy(src, out.at[rows_of(p.block(0), rows)], send.at[12])
        h = half
        self.xa = remote(0, src, 0, 0, h, p.xn)
        self.xb = remote(1, src, 0, h, h, p.xn)
        self.ya = remote(2, src, 0, 0, h, p.yn)
        self.yb = remote(3, src, 0, h, h, p.yn)
        self.s0 = remote(4, src, 0, 0, rows, p.sib)
        self.da = remote(5, out, 1, 0, h, p.yn)
        self.db = remote(6, out, 2, h, h, p.xn)
        self.s1 = remote(7, out, 1, 0, rows, p.sib)
        self.s2 = remote(8, out, 2, 0, rows, p.sib)
        self.s3a = remote(9, out, 3, 0, h, p.sib)
        self.s3b = remote(10, out, 3, h, h, p.sib)

    def start(self):
        for copy in (self.xa, self.yb, self.xb, self.ya, self.s0, self.local):
            copy.start()

    def forward(self):
        self.xa.wait_recv()
        self.da.start()
        self.yb.wait_recv()
        self.db.start()
        self.xb.wait_recv()
        self.s1.start()
        self.ya.wait_recv()
        self.s2.start()

    def finish(self):
        self.da.wait_recv()
        self.s3a.start()
        self.db.wait_recv()
        self.s3b.start()
        self.local.wait()
        for copy in (self.s0, self.s1, self.s2, self.s3a, self.s3b):
            copy.wait()
        for copy in (self.xa, self.xb, self.ya, self.yb, self.da, self.db):
            copy.wait_send()


class Reduce:
    @staticmethod
    def scratch(rows, columns):
        return [
            pltpu.VMEM((4, rows, columns), BF16),
            pltpu.VMEM((4, rows, columns), BF16),
            pltpu.VMEM((2, rows, columns), BF16),
            pltpu.VMEM((2, rows // 2, columns), BF16),
            pltpu.SemaphoreType.DMA((14,)),
            pltpu.SemaphoreType.DMA((10,)),
        ]

    def __init__(self, place, part, mine, theirs, got, across, send, recv):
        p = place
        rows = mine.shape[1]
        h = rows // 2
        self.rows, self.half = rows, h
        self.mine, self.theirs, self.got, self.across = mine, theirs, got, across

        def remote(k, source, target_ref, target):
            return pltpu.make_async_remote_copy(
                src_ref=source,
                dst_ref=target_ref,
                send_sem=send.at[k],
                recv_sem=recv.at[k],
                device_id=target,
                device_id_type=MESH,
            )

        a, b = pl.ds(0, h), pl.ds(h, h)
        self.load = [
            pltpu.make_async_copy(part.at[rows_of(p.block(j), rows)], mine.at[j], send.at[10 + j])
            for j in range(4)
        ]
        self.swap = [
            remote(j, part.at[rows_of(p.block(j, 1), rows)], theirs.at[j], p.sib) for j in range(4)
        ]
        self.da = remote(4, mine.at[3, a], across.at[0], p.xn)
        self.db = remote(5, mine.at[3, b], across.at[1], p.yn)
        self.xa = remote(6, mine.at[1, a], got.at[0, a], p.xn)
        self.xb = remote(7, mine.at[1, b], got.at[0, b], p.xn)
        self.ya = remote(8, mine.at[2, a], got.at[1, a], p.yn)
        self.yb = remote(9, mine.at[2, b], got.at[1, b], p.yn)

    def add(self, j, lo, n, other, other_lo):
        def body(i, carry):
            r = pl.ds(pl.multiple_of(lo + i * CHUNK, CHUNK), CHUNK)
            q = pl.ds(pl.multiple_of(other_lo + i * CHUNK, CHUNK), CHUNK)
            self.mine[j, r] = (self.mine[j, r].astype(F32) + other[q].astype(F32)).astype(BF16)
            return carry

        lax.fori_loop(0, n // CHUNK, body, 0)

    def start(self):
        for j in (3, 1, 2, 0):
            self.swap[j].start()
            self.load[j].start()

    def run(self):
        rows, h = self.rows, self.half
        for j, copies in ((3, (self.da, self.db)), (1, (self.xa,)), (2, (self.yb,))):
            self.load[j].wait()
            self.swap[j].wait_recv()
            self.add(j, 0, rows, self.theirs.at[j], 0)
            for copy in copies:
                copy.start()
        self.db.wait_recv()
        self.add(1, h, h, self.across.at[1], 0)
        self.xb.start()
        self.da.wait_recv()
        self.add(2, 0, h, self.across.at[0], 0)
        self.ya.start()
        self.load[0].wait()
        self.swap[0].wait_recv()
        for copy in (self.xa, self.yb, self.xb, self.ya):
            copy.wait_recv()

    def total(self, r):
        pieces = (self.mine[0, r], self.theirs[0, r], self.got[0, r], self.got[1, r])
        one, two, three, four = (piece.astype(F32) for piece in pieces)
        return (one + two) + (three + four)

    def finish(self):
        for copy in (*self.swap, self.da, self.db, self.xa, self.xb, self.ya, self.yb):
            copy.wait_send()


def chunks(rows, body):
    def step(i, carry):
        body(pl.ds(pl.multiple_of(i * CHUNK, CHUNK), CHUNK))
        return carry

    lax.fori_loop(0, rows // CHUNK, step, 0)


def first_kernel(x_ref, cot_ref, gains_ref, out_x, out_cot, normed, *sems):
    place = Place()
    greet(place)
    gain, shift = gains_ref[0:1, :], gains_ref[1:2, :]

    def body(r):
        hat, _ = normalize(x_ref[r].astype(F32), EPSILON)
        normed[r] = (hat * gain + shift).astype(BF16)

    chunks(x_ref.shape[0], body)
    one = Gather(place, normed, out_x, *sems[:2])
    two = Gather(place, cot_ref, out_cot, *sems[2:])
    one.start()
    two.start()
    one.forward()
    two.forward()
    one.finish()
    two.finish()


def second_kernel(part_ref, x_ref, gains_ref, out_all, middle_ref, normed, *scratch):
    place = Place()
    greet(place)
    reduce = Reduce(place, part_ref, *scratch[:6])
    reduce.start()
    reduce.run()
    gain, shift = gains_ref[2:3, :], gains_ref[3:4, :]

    def body(r):
        middle = x_ref[r].astype(F32) + reduce.total(r)
        middle_ref[r] = middle
        hat, _ = normalize(middle, EPSILON)
        normed[r] = (hat * gain + shift).astype(BF16)

    chunks(x_ref.shape[0], body)
    gather = Gather(place, normed, out_all, *scratch[6:])
    gather.start()
    gather.forward()
    gather.finish()
    reduce.finish()


def third_kernel(
    part_ref, middle_ref, cot_ref, gains_ref, out_all, back_ref, pieces_ref, low, *scratch
):
    place = Place()
    greet(place)
    reduce = Reduce(place, part_ref, *scratch[:6])
    reduce.start()
    pieces_ref[...] = jnp.zeros_like(pieces_ref)
    reduce.run()
    gain = gains_ref[2:3, :]

    def body(r):
        upstream = reduce.total(r)
        hat, inverse = normalize(middle_ref[r], EPSILON)
        scaled = upstream * hat
        pieces_ref[0] += scaled[0:8] + scaled[8:16]
        pieces_ref[1] += upstream[0:8] + upstream[8:16]
        back = cot_ref[r].astype(F32) + normalize_back(upstream * gain, hat, inverse)
        back_ref[r] = back
        low[r] = back.astype(BF16)

    chunks(middle_ref.shape[0], body)
    gather = Gather(place, low, out_all, *scratch[6:])
    gather.start()
    gather.forward()
    gather.finish()
    reduce.finish()


def fourth_kernel(
    first_ref, mixer_ref, x_ref, middle_ref, gains_ref, delta_ref, final_ref, pieces_ref, *scratch
):
    place = Place()
    greet(place)
    one = Reduce(place, first_ref, *scratch[:6])
    two = Reduce(place, mixer_ref, *scratch[6:])
    one.start()
    two.start()
    pieces_ref[...] = jnp.zeros_like(pieces_ref)
    one.run()
    two.run()
    gain = gains_ref[0:1, :]

    def body(r):
        upstream = one.total(r)
        hat, inverse = normalize(x_ref[r].astype(F32), EPSILON)
        scaled = upstream * hat
        pieces_ref[0] += scaled[0:8] + scaled[8:16]
        pieces_ref[1] += upstream[0:8] + upstream[8:16]
        delta_ref[r] = normalize_back(upstream * gain, hat, inverse)
        final_ref[r] = middle_ref[r] + two.total(r)

    chunks(x_ref.shape[0], body)
    one.finish()
    two.finish()


ANY = pl.BlockSpec(memory_space=pl.ANY)
VM = pl.BlockSpec(memory_space=pltpu.VMEM)


def call(kernel, ident, args, specs, outs, out_specs, scratch, nbytes):
    return pl.pallas_call(
        kernel,
        out_shape=outs,
        in_specs=specs,
        out_specs=out_specs,
        scratch_shapes=scratch,
        compiler_params=pltpu.CompilerParams(
            collective_id=ident, has_side_effects=True, vmem_limit_bytes=32 << 20
        ),
        cost_estimate=pl.CostEstimate(flops=0, bytes_accessed=nbytes, transcendentals=0),
        name=kernel.__name__,
    )(*args)


def per_device(
    groups,
    swap,
    incoming_signals,
    loss_sensitivity,
    token_counts_per_slot,
    leading_norm_multiplier,
    leading_norm_offset,
    question_projection,
    lookup_projection,
    content_projection,
    silu_switch_projection,
    retention_result_projection,
    trailing_norm_multiplier,
    trailing_norm_offset,
    feedforward_switch_projection,
    expanding_projection,
    contracting_projection,
):
    local_rows, hidden_size = incoming_signals.shape
    total_rows = 8 * local_rows
    slots_here = token_counts_per_slot.shape[0]
    dp_rank, tensor_rank = lax.axis_index("dp"), lax.axis_index("tensor")
    side = lax.rem(dp_rank, 2)
    row_ids = tensor_rank * local_rows + jnp.arange(local_rows, dtype=jnp.int32)
    slot_match = (row_ids // SEQ_LEN)[:, None] == jnp.arange(slots_here, dtype=jnp.int32)[None, :]
    row_lengths = jnp.sum(jnp.where(slot_match, token_counts_per_slot[None, :], 0), axis=1)
    valid_rows = (row_ids % SEQ_LEN < row_lengths)[:, None]

    def exchange(weight, axis, join):
        half = weight.shape[axis] // 2
        keep = lax.dynamic_slice_in_dim(weight, side * half, half, axis)
        give = lax.dynamic_slice_in_dim(weight, (1 - side) * half, half, axis)
        take = lax.ppermute(give, "dp", swap)
        return jnp.where(
            side == 0,
            jnp.concatenate([keep, take], axis=join),
            jnp.concatenate([take, keep], axis=join),
        )

    def spread(block, axis):
        return lax.all_gather(block, "dp", axis=axis, tiled=True, axis_index_groups=groups)

    query_half = exchange(question_projection, 1, 0)
    key_half = exchange(lookup_projection, 1, 0)
    query_key = spread(jnp.concatenate([query_half, key_half], axis=1), 0)
    value_full = spread(exchange(content_projection, 1, 0), 0)
    swish_full = spread(exchange(silu_switch_projection, 1, 0), 0)
    output_full = spread(exchange(retention_result_projection, 0, 1), 1)
    gate_full = spread(exchange(feedforward_switch_projection, 1, 0), 0)
    up_full = spread(exchange(expanding_projection, 1, 0), 0)
    down_full = spread(exchange(contracting_projection, 0, 1), 1)

    gains = jnp.stack(
        [leading_norm_multiplier, leading_norm_offset, trailing_norm_multiplier, trailing_norm_offset]
    )
    gains = lax.all_gather(gains, "dp", axis=1, tiled=True).astype(F32)
    gains = jnp.concatenate([gains, gains], axis=0)

    all_rows = jax.ShapeDtypeStruct((total_rows, hidden_size), BF16)
    own_rows = jax.ShapeDtypeStruct((local_rows, hidden_size), F32)
    pieces = jax.ShapeDtypeStruct((2, 8, hidden_size), F32)
    row_low = pltpu.VMEM((local_rows, hidden_size), BF16)
    reduce_scratch = Reduce.scratch(local_rows, hidden_size)
    moved = total_rows * hidden_size * 2

    out_low = jnp.where(valid_rows, loss_sensitivity, 0)
    normed_all, out_all = call(
        first_kernel,
        0,
        (incoming_signals, out_low, gains),
        [VM, VM, VM],
        (all_rows, all_rows),
        (ANY, ANY),
        [row_low, *Gather.scratch(), *Gather.scratch()],
        24 * moved,
    )

    slot_count = total_rows // SEQ_LEN
    shape_key = (slot_count, SEQ_LEN, KEY_DIM)
    shape_value = (slot_count, SEQ_LEN, VAL_DIM)
    query_key_proj = matmul(normed_all, query_key)
    query_proj = query_key_proj[:, :KEY_DIM].reshape(shape_key)
    key_proj = query_key_proj[:, KEY_DIM:].reshape(shape_key)
    value_heads = matmul(normed_all, value_full).reshape(shape_value).astype(BF16)
    swish_heads = matmul(normed_all, swish_full).reshape(shape_value)
    cosines, sines = rotary_tables(SEQ_LEN, KEY_DIM)
    decays = decay_table(SEQ_LEN, tensor_rank * 2 + side)
    query_rot = (query_proj * cosines + rotate_half(query_proj) * sines).astype(BF16)
    key_rot = ((key_proj * cosines + rotate_half(key_proj) * sines) * KEY_DIM ** (-0.5)).astype(BF16)
    scores = (
        jnp.einsum("snk,smk->snm", query_rot, key_rot, preferred_element_type=F32) * decays[None]
    ).astype(BF16)
    retained = jnp.einsum("snm,smv->snv", scores, value_heads, preferred_element_type=F32)
    group_hat, group_inverse = normalize(retained, GROUP_EPSILON)
    sigmoid_gate = jax.nn.sigmoid(swish_heads)
    gated = (swish_heads * sigmoid_gate * group_hat).reshape(total_rows, VAL_DIM).astype(BF16)
    retention_part = matmul(gated, output_full).astype(BF16)

    mixer_all, middle_rows = call(
        second_kernel,
        1,
        (retention_part, incoming_signals, gains),
        [ANY, VM, VM],
        (all_rows, own_rows),
        (ANY, VM),
        [row_low, *reduce_scratch, *Gather.scratch()],
        24 * moved,
    )

    gate_proj = matmul(mixer_all, gate_full)
    up_proj = matmul(mixer_all, up_full)
    gelu_gate, gelu_back = jax.vjp(gelu_tanh, gate_proj)
    hidden = (gelu_gate * up_proj).astype(BF16)
    down_gradient = matmul(hidden.T, out_all).astype(BF16)
    hidden_back = matmul(out_all, down_full.T)
    gate_back = gelu_back(hidden_back * up_proj)[0].astype(BF16)
    up_back = (hidden_back * gelu_gate).astype(BF16)
    gate_gradient = matmul(mixer_all.T, gate_back).astype(BF16)
    up_gradient = matmul(mixer_all.T, up_back).astype(BF16)
    mixer_input_part = (matmul(gate_back, gate_full.T) + matmul(up_back, up_full.T)).astype(BF16)
    mixer_part = matmul(hidden, down_full).astype(BF16)

    middle_all, middle_back, after_pieces = call(
        third_kernel,
        2,
        (mixer_input_part, middle_rows, out_low, gains),
        [ANY, VM, VM, VM],
        (all_rows, own_rows, pieces),
        (ANY, VM, VM),
        [row_low, *reduce_scratch, *Gather.scratch()],
        24 * moved,
    )

    output_gradient = matmul(gated.T, middle_all).astype(BF16)
    gated_back = matmul(middle_all, output_full.T).reshape(shape_value)
    swish_back = (
        (gated_back * group_hat * sigmoid_gate * (1.0 + swish_heads * (1.0 - sigmoid_gate)))
        .reshape(total_rows, VAL_DIM)
        .astype(BF16)
    )
    retained_back = normalize_back(
        gated_back * swish_heads * sigmoid_gate, group_hat, group_inverse
    ).astype(BF16)
    score_back = (
        jnp.einsum("snv,smv->snm", retained_back, value_heads, preferred_element_type=F32)
        * decays[None]
    ).astype(BF16)
    query_rot_back = jnp.einsum("snm,smk->snk", score_back, key_rot, preferred_element_type=F32)
    key_rot_back = jnp.einsum("snm,snk->smk", score_back, query_rot, preferred_element_type=F32)
    value_back = jnp.einsum("snm,snv->smv", scores, retained_back, preferred_element_type=F32)
    query_back = (
        (query_rot_back * cosines - rotate_half(query_rot_back) * sines)
        .reshape(total_rows, KEY_DIM)
        .astype(BF16)
    )
    key_back = (
        ((key_rot_back * cosines - rotate_half(key_rot_back) * sines) * KEY_DIM ** (-0.5))
        .reshape(total_rows, KEY_DIM)
        .astype(BF16)
    )
    value_low = value_back.reshape(total_rows, VAL_DIM).astype(BF16)
    swish_gradient = matmul(normed_all.T, swish_back).astype(BF16)
    value_gradient = matmul(normed_all.T, value_low).astype(BF16)
    query_key_back = jnp.concatenate([query_back, key_back], axis=1)
    query_key_gradient = matmul(normed_all.T, query_key_back).astype(BF16)
    first_part = (
        matmul(query_key_back, query_key.T)
        + matmul(value_low, value_full.T)
        + matmul(swish_back, swish_full.T)
    ).astype(BF16)

    delta, final_rows, before_pieces = call(
        fourth_kernel,
        3,
        (first_part, mixer_part, incoming_signals, middle_rows, gains),
        [ANY, ANY, VM, VM, VM],
        (own_rows, own_rows, pieces),
        (VM, VM, VM),
        [*reduce_scratch, *reduce_scratch],
        24 * moved,
    )
    layer_output = jnp.where(valid_rows, final_rows, 0.0).astype(BF16)
    input_delta = middle_back + delta

    gain_pieces = jnp.concatenate(
        [jnp.sum(before_pieces, axis=1), jnp.sum(after_pieces, axis=1)], axis=0
    )
    gain_sums = lax.psum(gain_pieces, ("dp", "tensor"))
    width = leading_norm_multiplier.shape[0]
    gain_sums = lax.dynamic_slice_in_dim(gain_sums, dp_rank * width, width, 1)

    def collect(gradient, axis):
        return lax.psum_scatter(
            gradient, "dp", scatter_dimension=axis, tiled=True, axis_index_groups=groups
        )

    def restore(block, axis, join):
        half = block.shape[axis] // 2
        keep = lax.dynamic_slice_in_dim(block, side * half, half, axis)
        give = lax.dynamic_slice_in_dim(block, (1 - side) * half, half, axis)
        take = lax.ppermute(give, "dp", swap)
        return jnp.where(
            side == 0,
            jnp.concatenate([keep, take], axis=join),
            jnp.concatenate([take, keep], axis=join),
        ).astype(F32)

    down_owned = restore(collect(down_gradient, 1), 1, 0)
    gate_owned = restore(collect(gate_gradient, 0), 0, 1)
    up_owned = restore(collect(up_gradient, 0), 0, 1)
    output_owned = restore(collect(output_gradient, 1), 1, 0)
    swish_owned = restore(collect(swish_gradient, 0), 0, 1)
    value_owned = restore(collect(value_gradient, 0), 0, 1)
    query_key_owned = collect(query_key_gradient, 0)
    query_owned = restore(query_key_owned[:, :KEY_DIM], 0, 1)
    key_owned = restore(query_key_owned[:, KEY_DIM:], 0, 1)
    return (
        layer_output,
        input_delta,
        gain_sums[0],
        gain_sums[1],
        query_owned,
        key_owned,
        value_owned,
        swish_owned,
        output_owned,
        gain_sums[2],
        gain_sums[3],
        gate_owned,
        up_owned,
        down_owned,
    )


PLANES = 4
QK, VALUE, SWISH, OUTPUT, GATE, UP, DOWN = range(7)
WIDE = 512
TILE = 256


def nt(left, right):
    return lax.dot_general(left, right, (((1,), (1,)), ((), ())), preferred_element_type=F32)


def loop(count, body):
    def step(i, carry):
        body(i)
        return carry

    lax.fori_loop(0, count, step, 0)


def at(index, size):
    return pl.ds(pl.multiple_of(index * size, size), size)


def mega_scratch(rows, hidden):
    total = 8 * rows
    dma = pltpu.SemaphoreType.DMA
    return dict(
        w=pltpu.VMEM((7, hidden, WIDE), BF16),
        xs=pltpu.VMEM((total, hidden), BF16),
        xt=pltpu.VMEM((hidden, total), BF16),
        outs=pltpu.VMEM((total, hidden), BF16),
        part=pltpu.VMEM((total, hidden), BF16),
        theirs=pltpu.VMEM((4, rows, hidden), BF16),
        got=pltpu.VMEM((2, rows, hidden), BF16),
        across=pltpu.VMEM((2, rows // 2, hidden), BF16),
        q=pltpu.VMEM((total, KEY_DIM), BF16),
        k=pltpu.VMEM((total, KEY_DIM), BF16),
        v=pltpu.VMEM((total, VAL_DIM), BF16),
        sc=pltpu.VMEM((total, SEQ_LEN), BF16),
        swish=pltpu.VMEM((total, VAL_DIM), F32),
        ghat=pltpu.VMEM((total, VAL_DIM), F32),
        ginv=pltpu.VMEM((total, 128), F32),
        gated=pltpu.VMEM((total, VAL_DIM), BF16),
        hid=pltpu.VMEM((total, WIDE), BF16),
        gate=pltpu.VMEM((total, WIDE), F32),
        up=pltpu.VMEM((total, WIDE), F32),
        gb=pltpu.VMEM((total, WIDE), BF16),
        ub=pltpu.VMEM((total, WIDE), BF16),
        sb=pltpu.VMEM((total, SEQ_LEN), BF16),
        qkb=pltpu.VMEM((total, 2 * KEY_DIM), BF16),
        turned=pltpu.VMEM((WIDE, total), BF16),
        st=pltpu.VMEM((4, WIDE, WIDE), BF16),
        decay=pltpu.VMEM((SEQ_LEN, SEQ_LEN), F32),
        low=pltpu.VMEM((rows, hidden), BF16),
        middle=pltpu.VMEM((rows, hidden), F32),
        back=pltpu.VMEM((rows, hidden), F32),
        pieces=pltpu.VMEM((4, 8, hidden), F32),
        gparts=pltpu.VMEM((8, 8, 256), F32),
        gain=pltpu.VMEM((8, hidden), F32),
        gsend=pltpu.VMEM((8, 8, 256), F32),
        gsum=pltpu.VMEM((4, 8, 256), F32),
        ex_s=dma((8,)),
        ex_r=dma((8,)),
        ex_l=dma((8,)),
        zs=dma((7, 5)),
        zr=dma((7, 4)),
        rs=dma((7, 4)),
        rr=dma((7, 4)),
        ra=dma((7,)),
        stl=dma((4,)),
        fl=dma((4,)),
        fe_s=dma((8,)),
        fe_r=dma((8,)),
        gg_s=dma((8,)),
        gg_r=dma((8,)),
        gt_s=dma((4,)),
        gt_r=dma((4,)),
        ga_s=dma((13,)),
        ga_r=dma((13,)),
        gc_s=dma((13,)),
        gc_r=dma((13,)),
        re_s=dma((10,)),
        re_r=dma((10,)),
        ol=dma((4,)),
        free=pltpu.SemaphoreType.REGULAR,
    )


class PlaneSum(Reduce):
    def __init__(self, place, part, theirs, got, across, send, recv):
        p = place
        rows = theirs.shape[1]
        h = rows // 2
        self.rows, self.half, self.part = rows, h, part
        self.theirs, self.got, self.across = theirs, got, across
        self.base = [p.block(j) * rows for j in range(4)]

        def remote(k, source, target_ref, target):
            return pltpu.make_async_remote_copy(
                src_ref=source,
                dst_ref=target_ref,
                send_sem=send.at[k],
                recv_sem=recv.at[k],
                device_id=target,
                device_id_type=MESH,
            )

        def piece(j, lo):
            return part.at[pl.ds(pl.multiple_of(self.base[j] + lo, 8), h)]

        a, b = pl.ds(0, h), pl.ds(h, h)
        self.swap = [
            remote(j, part.at[rows_of(p.block(j, 1), rows)], theirs.at[j], p.sib) for j in range(4)
        ]
        self.da = remote(4, piece(3, 0), across.at[0], p.xn)
        self.db = remote(5, piece(3, h), across.at[1], p.yn)
        self.xa = remote(6, piece(1, 0), got.at[0, a], p.xn)
        self.xb = remote(7, piece(1, h), got.at[0, b], p.xn)
        self.ya = remote(8, piece(2, 0), got.at[1, a], p.yn)
        self.yb = remote(9, piece(2, h), got.at[1, b], p.yn)

    def add(self, j, lo, n, other, other_lo):
        def body(i):
            r = pl.ds(pl.multiple_of(self.base[j] + lo + i * CHUNK, CHUNK), CHUNK)
            q = pl.ds(pl.multiple_of(other_lo + i * CHUNK, CHUNK), CHUNK)
            self.part[r] = (self.part[r].astype(F32) + other[q].astype(F32)).astype(BF16)

        loop(n // CHUNK, body)

    def start(self):
        for j in (3, 1, 2, 0):
            self.swap[j].start()

    def run(self):
        rows, h = self.rows, self.half
        for j, copies in ((3, (self.da, self.db)), (1, (self.xa,)), (2, (self.yb,))):
            self.swap[j].wait_recv()
            self.add(j, 0, rows, self.theirs.at[j], 0)
            for copy in copies:
                copy.start()
        self.db.wait_recv()
        self.add(1, h, h, self.across.at[1], 0)
        self.xb.start()
        self.da.wait_recv()
        self.add(2, 0, h, self.across.at[0], 0)
        self.ya.start()
        self.swap[0].wait_recv()
        for copy in (self.xa, self.yb, self.xb, self.ya):
            copy.wait_recv()

    def total(self, i):
        r = pl.ds(pl.multiple_of(i * CHUNK, CHUNK), CHUNK)
        mine = pl.ds(pl.multiple_of(self.base[0] + i * CHUNK, CHUNK), CHUNK)
        pieces = (self.part[mine], self.theirs[0, r], self.got[0, r], self.got[1, r])
        one, two, three, four = (piece.astype(F32) for piece in pieces)
        return (one + two) + (three + four)


def mega_kernel(names, count_in, count_out, *refs):
    x_ref, cot_ref, gains_ref, cos_ref, sin_ref, rate_ref = refs[:6]
    q_w, k_w, v_w, s_w, o_w, g_w, u_w, d_w = refs[6:count_in]
    outs = refs[count_in : count_in + count_out]
    final_out, delta_out, gains_out, q_g, k_g, v_g, s_g, o_g, g_g, u_g, d_g, stage, heard, added = outs
    b = {name: ref for name, ref in zip(names, refs[count_in + count_out :], strict=True)}
    w, xs, xt, st, part, turned = b["w"], b["xs"], b["xt"], b["st"], b["part"], b["turned"]
    rows, hidden = x_ref.shape
    width = hidden // 8

    dp, tensor = lax.axis_index("dp"), lax.axis_index("tensor")
    place = Place()
    x, z = place.x, dp // 2
    mid = (z == 1) | (z == 2)
    end = (z == 0) | (z == 3)

    barrier = pltpu.get_barrier_semaphore()
    for i in range(1, 8):
        other = (lax.rem(dp + i, 8), tensor)
        pl.semaphore_signal(barrier, inc=1, device_id=other, device_id_type=MESH)
    for i in range(1, 4):
        other = (dp, lax.rem(tensor + i, 4))
        pl.semaphore_signal(barrier, inc=1, device_id=other, device_id_type=MESH)
    pl.semaphore_wait(barrier, 10)

    def remote(source, target_ref, send, recv, target):
        return pltpu.make_async_remote_copy(
            src_ref=source,
            dst_ref=target_ref,
            send_sem=send,
            recv_sem=recv,
            device_id=target,
            device_id_type=MESH,
        )

    def plane(step):
        return ((z + step) * 2 + x, tensor)

    def column_exchange(n, weight, k, lane, half):
        where = w.at[k, pl.ds(pl.multiple_of(z * 512 + x * 256, 256), width), pl.ds(lane, half)]
        keep = pltpu.make_async_copy(weight.at[:, at(x, half)], where, b["ex_l"].at[n])
        give = remote(
            weight.at[:, at(1 - x, half)], where, b["ex_s"].at[n], b["ex_r"].at[n], place.xn
        )
        return keep, give

    def row_exchange(n, weight, k):
        where = w.at[k, at(z, 512), at(x, width)]
        keep = pltpu.make_async_copy(weight.at[at(x, 512)], where, b["ex_l"].at[n])
        give = remote(weight.at[at(1 - x, 512)], where, b["ex_s"].at[n], b["ex_r"].at[n], place.xn)
        return keep, give

    exchanges = [
        [column_exchange(0, q_w, QK, 0, 256), column_exchange(1, k_w, QK, 256, 256)],
        [column_exchange(2, v_w, VALUE, 0, 512)],
        [column_exchange(3, s_w, SWISH, 0, 512)],
        [row_exchange(4, o_w, OUTPUT)],
        [column_exchange(5, g_w, GATE, 0, 512)],
        [column_exchange(6, u_w, UP, 0, 512)],
        [row_exchange(7, d_w, DOWN)],
    ]

    def give(k):
        for keep, send in exchanges[k]:
            send.start()
            keep.start()

    steps = (2, -2, 1, -1)

    def block_copy(k, block, step, slot):
        ref = w.at[k, at(block, 512)]
        return remote(ref, ref, b["zs"].at[k, slot], b["zr"].at[k, block], plane(step))

    def reaches(step):
        return (z + step >= 0) & (z + step < PLANES)

    def spread(k):
        for keep, send in exchanges[k]:
            keep.wait()
            send.wait_recv()
        for slot, step in enumerate(steps):

            @pl.when(reaches(step))
            def _(slot=slot, step=step):
                block_copy(k, z, step, slot).start()

    far = jnp.where(z == 1, 3, 0)

    def pass_on(k):
        @pl.when(z == 1)
        def _():
            block_copy(k, 3, 1, 4).wait_recv()
            block_copy(k, 3, -1, 4).start()

        @pl.when(z == 2)
        def _():
            block_copy(k, 0, 1, 4).wait_recv()
            block_copy(k, 0, 1, 4).start()

    def arrive(k):
        for block in range(PLANES):
            skip = (z == block) | ((z == 1) & (block == 3)) | ((z == 2) & (block == 0))

            @pl.when(jnp.logical_not(skip))
            def _(block=block):
                block_copy(k, block, 1, 4).wait_recv()

    def weights_sent():
        for k in range(7):
            for _, send in exchanges[k]:
                send.wait_send()
            for slot, step in enumerate(steps):

                @pl.when(reaches(step))
                def _(k=k, slot=slot, step=step):
                    block_copy(k, z, step, slot).wait_send()

            @pl.when(mid)
            def _(k=k):
                block_copy(k, z, 1, 4).wait_send()

    def direct(c, step, slot, to_added=False):
        if to_added:
            block = 3 - z
            target, sem = added.at[c], b["ra"].at[c]
        else:
            block = z + step
            target, sem = heard.at[c, z], b["rr"].at[c, z]
        return remote(stage.at[c, block], target, b["rs"].at[c, slot], sem, plane(step))

    def staged(c, block, slot):
        return pltpu.make_async_copy(st.at[slot], stage.at[c, block], b["stl"].at[slot])

    def send_gradient(c):
        for block in range(PLANES):
            staged(c, block, block).wait()
        for here, step in ((0, 1), (3, -1)):

            @pl.when(z == here)
            def _(step=step):
                direct(c, step, 0, True).start()
                direct(c, 2 * step, 1).start()
                direct(c, step, 2).start()

        @pl.when(mid)
        def _():
            direct(c, 1, 1).start()
            direct(c, -1, 2).start()

    def rounds(count, body):
        def step(i):
            body(pl.ds(pl.multiple_of(i * 32, 32), 32))

        loop(count // 32, step)

    def combine(c):
        for here, step in ((1, 2), (2, -2)):

            @pl.when(z == here)
            def _(here=here, step=step):
                there = here + step
                remote(
                    stage.at[c, 0], added.at[c], b["rs"].at[c, 0], b["ra"].at[c], plane(step)
                ).wait_recv()
                one = pltpu.make_async_copy(added.at[c], st.at[0], b["fl"].at[0])
                two = pltpu.make_async_copy(stage.at[c, there], st.at[1], b["fl"].at[1])
                one.start()
                two.start()
                one.wait()
                two.wait()

                def body(r):
                    st[2, r] = (st[0, r].astype(F32) + st[1, r].astype(F32)).astype(BF16)

                rounds(WIDE, body)
                three = pltpu.make_async_copy(st.at[2], stage.at[c, there], b["fl"].at[2])
                three.start()
                three.wait()
                direct(c, step, 0).start()

    col_homes = {VALUE: v_g, SWISH: s_g, GATE: g_g, UP: u_g}
    row_homes = {OUTPUT: o_g, DOWN: d_g}

    def homes(c):
        if c == QK:
            return [
                ((at(x, 256), pl.ds(0, 256)), (at(1 - x, 256), pl.ds(0, 256)), q_g, 0),
                ((at(x, 256), pl.ds(256, 256)), (at(1 - x, 256), pl.ds(256, 256)), k_g, 7),
            ]
        if c in col_homes:
            every = pl.ds(0, 512)
            return [((at(x, 256), every), (at(1 - x, 256), every), col_homes[c], c)]
        every = pl.ds(0, 512)
        return [((every, at(x, 256)), (every, at(1 - x, 256)), row_homes[c], c)]

    def home_slot(c, home):
        if c in row_homes:
            return home.at[at(x, 512)]
        half = home.shape[1] // 2
        return home.at[:, at(x, half)]

    def home_copies(c):
        for kept, given, home, n in homes(c):
            slot = home_slot(c, home)
            yield (
                pltpu.make_async_copy(st.at[0].at[kept], slot, b["fl"].at[1 if n == 7 else 0]),
                remote(
                    stage.at[c, z].at[given],
                    slot,
                    b["fe_s"].at[n],
                    b["fe_r"].at[n],
                    place.xn,
                ),
            )

    def finish_gradient(c):
        own = pltpu.make_async_copy(stage.at[c, z], st.at[0], b["fl"].at[0])
        own.start()
        for src in range(PLANES):
            here = (jnp.abs(z - src) <= 2) & (z != src)

            @pl.when(here)
            def _(src=src):
                remote(
                    stage.at[c, 0], heard.at[c, src], b["rs"].at[c, 3], b["rr"].at[c, src], plane(1)
                ).wait_recv()

        def load(src, slot):
            return pltpu.make_async_copy(heard.at[c, src], st.at[slot], b["fl"].at[slot])

        sources = {0: (1, 2), 1: (0, 2, 3), 2: (0, 1, 3), 3: (1, 2)}
        for here, srcs in sources.items():

            @pl.when(z == here)
            def _(srcs=srcs):
                for slot, src in enumerate(srcs):
                    load(src, slot + 1).start()
                for slot, src in enumerate(srcs):
                    load(src, slot + 1).wait()

        own.wait()

        @pl.when(end)
        def _():
            def body(r):
                st[0, r] = (st[0, r].astype(F32) + (st[1, r].astype(F32) + st[2, r].astype(F32))).astype(BF16)

            rounds(WIDE, body)

        @pl.when(mid)
        def _():
            def body(r):
                st[0, r] = (
                    (st[0, r].astype(F32) + st[1, r].astype(F32))
                    + (st[2, r].astype(F32) + st[3, r].astype(F32))
                ).astype(BF16)

            rounds(WIDE, body)

        store = pltpu.make_async_copy(st.at[0], stage.at[c, z], b["fl"].at[2])
        store.start()
        copies = list(home_copies(c))
        for keep, _ in copies:
            keep.start()
        store.wait()
        for _, send in copies:
            send.start()
        for keep, _ in copies:
            keep.wait()

    def gradients_done():
        for c in range(7):
            for _, send in home_copies(c):
                send.wait()
            for here, step in ((0, 1), (3, -1)):

                @pl.when(z == here)
                def _(c=c, step=step):
                    direct(c, step, 0, True).wait_send()
                    direct(c, 2 * step, 1).wait_send()
                    direct(c, step, 2).wait_send()

            for here, step in ((1, 2), (2, -2)):

                @pl.when(z == here)
                def _(c=c, step=step):
                    direct(c, step, 0).wait_send()
                    direct(c, 1, 1).wait_send()
                    direct(c, -1, 2).wait_send()

    def gain_copy(i):
        target = lax.rem(dp + i, 8)
        return remote(
            gains_ref, b["gparts"].at[dp], b["gg_s"].at[i], b["gg_r"].at[dp], (target, tensor)
        )

    def gain_arrival(i):
        source = lax.rem(dp + i, 8)
        return remote(
            gains_ref, b["gparts"].at[source], b["gg_s"].at[i], b["gg_r"].at[source], (source, tensor)
        )

    gather_sems = (b["ga_s"], b["ga_r"])

    def plane_sum(ref):
        return PlaneSum(place, ref, b["theirs"], b["got"], b["across"], b["re_s"], b["re_r"])

    give(QK)
    for i in range(1, 8):
        gain_copy(i).start()
    give(VALUE)
    mine = pltpu.make_async_copy(gains_ref, b["gparts"].at[dp], b["ol"].at[0])
    mine.start()
    rate = rate_ref[0:1, 0:1]

    def body(i):
        r = at(i, 64)
        n = lax.broadcasted_iota(jnp.int32, (64, SEQ_LEN), 0) + i * 64
        m = lax.broadcasted_iota(jnp.int32, (64, SEQ_LEN), 1)
        gap = n - m
        b["decay"][r] = jnp.where(gap >= 0, jnp.exp(jnp.maximum(gap, 0).astype(F32) * rate), 0.0)

    loop(SEQ_LEN // 64, body)
    spread(QK)
    mine.wait()
    for i in range(1, 8):
        gain_arrival(i).wait_recv()
    for i in range(8):
        b["gain"][:, i * 256 : (i + 1) * 256] = b["gparts"][i]
    gain = b["gain"]
    low = b["low"]

    def body(i):
        r = at(i, CHUNK)
        hat, _ = normalize(x_ref[r].astype(F32), EPSILON)
        low[r] = (hat * gain[0:1, :] + gain[1:2, :]).astype(BF16)

    loop(rows // CHUNK, body)
    first = Gather(place, low, xs, *gather_sems)
    first.start()
    spread(VALUE)
    first.forward()
    for k in range(SWISH, DOWN + 1):
        give(k)
    cotangent = Gather(place, cot_ref, b["outs"], b["gc_s"], b["gc_r"])
    cotangent.start()
    first.finish()

    def body(i):
        xt[at(i, 256), :] = xs[:, at(i, 256)].T

    loop(hidden // 256, body)

    pass_on(QK)
    spread(SWISH)
    arrive(QK)

    def turn(acc, tile, scale):
        spot = at(lax.rem(tile, SEQ_LEN // TILE), TILE)
        cos, sin = cos_ref[spot], sin_ref[spot]
        one, two = acc[:, :128], acc[:, 128:]
        return (((one * cos - two * sin) * scale).astype(BF16), ((two * cos + one * sin) * scale).astype(BF16))

    def body(i):
        r = at(i, TILE)
        acc = matmul(xs[r], w[QK])
        b["q"][r, :128], b["q"][r, 128:] = turn(acc[:, :KEY_DIM], i, 1.0)
        b["k"][r, :128], b["k"][r, 128:] = turn(acc[:, KEY_DIM:], i, KEY_DIM ** (-0.5))

    tiles = 8 * rows // TILE
    per_slot = SEQ_LEN // TILE
    loop(tiles, body)

    def slot_rows(i):
        return at(i // per_slot, SEQ_LEN)

    def body(i):
        r = at(i, TILE)
        decay = b["decay"][at(lax.rem(i, per_slot), TILE)]
        b["sc"][r] = (nt(b["q"][r], b["k"][slot_rows(i)]) * decay).astype(BF16)

    loop(tiles, body)

    pass_on(VALUE)
    spread(OUTPUT)
    arrive(VALUE)

    def body(i):
        r = at(i, TILE)
        b["v"][r] = matmul(xs[r], w[VALUE]).astype(BF16)

    loop(tiles, body)

    def body(i):
        r = at(i, TILE)
        retained = matmul(b["sc"][r], b["v"][slot_rows(i)])
        hat, inverse = normalize(retained, GROUP_EPSILON)
        b["ghat"][r] = hat
        b["ginv"][r] = jnp.broadcast_to(inverse, (TILE, 128))

    loop(tiles, body)
    cotangent.forward()
    cotangent.finish()

    pass_on(SWISH)
    spread(GATE)
    arrive(SWISH)

    def body(i):
        r = at(i, TILE)
        swish = matmul(xs[r], w[SWISH])
        b["swish"][r] = swish
        b["gated"][r] = (swish * jax.nn.sigmoid(swish) * b["ghat"][r]).astype(BF16)

    loop(tiles, body)

    pass_on(OUTPUT)
    spread(UP)
    arrive(OUTPUT)

    def grid_of(i):
        return at(i // PLANES, TILE), at(lax.rem(i, PLANES), 512)

    def body(i):
        r, c = grid_of(i)
        part[r, c] = matmul(b["gated"][r], w[OUTPUT, c]).astype(BF16)

    loop(tiles * PLANES, body)
    reduce = plane_sum(part)
    reduce.start()
    reduce.run()

    def body(i):
        r = at(i, CHUNK)
        middle = x_ref[r].astype(F32) + reduce.total(i)
        b["middle"][r] = middle
        hat, _ = normalize(middle, EPSILON)
        low[r] = (hat * gain[2:3, :] + gain[3:4, :]).astype(BF16)

    loop(rows // CHUNK, body)
    second = Gather(place, low, xs, *gather_sems)
    second.start()
    pass_on(GATE)
    spread(DOWN)
    second.forward()
    second.finish()
    reduce.finish()

    arrive(GATE)

    def body(i):
        r = at(i, TILE)
        b["gate"][r] = matmul(xs[r], w[GATE])

    loop(tiles, body)
    pass_on(UP)
    arrive(UP)

    def gelu_of(t):
        inner = 0.7978845608028654 * (t + 0.044715 * t * t * t)
        return 0.5 * (1.0 + jnp.tanh(inner)), jnp.tanh(inner)

    def body(i):
        r = at(i, TILE)
        up = matmul(xs[r], w[UP])
        b["up"][r] = up
        gate = b["gate"][r]
        share, _ = gelu_of(gate)
        b["hid"][r] = (gate * share * up).astype(BF16)

    loop(tiles, body)

    def turned_of(ref):
        def body(i):
            turned[:, at(i, TILE)] = ref[at(i, TILE)].T

        loop(tiles, body)

    def stage_block(c, i, value):
        st[i] = value.astype(BF16)
        staged(c, i, i).start()

    turned_of(b["hid"])

    def body(i):
        stage_block(DOWN, i, matmul(turned[...], b["outs"][:, at(i, 512)]))

    loop(PLANES, body)
    send_gradient(DOWN)
    pass_on(DOWN)
    arrive(DOWN)

    def times_turned(left, r, k):
        acc = nt(left[r, 0:512], w[k, 0:512])
        for plane_at in range(1, PLANES):
            lanes = slice(plane_at * 512, plane_at * 512 + 512)
            acc = acc + nt(left[r, lanes], w[k, lanes])
        return acc

    def body(i):
        r = at(i, TILE)
        back = times_turned(b["outs"], r, DOWN)
        gate, up = b["gate"][r], b["up"][r]
        share, tanh = gelu_of(gate)
        slope = 0.5 * gate * (1.0 - tanh * tanh) * (0.7978845608028654 * (1.0 + 0.134145 * gate * gate))
        b["gb"][r] = (back * up * (share + slope)).astype(BF16)
        b["ub"][r] = (back * gate * share).astype(BF16)

    loop(tiles, body)

    def body(i):
        r, c = grid_of(i)
        part[r, c] = (nt(b["gb"][r], w[GATE, c]) + nt(b["ub"][r], w[UP, c])).astype(BF16)

    loop(tiles * PLANES, body)
    reduce = plane_sum(part)
    reduce.start()

    def weight_gradient(c, right):
        def body(i):
            def body_turn(j):
                turned[:, at(j, TILE)] = xs[at(j, TILE), at(i, 512)].T

            loop(tiles, body_turn)
            stage_block(c, i, matmul(turned[...], right[...]))

        loop(PLANES, body)
        send_gradient(c)

    weight_gradient(GATE, b["gb"])
    reduce.run()
    b["pieces"][...] = jnp.zeros_like(b["pieces"])

    def body(i):
        r = at(i, CHUNK)
        upstream = reduce.total(i)
        hat, inverse = normalize(b["middle"][r], EPSILON)
        scaled = upstream * hat
        b["pieces"][2] += scaled[0:8] + scaled[8:16]
        b["pieces"][3] += upstream[0:8] + upstream[8:16]
        back = cot_ref[r].astype(F32) + normalize_back(upstream * gain[2:3, :], hat, inverse)
        b["back"][r] = back
        low[r] = back.astype(BF16)

    loop(rows // CHUNK, body)
    third = Gather(place, low, b["outs"], *gather_sems)
    third.start()
    weight_gradient(UP, b["ub"])
    third.forward()
    combine(DOWN)

    def body(i):
        r, c = grid_of(i)
        xs[r, c] = matmul(b["hid"][r], w[DOWN, c]).astype(BF16)

    loop(tiles * PLANES, body)
    third.finish()
    reduce.finish()

    turned_of(b["gated"])

    def body(i):
        stage_block(OUTPUT, i, matmul(turned[...], b["outs"][:, at(i, 512)]))

    loop(PLANES, body)
    send_gradient(OUTPUT)
    combine(GATE)
    swb, rb, vlow = b["gb"], b["hid"], b["ub"]

    def body(i):
        r = at(i, TILE)
        back = times_turned(b["outs"], r, OUTPUT)
        swish, hat = b["swish"][r], b["ghat"][r]
        gate = jax.nn.sigmoid(swish)
        swb[r] = (back * hat * gate * (1.0 + swish * (1.0 - gate))).astype(BF16)
        rb[r] = normalize_back(back * swish * gate, hat, b["ginv"][r, 0:1]).astype(BF16)

    loop(tiles, body)

    def projection_gradient(c, right):
        def body(i):
            stage_block(c, i, matmul(xt[at(i, 512)], right[...]))

        loop(PLANES, body)
        send_gradient(c)

    projection_gradient(SWISH, swb)

    def body(i):
        r = at(i, TILE)
        decay = b["decay"][at(lax.rem(i, per_slot), TILE)]
        b["sb"][r] = (nt(rb[r], b["v"][slot_rows(i)]) * decay).astype(BF16)

    loop(tiles, body)
    turned_of(b["sc"])

    def body(i):
        vlow[at(i, TILE)] = matmul(
            turned[at(lax.rem(i, per_slot), TILE), slot_rows(i)], rb[slot_rows(i)]
        ).astype(BF16)

    loop(tiles, body)
    projection_gradient(VALUE, vlow)
    combine(UP)
    turned_of(b["sb"])

    def turn_back(acc, tile, scale):
        spot = at(lax.rem(tile, per_slot), TILE)
        cos, sin = cos_ref[spot], sin_ref[spot]
        one, two = acc[:, :128], acc[:, 128:]
        return (((one * cos + two * sin) * scale).astype(BF16), ((two * cos - one * sin) * scale).astype(BF16))

    def body(i):
        r = at(i, TILE)
        qkb = b["qkb"]
        query = matmul(b["sb"][r], b["k"][slot_rows(i)])
        qkb[r, 0:128], qkb[r, 128:256] = turn_back(query, i, 1.0)
        key = matmul(turned[at(lax.rem(i, per_slot), TILE), slot_rows(i)], b["q"][slot_rows(i)])
        qkb[r, 256:384], qkb[r, 384:512] = turn_back(key, i, KEY_DIM ** (-0.5))

    loop(tiles, body)
    projection_gradient(QK, b["qkb"])
    combine(OUTPUT)

    def body(i):
        r, c = grid_of(i)
        part[r, c] = (
            nt(b["qkb"][r], w[QK, c]) + nt(vlow[r], w[VALUE, c]) + nt(swb[r], w[SWISH, c])
        ).astype(BF16)

    loop(tiles * PLANES, body)
    finish_gradient(DOWN)
    combine(SWISH)

    reduce = plane_sum(xs)
    reduce.start()
    reduce.run()

    def body(i):
        b["middle"][at(i, CHUNK)] += reduce.total(i)

    loop(rows // CHUNK, body)
    reduce.finish()
    for partner in (place.sib, place.xn, place.yn):
        pl.semaphore_signal(b["free"], inc=1, device_id=partner, device_id_type=MESH)
    final_copy = pltpu.make_async_copy(b["middle"], final_out, b["ol"].at[1])
    final_copy.start()
    finish_gradient(GATE)
    combine(VALUE)
    pl.semaphore_wait(b["free"], 3)
    reduce = plane_sum(part)
    reduce.start()
    reduce.run()

    def body(i):
        r = at(i, CHUNK)
        upstream = reduce.total(i)
        hat, inverse = normalize(x_ref[r].astype(F32), EPSILON)
        scaled = upstream * hat
        b["pieces"][0] += scaled[0:8] + scaled[8:16]
        b["pieces"][1] += upstream[0:8] + upstream[8:16]
        b["back"][r] += normalize_back(upstream * gain[0:1, :], hat, inverse)

    loop(rows // CHUNK, body)
    reduce.finish()
    delta_copy = pltpu.make_async_copy(b["back"], delta_out, b["ol"].at[2])
    delta_copy.start()
    combine(QK)

    for i in range(1, 8):
        gain_copy(i).wait_send()
    gsend, gparts, gsum = b["gsend"], b["gparts"], b["gsum"]
    for i in range(8):
        for n in range(4):
            lanes = slice(i * 256, i * 256 + 256)
            gsend[i, n : n + 1, :] = jnp.sum(b["pieces"][n, :, lanes], axis=0, keepdims=True)
            gsend[i, n + 4 : n + 5, :] = jnp.zeros((1, 256), F32)

    def share_copy(i):
        target = lax.rem(dp + i, 8)
        return remote(
            gsend.at[target], gparts.at[dp], b["gg_s"].at[i], b["gg_r"].at[dp], (target, tensor)
        )

    for i in range(1, 8):
        share_copy(i).start()
    acc = gsend[dp]
    for i in range(1, 8):
        gain_arrival(i).wait_recv()
        acc = acc + gparts[lax.rem(dp + i, 8)]
    gsum[tensor] = acc

    def sum_copy(i, source):
        target = lax.rem(tensor + i, 4)
        return remote(
            gsum.at[source], gsum.at[source], b["gt_s"].at[i], b["gt_r"].at[source], (dp, target)
        )

    for i in range(1, 4):
        sum_copy(i, tensor).start()
    for i in range(1, 4):
        sum_copy(i, lax.rem(tensor + i, 4)).wait_recv()
    for i in range(1, 4):
        sum_copy(i, tensor).wait_send()
    for i in range(1, 8):
        share_copy(i).wait_send()
    gains_out[...] = (gsum[0] + gsum[1]) + (gsum[2] + gsum[3])

    finish_gradient(UP)
    finish_gradient(OUTPUT)
    finish_gradient(SWISH)
    finish_gradient(VALUE)
    finish_gradient(QK)
    final_copy.wait()
    delta_copy.wait()
    weights_sent()
    gradients_done()


def whole_layer(
    incoming_signals,
    loss_sensitivity,
    token_counts_per_slot,
    leading_norm_multiplier,
    leading_norm_offset,
    question_projection,
    lookup_projection,
    content_projection,
    silu_switch_projection,
    retention_result_projection,
    trailing_norm_multiplier,
    trailing_norm_offset,
    feedforward_switch_projection,
    expanding_projection,
    contracting_projection,
):
    rows, hidden = incoming_signals.shape
    slots_here = token_counts_per_slot.shape[0]
    dp_rank, tensor_rank = lax.axis_index("dp"), lax.axis_index("tensor")
    row_ids = tensor_rank * rows + jnp.arange(rows, dtype=jnp.int32)
    slot_match = (row_ids // SEQ_LEN)[:, None] == jnp.arange(slots_here, dtype=jnp.int32)[None, :]
    row_lengths = jnp.sum(jnp.where(slot_match, token_counts_per_slot[None, :], 0), axis=1)
    valid_rows = (row_ids % SEQ_LEN < row_lengths)[:, None]
    gains = jnp.stack(
        [leading_norm_multiplier, leading_norm_offset, trailing_norm_multiplier, trailing_norm_offset]
    ).astype(F32)
    gains = jnp.concatenate([gains, gains], axis=0)
    places = np.arange(SEQ_LEN, dtype=np.float32)
    spectrum = np.float32(10000.0) ** (-np.arange(KEY_DIM // 2, dtype=np.float32) / np.float32(KEY_DIM // 2))
    angles = places[:, None] * spectrum[None, :]
    head = tensor_rank * 2 + lax.rem(dp_rank, 2)
    rate = jnp.log(1.0 - jnp.exp2(-5.0 - head.astype(F32)))
    weights = (
        question_projection,
        lookup_projection,
        content_projection,
        silu_switch_projection,
        retention_result_projection,
        feedforward_switch_projection,
        expanding_projection,
        contracting_projection,
    )
    args = (
        incoming_signals,
        jnp.where(valid_rows, loss_sensitivity, 0),
        gains,
        jnp.asarray(np.cos(angles)),
        jnp.asarray(np.sin(angles)),
        jnp.full((8, 128), rate, F32),
        *weights,
    )
    scratch = mega_scratch(rows, hidden)
    shape = jax.ShapeDtypeStruct
    outs = (
        shape((rows, hidden), F32),
        shape((rows, hidden), F32),
        shape((8, 256), F32),
        *(shape(weight.shape, BF16) for weight in weights),
        shape((7, PLANES, WIDE, WIDE), BF16),
        shape((7, PLANES, WIDE, WIDE), BF16),
        shape((7, WIDE, WIDE), BF16),
    )
    results = pl.pallas_call(
        functools.partial(mega_kernel, tuple(scratch), len(args), len(outs)),
        out_shape=outs,
        in_specs=[VM] * 6 + [ANY] * 8,
        out_specs=tuple([ANY, ANY, VM] + [ANY] * 11),
        scratch_shapes=list(scratch.values()),
        compiler_params=pltpu.CompilerParams(
            collective_id=0, has_side_effects=True, vmem_limit_bytes=67043328
        ),
        name="whole_layer",
    )(*args)
    final_rows, delta, gain_sums = results[:3]
    grads = [grad.astype(F32) for grad in results[3:11]]
    layer_output = jnp.where(valid_rows, final_rows, 0.0).astype(BF16)
    query, key, value, swish, output, gate, up, down = grads
    return (
        layer_output,
        delta,
        gain_sums[0],
        gain_sums[1],
        query,
        key,
        value,
        swish,
        output,
        gain_sums[2],
        gain_sums[3],
        gate,
        up,
        down,
    )


def solution(mesh):
    ranks = mesh.shape["dp"]
    groups = [[2 * k + side for k in range(ranks // 2)] for side in range(2)]
    swap = [(rank, rank + 1 - 2 * (rank % 2)) for rank in range(ranks)]
    rows, gain, column, row = P(("dp", "tensor"), None), P("dp"), P("dp", "tensor"), P("tensor", "dp")
    weights = (gain, gain, column, column, column, column, row, gain, gain, column, column, row)
    one_kernel = ranks == 8 and mesh.shape["tensor"] == 4
    return jax.shard_map(
        whole_layer if one_kernel else functools.partial(per_device, groups, swap),
        mesh=mesh,
        in_specs=(rows, rows, P("dp"), *weights),
        out_specs=(rows, rows, *weights),
        check_vma=False,
    )
```

```python
import functools

import jax
import jax.numpy as jnp
import numpy as np
from jax import lax
from jax.experimental import pallas as pl
from jax.experimental.pallas import tpu as pltpu
from jax.sharding import PartitionSpec as P

KEY_DIM = 256
VAL_DIM = 512
SEQ_LEN = 512

EPSILON = 1e-05
GROUP_EPSILON = 0.1

MESH = pl.DeviceIdType.MESH
F32 = jnp.float32
BF16 = jnp.bfloat16
CHUNK = 16


def normalize(values, epsilon):
    centre = values - jnp.mean(values, axis=-1, keepdims=True)
    inverse = lax.rsqrt(jnp.mean(centre * centre, axis=-1, keepdims=True) + epsilon)
    return (centre * inverse, inverse)


def normalize_back(upstream, normed, inverse):
    return inverse * (
        upstream
        - jnp.mean(upstream, axis=-1, keepdims=True)
        - normed * jnp.mean(upstream * normed, axis=-1, keepdims=True)
    )


def rotate_half(values):
    middle = values.shape[-1] // 2
    return jnp.concatenate([-values[..., middle:], values[..., :middle]], axis=-1)


def rotary_tables(span, columns):
    middle = columns // 2
    places = jnp.arange(span, dtype=jnp.int32).astype(jnp.float32)
    spectrum = 10000.0 ** (-jnp.arange(middle, dtype=jnp.int32).astype(jnp.float32) / middle)
    angles = places[:, None] * spectrum[None, :]
    angles = jnp.concatenate([angles, angles], axis=1)
    return (jnp.cos(angles)[None], jnp.sin(angles)[None])


def decay_table(span, head_id):
    log_rate = jnp.log(1.0 - jnp.exp2(-5.0 - head_id.astype(jnp.float32)))
    places = jnp.arange(span, dtype=jnp.int32)
    offsets = places[:, None] - places[None, :]
    decayed = jnp.exp(jnp.maximum(offsets, 0).astype(jnp.float32) * log_rate)
    return jnp.where(offsets >= 0, decayed, 0.0)


def gelu_tanh(values):
    return jax.nn.gelu(values, approximate=True)


def matmul(left, right):
    return jnp.dot(left, right, preferred_element_type=jnp.float32)


class Place:
    def __init__(self):
        d, t = lax.axis_index("dp"), lax.axis_index("tensor")
        self.x, self.y, self.c = lax.rem(d, 2), t // 2, lax.rem(t, 2)
        dx, ty = d + 1 - 2 * self.x, (1 - self.y) * 2 + self.c
        self.sib = (d, t + 1 - 2 * self.c)
        self.xn = (dx, t)
        self.yn = (d, ty)

    def block(self, j, other_core=0):
        x = 1 - self.x if j in (1, 3) else self.x
        y = 1 - self.y if j in (2, 3) else self.y
        c = 1 - self.c if other_core else self.c
        return x * 4 + y * 2 + c


def greet(place):
    barrier = pltpu.get_barrier_semaphore()
    for partner in (place.sib, place.xn, place.yn):
        pl.semaphore_signal(barrier, inc=1, device_id=partner, device_id_type=MESH)
    pl.semaphore_wait(barrier, 3)


def rows_of(index, rows):
    return pl.ds(pl.multiple_of(index * rows, rows), rows)


class Gather:
    @staticmethod
    def scratch():
        return [pltpu.SemaphoreType.DMA((13,)), pltpu.SemaphoreType.DMA((13,))]

    def __init__(self, place, src, out, send, recv):
        rows = src.shape[0]
        half = rows // 2
        p = place

        def remote(k, source, j, lo, n, target, core=0):
            where = pl.ds(pl.multiple_of(p.block(j, core) * rows + lo, 8), n)
            source = source.at[pl.ds(lo, n)] if source is src else source.at[where]
            return pltpu.make_async_remote_copy(
                src_ref=source,
                dst_ref=out.at[where],
                send_sem=send.at[k],
                recv_sem=recv.at[k],
                device_id=target,
                device_id_type=MESH,
            )

        self.p, self.rows, self.half = p, rows, half
        self.local = pltpu.make_async_copy(src, out.at[rows_of(p.block(0), rows)], send.at[12])
        h = half
        self.xa = remote(0, src, 0, 0, h, p.xn)
        self.xb = remote(1, src, 0, h, h, p.xn)
        self.ya = remote(2, src, 0, 0, h, p.yn)
        self.yb = remote(3, src, 0, h, h, p.yn)
        self.s0 = remote(4, src, 0, 0, rows, p.sib)
        self.da = remote(5, out, 1, 0, h, p.yn)
        self.db = remote(6, out, 2, h, h, p.xn)
        self.s1 = remote(7, out, 1, 0, rows, p.sib)
        self.s2 = remote(8, out, 2, 0, rows, p.sib)
        self.s3a = remote(9, out, 3, 0, h, p.sib)
        self.s3b = remote(10, out, 3, h, h, p.sib)

    def start(self):
        for copy in (self.xa, self.yb, self.xb, self.ya, self.s0, self.local):
            copy.start()

    def forward(self):
        self.xa.wait_recv()
        self.da.start()
        self.yb.wait_recv()
        self.db.start()
        self.xb.wait_recv()
        self.s1.start()
        self.ya.wait_recv()
        self.s2.start()

    def finish(self):
        self.da.wait_recv()
        self.s3a.start()
        self.db.wait_recv()
        self.s3b.start()
        self.local.wait()
        for copy in (self.s0, self.s1, self.s2, self.s3a, self.s3b):
            copy.wait()
        for copy in (self.xa, self.xb, self.ya, self.yb, self.da, self.db):
            copy.wait_send()


class Reduce:
    @staticmethod
    def scratch(rows, columns):
        return [
            pltpu.VMEM((4, rows, columns), BF16),
            pltpu.VMEM((4, rows, columns), BF16),
            pltpu.VMEM((2, rows, columns), BF16),
            pltpu.VMEM((2, rows // 2, columns), BF16),
            pltpu.SemaphoreType.DMA((14,)),
            pltpu.SemaphoreType.DMA((10,)),
        ]

    def __init__(self, place, part, mine, theirs, got, across, send, recv):
        p = place
        rows = mine.shape[1]
        h = rows // 2
        self.rows, self.half = rows, h
        self.mine, self.theirs, self.got, self.across = mine, theirs, got, across

        def remote(k, source, target_ref, target):
            return pltpu.make_async_remote_copy(
                src_ref=source,
                dst_ref=target_ref,
                send_sem=send.at[k],
                recv_sem=recv.at[k],
                device_id=target,
                device_id_type=MESH,
            )

        a, b = pl.ds(0, h), pl.ds(h, h)
        self.load = [
            pltpu.make_async_copy(part.at[rows_of(p.block(j), rows)], mine.at[j], send.at[10 + j])
            for j in range(4)
        ]
        self.swap = [
            remote(j, part.at[rows_of(p.block(j, 1), rows)], theirs.at[j], p.sib) for j in range(4)
        ]
        self.da = remote(4, mine.at[3, a], across.at[0], p.xn)
        self.db = remote(5, mine.at[3, b], across.at[1], p.yn)
        self.xa = remote(6, mine.at[1, a], got.at[0, a], p.xn)
        self.xb = remote(7, mine.at[1, b], got.at[0, b], p.xn)
        self.ya = remote(8, mine.at[2, a], got.at[1, a], p.yn)
        self.yb = remote(9, mine.at[2, b], got.at[1, b], p.yn)

    def add(self, j, lo, n, other, other_lo):
        def body(i, carry):
            r = pl.ds(pl.multiple_of(lo + i * CHUNK, CHUNK), CHUNK)
            q = pl.ds(pl.multiple_of(other_lo + i * CHUNK, CHUNK), CHUNK)
            self.mine[j, r] = (self.mine[j, r].astype(F32) + other[q].astype(F32)).astype(BF16)
            return carry

        lax.fori_loop(0, n // CHUNK, body, 0)

    def start(self):
        for j in (3, 1, 2, 0):
            self.swap[j].start()
            self.load[j].start()

    def run(self):
        rows, h = self.rows, self.half
        for j, copies in ((3, (self.da, self.db)), (1, (self.xa,)), (2, (self.yb,))):
            self.load[j].wait()
            self.swap[j].wait_recv()
            self.add(j, 0, rows, self.theirs.at[j], 0)
            for copy in copies:
                copy.start()
        self.db.wait_recv()
        self.add(1, h, h, self.across.at[1], 0)
        self.xb.start()
        self.da.wait_recv()
        self.add(2, 0, h, self.across.at[0], 0)
        self.ya.start()
        self.load[0].wait()
        self.swap[0].wait_recv()
        for copy in (self.xa, self.yb, self.xb, self.ya):
            copy.wait_recv()

    def total(self, r):
        pieces = (self.mine[0, r], self.theirs[0, r], self.got[0, r], self.got[1, r])
        one, two, three, four = (piece.astype(F32) for piece in pieces)
        return (one + two) + (three + four)

    def finish(self):
        for copy in (*self.swap, self.da, self.db, self.xa, self.xb, self.ya, self.yb):
            copy.wait_send()


def chunks(rows, body):
    def step(i, carry):
        body(pl.ds(pl.multiple_of(i * CHUNK, CHUNK), CHUNK))
        return carry

    lax.fori_loop(0, rows // CHUNK, step, 0)


def first_kernel(x_ref, cot_ref, gains_ref, out_x, out_cot, normed, *sems):
    place = Place()
    greet(place)
    gain, shift = gains_ref[0:1, :], gains_ref[1:2, :]

    def body(r):
        hat, _ = normalize(x_ref[r].astype(F32), EPSILON)
        normed[r] = (hat * gain + shift).astype(BF16)

    chunks(x_ref.shape[0], body)
    one = Gather(place, normed, out_x, *sems[:2])
    two = Gather(place, cot_ref, out_cot, *sems[2:])
    one.start()
    two.start()
    one.forward()
    two.forward()
    one.finish()
    two.finish()


def second_kernel(part_ref, x_ref, gains_ref, out_all, middle_ref, normed, *scratch):
    place = Place()
    greet(place)
    reduce = Reduce(place, part_ref, *scratch[:6])
    reduce.start()
    reduce.run()
    gain, shift = gains_ref[2:3, :], gains_ref[3:4, :]

    def body(r):
        middle = x_ref[r].astype(F32) + reduce.total(r)
        middle_ref[r] = middle
        hat, _ = normalize(middle, EPSILON)
        normed[r] = (hat * gain + shift).astype(BF16)

    chunks(x_ref.shape[0], body)
    gather = Gather(place, normed, out_all, *scratch[6:])
    gather.start()
    gather.forward()
    gather.finish()
    reduce.finish()


def third_kernel(
    part_ref, middle_ref, cot_ref, gains_ref, out_all, back_ref, pieces_ref, low, *scratch
):
    place = Place()
    greet(place)
    reduce = Reduce(place, part_ref, *scratch[:6])
    reduce.start()
    pieces_ref[...] = jnp.zeros_like(pieces_ref)
    reduce.run()
    gain = gains_ref[2:3, :]

    def body(r):
        upstream = reduce.total(r)
        hat, inverse = normalize(middle_ref[r], EPSILON)
        scaled = upstream * hat
        pieces_ref[0] += scaled[0:8] + scaled[8:16]
        pieces_ref[1] += upstream[0:8] + upstream[8:16]
        back = cot_ref[r].astype(F32) + normalize_back(upstream * gain, hat, inverse)
        back_ref[r] = back
        low[r] = back.astype(BF16)

    chunks(middle_ref.shape[0], body)
    gather = Gather(place, low, out_all, *scratch[6:])
    gather.start()
    gather.forward()
    gather.finish()
    reduce.finish()


def fourth_kernel(
    first_ref, mixer_ref, x_ref, middle_ref, gains_ref, delta_ref, final_ref, pieces_ref, *scratch
):
    place = Place()
    greet(place)
    one = Reduce(place, first_ref, *scratch[:6])
    two = Reduce(place, mixer_ref, *scratch[6:])
    one.start()
    two.start()
    pieces_ref[...] = jnp.zeros_like(pieces_ref)
    one.run()
    two.run()
    gain = gains_ref[0:1, :]

    def body(r):
        upstream = one.total(r)
        hat, inverse = normalize(x_ref[r].astype(F32), EPSILON)
        scaled = upstream * hat
        pieces_ref[0] += scaled[0:8] + scaled[8:16]
        pieces_ref[1] += upstream[0:8] + upstream[8:16]
        delta_ref[r] = normalize_back(upstream * gain, hat, inverse)
        final_ref[r] = middle_ref[r] + two.total(r)

    chunks(x_ref.shape[0], body)
    one.finish()
    two.finish()


ANY = pl.BlockSpec(memory_space=pl.ANY)
VM = pl.BlockSpec(memory_space=pltpu.VMEM)


def call(kernel, ident, args, specs, outs, out_specs, scratch, nbytes):
    return pl.pallas_call(
        kernel,
        out_shape=outs,
        in_specs=specs,
        out_specs=out_specs,
        scratch_shapes=scratch,
        compiler_params=pltpu.CompilerParams(
            collective_id=ident, has_side_effects=True, vmem_limit_bytes=32 << 20
        ),
        cost_estimate=pl.CostEstimate(flops=0, bytes_accessed=nbytes, transcendentals=0),
        name=kernel.__name__,
    )(*args)


def per_device(
    groups,
    swap,
    incoming_signals,
    loss_sensitivity,
    token_counts_per_slot,
    leading_norm_multiplier,
    leading_norm_offset,
    question_projection,
    lookup_projection,
    content_projection,
    silu_switch_projection,
    retention_result_projection,
    trailing_norm_multiplier,
    trailing_norm_offset,
    feedforward_switch_projection,
    expanding_projection,
    contracting_projection,
):
    local_rows, hidden_size = incoming_signals.shape
    total_rows = 8 * local_rows
    slots_here = token_counts_per_slot.shape[0]
    dp_rank, tensor_rank = lax.axis_index("dp"), lax.axis_index("tensor")
    side = lax.rem(dp_rank, 2)
    row_ids = tensor_rank * local_rows + jnp.arange(local_rows, dtype=jnp.int32)
    slot_match = (row_ids // SEQ_LEN)[:, None] == jnp.arange(slots_here, dtype=jnp.int32)[None, :]
    row_lengths = jnp.sum(jnp.where(slot_match, token_counts_per_slot[None, :], 0), axis=1)
    valid_rows = (row_ids % SEQ_LEN < row_lengths)[:, None]

    def exchange(weight, axis, join):
        half = weight.shape[axis] // 2
        keep = lax.dynamic_slice_in_dim(weight, side * half, half, axis)
        give = lax.dynamic_slice_in_dim(weight, (1 - side) * half, half, axis)
        take = lax.ppermute(give, "dp", swap)
        return jnp.where(
            side == 0,
            jnp.concatenate([keep, take], axis=join),
            jnp.concatenate([take, keep], axis=join),
        )

    def spread(block, axis):
        return lax.all_gather(block, "dp", axis=axis, tiled=True, axis_index_groups=groups)

    query_half = exchange(question_projection, 1, 0)
    key_half = exchange(lookup_projection, 1, 0)
    query_key = spread(jnp.concatenate([query_half, key_half], axis=1), 0)
    value_full = spread(exchange(content_projection, 1, 0), 0)
    swish_full = spread(exchange(silu_switch_projection, 1, 0), 0)
    output_full = spread(exchange(retention_result_projection, 0, 1), 1)
    gate_full = spread(exchange(feedforward_switch_projection, 1, 0), 0)
    up_full = spread(exchange(expanding_projection, 1, 0), 0)
    down_full = spread(exchange(contracting_projection, 0, 1), 1)

    gains = jnp.stack(
        [leading_norm_multiplier, leading_norm_offset, trailing_norm_multiplier, trailing_norm_offset]
    )
    gains = lax.all_gather(gains, "dp", axis=1, tiled=True).astype(F32)
    gains = jnp.concatenate([gains, gains], axis=0)

    all_rows = jax.ShapeDtypeStruct((total_rows, hidden_size), BF16)
    own_rows = jax.ShapeDtypeStruct((local_rows, hidden_size), F32)
    pieces = jax.ShapeDtypeStruct((2, 8, hidden_size), F32)
    row_low = pltpu.VMEM((local_rows, hidden_size), BF16)
    reduce_scratch = Reduce.scratch(local_rows, hidden_size)
    moved = total_rows * hidden_size * 2

    out_low = jnp.where(valid_rows, loss_sensitivity, 0)
    normed_all, out_all = call(
        first_kernel,
        0,
        (incoming_signals, out_low, gains),
        [VM, VM, VM],
        (all_rows, all_rows),
        (ANY, ANY),
        [row_low, *Gather.scratch(), *Gather.scratch()],
        24 * moved,
    )

    slot_count = total_rows // SEQ_LEN
    shape_key = (slot_count, SEQ_LEN, KEY_DIM)
    shape_value = (slot_count, SEQ_LEN, VAL_DIM)
    query_key_proj = matmul(normed_all, query_key)
    query_proj = query_key_proj[:, :KEY_DIM].reshape(shape_key)
    key_proj = query_key_proj[:, KEY_DIM:].reshape(shape_key)
    value_heads = matmul(normed_all, value_full).reshape(shape_value).astype(BF16)
    swish_heads = matmul(normed_all, swish_full).reshape(shape_value)
    cosines, sines = rotary_tables(SEQ_LEN, KEY_DIM)
    decays = decay_table(SEQ_LEN, tensor_rank * 2 + side)
    query_rot = (query_proj * cosines + rotate_half(query_proj) * sines).astype(BF16)
    key_rot = ((key_proj * cosines + rotate_half(key_proj) * sines) * KEY_DIM ** (-0.5)).astype(BF16)
    scores = (
        jnp.einsum("snk,smk->snm", query_rot, key_rot, preferred_element_type=F32) * decays[None]
    ).astype(BF16)
    retained = jnp.einsum("snm,smv->snv", scores, value_heads, preferred_element_type=F32)
    group_hat, group_inverse = normalize(retained, GROUP_EPSILON)
    sigmoid_gate = jax.nn.sigmoid(swish_heads)
    gated = (swish_heads * sigmoid_gate * group_hat).reshape(total_rows, VAL_DIM).astype(BF16)
    retention_part = matmul(gated, output_full).astype(BF16)

    mixer_all, middle_rows = call(
        second_kernel,
        1,
        (retention_part, incoming_signals, gains),
        [ANY, VM, VM],
        (all_rows, own_rows),
        (ANY, VM),
        [row_low, *reduce_scratch, *Gather.scratch()],
        24 * moved,
    )

    gate_proj = matmul(mixer_all, gate_full)
    up_proj = matmul(mixer_all, up_full)
    gelu_gate, gelu_back = jax.vjp(gelu_tanh, gate_proj)
    hidden = (gelu_gate * up_proj).astype(BF16)
    down_gradient = matmul(hidden.T, out_all).astype(BF16)
    hidden_back = matmul(out_all, down_full.T)
    gate_back = gelu_back(hidden_back * up_proj)[0].astype(BF16)
    up_back = (hidden_back * gelu_gate).astype(BF16)
    gate_gradient = matmul(mixer_all.T, gate_back).astype(BF16)
    up_gradient = matmul(mixer_all.T, up_back).astype(BF16)
    mixer_input_part = (matmul(gate_back, gate_full.T) + matmul(up_back, up_full.T)).astype(BF16)
    mixer_part = matmul(hidden, down_full).astype(BF16)

    middle_all, middle_back, after_pieces = call(
        third_kernel,
        2,
        (mixer_input_part, middle_rows, out_low, gains),
        [ANY, VM, VM, VM],
        (all_rows, own_rows, pieces),
        (ANY, VM, VM),
        [row_low, *reduce_scratch, *Gather.scratch()],
        24 * moved,
    )

    output_gradient = matmul(gated.T, middle_all).astype(BF16)
    gated_back = matmul(middle_all, output_full.T).reshape(shape_value)
    swish_back = (
        (gated_back * group_hat * sigmoid_gate * (1.0 + swish_heads * (1.0 - sigmoid_gate)))
        .reshape(total_rows, VAL_DIM)
        .astype(BF16)
    )
    retained_back = normalize_back(
        gated_back * swish_heads * sigmoid_gate, group_hat, group_inverse
    ).astype(BF16)
    score_back = (
        jnp.einsum("snv,smv->snm", retained_back, value_heads, preferred_element_type=F32)
        * decays[None]
    ).astype(BF16)
    query_rot_back = jnp.einsum("snm,smk->snk", score_back, key_rot, preferred_element_type=F32)
    key_rot_back = jnp.einsum("snm,snk->smk", score_back, query_rot, preferred_element_type=F32)
    value_back = jnp.einsum("snm,snv->smv", scores, retained_back, preferred_element_type=F32)
    query_back = (
        (query_rot_back * cosines - rotate_half(query_rot_back) * sines)
        .reshape(total_rows, KEY_DIM)
        .astype(BF16)
    )
    key_back = (
        ((key_rot_back * cosines - rotate_half(key_rot_back) * sines) * KEY_DIM ** (-0.5))
        .reshape(total_rows, KEY_DIM)
        .astype(BF16)
    )
    value_low = value_back.reshape(total_rows, VAL_DIM).astype(BF16)
    swish_gradient = matmul(normed_all.T, swish_back).astype(BF16)
    value_gradient = matmul(normed_all.T, value_low).astype(BF16)
    query_key_back = jnp.concatenate([query_back, key_back], axis=1)
    query_key_gradient = matmul(normed_all.T, query_key_back).astype(BF16)
    first_part = (
        matmul(query_key_back, query_key.T)
        + matmul(value_low, value_full.T)
        + matmul(swish_back, swish_full.T)
    ).astype(BF16)

    delta, final_rows, before_pieces = call(
        fourth_kernel,
        3,
        (first_part, mixer_part, incoming_signals, middle_rows, gains),
        [ANY, ANY, VM, VM, VM],
        (own_rows, own_rows, pieces),
        (VM, VM, VM),
        [*reduce_scratch, *reduce_scratch],
        24 * moved,
    )
    layer_output = jnp.where(valid_rows, final_rows, 0.0).astype(BF16)
    input_delta = middle_back + delta

    gain_pieces = jnp.concatenate(
        [jnp.sum(before_pieces, axis=1), jnp.sum(after_pieces, axis=1)], axis=0
    )
    gain_sums = lax.psum(gain_pieces, ("dp", "tensor"))
    width = leading_norm_multiplier.shape[0]
    gain_sums = lax.dynamic_slice_in_dim(gain_sums, dp_rank * width, width, 1)

    def collect(gradient, axis):
        return lax.psum_scatter(
            gradient, "dp", scatter_dimension=axis, tiled=True, axis_index_groups=groups
        )

    def restore(block, axis, join):
        half = block.shape[axis] // 2
        keep = lax.dynamic_slice_in_dim(block, side * half, half, axis)
        give = lax.dynamic_slice_in_dim(block, (1 - side) * half, half, axis)
        take = lax.ppermute(give, "dp", swap)
        return jnp.where(
            side == 0,
            jnp.concatenate([keep, take], axis=join),
            jnp.concatenate([take, keep], axis=join),
        ).astype(F32)

    down_owned = restore(collect(down_gradient, 1), 1, 0)
    gate_owned = restore(collect(gate_gradient, 0), 0, 1)
    up_owned = restore(collect(up_gradient, 0), 0, 1)
    output_owned = restore(collect(output_gradient, 1), 1, 0)
    swish_owned = restore(collect(swish_gradient, 0), 0, 1)
    value_owned = restore(collect(value_gradient, 0), 0, 1)
    query_key_owned = collect(query_key_gradient, 0)
    query_owned = restore(query_key_owned[:, :KEY_DIM], 0, 1)
    key_owned = restore(query_key_owned[:, KEY_DIM:], 0, 1)
    return (
        layer_output,
        input_delta,
        gain_sums[0],
        gain_sums[1],
        query_owned,
        key_owned,
        value_owned,
        swish_owned,
        output_owned,
        gain_sums[2],
        gain_sums[3],
        gate_owned,
        up_owned,
        down_owned,
    )


PLANES = 4
QK, VALUE, SWISH, OUTPUT, GATE, UP, DOWN = range(7)
WIDE = 512
QUERY, KEY = 7, 8
GRADIENTS = (DOWN, GATE, UP, OUTPUT, SWISH, VALUE, QUERY, KEY)
TILE = 256


def nt(left, right):
    return lax.dot_general(left, right, (((1,), (1,)), ((), ())), preferred_element_type=F32)


def loop(count, body):
    def step(i, carry):
        body(i)
        return carry

    lax.fori_loop(0, count, step, 0)


def at(index, size):
    return pl.ds(pl.multiple_of(index * size, size), size)


def mega_scratch(rows, hidden):
    total = 8 * rows
    dma = pltpu.SemaphoreType.DMA
    return dict(
        w=pltpu.VMEM((7, hidden, WIDE), BF16),
        xs=pltpu.VMEM((total, hidden), BF16),
        xt=pltpu.VMEM((hidden, total), BF16),
        outs=pltpu.VMEM((total, hidden), BF16),
        part=pltpu.VMEM((total, hidden), BF16),
        theirs=pltpu.VMEM((4, rows, hidden), BF16),
        got=pltpu.VMEM((2, rows, hidden), BF16),
        across=pltpu.VMEM((2, rows // 2, hidden), BF16),
        q=pltpu.VMEM((total, KEY_DIM), BF16),
        k=pltpu.VMEM((total, KEY_DIM), BF16),
        v=pltpu.VMEM((total, VAL_DIM), BF16),
        sc=pltpu.VMEM((total, SEQ_LEN), BF16),
        swish=pltpu.VMEM((total, VAL_DIM), F32),
        ghat=pltpu.VMEM((total, VAL_DIM), F32),
        ginv=pltpu.VMEM((total, 128), F32),
        gated=pltpu.VMEM((total, VAL_DIM), BF16),
        hid=pltpu.VMEM((total, WIDE), BF16),
        gate=pltpu.VMEM((total, WIDE), F32),
        up=pltpu.VMEM((total, WIDE), F32),
        gb=pltpu.VMEM((total, WIDE), BF16),
        ub=pltpu.VMEM((total, WIDE), BF16),
        sb=pltpu.VMEM((total, SEQ_LEN), BF16),
        qkb=pltpu.VMEM((total, 2 * KEY_DIM), BF16),
        turned=pltpu.VMEM((WIDE, total), BF16),
        st=pltpu.VMEM((4, WIDE, WIDE), BF16),
        decay=pltpu.VMEM((SEQ_LEN, SEQ_LEN), F32),
        low=pltpu.VMEM((rows, hidden), BF16),
        middle=pltpu.VMEM((rows, hidden), F32),
        back=pltpu.VMEM((rows, hidden), F32),
        pieces=pltpu.VMEM((4, 8, hidden), F32),
        gparts=pltpu.VMEM((8, 8, 256), F32),
        gain=pltpu.VMEM((8, hidden), F32),
        gsend=pltpu.VMEM((8, 8, 256), F32),
        gsum=pltpu.VMEM((4, 8, 256), F32),
        xr=pltpu.VMEM((rows, hidden), BF16),
        cr=pltpu.VMEM((rows, hidden), BF16),
        gown=pltpu.VMEM((8, 256), F32),
        ex_s=dma((8,)),
        ex_r=dma((8,)),
        ex_l=dma((8,)),
        zs=dma((7, 2, 4)),
        zr=dma((7, 2, 4)),
        rs=dma((8, 3)),
        rr=dma((8, 4)),
        ra=dma((8, 2)),
        stl=dma((4,)),
        fl=dma((4,)),
        fe_s=dma((8,)),
        fe_r=dma((8,)),
        gg_s=dma((8,)),
        gg_r=dma((8,)),
        gt_s=dma((4,)),
        gt_r=dma((4,)),
        ga_s=dma((13,)),
        ga_r=dma((13,)),
        gc_s=dma((13,)),
        gc_r=dma((13,)),
        re_s=dma((10,)),
        re_r=dma((10,)),
        ol=dma((6,)),
        free=pltpu.SemaphoreType.REGULAR,
    )


class PlaneSum(Reduce):
    def __init__(self, place, part, theirs, got, across, send, recv):
        p = place
        rows = theirs.shape[1]
        h = rows // 2
        self.rows, self.half, self.part = rows, h, part
        self.theirs, self.got, self.across = theirs, got, across
        self.base = [p.block(j) * rows for j in range(4)]

        def remote(k, source, target_ref, target):
            return pltpu.make_async_remote_copy(
                src_ref=source,
                dst_ref=target_ref,
                send_sem=send.at[k],
                recv_sem=recv.at[k],
                device_id=target,
                device_id_type=MESH,
            )

        def piece(j, lo):
            return part.at[pl.ds(pl.multiple_of(self.base[j] + lo, 8), h)]

        a, b = pl.ds(0, h), pl.ds(h, h)
        self.swap = [
            remote(j, part.at[rows_of(p.block(j, 1), rows)], theirs.at[j], p.sib) for j in range(4)
        ]
        self.da = remote(4, piece(3, 0), across.at[0], p.xn)
        self.db = remote(5, piece(3, h), across.at[1], p.yn)
        self.xa = remote(6, piece(1, 0), got.at[0, a], p.xn)
        self.xb = remote(7, piece(1, h), got.at[0, b], p.xn)
        self.ya = remote(8, piece(2, 0), got.at[1, a], p.yn)
        self.yb = remote(9, piece(2, h), got.at[1, b], p.yn)

    def add(self, j, lo, n, other, other_lo):
        def body(i):
            r = pl.ds(pl.multiple_of(self.base[j] + lo + i * CHUNK, CHUNK), CHUNK)
            q = pl.ds(pl.multiple_of(other_lo + i * CHUNK, CHUNK), CHUNK)
            self.part[r] = (self.part[r].astype(F32) + other[q].astype(F32)).astype(BF16)

        loop(n // CHUNK, body)

    def start(self):
        for j in (3, 1, 2, 0):
            self.swap[j].start()

    def run(self):
        rows, h = self.rows, self.half
        for j, copies in ((3, (self.da, self.db)), (1, (self.xa,)), (2, (self.yb,))):
            self.swap[j].wait_recv()
            self.add(j, 0, rows, self.theirs.at[j], 0)
            for copy in copies:
                copy.start()
        self.db.wait_recv()
        self.add(1, h, h, self.across.at[1], 0)
        self.xb.start()
        self.da.wait_recv()
        self.add(2, 0, h, self.across.at[0], 0)
        self.ya.start()
        self.swap[0].wait_recv()
        for copy in (self.xa, self.yb, self.xb, self.ya):
            copy.wait_recv()

    def total(self, i):
        r = pl.ds(pl.multiple_of(i * CHUNK, CHUNK), CHUNK)
        mine = pl.ds(pl.multiple_of(self.base[0] + i * CHUNK, CHUNK), CHUNK)
        pieces = (self.part[mine], self.theirs[0, r], self.got[0, r], self.got[1, r])
        one, two, three, four = (piece.astype(F32) for piece in pieces)
        return (one + two) + (three + four)


def mega_kernel(names, count_in, count_out, *refs):
    x_hbm, cot_hbm, counts_ref, cos_ref, sin_ref = refs[:5]
    gain_refs = refs[5:9]
    q_w, k_w, v_w, s_w, o_w, g_w, u_w, d_w = refs[9:count_in]
    outs = refs[count_in : count_in + count_out]
    final_out, delta_out, gains_out, q_g, k_g, v_g, s_g, o_g, g_g, u_g, d_g, stage, heard, added = outs
    b = {name: ref for name, ref in zip(names, refs[count_in + count_out :], strict=True)}
    w, xs, xt, st, part, turned = b["w"], b["xs"], b["xt"], b["st"], b["part"], b["turned"]
    x_ref, cot_ref = b["xr"], b["cr"]
    rows, hidden = x_ref.shape
    width = hidden // 8

    dp, tensor = lax.axis_index("dp"), lax.axis_index("tensor")
    place = Place()
    x, z = place.x, dp // 2
    first_plane, inner = z == 0, (z == 1) | (z == 2)
    outer = jnp.logical_not(inner)

    barrier = pltpu.get_barrier_semaphore()
    for i in range(1, 8):
        other = (lax.rem(dp + i, 8), tensor)
        pl.semaphore_signal(barrier, inc=1, device_id=other, device_id_type=MESH)
    for i in range(1, 4):
        other = (dp, lax.rem(tensor + i, 4))
        pl.semaphore_signal(barrier, inc=1, device_id=other, device_id_type=MESH)

    def remote(source, target_ref, send, recv, target):
        return pltpu.make_async_remote_copy(
            src_ref=source,
            dst_ref=target_ref,
            send_sem=send,
            recv_sem=recv,
            device_id=target,
            device_id_type=MESH,
        )

    def plane(step):
        return ((z + step) * 2 + x, tensor)

    def column_exchange(n, weight, k, lane, half):
        where = w.at[k, pl.ds(pl.multiple_of(z * 512 + x * 256, 256), width), pl.ds(lane, half)]
        keep = pltpu.make_async_copy(weight.at[:, at(x, half)], where, b["ex_l"].at[n])
        give = remote(
            weight.at[:, at(1 - x, half)], where, b["ex_s"].at[n], b["ex_r"].at[n], place.xn
        )
        return keep, give

    def row_exchange(n, weight, k):
        where = w.at[k, at(z, 512), at(x, width)]
        keep = pltpu.make_async_copy(weight.at[at(x, 512)], where, b["ex_l"].at[n])
        give = remote(weight.at[at(1 - x, 512)], where, b["ex_s"].at[n], b["ex_r"].at[n], place.xn)
        return keep, give

    exchanges = [
        [column_exchange(0, q_w, QK, 0, 256), column_exchange(1, k_w, QK, 256, 256)],
        [column_exchange(2, v_w, VALUE, 0, 512)],
        [column_exchange(3, s_w, SWISH, 0, 512)],
        [row_exchange(4, o_w, OUTPUT)],
        [column_exchange(5, g_w, GATE, 0, 512)],
        [column_exchange(6, u_w, UP, 0, 512)],
        [row_exchange(7, d_w, DOWN)],
    ]

    def keep(k):
        for local, _ in exchanges[k]:
            local.start()

    def give(k):
        for _, send in exchanges[k]:
            send.start()

    towards = jnp.where(z == 1, -1, 1)
    near, far = jnp.where(z == 1, 2, 1), jnp.where(z == 1, 3, 0)
    own_steps = (
        jnp.where(first_plane, 2, jnp.where(inner, 1, -2)),
        jnp.where(first_plane, 1, -1),
    )
    beside = place.xn

    def parts(k):
        return (0, 1) if k == QK else (0,)

    def block_copy(k, block, half, slot, target):
        if k == QK:
            side = x if half == 0 else 1 - x
            ref = w.at[k, pl.ds(pl.multiple_of(block * 512 + side * 256, 256), 256)]
        else:
            ref = w.at[k, at(block, 512)]
        return remote(ref, ref, b["zs"].at[k, half, slot], b["zr"].at[k, half, block], target)

    def kept(k):
        for local, _ in exchanges[k]:
            local.wait()

    def swapped(k):
        for _, send in exchanges[k]:
            send.wait_recv()

    def spread_half(k, half):
        for slot, step in enumerate(own_steps):
            block_copy(k, z, half, slot, plane(step)).start()

    def spread(k):
        kept(k)
        swapped(k)
        spread_half(k, 0)

    def pass_on(k):
        @pl.when(inner)
        def _():
            for half in parts(k):
                for slot, block in ((2, near), (3, far)):
                    copy = block_copy(k, block, half, slot, plane(towards))
                    copy.wait_recv()
                    copy.start()

    def arrive(k):
        for half in parts(k):

            @pl.when(inner)
            def _(half=half):
                block_copy(k, jnp.where(z == 1, 0, 3), half, 0, beside).wait_recv()

            @pl.when(outer)
            def _(half=half):
                for i in range(3):
                    block = jnp.where(first_plane, i + 1, i)
                    block_copy(k, block, half, 0, beside).wait_recv()

    def weights_sent():
        for k in range(7):
            for _, send in exchanges[k]:
                send.wait_send()
            for half in parts(k):
                for slot in range(2):
                    block_copy(k, z, half, slot, beside).wait_send()

                @pl.when(inner)
                def _(k=k, half=half):
                    for slot in (2, 3):
                        block_copy(k, z, half, slot, beside).wait_send()

    def lanes_of(c):
        if c in (QUERY, KEY):
            return QK, pl.ds(256 * (c - QUERY), 256)
        return c, pl.ds(0, 512)

    def share(ref, c, *index):
        chunk, lanes = lanes_of(c)
        return ref.at[(chunk, *index, slice(None), lanes)]

    def slot_of(c, slot):
        return st.at[slot, :, pl.ds(0, 256 if c in (QUERY, KEY) else 512)]

    def number(c):
        return c if c < QUERY else c - QUERY + (0 if c == QUERY else 6)

    def staged(c, block, slot):
        return pltpu.make_async_copy(slot_of(c, slot), share(stage, c, block), b["stl"].at[slot])

    def to_added(c, block, which, target):
        n = number(c)
        return remote(
            share(stage, c, block),
            share(added, c, which),
            b["rs"].at[n, which],
            b["ra"].at[n, which],
            target,
        )

    def to_heard(c, block, slot, target):
        n = number(c)
        return remote(
            share(stage, c, block), share(heard, c, z), b["rs"].at[n, slot], b["rr"].at[n, z], target
        )

    def send_gradient(c):
        for block in range(PLANES):
            staged(c, block, block).wait()
        step = jnp.where(first_plane, 1, -1)

        @pl.when(outer)
        def _():
            to_added(c, 3 - z, 0, plane(step)).start()
            to_added(c, z + 2 * step, 1, plane(step)).start()
            to_heard(c, z + step, 2, plane(step)).start()

        @pl.when(inner)
        def _():
            to_heard(c, z + towards, 2, plane(towards)).start()

    def rounds(c, body):
        lanes = 256 if c in (QUERY, KEY) else 512

        def step(i):
            body(pl.ds(pl.multiple_of(i * 32, 32), 32), pl.ds(0, lanes))

        loop(WIDE // 32, step)

    def local(source, target, n):
        return pltpu.make_async_copy(source, target, b["fl"].at[n])

    def combine(c):
        @pl.when(inner)
        def _():
            blocks = (far, near)
            mine = [local(share(stage, c, blocks[i]), slot_of(c, i), i) for i in range(2)]
            for copy in mine:
                copy.start()
            theirs = [local(share(added, c, i), slot_of(c, 2 + i), 2 + i) for i in range(2)]
            for i in range(2):
                to_added(c, blocks[i], i, beside).wait_recv()
                theirs[i].start()
            for i in range(2):
                mine[i].wait()
                theirs[i].wait()

                def body(r, lanes, i=i):
                    st[i, r, lanes] = (
                        st[i, r, lanes].astype(F32) + st[2 + i, r, lanes].astype(F32)
                    ).astype(BF16)

                rounds(c, body)
                back = local(slot_of(c, i), share(stage, c, blocks[i]), i)
                back.start()
            for i, step in enumerate((-2 * towards, -towards)):
                local(slot_of(c, i), share(stage, c, blocks[i]), i).wait()
                to_heard(c, blocks[i], i, plane(step)).start()

    homes = {
        QUERY: q_g, KEY: k_g, VALUE: v_g, SWISH: s_g, OUTPUT: o_g, GATE: g_g, UP: u_g, DOWN: d_g
    }

    def home_copies(c, source):
        home, (_, lanes) = homes[c], lanes_of(c)
        if c in (OUTPUT, DOWN):
            kept_half, given_half = (slice(None), at(x, 256)), (slice(None), at(1 - x, 256))
            slot = home.at[at(x, 512)]
        else:
            kept_half, given_half = (at(x, 256),), (at(1 - x, 256),)
            slot = home.at[:, at(x, home.shape[1] // 2)]
        n = number(c)
        return (
            local(slot_of(c, 0).at[kept_half], slot, 3),
            remote(source.at[given_half], slot, b["fe_s"].at[n], b["fe_r"].at[n], beside),
        )

    sources = (jnp.where(z == 1, 0, 1), jnp.where(z == 2, 3, 2))

    def finish_gradient(c, last=False):
        n = number(c)
        own = local(share(stage, c, z), slot_of(c, 0), 0)
        own.start()
        loads = []
        for i, source in enumerate(sources):
            remote(
                share(stage, c, 0), share(heard, c, source), b["rs"].at[n, 2], b["rr"].at[n, source], beside
            ).wait_recv()
            loads.append(local(share(heard, c, source), slot_of(c, 1 + i), 1 + i))
            loads[-1].start()
        own.wait()
        for load in loads:
            load.wait()

        def body(r, lanes):
            st[0, r, lanes] = (
                st[0, r, lanes].astype(F32)
                + (st[1, r, lanes].astype(F32) + st[2, r, lanes].astype(F32))
            ).astype(BF16)

        rounds(c, body)
        source = slot_of(c, 0) if last else share(stage, c, z)
        stay, send = home_copies(c, source)
        if not last:
            store = local(slot_of(c, 0), share(stage, c, z), 0)
            store.start()
            stay.start()
            store.wait()
            send.start()
            stay.wait()
        else:
            send.start()
            stay.start()
            stay.wait()

    def gradients_done():
        for c in GRADIENTS:
            n = number(c)
            source = slot_of(c, 0) if c == KEY else share(stage, c, z)
            _, send = home_copies(c, source)
            send.wait()
            for slot in range(3):
                remote(
                    share(stage, c, 0), share(heard, c, 0), b["rs"].at[n, slot], b["rr"].at[n, 0], beside
                ).wait_send()

    def gain_copy(i):
        target = lax.rem(dp + i, 8)
        return remote(
            b["gown"], b["gparts"].at[dp], b["gg_s"].at[i], b["gg_r"].at[dp], (target, tensor)
        )

    def gain_arrival(i):
        source = lax.rem(dp + i, 8)
        return remote(
            b["gown"], b["gparts"].at[source], b["gg_s"].at[i], b["gg_r"].at[source], (source, tensor)
        )

    gather_sems = (b["ga_s"], b["ga_r"])

    def plane_sum(ref):
        return PlaneSum(place, ref, b["theirs"], b["got"], b["across"], b["re_s"], b["re_r"])

    for k in range(7):
        keep(k)
    gown = b["gown"]
    for n in range(8):
        gown[n : n + 1, :] = gain_refs[n % 4][...].astype(F32).reshape(1, 256)
    load_x = pltpu.make_async_copy(x_hbm, x_ref, b["ol"].at[3])
    load_cot = pltpu.make_async_copy(cot_hbm, cot_ref, b["ol"].at[4])
    load_x.start()
    load_cot.start()
    mine = pltpu.make_async_copy(gown, b["gparts"].at[dp], b["ol"].at[0])
    mine.start()
    kept(QK)
    pl.semaphore_wait(barrier, 10)
    for i in range(1, 8):
        gain_copy(i).start()
    give(QK)
    spread_half(QK, 0)
    give(VALUE)
    head = (tensor * 2 + x).astype(F32)
    rate = jnp.log(1.0 - jnp.exp2(-5.0 - jnp.full((8, SEQ_LEN), head, F32)))[0:1]

    def body(i):
        r = at(i, 64)
        n = lax.broadcasted_iota(jnp.int32, (64, SEQ_LEN), 0) + i * 64
        m = lax.broadcasted_iota(jnp.int32, (64, SEQ_LEN), 1)
        gap = n - m
        b["decay"][r] = jnp.where(gap >= 0, jnp.exp(jnp.maximum(gap, 0).astype(F32) * rate), 0.0)

    loop(SEQ_LEN // 64, body)
    load_x.wait()
    swapped(QK)
    spread_half(QK, 1)
    mine.wait()
    for i in range(1, 8):
        gain_arrival(i).wait_recv()
    for i in range(8):
        b["gain"][:, i * 256 : (i + 1) * 256] = b["gparts"][i]
    gain = b["gain"]
    low = b["low"]

    def body(i):
        r = at(i, CHUNK)
        hat, _ = normalize(x_ref[r].astype(F32), EPSILON)
        low[r] = (hat * gain[0:1, :] + gain[1:2, :]).astype(BF16)

    loop(rows // CHUNK, body)
    first = Gather(place, low, xs, *gather_sems)
    first.start()
    spread(VALUE)
    load_cot.wait()
    count = counts_ref[0]

    def body(i):
        r = at(i, CHUNK)
        row = lax.broadcasted_iota(jnp.int32, (CHUNK, hidden), 0) + (tensor * rows + i * CHUNK)
        cot_ref[r] = jnp.where(row < count, cot_ref[r].astype(F32), 0.0).astype(BF16)

    loop(rows // CHUNK, body)
    first.forward()
    for k in range(SWISH, DOWN + 1):
        give(k)
    cotangent = Gather(place, cot_ref, b["outs"], b["gc_s"], b["gc_r"])
    cotangent.start()
    pass_on(QK)
    spread(SWISH)
    first.finish()

    def body(i):
        xt[at(i, 256), :] = xs[:, at(i, 256)].T

    loop(hidden // 256, body)

    arrive(QK)

    def turn(acc, tile, scale):
        spot = at(lax.rem(tile, SEQ_LEN // TILE), TILE)
        cos, sin = cos_ref[spot], sin_ref[spot]
        one, two = acc[:, :128], acc[:, 128:]
        return (((one * cos - two * sin) * scale).astype(BF16), ((two * cos + one * sin) * scale).astype(BF16))

    def body(i):
        r = at(i, TILE)
        acc = matmul(xs[r], w[QK])
        b["q"][r, :128], b["q"][r, 128:] = turn(acc[:, :KEY_DIM], i, 1.0)
        b["k"][r, :128], b["k"][r, 128:] = turn(acc[:, KEY_DIM:], i, KEY_DIM ** (-0.5))

    tiles = 8 * rows // TILE
    per_slot = SEQ_LEN // TILE
    loop(tiles, body)

    def slot_rows(i):
        return at(i // per_slot, SEQ_LEN)

    def body(i):
        r = at(i, TILE)
        decay = b["decay"][at(lax.rem(i, per_slot), TILE)]
        b["sc"][r] = (nt(b["q"][r], b["k"][slot_rows(i)]) * decay).astype(BF16)

    loop(tiles, body)

    pass_on(VALUE)
    spread(OUTPUT)
    arrive(VALUE)

    def body(i):
        r = at(i, TILE)
        b["v"][r] = matmul(xs[r], w[VALUE]).astype(BF16)

    loop(tiles, body)

    def body(i):
        r = at(i, TILE)
        retained = matmul(b["sc"][r], b["v"][slot_rows(i)])
        hat, inverse = normalize(retained, GROUP_EPSILON)
        b["ghat"][r] = hat
        b["ginv"][r] = jnp.broadcast_to(inverse, (TILE, 128))

    loop(tiles, body)
    cotangent.forward()
    cotangent.finish()

    pass_on(SWISH)
    spread(GATE)
    arrive(SWISH)

    def body(i):
        r = at(i, TILE)
        swish = matmul(xs[r], w[SWISH])
        b["swish"][r] = swish
        b["gated"][r] = (swish * jax.nn.sigmoid(swish) * b["ghat"][r]).astype(BF16)

    loop(tiles, body)

    pass_on(OUTPUT)
    spread(UP)
    pl.when(outer)(lambda: spread(DOWN))
    arrive(OUTPUT)

    def grid_of(i):
        return at(i // PLANES, TILE), at(lax.rem(i, PLANES), 512)

    def body(i):
        r, c = grid_of(i)
        part[r, c] = matmul(b["gated"][r], w[OUTPUT, c]).astype(BF16)

    loop(tiles * PLANES, body)
    reduce = plane_sum(part)
    reduce.start()
    reduce.run()
    pass_on(GATE)

    def body(i):
        r = at(i, CHUNK)
        middle = x_ref[r].astype(F32) + reduce.total(i)
        b["middle"][r] = middle
        hat, _ = normalize(middle, EPSILON)
        low[r] = (hat * gain[2:3, :] + gain[3:4, :]).astype(BF16)

    loop(rows // CHUNK, body)
    second = Gather(place, low, xs, *gather_sems)
    second.start()
    second.forward()
    second.finish()
    reduce.finish()

    pass_on(UP)
    pl.when(inner)(lambda: spread(DOWN))
    arrive(GATE)

    def body(i):
        r = at(i, TILE)
        b["gate"][r] = matmul(xs[r], w[GATE])

    loop(tiles, body)
    arrive(UP)

    def gelu_of(t):
        inner = 0.7978845608028654 * (t + 0.044715 * t * t * t)
        return 0.5 * (1.0 + jnp.tanh(inner)), jnp.tanh(inner)

    def body(i):
        r = at(i, TILE)
        up = matmul(xs[r], w[UP])
        b["up"][r] = up
        gate = b["gate"][r]
        share, _ = gelu_of(gate)
        b["hid"][r] = (gate * share * up).astype(BF16)

    loop(tiles, body)

    def turned_of(ref):
        def body(i):
            turned[:, at(i, TILE)] = ref[at(i, TILE)].T

        loop(tiles, body)

    def stage_block(c, i, value):
        st[i] = value.astype(BF16)
        staged(c, i, i).start()

    pass_on(DOWN)
    turned_of(b["hid"])

    def body(i):
        stage_block(DOWN, i, matmul(turned[...], b["outs"][:, at(i, 512)]))

    loop(PLANES, body)
    send_gradient(DOWN)
    arrive(DOWN)

    def times_turned(left, r, k):
        acc = nt(left[r, 0:512], w[k, 0:512])
        for plane_at in range(1, PLANES):
            lanes = slice(plane_at * 512, plane_at * 512 + 512)
            acc = acc + nt(left[r, lanes], w[k, lanes])
        return acc

    def body(i):
        r = at(i, TILE)
        back = times_turned(b["outs"], r, DOWN)
        gate, up = b["gate"][r], b["up"][r]
        share, tanh = gelu_of(gate)
        slope = 0.5 * gate * (1.0 - tanh * tanh) * (0.7978845608028654 * (1.0 + 0.134145 * gate * gate))
        b["gb"][r] = (back * up * (share + slope)).astype(BF16)
        b["ub"][r] = (back * gate * share).astype(BF16)

    loop(tiles, body)

    def weight_gradient(c, right):
        def body(i):
            def body_turn(j):
                turned[:, at(j, TILE)] = xs[at(j, TILE), at(i, 512)].T

            loop(tiles, body_turn)
            stage_block(c, i, matmul(turned[...], right[...]))

        loop(PLANES, body)
        send_gradient(c)

    weight_gradient(GATE, b["gb"])

    def body(i):
        r, c = grid_of(i)
        part[r, c] = (nt(b["gb"][r], w[GATE, c]) + nt(b["ub"][r], w[UP, c])).astype(BF16)

    loop(tiles * PLANES, body)
    reduce = plane_sum(part)
    reduce.start()
    weight_gradient(UP, b["ub"])
    reduce.run()
    b["pieces"][...] = jnp.zeros_like(b["pieces"])

    def body(i):
        r = at(i, CHUNK)
        upstream = reduce.total(i)
        hat, inverse = normalize(b["middle"][r], EPSILON)
        scaled = upstream * hat
        b["pieces"][2] += scaled[0:8] + scaled[8:16]
        b["pieces"][3] += upstream[0:8] + upstream[8:16]
        back = cot_ref[r].astype(F32) + normalize_back(upstream * gain[2:3, :], hat, inverse)
        b["back"][r] = back
        low[r] = back.astype(BF16)

    loop(rows // CHUNK, body)
    third = Gather(place, low, b["outs"], *gather_sems)
    third.start()
    third.forward()

    def body(i):
        r, c = grid_of(i)
        xs[r, c] = matmul(b["hid"][r], w[DOWN, c]).astype(BF16)

    loop(tiles * PLANES, body)
    third.finish()
    reduce.finish()

    turned_of(b["gated"])

    def body(i):
        stage_block(OUTPUT, i, matmul(turned[...], b["outs"][:, at(i, 512)]))

    loop(PLANES, body)
    send_gradient(OUTPUT)
    swb, rb, vlow = b["gb"], b["hid"], b["ub"]

    def body(i):
        r = at(i, TILE)
        back = times_turned(b["outs"], r, OUTPUT)
        swish, hat = b["swish"][r], b["ghat"][r]
        gate = jax.nn.sigmoid(swish)
        swb[r] = (back * hat * gate * (1.0 + swish * (1.0 - gate))).astype(BF16)
        rb[r] = normalize_back(back * swish * gate, hat, b["ginv"][r, 0:1]).astype(BF16)

    loop(tiles, body)

    def projection_gradient(c, right, lanes=slice(None)):
        def body(i):
            value = matmul(xt[at(i, 512)], right[:, lanes]).astype(BF16)
            st[i, :, 0 : value.shape[1]] = value
            staged(c, i, i).start()

        loop(PLANES, body)
        send_gradient(c)

    projection_gradient(SWISH, swb)
    combine(DOWN)

    def body(i):
        r = at(i, TILE)
        decay = b["decay"][at(lax.rem(i, per_slot), TILE)]
        b["sb"][r] = (nt(rb[r], b["v"][slot_rows(i)]) * decay).astype(BF16)

    loop(tiles, body)
    turned_of(b["sc"])

    def body(i):
        vlow[at(i, TILE)] = matmul(
            turned[at(lax.rem(i, per_slot), TILE), slot_rows(i)], rb[slot_rows(i)]
        ).astype(BF16)

    loop(tiles, body)
    projection_gradient(VALUE, vlow)
    turned_of(b["sb"])

    def turn_back(acc, tile, scale):
        spot = at(lax.rem(tile, per_slot), TILE)
        cos, sin = cos_ref[spot], sin_ref[spot]
        one, two = acc[:, :128], acc[:, 128:]
        return (((one * cos + two * sin) * scale).astype(BF16), ((two * cos - one * sin) * scale).astype(BF16))

    def body(i):
        r = at(i, TILE)
        qkb = b["qkb"]
        query = matmul(b["sb"][r], b["k"][slot_rows(i)])
        qkb[r, 0:128], qkb[r, 128:256] = turn_back(query, i, 1.0)
        key = matmul(turned[at(lax.rem(i, per_slot), TILE), slot_rows(i)], b["q"][slot_rows(i)])
        qkb[r, 256:384], qkb[r, 384:512] = turn_back(key, i, KEY_DIM ** (-0.5))

    loop(tiles, body)
    projection_gradient(QUERY, b["qkb"], slice(0, 256))
    projection_gradient(KEY, b["qkb"], slice(256, 512))
    combine(GATE)

    def body(i):
        r, c = grid_of(i)
        part[r, c] = (
            nt(b["qkb"][r], w[QK, c]) + nt(vlow[r], w[VALUE, c]) + nt(swb[r], w[SWISH, c])
        ).astype(BF16)

    loop(tiles * PLANES, body)
    reduce = plane_sum(xs)
    reduce.start()
    reduce.run()

    def body(i):
        b["middle"][at(i, CHUNK)] += reduce.total(i)

    loop(rows // CHUNK, body)
    reduce.finish()
    for partner in (place.sib, place.xn, place.yn):
        pl.semaphore_signal(b["free"], inc=1, device_id=partner, device_id_type=MESH)
    final_copy = pltpu.make_async_copy(b["middle"], final_out, b["ol"].at[1])
    final_copy.start()
    combine(UP)
    finish_gradient(DOWN)
    pl.semaphore_wait(b["free"], 3)
    reduce = plane_sum(part)
    reduce.start()
    reduce.run()

    def body(i):
        r = at(i, CHUNK)
        upstream = reduce.total(i)
        hat, inverse = normalize(x_ref[r].astype(F32), EPSILON)
        scaled = upstream * hat
        b["pieces"][0] += scaled[0:8] + scaled[8:16]
        b["pieces"][1] += upstream[0:8] + upstream[8:16]
        b["back"][r] += normalize_back(upstream * gain[0:1, :], hat, inverse)

    loop(rows // CHUNK, body)
    reduce.finish()
    delta_copy = pltpu.make_async_copy(b["back"], delta_out, b["ol"].at[2])
    delta_copy.start()
    combine(OUTPUT)
    finish_gradient(GATE)

    for i in range(1, 8):
        gain_copy(i).wait_send()
    gsend, gparts, gsum = b["gsend"], b["gparts"], b["gsum"]
    for i in range(8):
        for n in range(4):
            lanes = slice(i * 256, i * 256 + 256)
            gsend[i, n : n + 1, :] = jnp.sum(b["pieces"][n, :, lanes], axis=0, keepdims=True)
            gsend[i, n + 4 : n + 5, :] = jnp.zeros((1, 256), F32)

    def share_copy(i):
        target = lax.rem(dp + i, 8)
        return remote(
            gsend.at[target], gparts.at[dp], b["gg_s"].at[i], b["gg_r"].at[dp], (target, tensor)
        )

    for i in range(1, 8):
        share_copy(i).start()
    combine(SWISH)
    finish_gradient(UP)
    combine(VALUE)
    finish_gradient(OUTPUT)
    combine(QUERY)
    finish_gradient(SWISH)
    combine(KEY)
    finish_gradient(VALUE)
    finish_gradient(QUERY)
    acc = gsend[dp]
    for i in range(1, 8):
        gain_arrival(i).wait_recv()
        acc = acc + gparts[lax.rem(dp + i, 8)]
    gsum[tensor] = acc

    def sum_copy(i, source):
        target = lax.rem(tensor + i, 4)
        return remote(
            gsum.at[source], gsum.at[source], b["gt_s"].at[i], b["gt_r"].at[source], (dp, target)
        )

    for i in range(1, 4):
        sum_copy(i, tensor).start()
    finish_gradient(KEY, last=True)
    for i in range(1, 4):
        sum_copy(i, lax.rem(tensor + i, 4)).wait_recv()
    for i in range(1, 4):
        sum_copy(i, tensor).wait_send()
    for i in range(1, 8):
        share_copy(i).wait_send()
    gains_out[...] = (gsum[0] + gsum[1]) + (gsum[2] + gsum[3])
    final_copy.wait()
    delta_copy.wait()
    weights_sent()
    gradients_done()


def whole_layer(
    incoming_signals,
    loss_sensitivity,
    token_counts_per_slot,
    leading_norm_multiplier,
    leading_norm_offset,
    question_projection,
    lookup_projection,
    content_projection,
    silu_switch_projection,
    retention_result_projection,
    trailing_norm_multiplier,
    trailing_norm_offset,
    feedforward_switch_projection,
    expanding_projection,
    contracting_projection,
):
    rows, hidden = incoming_signals.shape
    places = np.arange(SEQ_LEN, dtype=np.float32)
    middle = KEY_DIM // 2
    spectrum = np.float32(10000.0) ** (-np.arange(middle, dtype=np.float32) / np.float32(middle))
    angles = places[:, None] * spectrum[None, :]
    weights = (
        question_projection,
        lookup_projection,
        content_projection,
        silu_switch_projection,
        retention_result_projection,
        feedforward_switch_projection,
        expanding_projection,
        contracting_projection,
    )
    gains = (
        leading_norm_multiplier, leading_norm_offset, trailing_norm_multiplier, trailing_norm_offset
    )
    tables = (jnp.asarray(np.cos(angles)), jnp.asarray(np.sin(angles)))
    args = (incoming_signals, loss_sensitivity, token_counts_per_slot, *tables, *gains, *weights)
    scratch = mega_scratch(rows, hidden)
    shape = jax.ShapeDtypeStruct
    outs = (
        shape((rows, hidden), F32),
        shape((rows, hidden), F32),
        shape((8, 256), F32),
        *(shape(weight.shape, BF16) for weight in weights),
        shape((7, PLANES, WIDE, WIDE), BF16),
        shape((7, PLANES, WIDE, WIDE), BF16),
        shape((7, 2, WIDE, WIDE), BF16),
    )
    scalar = pl.BlockSpec(memory_space=pltpu.SMEM)
    results = pl.pallas_call(
        functools.partial(mega_kernel, tuple(scratch), len(args), len(outs)),
        out_shape=outs,
        in_specs=[ANY, ANY, scalar] + [VM] * 6 + [ANY] * 8,
        out_specs=tuple([ANY, ANY, VM] + [ANY] * 11),
        scratch_shapes=list(scratch.values()),
        compiler_params=pltpu.CompilerParams(
            collective_id=0, has_side_effects=True, vmem_limit_bytes=67043328
        ),
        name="whole_layer",
    )(*args)
    final_rows, delta, gain_sums = results[:3]
    owned = results[3:11]
    wide = pl.pallas_call(
        widen_kernel,
        out_shape=(
            shape((rows, hidden), BF16),
            shape((rows, hidden), F32),
            *(shape(weight.shape, F32) for weight in weights),
        ),
        in_specs=[scalar] + [ANY] * 10,
        out_specs=(ANY,) * 10,
        scratch_shapes=[
            pltpu.VMEM((rows, hidden), F32),
            pltpu.VMEM((rows, hidden), F32),
            pltpu.VMEM((rows, hidden), BF16),
            *(pltpu.VMEM(weight.shape, BF16) for weight in weights),
            *(pltpu.VMEM(weight.shape, F32) for weight in weights),
            pltpu.SemaphoreType.DMA((10,)),
            pltpu.SemaphoreType.DMA((10,)),
        ],
        compiler_params=pltpu.CompilerParams(vmem_limit_bytes=67043328),
        name="widen",
    )(token_counts_per_slot, final_rows, delta, *owned)
    query, key, value, swish, output, gate, up, down = wide[2:]
    return (
        wide[0],
        wide[1],
        gain_sums[0],
        gain_sums[1],
        query,
        key,
        value,
        swish,
        output,
        gain_sums[2],
        gain_sums[3],
        gate,
        up,
        down,
    )


def widen_kernel(counts_ref, *refs):
    sources, targets, scratch = refs[:10], refs[10:20], refs[20:]
    final, delta, low = scratch[:3]
    narrow, wide, (came, went) = scratch[3:11], scratch[11:19], scratch[19:]
    buffers = (final, delta, *narrow)
    loads = [
        pltpu.make_async_copy(source, buffer, came.at[i])
        for i, (source, buffer) in enumerate(zip(sources, buffers, strict=True))
    ]
    stores = [
        pltpu.make_async_copy(buffer, target, went.at[i])
        for i, (buffer, target) in enumerate(zip((low, delta, *wide), targets, strict=True))
    ]
    for load in loads:
        load.start()
    rows, hidden = final.shape
    tensor, count = lax.axis_index("tensor"), counts_ref[0]
    loads[0].wait()

    def body(i):
        r = at(i, CHUNK)
        row = lax.broadcasted_iota(jnp.int32, (CHUNK, hidden), 0) + (tensor * rows + i * CHUNK)
        low[r] = jnp.where(row < count, final[r], 0.0).astype(BF16)

    loop(rows // CHUNK, body)
    stores[0].start()
    loads[1].wait()
    stores[1].start()
    for n in range(8):
        loads[n + 2].wait()

        def body(i, n=n):
            r = at(i, 32)
            wide[n][r] = narrow[n][r].astype(F32)

        loop(narrow[n].shape[0] // 32, body)
        stores[n + 2].start()
    for store in stores:
        store.wait()


def solution(mesh):
    ranks = mesh.shape["dp"]
    groups = [[2 * k + side for k in range(ranks // 2)] for side in range(2)]
    swap = [(rank, rank + 1 - 2 * (rank % 2)) for rank in range(ranks)]
    rows, gain, column, row = P(("dp", "tensor"), None), P("dp"), P("dp", "tensor"), P("tensor", "dp")
    weights = (gain, gain, column, column, column, column, row, gain, gain, column, column, row)
    one_kernel = ranks == 8 and mesh.shape["tensor"] == 4
    return jax.shard_map(
        whole_layer if one_kernel else functools.partial(per_device, groups, swap),
        mesh=mesh,
        in_specs=(rows, rows, P("dp"), *weights),
        out_specs=(rows, rows, *weights),
        check_vma=False,
    )
```

```python
import functools

import jax
import jax.numpy as jnp
import numpy as np
from jax import lax
from jax.experimental import pallas as pl
from jax.experimental.pallas import tpu as pltpu
from jax.sharding import PartitionSpec as P

KEY_DIM = 256
VAL_DIM = 512
SEQ_LEN = 512

EPSILON = 1e-05
GROUP_EPSILON = 0.1

MESH = pl.DeviceIdType.MESH
F32 = jnp.float32
BF16 = jnp.bfloat16
CHUNK = 16


def normalize(values, epsilon):
    centre = values - jnp.mean(values, axis=-1, keepdims=True)
    inverse = lax.rsqrt(jnp.mean(centre * centre, axis=-1, keepdims=True) + epsilon)
    return (centre * inverse, inverse)


def normalize_back(upstream, normed, inverse):
    return inverse * (
        upstream
        - jnp.mean(upstream, axis=-1, keepdims=True)
        - normed * jnp.mean(upstream * normed, axis=-1, keepdims=True)
    )


def rotate_half(values):
    middle = values.shape[-1] // 2
    return jnp.concatenate([-values[..., middle:], values[..., :middle]], axis=-1)


def rotary_tables(span, columns):
    middle = columns // 2
    places = jnp.arange(span, dtype=jnp.int32).astype(jnp.float32)
    spectrum = 10000.0 ** (-jnp.arange(middle, dtype=jnp.int32).astype(jnp.float32) / middle)
    angles = places[:, None] * spectrum[None, :]
    angles = jnp.concatenate([angles, angles], axis=1)
    return (jnp.cos(angles)[None], jnp.sin(angles)[None])


def decay_table(span, head_id):
    log_rate = jnp.log(1.0 - jnp.exp2(-5.0 - head_id.astype(jnp.float32)))
    places = jnp.arange(span, dtype=jnp.int32)
    offsets = places[:, None] - places[None, :]
    decayed = jnp.exp(jnp.maximum(offsets, 0).astype(jnp.float32) * log_rate)
    return jnp.where(offsets >= 0, decayed, 0.0)


def gelu_tanh(values):
    return jax.nn.gelu(values, approximate=True)


def matmul(left, right):
    return jnp.dot(left, right, preferred_element_type=jnp.float32)


class Place:
    def __init__(self):
        d, t = lax.axis_index("dp"), lax.axis_index("tensor")
        self.x, self.y, self.c = lax.rem(d, 2), t // 2, lax.rem(t, 2)
        dx, ty = d + 1 - 2 * self.x, (1 - self.y) * 2 + self.c
        self.sib = (d, t + 1 - 2 * self.c)
        self.xn = (dx, t)
        self.yn = (d, ty)

    def block(self, j, other_core=0):
        x = 1 - self.x if j in (1, 3) else self.x
        y = 1 - self.y if j in (2, 3) else self.y
        c = 1 - self.c if other_core else self.c
        return x * 4 + y * 2 + c


def greet(place):
    barrier = pltpu.get_barrier_semaphore()
    for partner in (place.sib, place.xn, place.yn):
        pl.semaphore_signal(barrier, inc=1, device_id=partner, device_id_type=MESH)
    pl.semaphore_wait(barrier, 3)


def rows_of(index, rows):
    return pl.ds(pl.multiple_of(index * rows, rows), rows)


class Gather:
    @staticmethod
    def scratch():
        return [pltpu.SemaphoreType.DMA((13,)), pltpu.SemaphoreType.DMA((13,))]

    def __init__(self, place, src, out, send, recv):
        rows = src.shape[0]
        half = rows // 2
        p = place

        def remote(k, source, j, lo, n, target, core=0):
            where = pl.ds(pl.multiple_of(p.block(j, core) * rows + lo, 8), n)
            source = source.at[pl.ds(lo, n)] if source is src else source.at[where]
            return pltpu.make_async_remote_copy(
                src_ref=source,
                dst_ref=out.at[where],
                send_sem=send.at[k],
                recv_sem=recv.at[k],
                device_id=target,
                device_id_type=MESH,
            )

        self.p, self.rows, self.half = p, rows, half
        self.local = pltpu.make_async_copy(src, out.at[rows_of(p.block(0), rows)], send.at[12])
        h = half
        self.xa = remote(0, src, 0, 0, h, p.xn)
        self.xb = remote(1, src, 0, h, h, p.xn)
        self.ya = remote(2, src, 0, 0, h, p.yn)
        self.yb = remote(3, src, 0, h, h, p.yn)
        self.s0 = remote(4, src, 0, 0, rows, p.sib)
        self.da = remote(5, out, 1, 0, h, p.yn)
        self.db = remote(6, out, 2, h, h, p.xn)
        self.s1 = remote(7, out, 1, 0, rows, p.sib)
        self.s2 = remote(8, out, 2, 0, rows, p.sib)
        self.s3a = remote(9, out, 3, 0, h, p.sib)
        self.s3b = remote(10, out, 3, h, h, p.sib)

    def start(self):
        for copy in (self.xa, self.yb, self.xb, self.ya, self.s0, self.local):
            copy.start()

    def start_first_half(self):
        self.xa.start()
        self.ya.start()

    def start_second_half(self):
        for copy in (self.yb, self.xb, self.s0, self.local):
            copy.start()

    def forward(self):
        self.xa.wait_recv()
        self.da.start()
        self.yb.wait_recv()
        self.db.start()
        self.xb.wait_recv()
        self.s1.start()
        self.ya.wait_recv()
        self.s2.start()

    def finish(self):
        self.da.wait_recv()
        self.s3a.start()
        self.db.wait_recv()
        self.s3b.start()
        self.local.wait()
        for copy in (self.s0, self.s1, self.s2, self.s3a, self.s3b):
            copy.wait()
        for copy in (self.xa, self.xb, self.ya, self.yb, self.da, self.db):
            copy.wait_send()


class Reduce:
    @staticmethod
    def scratch(rows, columns):
        return [
            pltpu.VMEM((4, rows, columns), BF16),
            pltpu.VMEM((4, rows, columns), BF16),
            pltpu.VMEM((2, rows, columns), BF16),
            pltpu.VMEM((2, rows // 2, columns), BF16),
            pltpu.SemaphoreType.DMA((14,)),
            pltpu.SemaphoreType.DMA((10,)),
        ]

    def __init__(self, place, part, mine, theirs, got, across, send, recv):
        p = place
        rows = mine.shape[1]
        h = rows // 2
        self.rows, self.half = rows, h
        self.mine, self.theirs, self.got, self.across = mine, theirs, got, across

        def remote(k, source, target_ref, target):
            return pltpu.make_async_remote_copy(
                src_ref=source,
                dst_ref=target_ref,
                send_sem=send.at[k],
                recv_sem=recv.at[k],
                device_id=target,
                device_id_type=MESH,
            )

        a, b = pl.ds(0, h), pl.ds(h, h)
        self.load = [
            pltpu.make_async_copy(part.at[rows_of(p.block(j), rows)], mine.at[j], send.at[10 + j])
            for j in range(4)
        ]
        self.swap = [
            remote(j, part.at[rows_of(p.block(j, 1), rows)], theirs.at[j], p.sib) for j in range(4)
        ]
        self.da = remote(4, mine.at[3, a], across.at[0], p.xn)
        self.db = remote(5, mine.at[3, b], across.at[1], p.yn)
        self.xa = remote(6, mine.at[1, a], got.at[0, a], p.xn)
        self.xb = remote(7, mine.at[1, b], got.at[0, b], p.xn)
        self.ya = remote(8, mine.at[2, a], got.at[1, a], p.yn)
        self.yb = remote(9, mine.at[2, b], got.at[1, b], p.yn)

    def add(self, j, lo, n, other, other_lo):
        def body(i, carry):
            r = pl.ds(pl.multiple_of(lo + i * CHUNK, CHUNK), CHUNK)
            q = pl.ds(pl.multiple_of(other_lo + i * CHUNK, CHUNK), CHUNK)
            self.mine[j, r] = (self.mine[j, r].astype(F32) + other[q].astype(F32)).astype(BF16)
            return carry

        lax.fori_loop(0, n // CHUNK, body, 0)

    def start(self):
        for j in (3, 1, 2, 0):
            self.swap[j].start()
            self.load[j].start()

    def run(self):
        rows, h = self.rows, self.half
        for j, copies in ((3, (self.da, self.db)), (1, (self.xa,)), (2, (self.yb,))):
            self.load[j].wait()
            self.swap[j].wait_recv()
            self.add(j, 0, rows, self.theirs.at[j], 0)
            for copy in copies:
                copy.start()
        self.db.wait_recv()
        self.add(1, h, h, self.across.at[1], 0)
        self.xb.start()
        self.da.wait_recv()
        self.add(2, 0, h, self.across.at[0], 0)
        self.ya.start()
        self.load[0].wait()
        self.swap[0].wait_recv()
        for copy in (self.xa, self.yb, self.xb, self.ya):
            copy.wait_recv()

    def total(self, r):
        pieces = (self.mine[0, r], self.theirs[0, r], self.got[0, r], self.got[1, r])
        one, two, three, four = (piece.astype(F32) for piece in pieces)
        return (one + two) + (three + four)

    def finish(self):
        for copy in (*self.swap, self.da, self.db, self.xa, self.xb, self.ya, self.yb):
            copy.wait_send()


def chunks(rows, body):
    def step(i, carry):
        body(pl.ds(pl.multiple_of(i * CHUNK, CHUNK), CHUNK))
        return carry

    lax.fori_loop(0, rows // CHUNK, step, 0)


def first_kernel(x_ref, cot_ref, gains_ref, out_x, out_cot, normed, *sems):
    place = Place()
    greet(place)
    gain, shift = gains_ref[0:1, :], gains_ref[1:2, :]

    def body(r):
        hat, _ = normalize(x_ref[r].astype(F32), EPSILON)
        normed[r] = (hat * gain + shift).astype(BF16)

    chunks(x_ref.shape[0], body)
    one = Gather(place, normed, out_x, *sems[:2])
    two = Gather(place, cot_ref, out_cot, *sems[2:])
    one.start()
    two.start()
    one.forward()
    two.forward()
    one.finish()
    two.finish()


def second_kernel(part_ref, x_ref, gains_ref, out_all, middle_ref, normed, *scratch):
    place = Place()
    greet(place)
    reduce = Reduce(place, part_ref, *scratch[:6])
    reduce.start()
    reduce.run()
    gain, shift = gains_ref[2:3, :], gains_ref[3:4, :]

    def body(r):
        middle = x_ref[r].astype(F32) + reduce.total(r)
        middle_ref[r] = middle
        hat, _ = normalize(middle, EPSILON)
        normed[r] = (hat * gain + shift).astype(BF16)

    chunks(x_ref.shape[0], body)
    gather = Gather(place, normed, out_all, *scratch[6:])
    gather.start()
    gather.forward()
    gather.finish()
    reduce.finish()


def third_kernel(
    part_ref, middle_ref, cot_ref, gains_ref, out_all, back_ref, pieces_ref, low, *scratch
):
    place = Place()
    greet(place)
    reduce = Reduce(place, part_ref, *scratch[:6])
    reduce.start()
    pieces_ref[...] = jnp.zeros_like(pieces_ref)
    reduce.run()
    gain = gains_ref[2:3, :]

    def body(r):
        upstream = reduce.total(r)
        hat, inverse = normalize(middle_ref[r], EPSILON)
        scaled = upstream * hat
        pieces_ref[0] += scaled[0:8] + scaled[8:16]
        pieces_ref[1] += upstream[0:8] + upstream[8:16]
        back = cot_ref[r].astype(F32) + normalize_back(upstream * gain, hat, inverse)
        back_ref[r] = back
        low[r] = back.astype(BF16)

    chunks(middle_ref.shape[0], body)
    gather = Gather(place, low, out_all, *scratch[6:])
    gather.start()
    gather.forward()
    gather.finish()
    reduce.finish()


def fourth_kernel(
    first_ref, mixer_ref, x_ref, middle_ref, gains_ref, delta_ref, final_ref, pieces_ref, *scratch
):
    place = Place()
    greet(place)
    one = Reduce(place, first_ref, *scratch[:6])
    two = Reduce(place, mixer_ref, *scratch[6:])
    one.start()
    two.start()
    pieces_ref[...] = jnp.zeros_like(pieces_ref)
    one.run()
    two.run()
    gain = gains_ref[0:1, :]

    def body(r):
        upstream = one.total(r)
        hat, inverse = normalize(x_ref[r].astype(F32), EPSILON)
        scaled = upstream * hat
        pieces_ref[0] += scaled[0:8] + scaled[8:16]
        pieces_ref[1] += upstream[0:8] + upstream[8:16]
        delta_ref[r] = normalize_back(upstream * gain, hat, inverse)
        final_ref[r] = middle_ref[r] + two.total(r)

    chunks(x_ref.shape[0], body)
    one.finish()
    two.finish()


ANY = pl.BlockSpec(memory_space=pl.ANY)
VM = pl.BlockSpec(memory_space=pltpu.VMEM)


def call(kernel, ident, args, specs, outs, out_specs, scratch, nbytes):
    return pl.pallas_call(
        kernel,
        out_shape=outs,
        in_specs=specs,
        out_specs=out_specs,
        scratch_shapes=scratch,
        compiler_params=pltpu.CompilerParams(
            collective_id=ident, has_side_effects=True, vmem_limit_bytes=32 << 20
        ),
        cost_estimate=pl.CostEstimate(flops=0, bytes_accessed=nbytes, transcendentals=0),
        name=kernel.__name__,
    )(*args)


def per_device(
    groups,
    swap,
    incoming_signals,
    loss_sensitivity,
    token_counts_per_slot,
    leading_norm_multiplier,
    leading_norm_offset,
    question_projection,
    lookup_projection,
    content_projection,
    silu_switch_projection,
    retention_result_projection,
    trailing_norm_multiplier,
    trailing_norm_offset,
    feedforward_switch_projection,
    expanding_projection,
    contracting_projection,
):
    local_rows, hidden_size = incoming_signals.shape
    total_rows = 8 * local_rows
    slots_here = token_counts_per_slot.shape[0]
    dp_rank, tensor_rank = lax.axis_index("dp"), lax.axis_index("tensor")
    side = lax.rem(dp_rank, 2)
    row_ids = tensor_rank * local_rows + jnp.arange(local_rows, dtype=jnp.int32)
    slot_match = (row_ids // SEQ_LEN)[:, None] == jnp.arange(slots_here, dtype=jnp.int32)[None, :]
    row_lengths = jnp.sum(jnp.where(slot_match, token_counts_per_slot[None, :], 0), axis=1)
    valid_rows = (row_ids % SEQ_LEN < row_lengths)[:, None]

    def exchange(weight, axis, join):
        half = weight.shape[axis] // 2
        keep = lax.dynamic_slice_in_dim(weight, side * half, half, axis)
        give = lax.dynamic_slice_in_dim(weight, (1 - side) * half, half, axis)
        take = lax.ppermute(give, "dp", swap)
        return jnp.where(
            side == 0,
            jnp.concatenate([keep, take], axis=join),
            jnp.concatenate([take, keep], axis=join),
        )

    def spread(block, axis):
        return lax.all_gather(block, "dp", axis=axis, tiled=True, axis_index_groups=groups)

    query_half = exchange(question_projection, 1, 0)
    key_half = exchange(lookup_projection, 1, 0)
    query_key = spread(jnp.concatenate([query_half, key_half], axis=1), 0)
    value_full = spread(exchange(content_projection, 1, 0), 0)
    swish_full = spread(exchange(silu_switch_projection, 1, 0), 0)
    output_full = spread(exchange(retention_result_projection, 0, 1), 1)
    gate_full = spread(exchange(feedforward_switch_projection, 1, 0), 0)
    up_full = spread(exchange(expanding_projection, 1, 0), 0)
    down_full = spread(exchange(contracting_projection, 0, 1), 1)

    gains = jnp.stack(
        [leading_norm_multiplier, leading_norm_offset, trailing_norm_multiplier, trailing_norm_offset]
    )
    gains = lax.all_gather(gains, "dp", axis=1, tiled=True).astype(F32)
    gains = jnp.concatenate([gains, gains], axis=0)

    all_rows = jax.ShapeDtypeStruct((total_rows, hidden_size), BF16)
    own_rows = jax.ShapeDtypeStruct((local_rows, hidden_size), F32)
    pieces = jax.ShapeDtypeStruct((2, 8, hidden_size), F32)
    row_low = pltpu.VMEM((local_rows, hidden_size), BF16)
    reduce_scratch = Reduce.scratch(local_rows, hidden_size)
    moved = total_rows * hidden_size * 2

    out_low = jnp.where(valid_rows, loss_sensitivity, 0)
    normed_all, out_all = call(
        first_kernel,
        0,
        (incoming_signals, out_low, gains),
        [VM, VM, VM],
        (all_rows, all_rows),
        (ANY, ANY),
        [row_low, *Gather.scratch(), *Gather.scratch()],
        24 * moved,
    )

    slot_count = total_rows // SEQ_LEN
    shape_key = (slot_count, SEQ_LEN, KEY_DIM)
    shape_value = (slot_count, SEQ_LEN, VAL_DIM)
    query_key_proj = matmul(normed_all, query_key)
    query_proj = query_key_proj[:, :KEY_DIM].reshape(shape_key)
    key_proj = query_key_proj[:, KEY_DIM:].reshape(shape_key)
    value_heads = matmul(normed_all, value_full).reshape(shape_value).astype(BF16)
    swish_heads = matmul(normed_all, swish_full).reshape(shape_value)
    cosines, sines = rotary_tables(SEQ_LEN, KEY_DIM)
    decays = decay_table(SEQ_LEN, tensor_rank * 2 + side)
    query_rot = (query_proj * cosines + rotate_half(query_proj) * sines).astype(BF16)
    key_rot = ((key_proj * cosines + rotate_half(key_proj) * sines) * KEY_DIM ** (-0.5)).astype(BF16)
    scores = (
        jnp.einsum("snk,smk->snm", query_rot, key_rot, preferred_element_type=F32) * decays[None]
    ).astype(BF16)
    retained = jnp.einsum("snm,smv->snv", scores, value_heads, preferred_element_type=F32)
    group_hat, group_inverse = normalize(retained, GROUP_EPSILON)
    sigmoid_gate = jax.nn.sigmoid(swish_heads)
    gated = (swish_heads * sigmoid_gate * group_hat).reshape(total_rows, VAL_DIM).astype(BF16)
    retention_part = matmul(gated, output_full).astype(BF16)

    mixer_all, middle_rows = call(
        second_kernel,
        1,
        (retention_part, incoming_signals, gains),
        [ANY, VM, VM],
        (all_rows, own_rows),
        (ANY, VM),
        [row_low, *reduce_scratch, *Gather.scratch()],
        24 * moved,
    )

    gate_proj = matmul(mixer_all, gate_full)
    up_proj = matmul(mixer_all, up_full)
    gelu_gate, gelu_back = jax.vjp(gelu_tanh, gate_proj)
    hidden = (gelu_gate * up_proj).astype(BF16)
    down_gradient = matmul(hidden.T, out_all).astype(BF16)
    hidden_back = matmul(out_all, down_full.T)
    gate_back = gelu_back(hidden_back * up_proj)[0].astype(BF16)
    up_back = (hidden_back * gelu_gate).astype(BF16)
    gate_gradient = matmul(mixer_all.T, gate_back).astype(BF16)
    up_gradient = matmul(mixer_all.T, up_back).astype(BF16)
    mixer_input_part = (matmul(gate_back, gate_full.T) + matmul(up_back, up_full.T)).astype(BF16)
    mixer_part = matmul(hidden, down_full).astype(BF16)

    middle_all, middle_back, after_pieces = call(
        third_kernel,
        2,
        (mixer_input_part, middle_rows, out_low, gains),
        [ANY, VM, VM, VM],
        (all_rows, own_rows, pieces),
        (ANY, VM, VM),
        [row_low, *reduce_scratch, *Gather.scratch()],
        24 * moved,
    )

    output_gradient = matmul(gated.T, middle_all).astype(BF16)
    gated_back = matmul(middle_all, output_full.T).reshape(shape_value)
    swish_back = (
        (gated_back * group_hat * sigmoid_gate * (1.0 + swish_heads * (1.0 - sigmoid_gate)))
        .reshape(total_rows, VAL_DIM)
        .astype(BF16)
    )
    retained_back = normalize_back(
        gated_back * swish_heads * sigmoid_gate, group_hat, group_inverse
    ).astype(BF16)
    score_back = (
        jnp.einsum("snv,smv->snm", retained_back, value_heads, preferred_element_type=F32)
        * decays[None]
    ).astype(BF16)
    query_rot_back = jnp.einsum("snm,smk->snk", score_back, key_rot, preferred_element_type=F32)
    key_rot_back = jnp.einsum("snm,snk->smk", score_back, query_rot, preferred_element_type=F32)
    value_back = jnp.einsum("snm,snv->smv", scores, retained_back, preferred_element_type=F32)
    query_back = (
        (query_rot_back * cosines - rotate_half(query_rot_back) * sines)
        .reshape(total_rows, KEY_DIM)
        .astype(BF16)
    )
    key_back = (
        ((key_rot_back * cosines - rotate_half(key_rot_back) * sines) * KEY_DIM ** (-0.5))
        .reshape(total_rows, KEY_DIM)
        .astype(BF16)
    )
    value_low = value_back.reshape(total_rows, VAL_DIM).astype(BF16)
    swish_gradient = matmul(normed_all.T, swish_back).astype(BF16)
    value_gradient = matmul(normed_all.T, value_low).astype(BF16)
    query_key_back = jnp.concatenate([query_back, key_back], axis=1)
    query_key_gradient = matmul(normed_all.T, query_key_back).astype(BF16)
    first_part = (
        matmul(query_key_back, query_key.T)
        + matmul(value_low, value_full.T)
        + matmul(swish_back, swish_full.T)
    ).astype(BF16)

    delta, final_rows, before_pieces = call(
        fourth_kernel,
        3,
        (first_part, mixer_part, incoming_signals, middle_rows, gains),
        [ANY, ANY, VM, VM, VM],
        (own_rows, own_rows, pieces),
        (VM, VM, VM),
        [*reduce_scratch, *reduce_scratch],
        24 * moved,
    )
    layer_output = jnp.where(valid_rows, final_rows, 0.0).astype(BF16)
    input_delta = middle_back + delta

    gain_pieces = jnp.concatenate(
        [jnp.sum(before_pieces, axis=1), jnp.sum(after_pieces, axis=1)], axis=0
    )
    gain_sums = lax.psum(gain_pieces, ("dp", "tensor"))
    width = leading_norm_multiplier.shape[0]
    gain_sums = lax.dynamic_slice_in_dim(gain_sums, dp_rank * width, width, 1)

    def collect(gradient, axis):
        return lax.psum_scatter(
            gradient, "dp", scatter_dimension=axis, tiled=True, axis_index_groups=groups
        )

    def restore(block, axis, join):
        half = block.shape[axis] // 2
        keep = lax.dynamic_slice_in_dim(block, side * half, half, axis)
        give = lax.dynamic_slice_in_dim(block, (1 - side) * half, half, axis)
        take = lax.ppermute(give, "dp", swap)
        return jnp.where(
            side == 0,
            jnp.concatenate([keep, take], axis=join),
            jnp.concatenate([take, keep], axis=join),
        ).astype(F32)

    down_owned = restore(collect(down_gradient, 1), 1, 0)
    gate_owned = restore(collect(gate_gradient, 0), 0, 1)
    up_owned = restore(collect(up_gradient, 0), 0, 1)
    output_owned = restore(collect(output_gradient, 1), 1, 0)
    swish_owned = restore(collect(swish_gradient, 0), 0, 1)
    value_owned = restore(collect(value_gradient, 0), 0, 1)
    query_key_owned = collect(query_key_gradient, 0)
    query_owned = restore(query_key_owned[:, :KEY_DIM], 0, 1)
    key_owned = restore(query_key_owned[:, KEY_DIM:], 0, 1)
    return (
        layer_output,
        input_delta,
        gain_sums[0],
        gain_sums[1],
        query_owned,
        key_owned,
        value_owned,
        swish_owned,
        output_owned,
        gain_sums[2],
        gain_sums[3],
        gate_owned,
        up_owned,
        down_owned,
    )


PLANES = 4
QK, VALUE, SWISH, OUTPUT, GATE, UP, DOWN = range(7)
WIDE = 512
QUERY, KEY = 7, 8
FEED_FORWARD = (DOWN, GATE, UP)
GRADIENTS = (*FEED_FORWARD, OUTPUT, SWISH, VALUE, QUERY, KEY)
TILE = 256


def nt(left, right):
    return lax.dot_general(left, right, (((1,), (1,)), ((), ())), preferred_element_type=F32)


def loop(count, body):
    def step(i, carry):
        body(i)
        return carry

    lax.fori_loop(0, count, step, 0)


def at(index, size):
    return pl.ds(pl.multiple_of(index * size, size), size)


def mega_scratch(rows, hidden):
    total = 8 * rows
    dma = pltpu.SemaphoreType.DMA
    return dict(
        w=pltpu.VMEM((7, hidden, WIDE), BF16),
        xs=pltpu.VMEM((total, hidden), BF16),
        xt=pltpu.VMEM((hidden, total), BF16),
        outs=pltpu.VMEM((total, hidden), BF16),
        part=pltpu.VMEM((total, hidden), BF16),
        theirs=pltpu.VMEM((4, rows, hidden), BF16),
        got=pltpu.VMEM((2, rows, hidden), BF16),
        across=pltpu.VMEM((2, rows // 2, hidden), BF16),
        q=pltpu.VMEM((total, KEY_DIM), BF16),
        k=pltpu.VMEM((total, KEY_DIM), BF16),
        v=pltpu.VMEM((total, VAL_DIM), BF16),
        sc=pltpu.VMEM((total, SEQ_LEN), BF16),
        swish=pltpu.VMEM((total, VAL_DIM), F32),
        ghat=pltpu.VMEM((total, VAL_DIM), F32),
        ginv=pltpu.VMEM((total, 128), F32),
        gated=pltpu.VMEM((total, VAL_DIM), BF16),
        hid=pltpu.VMEM((total, WIDE), BF16),
        gate=pltpu.VMEM((total, WIDE), F32),
        up=pltpu.VMEM((total, WIDE), F32),
        gb=pltpu.VMEM((total, WIDE), BF16),
        ub=pltpu.VMEM((total, WIDE), BF16),
        sb=pltpu.VMEM((total, SEQ_LEN), BF16),
        qkb=pltpu.VMEM((total, 2 * KEY_DIM), BF16),
        turned=pltpu.VMEM((WIDE, total), BF16),
        st=pltpu.VMEM((4, WIDE, WIDE), BF16),
        decay=pltpu.VMEM((SEQ_LEN, SEQ_LEN), F32),
        low=pltpu.VMEM((rows, hidden), BF16),
        middle=pltpu.VMEM((rows, hidden), F32),
        back=pltpu.VMEM((rows, hidden), F32),
        pieces=pltpu.VMEM((4, 8, hidden), F32),
        gparts=pltpu.VMEM((8, 8, 256), F32),
        gain=pltpu.VMEM((8, hidden), F32),
        gsend=pltpu.VMEM((8, 8, 256), F32),
        gsum=pltpu.VMEM((4, 8, 256), F32),
        xr=pltpu.VMEM((rows, hidden), BF16),
        cr=pltpu.VMEM((rows, hidden), BF16),
        rows2=pltpu.VMEM((rows, hidden), BF16),
        cot2=pltpu.VMEM((rows, hidden), BF16),
        ub2=pltpu.VMEM((total, WIDE), BF16),
        hop_s=dma((6,)),
        hop_r=dma((6,)),
        gd_s=dma((13,)),
        gd_r=dma((13,)),
        gown=pltpu.VMEM((8, 256), F32),
        ex_s=dma((8,)),
        ex_r=dma((8,)),
        ex_l=dma((8,)),
        zs=dma((7, 2, 4)),
        zr=dma((7, 2, 4)),
        rs=dma((8, 3)),
        rr=dma((8, 4)),
        ra=dma((8, 2)),
        stl=dma((4,)),
        fl=dma((4,)),
        fe_s=dma((8,)),
        fe_r=dma((8,)),
        gg_s=dma((8,)),
        gg_r=dma((8,)),
        gt_s=dma((4,)),
        gt_r=dma((4,)),
        ga_s=dma((13,)),
        ga_r=dma((13,)),
        gc_s=dma((13,)),
        gc_r=dma((13,)),
        re_s=dma((10,)),
        re_r=dma((10,)),
        ol=dma((6,)),
        free=pltpu.SemaphoreType.REGULAR,
    )


class PlaneSum(Reduce):
    def __init__(self, place, part, theirs, got, across, send, recv):
        p = place
        rows = theirs.shape[1]
        h = rows // 2
        self.rows, self.half, self.part = rows, h, part
        self.theirs, self.got, self.across = theirs, got, across
        self.base = [p.block(j) * rows for j in range(4)]

        def remote(k, source, target_ref, target):
            return pltpu.make_async_remote_copy(
                src_ref=source,
                dst_ref=target_ref,
                send_sem=send.at[k],
                recv_sem=recv.at[k],
                device_id=target,
                device_id_type=MESH,
            )

        def piece(j, lo):
            return part.at[pl.ds(pl.multiple_of(self.base[j] + lo, 8), h)]

        self.place, self.remote = p, remote
        a, b = pl.ds(0, h), pl.ds(h, h)
        self.swap = [
            remote(j, part.at[rows_of(p.block(j, 1), rows)], theirs.at[j], p.sib) for j in range(4)
        ]
        self.da = remote(4, piece(3, 0), across.at[0], p.xn)
        self.db = remote(5, piece(3, h), across.at[1], p.yn)
        self.xa = remote(6, piece(1, 0), got.at[0, a], p.xn)
        self.xb = remote(7, piece(1, h), got.at[0, b], p.xn)
        self.ya = remote(8, piece(2, 0), got.at[1, a], p.yn)
        self.yb = remote(9, piece(2, h), got.at[1, b], p.yn)

    def add(self, j, lo, n, other, other_lo):
        def body(i):
            r = pl.ds(pl.multiple_of(self.base[j] + lo + i * CHUNK, CHUNK), CHUNK)
            q = pl.ds(pl.multiple_of(other_lo + i * CHUNK, CHUNK), CHUNK)
            self.part[r] = (self.part[r].astype(F32) + other[q].astype(F32)).astype(BF16)

        loop(n // CHUNK, body)

    def start(self):
        for j in (3, 1, 2, 0):
            self.swap[j].start()

    def fill(self, tile_value):
        p, tile = self.place, 2 * self.rows

        def body(i):
            j = jnp.where(i == 0, 3, jnp.where(i == 3, 0, i))
            chip_x = jnp.where(lax.rem(j, 2) == 1, 1 - p.x, p.x)
            chip_y = jnp.where(j >= 2, 1 - p.y, p.y)
            chip = chip_x * 2 + chip_y
            r = at(chip, tile)

            def inner(n):
                c = at(n, WIDE)
                self.part[r, c] = tile_value(r, c).astype(BF16)

            loop(self.part.shape[1] // WIDE, inner)
            source = self.part.at[rows_of(chip * 2 + 1 - p.c, self.rows)]
            self.remote(j, source, self.theirs.at[j], p.sib).start()

        loop(4, body)

    def run1(self):
        for j, copies in ((3, (self.da, self.db)), (1, (self.xa,)), (2, (self.yb,))):
            self.swap[j].wait_recv()
            self.add(j, 0, self.rows, self.theirs.at[j], 0)
            for copy in copies:
                copy.start()

    def run2(self):
        h = self.half
        self.db.wait_recv()
        self.add(1, h, h, self.across.at[1], 0)
        self.xb.start()
        self.da.wait_recv()
        self.add(2, 0, h, self.across.at[0], 0)
        self.ya.start()

    def run3(self):
        self.swap[0].wait_recv()
        for copy in (self.xa, self.yb, self.xb, self.ya):
            copy.wait_recv()

    def run(self):
        self.run1()
        self.run2()
        self.run3()

    def total(self, i):
        r = pl.ds(pl.multiple_of(i * CHUNK, CHUNK), CHUNK)
        mine = pl.ds(pl.multiple_of(self.base[0] + i * CHUNK, CHUNK), CHUNK)
        pieces = (self.part[mine], self.theirs[0, r], self.got[0, r], self.got[1, r])
        one, two, three, four = (piece.astype(F32) for piece in pieces)
        return (one + two) + (three + four)


def mega_kernel(names, count_in, count_out, *refs):
    x_hbm, cot_hbm, counts_ref, cos_ref, sin_ref = refs[:5]
    gain_refs = refs[5:9]
    q_w, k_w, v_w, s_w, o_w, g_w, u_w, d_w = refs[9:count_in]
    outs = refs[count_in : count_in + count_out]
    final_out, delta_out, gains_out, q_g, k_g, v_g, s_g, o_g, g_g, u_g, d_g, stage, heard, added = outs
    b = {name: ref for name, ref in zip(names, refs[count_in + count_out :], strict=True)}
    w, xs, xt, st, part, turned = b["w"], b["xs"], b["xt"], b["st"], b["part"], b["turned"]
    x_ref, cot_ref = b["xr"], b["cr"]
    rows, hidden = x_ref.shape
    width = hidden // 8

    dp, tensor = lax.axis_index("dp"), lax.axis_index("tensor")
    place = Place()
    x, z = place.x, dp // 2
    first_plane, inner = z == 0, (z == 1) | (z == 2)
    outer = jnp.logical_not(inner)

    barrier = pltpu.get_barrier_semaphore()
    for i in range(1, 8):
        other = (lax.rem(dp + i, 8), tensor)
        pl.semaphore_signal(barrier, inc=1, device_id=other, device_id_type=MESH)
    for i in range(1, 4):
        other = (dp, lax.rem(tensor + i, 4))
        pl.semaphore_signal(barrier, inc=1, device_id=other, device_id_type=MESH)

    def remote(source, target_ref, send, recv, target):
        return pltpu.make_async_remote_copy(
            src_ref=source,
            dst_ref=target_ref,
            send_sem=send,
            recv_sem=recv,
            device_id=target,
            device_id_type=MESH,
        )

    def plane(step):
        return ((z + step) * 2 + x, tensor)

    def column_exchange(n, weight, k, lane, half):
        where = w.at[k, pl.ds(pl.multiple_of(z * 512 + x * 256, 256), width), pl.ds(lane, half)]
        keep = pltpu.make_async_copy(weight.at[:, at(x, half)], where, b["ex_l"].at[n])
        give = remote(
            weight.at[:, at(1 - x, half)], where, b["ex_s"].at[n], b["ex_r"].at[n], place.xn
        )
        return keep, give

    def row_exchange(n, weight, k):
        where = w.at[k, at(z, 512), at(x, width)]
        keep = pltpu.make_async_copy(weight.at[at(x, 512)], where, b["ex_l"].at[n])
        give = remote(weight.at[at(1 - x, 512)], where, b["ex_s"].at[n], b["ex_r"].at[n], place.xn)
        return keep, give

    exchanges = [
        [column_exchange(0, q_w, QK, 0, 256), column_exchange(1, k_w, QK, 256, 256)],
        [column_exchange(2, v_w, VALUE, 0, 512)],
        [column_exchange(3, s_w, SWISH, 0, 512)],
        [row_exchange(4, o_w, OUTPUT)],
        [column_exchange(5, g_w, GATE, 0, 512)],
        [column_exchange(6, u_w, UP, 0, 512)],
        [row_exchange(7, d_w, DOWN)],
    ]

    def keep(k):
        for local, _ in exchanges[k]:
            local.start()

    def give(k):
        for _, send in exchanges[k]:
            send.start()

    towards = jnp.where(z == 1, -1, 1)
    near, far = jnp.where(z == 1, 2, 1), jnp.where(z == 1, 3, 0)
    own_steps = (
        jnp.where(first_plane, 2, jnp.where(inner, 1, -2)),
        jnp.where(first_plane, 1, -1),
    )
    beside = place.xn

    def parts(k):
        return (0, 1) if k == QK else (0,)

    def block_copy(k, block, half, slot, target):
        if k == QK:
            side = x if half == 0 else 1 - x
            ref = w.at[k, pl.ds(pl.multiple_of(block * 512 + side * 256, 256), 256)]
        else:
            ref = w.at[k, at(block, 512)]
        return remote(ref, ref, b["zs"].at[k, half, slot], b["zr"].at[k, half, block], target)

    def kept(k):
        for local, _ in exchanges[k]:
            local.wait()

    def swapped(k):
        for _, send in exchanges[k]:
            send.wait_recv()

    def spread_half(k, half):
        def both():
            for slot, step in enumerate(own_steps):
                block_copy(k, z, half, slot, plane(step)).start()

        if k in FEED_FORWARD:
            pl.when(outer)(both)
            pl.when(inner)(lambda: block_copy(k, z, half, 0, plane(-towards)).start())
        else:
            both()

    def spread(k):
        kept(k)
        swapped(k)
        spread_half(k, 0)

    def pass_on(k):
        @pl.when(inner)
        def _():
            for half in parts(k):
                for slot, block in ((2, near), (3, far)):
                    copy = block_copy(k, block, half, slot, plane(towards))
                    copy.wait_recv()
                    copy.start()

    def arrive(k):
        for half in parts(k):

            @pl.when(inner)
            def _(half=half):
                block_copy(k, jnp.where(z == 1, 0, 3), half, 0, beside).wait_recv()

            @pl.when(outer)
            def _(half=half):
                for i in range(3):
                    block = jnp.where(first_plane, i + 1, i)
                    block_copy(k, block, half, 0, beside).wait_recv()

    def arrive_inner(k):
        for i in range(3):
            block = jnp.where(z == 1, (0, 2, 3)[i], (0, 1, 3)[i])
            block_copy(k, block, 0, 0, beside).wait_recv()

    def weights_sent():
        for k in range(7):
            for _, send in exchanges[k]:
                send.wait_send()
            for half in parts(k):
                block_copy(k, z, half, 0, beside).wait_send()
                if k in FEED_FORWARD:
                    pl.when(outer)(lambda k=k, half=half: block_copy(k, z, half, 1, beside).wait_send())
                else:
                    block_copy(k, z, half, 1, beside).wait_send()

                    @pl.when(inner)
                    def _(k=k, half=half):
                        for slot in (2, 3):
                            block_copy(k, z, half, slot, beside).wait_send()

    def lanes_of(c):
        if c in (QUERY, KEY):
            return QK, pl.ds(256 * (c - QUERY), 256)
        return c, pl.ds(0, 512)

    def share(ref, c, *index):
        chunk, lanes = lanes_of(c)
        return ref.at[(chunk, *index, slice(None), lanes)]

    def slot_of(c, slot):
        return st.at[slot, :, pl.ds(0, 256 if c in (QUERY, KEY) else 512)]

    def number(c):
        return c if c < QUERY else c - QUERY + (0 if c == QUERY else 6)

    def staged(c, block, slot):
        return pltpu.make_async_copy(slot_of(c, slot), share(stage, c, block), b["stl"].at[slot])

    def to_added(c, block, which, target):
        n = number(c)
        return remote(
            share(stage, c, block),
            share(added, c, which),
            b["rs"].at[n, which],
            b["ra"].at[n, which],
            target,
        )

    def to_heard(c, block, slot, target):
        n = number(c)
        return remote(
            share(stage, c, block), share(heard, c, z), b["rs"].at[n, slot], b["rr"].at[n, z], target
        )

    def all_staged(c):
        for block in range(PLANES):
            staged(c, block, block).wait()

    def send_gradient(c):
        all_staged(c)
        step = jnp.where(first_plane, 1, -1)

        @pl.when(outer)
        def _():
            to_added(c, 3 - z, 0, plane(step)).start()
            to_added(c, z + 2 * step, 1, plane(step)).start()
            to_heard(c, z + step, 2, plane(step)).start()

        @pl.when(inner)
        def _():
            to_heard(c, z + towards, 2, plane(towards)).start()

    def send_inner(c):
        to_added(c, far, 0, plane(-towards)).start()
        to_heard(c, near, 1, plane(-towards)).start()

    def rounds(c, body):
        lanes = 256 if c in (QUERY, KEY) else 512

        def step(i):
            body(pl.ds(pl.multiple_of(i * 32, 32), 32), pl.ds(0, lanes))

        loop(WIDE // 32, step)

    def local(source, target, n):
        return pltpu.make_async_copy(source, target, b["fl"].at[n])

    def combine(c):
        @pl.when(inner)
        def _():
            blocks = (far, near)
            mine = [local(share(stage, c, blocks[i]), slot_of(c, i), i) for i in range(2)]
            for copy in mine:
                copy.start()
            theirs = [local(share(added, c, i), slot_of(c, 2 + i), 2 + i) for i in range(2)]
            for i in range(2):
                to_added(c, blocks[i], i, beside).wait_recv()
                theirs[i].start()
            for i in range(2):
                mine[i].wait()
                theirs[i].wait()

                def body(r, lanes, i=i):
                    st[i, r, lanes] = (
                        st[i, r, lanes].astype(F32) + st[2 + i, r, lanes].astype(F32)
                    ).astype(BF16)

                rounds(c, body)
                back = local(slot_of(c, i), share(stage, c, blocks[i]), i)
                back.start()
            for i, step in enumerate((-2 * towards, -towards)):
                local(slot_of(c, i), share(stage, c, blocks[i]), i).wait()
                to_heard(c, blocks[i], i, plane(step)).start()

    def combine_inner(c):
        block = z + towards
        mine = local(share(stage, c, block), slot_of(c, 0), 0)
        theirs = local(share(added, c, 0), slot_of(c, 1), 1)
        mine.start()
        to_added(c, block, 0, beside).wait_recv()
        theirs.start()
        mine.wait()
        theirs.wait()

        def body(r, lanes):
            st[0, r, lanes] = (
                st[0, r, lanes].astype(F32) + st[1, r, lanes].astype(F32)
            ).astype(BF16)

        rounds(c, body)
        back = local(slot_of(c, 0), share(stage, c, block), 0)
        back.start()
        back.wait()
        to_heard(c, block, 2, plane(towards)).start()

    homes = {
        QUERY: q_g, KEY: k_g, VALUE: v_g, SWISH: s_g, OUTPUT: o_g, GATE: g_g, UP: u_g, DOWN: d_g
    }

    def home_copies(c, source):
        home, (_, lanes) = homes[c], lanes_of(c)
        if c in (OUTPUT, DOWN):
            kept_half, given_half = (slice(None), at(x, 256)), (slice(None), at(1 - x, 256))
            slot = home.at[at(x, 512)]
        else:
            kept_half, given_half = (at(x, 256),), (at(1 - x, 256),)
            slot = home.at[:, at(x, home.shape[1] // 2)]
        n = number(c)
        return (
            local(slot_of(c, 0).at[kept_half], slot, 3),
            remote(source.at[given_half], slot, b["fe_s"].at[n], b["fe_r"].at[n], beside),
        )

    sources = (jnp.where(z == 1, 0, 1), jnp.where(z == 2, 3, 2))

    def finish_gradient(c, last=False):
        n = number(c)

        def own_load():
            return local(share(stage, c, z), slot_of(c, 0), 0)

        def arrival(i, source):
            remote(
                share(stage, c, 0), share(heard, c, source), b["rs"].at[n, 2], b["rr"].at[n, source], beside
            ).wait_recv()
            load = local(share(heard, c, source), slot_of(c, i), i)
            load.start()
            return load

        if c in FEED_FORWARD:
            source = jnp.where((z == 0) | (z == 2), 1, 2)

            @pl.when(outer)
            def _():
                arrival(0, source).wait()

            @pl.when(inner)
            def _():
                own_load().start()
                arrival(1, source).wait()
                own_load().wait()

                def body(r, lanes):
                    st[0, r, lanes] = (
                        st[0, r, lanes].astype(F32) + st[1, r, lanes].astype(F32)
                    ).astype(BF16)

                rounds(c, body)

        else:
            own_load().start()
            loads = [arrival(1 + i, source) for i, source in enumerate(sources)]
            own_load().wait()
            for load in loads:
                load.wait()

            def body(r, lanes):
                st[0, r, lanes] = (
                    st[0, r, lanes].astype(F32)
                    + (st[1, r, lanes].astype(F32) + st[2, r, lanes].astype(F32))
                ).astype(BF16)

            rounds(c, body)

        source = slot_of(c, 0) if last else share(stage, c, z)
        stay, send = home_copies(c, source)
        if not last:
            store = local(slot_of(c, 0), share(stage, c, z), 0)
            store.start()
            stay.start()
            store.wait()
            send.start()
            stay.wait()
        else:
            send.start()
            stay.start()
            stay.wait()

    def gradients_done():
        for c in GRADIENTS:
            n = number(c)
            source = slot_of(c, 0) if c == KEY else share(stage, c, z)
            _, send = home_copies(c, source)
            send.wait()

            def sent(c=c, n=n):
                for slot in range(3):
                    remote(
                        share(stage, c, 0), share(heard, c, 0), b["rs"].at[n, slot], b["rr"].at[n, 0], beside
                    ).wait_send()

            if c in FEED_FORWARD:
                pl.when(inner)(sent)
            else:
                sent()

    across_step = jnp.where(outer, jnp.where(first_plane, 1, -1), towards)

    def hop(n, source, target, part_of=slice(None)):
        return remote(
            source.at[part_of], target.at[part_of], b["hop_s"].at[n], b["hop_r"].at[n], plane(across_step)
        )

    halves = (pl.ds(0, rows // 2), pl.ds(rows // 2, rows // 2))

    def neighbours_may_write():
        for partner in (place.sib, place.xn, place.yn):
            pl.semaphore_signal(b["free"], inc=1, device_id=partner, device_id_type=MESH)

    def may_write():
        pl.semaphore_wait(b["free"], 3)

    def gain_copy(i):
        target = lax.rem(dp + i, 8)
        return remote(
            b["gown"], b["gparts"].at[dp], b["gg_s"].at[i], b["gg_r"].at[dp], (target, tensor)
        )

    def gain_arrival(i):
        source = lax.rem(dp + i, 8)
        return remote(
            b["gown"], b["gparts"].at[source], b["gg_s"].at[i], b["gg_r"].at[source], (source, tensor)
        )

    gather_sems = (b["ga_s"], b["ga_r"])

    def plane_sum(ref):
        return PlaneSum(place, ref, b["theirs"], b["got"], b["across"], b["re_s"], b["re_r"])

    for k in range(7):
        keep(k)
    gown = b["gown"]
    for n in range(8):
        gown[n : n + 1, :] = gain_refs[n % 4][...].astype(F32).reshape(1, 256)
    load_x = pltpu.make_async_copy(x_hbm, x_ref, b["ol"].at[3])
    load_cot = pltpu.make_async_copy(cot_hbm, cot_ref, b["ol"].at[4])
    load_x.start()
    load_cot.start()
    mine = pltpu.make_async_copy(gown, b["gparts"].at[dp], b["ol"].at[0])
    mine.start()
    kept(QK)
    pl.semaphore_wait(barrier, 10)
    for i in range(1, 8):
        gain_copy(i).start()
    give(QK)
    spread_half(QK, 0)
    give(VALUE)
    head = (tensor * 2 + x).astype(F32)
    rate = jnp.log(1.0 - jnp.exp2(-5.0 - jnp.full((8, SEQ_LEN), head, F32)))[0:1]

    def body(i):
        r = at(i, 64)
        n = lax.broadcasted_iota(jnp.int32, (64, SEQ_LEN), 0) + i * 64
        m = lax.broadcasted_iota(jnp.int32, (64, SEQ_LEN), 1)
        gap = n - m
        b["decay"][r] = jnp.where(gap >= 0, jnp.exp(jnp.maximum(gap, 0).astype(F32) * rate), 0.0)

    loop(SEQ_LEN // 64, body)
    load_x.wait()
    swapped(QK)
    spread_half(QK, 1)
    mine.wait()
    for i in range(1, 8):
        gain_arrival(i).wait_recv()
    for i in range(8):
        b["gain"][:, i * 256 : (i + 1) * 256] = b["gparts"][i]
    gain = b["gain"]
    low = b["low"]

    def body(i):
        r = at(i, CHUNK)
        hat, _ = normalize(x_ref[r].astype(F32), EPSILON)
        low[r] = (hat * gain[0:1, :] + gain[1:2, :]).astype(BF16)

    loop(rows // CHUNK, body)
    first = Gather(place, low, xs, *gather_sems)
    first.start()
    spread(VALUE)
    load_cot.wait()
    count = counts_ref[0]

    def body(i):
        r = at(i, CHUNK)
        row = lax.broadcasted_iota(jnp.int32, (CHUNK, hidden), 0) + (tensor * rows + i * CHUNK)
        cot_ref[r] = jnp.where(row < count, cot_ref[r].astype(F32), 0.0).astype(BF16)

    loop(rows // CHUNK, body)
    pl.when(outer)(lambda: hop(2, cot_ref, b["cot2"]).start())
    first.forward()
    for k in range(SWISH, DOWN + 1):
        give(k)
    cotangent = Gather(place, cot_ref, b["outs"], b["gc_s"], b["gc_r"])
    pl.when(inner)(cotangent.start)
    pass_on(QK)
    spread(SWISH)
    first.finish()

    def body(i):
        xt[at(i, 256), :] = xs[:, at(i, 256)].T

    loop(hidden // 256, body)
    spread(OUTPUT)

    arrive(QK)

    def turn(acc, tile, scale):
        spot = at(lax.rem(tile, SEQ_LEN // TILE), TILE)
        cos, sin = cos_ref[spot], sin_ref[spot]
        one, two = acc[:, :128], acc[:, 128:]
        return (((one * cos - two * sin) * scale).astype(BF16), ((two * cos + one * sin) * scale).astype(BF16))

    def body(i):
        r = at(i, TILE)
        acc = matmul(xs[r], w[QK])
        b["q"][r, :128], b["q"][r, 128:] = turn(acc[:, :KEY_DIM], i, 1.0)
        b["k"][r, :128], b["k"][r, 128:] = turn(acc[:, KEY_DIM:], i, KEY_DIM ** (-0.5))

    tiles = 8 * rows // TILE
    per_slot = SEQ_LEN // TILE
    loop(tiles, body)

    def slot_rows(i):
        return at(i // per_slot, SEQ_LEN)

    def body(i):
        r = at(i, TILE)
        decay = b["decay"][at(lax.rem(i, per_slot), TILE)]
        b["sc"][r] = (nt(b["q"][r], b["k"][slot_rows(i)]) * decay).astype(BF16)

    loop(tiles, body)

    for k in (GATE, UP, DOWN):
        spread(k)
    pass_on(VALUE)
    arrive(VALUE)

    def body(i):
        r = at(i, TILE)
        b["v"][r] = matmul(xs[r], w[VALUE]).astype(BF16)

    loop(tiles, body)

    def body(i):
        r = at(i, TILE)
        retained = matmul(b["sc"][r], b["v"][slot_rows(i)])
        hat, inverse = normalize(retained, GROUP_EPSILON)
        b["ghat"][r] = hat
        b["ginv"][r] = jnp.broadcast_to(inverse, (TILE, 128))

    loop(tiles, body)
    @pl.when(inner)
    def _():
        cotangent.forward()
        cotangent.finish()

    pass_on(SWISH)
    arrive(SWISH)

    def body(i):
        r = at(i, TILE)
        swish = matmul(xs[r], w[SWISH])
        b["swish"][r] = swish
        b["gated"][r] = (swish * jax.nn.sigmoid(swish) * b["ghat"][r]).astype(BF16)

    loop(tiles, body)

    pass_on(OUTPUT)
    arrive(OUTPUT)

    def grid_of(i):
        return at(i // PLANES, TILE), at(lax.rem(i, PLANES), 512)

    reduce = plane_sum(part)
    reduce.fill(lambda r, c: matmul(b["gated"][r], w[OUTPUT, c]))
    reduce.run()
    def body(i):
        r = at(i, CHUNK)
        middle = x_ref[r].astype(F32) + reduce.total(i)
        b["middle"][r] = middle
        hat, _ = normalize(middle, EPSILON)
        low[r] = (hat * gain[2:3, :] + gain[3:4, :]).astype(BF16)

    loop(rows // CHUNK, body)

    @pl.when(outer)
    def _():
        for n in range(2):
            hop(n, low, b["rows2"], halves[n]).start()

    def gelu_of(t):
        inner_value = 0.7978845608028654 * (t + 0.044715 * t * t * t)
        tanh = jnp.tanh(inner_value)
        return 0.5 * (1.0 + tanh), tanh

    def turned_of(ref):
        def body(i):
            turned[:, at(i, TILE)] = ref[at(i, TILE)].T

        loop(tiles, body)

    def stage_block(c, i, value):
        st[i] = value.astype(BF16)
        staged(c, i, i).start()

    def times_turned(left, r, k):
        acc = nt(left[r, 0:512], w[k, 0:512])
        for plane_at in range(1, PLANES):
            lanes = slice(plane_at * 512, plane_at * 512 + 512)
            acc = acc + nt(left[r, lanes], w[k, lanes])
        return acc

    def gate_projection(mixer):
        def body(i):
            r = at(i, TILE)
            b["gate"][r] = matmul(mixer[r], w[GATE])

        loop(tiles, body)

    def up_projection(mixer, hid):
        def body(i):
            r = at(i, TILE)
            up = matmul(mixer[r], w[UP])
            b["up"][r] = up
            gate = b["gate"][r]
            share_of, _ = gelu_of(gate)
            hid[r] = (gate * share_of * up).astype(BF16)

        loop(tiles, body)

    def hidden_backward(cots, gb, ub):
        def body(i):
            r = at(i, TILE)
            back = times_turned(cots, r, DOWN)
            gate, up = b["gate"][r], b["up"][r]
            share_of, tanh = gelu_of(gate)
            slope = 0.5 * gate * (1.0 - tanh * tanh) * (0.7978845608028654 * (1.0 + 0.134145 * gate * gate))
            gb[r] = (back * up * (share_of + slope)).astype(BF16)
            ub[r] = (back * gate * share_of).astype(BF16)

        loop(tiles, body)

    def refill(c):
        copies = [pltpu.make_async_copy(stage.at[c, i], st.at[i], b["fl"].at[i]) for i in range(PLANES)]
        for copy in copies:
            copy.start()
        for copy in copies:
            copy.wait()

    def product_of(c, i, value, more):
        stage_block(c, i, value + st[i].astype(F32) if more else value)

    def down_gradient(hid, cots, more):
        if more:
            refill(DOWN)
        turned_of(hid)

        def body(i):
            product_of(DOWN, i, matmul(turned[...], cots[:, at(i, 512)]), more)

        loop(PLANES, body)
        all_staged(DOWN)

    def weight_gradient(c, mixer, right, more):
        if more:
            refill(c)

        def body(i):
            def body_turn(j):
                turned[:, at(j, TILE)] = mixer[at(j, TILE), at(i, 512)].T

            loop(tiles, body_turn)
            product_of(c, i, matmul(turned[...], right[...]), more)

        loop(PLANES, body)
        all_staged(c)

    def mixer_input(gb, ub):
        return lambda r, c: nt(gb[r], w[GATE, c]) + nt(ub[r], w[UP, c])

    def mixer_output(hid, target):
        def body(i):
            r, c = grid_of(i)
            target[r, c] = matmul(hid[r], w[DOWN, c]).astype(BF16)

        loop(tiles * PLANES, body)

    b["pieces"][...] = jnp.zeros_like(b["pieces"])

    def second_norm_backward(r, upstream):
        hat, inverse = normalize(b["middle"][r], EPSILON)
        scaled = upstream * hat
        b["pieces"][2] += scaled[0:8] + scaled[8:16]
        b["pieces"][3] += upstream[0:8] + upstream[8:16]
        back = cot_ref[r].astype(F32) + normalize_back(upstream * gain[2:3, :], hat, inverse)
        b["back"][r] = back
        low[r] = back.astype(BF16)

    hid2, gb2, ub2 = b["sb"], b["qkb"], b["ub2"]
    outs_ref = b["outs"]

    @pl.when(inner)
    def _():
        second = Gather(place, low, xs, *gather_sems)
        second.start()
        hop(2, cot_ref, b["cot2"]).wait_recv()
        second.forward()
        other_cot = Gather(place, b["cot2"], part, b["gc_s"], b["gc_r"])
        reduce.finish()
        neighbours_may_write()
        may_write()
        other_cot.start()
        second.finish()
        arrive_inner(GATE)
        gate_projection(xs)
        arrive_inner(UP)
        up_projection(xs, b["hid"])
        other_cot.forward()
        arrive_inner(DOWN)
        hidden_backward(outs_ref, b["gb"], b["ub"])
        down_gradient(b["hid"], outs_ref, False)
        neighbours_may_write()
        other_cot.finish()
        other = Gather(place, b["rows2"], outs_ref, b["gd_s"], b["gd_r"])
        may_write()
        hop(0, low, b["rows2"], halves[0]).wait_recv()
        other.start_first_half()
        hop(1, low, b["rows2"], halves[1]).wait_recv()
        other.start_second_half()
        weight_gradient(GATE, xs, b["gb"], False)
        other.forward()
        weight_gradient(UP, xs, b["ub"], False)
        other.finish()
        gate_projection(outs_ref)
        up_projection(outs_ref, hid2)
        hidden_backward(part, gb2, ub2)
        reduce2 = plane_sum(xs)
        reduce2.fill(mixer_input(gb2, ub2))
        reduce2.run1()
        down_gradient(hid2, part, True)
        send_inner(DOWN)
        reduce2.run2()
        reduce2.run3()

        for n in range(2):

            def body(i, n=n):
                i = n * (rows // 2 // CHUNK) + i
                b["rows2"][at(i, CHUNK)] = reduce2.total(i).astype(BF16)

            loop(rows // 2 // CHUNK, body)
            hop(3 + n, b["rows2"], b["rows2"], halves[n]).start()
        reduce2.finish()
        neighbours_may_write()
        may_write()
        reduce3 = plane_sum(part)
        reduce3.fill(mixer_input(b["gb"], b["ub"]))
        reduce3.run1()
        weight_gradient(GATE, outs_ref, gb2, True)
        send_inner(GATE)
        reduce3.run2()
        combine_inner(DOWN)
        weight_gradient(UP, outs_ref, ub2, True)
        send_inner(UP)
        neighbours_may_write()
        reduce3.run3()

        def body(i):
            second_norm_backward(at(i, CHUNK), reduce3.total(i))

        loop(rows // CHUNK, body)
        reduce3.finish()
        may_write()

    third = Gather(place, low, outs_ref, *gather_sems)

    @pl.when(outer)
    def _():
        reduce.finish()
        for n in range(2):
            hop(n, low, b["rows2"], halves[n]).wait_send()
        for n in range(2):
            hop(3 + n, b["rows2"], b["rows2"], halves[n]).wait_recv()

            def body(i, n=n):
                r = pl.ds(pl.multiple_of(n * (rows // 2) + i * CHUNK, CHUNK), CHUNK)
                second_norm_backward(r, b["rows2"][r].astype(F32))

            loop(rows // 2 // CHUNK, body)
            if n == 0:
                third.start_first_half()
            else:
                third.start_second_half()

    pl.when(inner)(third.start)
    third.forward()
    pl.when(inner)(lambda: combine_inner(GATE))
    pl.when(inner)(lambda: mixer_output(hid2, xs))
    third.finish()
    reduce5 = plane_sum(xs)
    pl.when(inner)(reduce5.start)
    pl.when(inner)(lambda: combine_inner(UP))

    turned_of(b["gated"])

    def body(i):
        stage_block(OUTPUT, i, matmul(turned[...], b["outs"][:, at(i, 512)]))

    loop(PLANES, body)
    send_gradient(OUTPUT)
    pl.when(inner)(reduce5.run1)
    swb, rb, vlow = b["gb"], b["ub2"], b["ub"]

    def body(i):
        r = at(i, TILE)
        back = times_turned(b["outs"], r, OUTPUT)
        swish, hat = b["swish"][r], b["ghat"][r]
        gate = jax.nn.sigmoid(swish)
        swb[r] = (back * hat * gate * (1.0 + swish * (1.0 - gate))).astype(BF16)
        rb[r] = normalize_back(back * swish * gate, hat, b["ginv"][r, 0:1]).astype(BF16)

    loop(tiles, body)

    def projection_gradient(c, right, lanes=slice(None)):
        def body(i):
            value = matmul(xt[at(i, 512)], right[:, lanes]).astype(BF16)
            st[i, :, 0 : value.shape[1]] = value
            staged(c, i, i).start()

        loop(PLANES, body)
        send_gradient(c)

    pl.when(inner)(reduce5.run2)
    projection_gradient(SWISH, swb)

    @pl.when(inner)
    def _():
        reduce5.run3()

        def body(i):
            b["cot2"][at(i, CHUNK)] = reduce5.total(i).astype(BF16)

        loop(rows // CHUNK, body)
        hop(5, b["cot2"], b["cot2"]).start()
        reduce5.finish()
        neighbours_may_write()
        mixer_output(b["hid"], xs)
        may_write()
        plane_sum(xs).start()

    reduce6 = plane_sum(xs)
    combine(OUTPUT)
    pl.when(inner)(reduce6.run1)
    def body(i):
        r = at(i, TILE)
        decay = b["decay"][at(lax.rem(i, per_slot), TILE)]
        b["sb"][r] = (nt(rb[r], b["v"][slot_rows(i)]) * decay).astype(BF16)

    loop(tiles, body)
    turned_of(b["sc"])

    def body(i):
        vlow[at(i, TILE)] = matmul(
            turned[at(lax.rem(i, per_slot), TILE), slot_rows(i)], rb[slot_rows(i)]
        ).astype(BF16)

    loop(tiles, body)
    pl.when(inner)(reduce6.run2)
    projection_gradient(VALUE, vlow)
    turned_of(b["sb"])

    def turn_back(acc, tile, scale):
        spot = at(lax.rem(tile, per_slot), TILE)
        cos, sin = cos_ref[spot], sin_ref[spot]
        one, two = acc[:, :128], acc[:, 128:]
        return (((one * cos + two * sin) * scale).astype(BF16), ((two * cos - one * sin) * scale).astype(BF16))

    def body(i):
        r = at(i, TILE)
        qkb = b["qkb"]
        query = matmul(b["sb"][r], b["k"][slot_rows(i)])
        qkb[r, 0:128], qkb[r, 128:256] = turn_back(query, i, 1.0)
        key = matmul(turned[at(lax.rem(i, per_slot), TILE), slot_rows(i)], b["q"][slot_rows(i)])
        qkb[r, 256:384], qkb[r, 384:512] = turn_back(key, i, KEY_DIM ** (-0.5))

    loop(tiles, body)
    projection_gradient(QUERY, b["qkb"], slice(0, 256))
    projection_gradient(KEY, b["qkb"], slice(256, 512))
    combine(SWISH)

    @pl.when(inner)
    def _():
        reduce6.run3()

        def body(i):
            b["middle"][at(i, CHUNK)] += reduce6.total(i)

        loop(rows // CHUNK, body)
        reduce6.finish()
        neighbours_may_write()
        may_write()

    reduce = plane_sum(part)
    reduce.fill(
        lambda r, c: nt(b["qkb"][r], w[QK, c]) + nt(vlow[r], w[VALUE, c]) + nt(swb[r], w[SWISH, c])
    )
    reduce.run1()
    finish_gradient(DOWN)
    reduce.run2()
    combine(VALUE)
    finish_gradient(GATE)
    reduce.run3()

    def body(i):
        r = at(i, CHUNK)
        upstream = reduce.total(i)
        hat, inverse = normalize(x_ref[r].astype(F32), EPSILON)
        scaled = upstream * hat
        b["pieces"][0] += scaled[0:8] + scaled[8:16]
        b["pieces"][1] += upstream[0:8] + upstream[8:16]
        b["back"][r] += normalize_back(upstream * gain[0:1, :], hat, inverse)

    loop(rows // CHUNK, body)
    reduce.finish()
    delta_copy = pltpu.make_async_copy(b["back"], delta_out, b["ol"].at[2])
    delta_copy.start()

    for i in range(1, 8):
        gain_copy(i).wait_send()
    gsend, gparts, gsum = b["gsend"], b["gparts"], b["gsum"]
    for i in range(8):
        for n in range(4):
            lanes = slice(i * 256, i * 256 + 256)
            gsend[i, n : n + 1, :] = jnp.sum(b["pieces"][n, :, lanes], axis=0, keepdims=True)
            gsend[i, n + 4 : n + 5, :] = jnp.zeros((1, 256), F32)

    def share_copy(i):
        target = lax.rem(dp + i, 8)
        return remote(
            gsend.at[target], gparts.at[dp], b["gg_s"].at[i], b["gg_r"].at[dp], (target, tensor)
        )

    for i in range(1, 8):
        share_copy(i).start()
    finish_gradient(UP)
    combine(QUERY)
    @pl.when(outer)
    def _():
        hop(2, cot_ref, b["cot2"]).wait_send()
        hop(5, b["cot2"], b["cot2"]).wait_recv()

        def body(i):
            r = at(i, CHUNK)
            b["middle"][r] += b["cot2"][r].astype(F32)

        loop(rows // CHUNK, body)

    final_copy = pltpu.make_async_copy(b["middle"], final_out, b["ol"].at[1])
    final_copy.start()
    finish_gradient(OUTPUT)
    combine(KEY)
    finish_gradient(SWISH)
    finish_gradient(VALUE)
    finish_gradient(QUERY)
    acc = gsend[dp]
    for i in range(1, 8):
        gain_arrival(i).wait_recv()
        acc = acc + gparts[lax.rem(dp + i, 8)]
    gsum[tensor] = acc

    def sum_copy(i, source):
        target = lax.rem(tensor + i, 4)
        return remote(
            gsum.at[source], gsum.at[source], b["gt_s"].at[i], b["gt_r"].at[source], (dp, target)
        )

    for i in range(1, 4):
        sum_copy(i, tensor).start()
    finish_gradient(KEY, last=True)
    for i in range(1, 4):
        sum_copy(i, lax.rem(tensor + i, 4)).wait_recv()
    for i in range(1, 4):
        sum_copy(i, tensor).wait_send()
    for i in range(1, 8):
        share_copy(i).wait_send()
    gains_out[...] = (gsum[0] + gsum[1]) + (gsum[2] + gsum[3])
    final_copy.wait()
    delta_copy.wait()
    weights_sent()

    @pl.when(inner)
    def _():
        for n in range(2):
            hop(3 + n, b["rows2"], b["rows2"], halves[n]).wait_send()
        hop(5, b["cot2"], b["cot2"]).wait_send()

    gradients_done()


def whole_layer(
    incoming_signals,
    loss_sensitivity,
    token_counts_per_slot,
    leading_norm_multiplier,
    leading_norm_offset,
    question_projection,
    lookup_projection,
    content_projection,
    silu_switch_projection,
    retention_result_projection,
    trailing_norm_multiplier,
    trailing_norm_offset,
    feedforward_switch_projection,
    expanding_projection,
    contracting_projection,
):
    rows, hidden = incoming_signals.shape
    places = np.arange(SEQ_LEN, dtype=np.float32)
    middle = KEY_DIM // 2
    spectrum = np.float32(10000.0) ** (-np.arange(middle, dtype=np.float32) / np.float32(middle))
    angles = places[:, None] * spectrum[None, :]
    weights = (
        question_projection,
        lookup_projection,
        content_projection,
        silu_switch_projection,
        retention_result_projection,
        feedforward_switch_projection,
        expanding_projection,
        contracting_projection,
    )
    gains = (
        leading_norm_multiplier, leading_norm_offset, trailing_norm_multiplier, trailing_norm_offset
    )
    tables = (jnp.asarray(np.cos(angles)), jnp.asarray(np.sin(angles)))
    args = (incoming_signals, loss_sensitivity, token_counts_per_slot, *tables, *gains, *weights)
    scratch = mega_scratch(rows, hidden)
    shape = jax.ShapeDtypeStruct
    outs = (
        shape((rows, hidden), F32),
        shape((rows, hidden), F32),
        shape((8, 256), F32),
        *(shape(weight.shape, BF16) for weight in weights),
        shape((7, PLANES, WIDE, WIDE), BF16),
        shape((7, PLANES, WIDE, WIDE), BF16),
        shape((7, 2, WIDE, WIDE), BF16),
    )
    scalar = pl.BlockSpec(memory_space=pltpu.SMEM)
    results = pl.pallas_call(
        functools.partial(mega_kernel, tuple(scratch), len(args), len(outs)),
        out_shape=outs,
        in_specs=[ANY, ANY, scalar] + [VM] * 6 + [ANY] * 8,
        out_specs=tuple([ANY, ANY, VM] + [ANY] * 11),
        scratch_shapes=list(scratch.values()),
        compiler_params=pltpu.CompilerParams(
            collective_id=0, has_side_effects=True, vmem_limit_bytes=67043328
        ),
        name="whole_layer",
    )(*args)
    final_rows, delta, gain_sums = results[:3]
    owned = results[3:11]
    wide = pl.pallas_call(
        widen_kernel,
        out_shape=(
            shape((rows, hidden), BF16),
            shape((rows, hidden), F32),
            *(shape(weight.shape, F32) for weight in weights),
        ),
        in_specs=[scalar] + [ANY] * 10,
        out_specs=(ANY,) * 10,
        scratch_shapes=[
            pltpu.VMEM((rows, hidden), F32),
            pltpu.VMEM((rows, hidden), F32),
            pltpu.VMEM((rows, hidden), BF16),
            *(pltpu.VMEM(weight.shape, BF16) for weight in weights),
            *(pltpu.VMEM(weight.shape, F32) for weight in weights),
            pltpu.SemaphoreType.DMA((10,)),
            pltpu.SemaphoreType.DMA((10,)),
        ],
        compiler_params=pltpu.CompilerParams(vmem_limit_bytes=67043328),
        name="widen",
    )(token_counts_per_slot, final_rows, delta, *owned)
    query, key, value, swish, output, gate, up, down = wide[2:]
    return (
        wide[0],
        wide[1],
        gain_sums[0],
        gain_sums[1],
        query,
        key,
        value,
        swish,
        output,
        gain_sums[2],
        gain_sums[3],
        gate,
        up,
        down,
    )


def widen_kernel(counts_ref, *refs):
    sources, targets, scratch = refs[:10], refs[10:20], refs[20:]
    final, delta, low = scratch[:3]
    narrow, wide, (came, went) = scratch[3:11], scratch[11:19], scratch[19:]
    buffers = (final, delta, *narrow)
    loads = [
        pltpu.make_async_copy(source, buffer, came.at[i])
        for i, (source, buffer) in enumerate(zip(sources, buffers, strict=True))
    ]
    stores = [
        pltpu.make_async_copy(buffer, target, went.at[i])
        for i, (buffer, target) in enumerate(zip((low, delta, *wide), targets, strict=True))
    ]
    for load in loads:
        load.start()
    rows, hidden = final.shape
    tensor, count = lax.axis_index("tensor"), counts_ref[0]
    loads[0].wait()

    def body(i):
        r = at(i, CHUNK)
        row = lax.broadcasted_iota(jnp.int32, (CHUNK, hidden), 0) + (tensor * rows + i * CHUNK)
        low[r] = jnp.where(row < count, final[r], 0.0).astype(BF16)

    loop(rows // CHUNK, body)
    stores[0].start()
    loads[1].wait()
    stores[1].start()
    for n in range(8):
        loads[n + 2].wait()

        def body(i, n=n):
            r = at(i, 32)
            wide[n][r] = narrow[n][r].astype(F32)

        loop(narrow[n].shape[0] // 32, body)
        stores[n + 2].start()
    for store in stores:
        store.wait()


def solution(mesh):
    ranks = mesh.shape["dp"]
    groups = [[2 * k + side for k in range(ranks // 2)] for side in range(2)]
    swap = [(rank, rank + 1 - 2 * (rank % 2)) for rank in range(ranks)]
    rows, gain, column, row = P(("dp", "tensor"), None), P("dp"), P("dp", "tensor"), P("tensor", "dp")
    weights = (gain, gain, column, column, column, column, row, gain, gain, column, column, row)
    one_kernel = ranks == 8 and mesh.shape["tensor"] == 4
    return jax.shard_map(
        whole_layer if one_kernel else functools.partial(per_device, groups, swap),
        mesh=mesh,
        in_specs=(rows, rows, P("dp"), *weights),
        out_specs=(rows, rows, *weights),
        check_vma=False,
    )
```

```python
import functools

import jax
import jax.numpy as jnp
import numpy as np
from jax import lax
from jax.experimental import pallas as pl
from jax.experimental.pallas import tpu as pltpu
from jax.sharding import PartitionSpec as P

KEY_DIM = 256
VAL_DIM = 512
SEQ_LEN = 512

EPSILON = 1e-05
GROUP_EPSILON = 0.1

MESH = pl.DeviceIdType.MESH
F32 = jnp.float32
BF16 = jnp.bfloat16
CHUNK = 16


def normalize(values, epsilon):
    centre = values - jnp.mean(values, axis=-1, keepdims=True)
    inverse = lax.rsqrt(jnp.mean(centre * centre, axis=-1, keepdims=True) + epsilon)
    return (centre * inverse, inverse)


def normalize_back(upstream, normed, inverse):
    return inverse * (
        upstream
        - jnp.mean(upstream, axis=-1, keepdims=True)
        - normed * jnp.mean(upstream * normed, axis=-1, keepdims=True)
    )


def rotate_half(values):
    middle = values.shape[-1] // 2
    return jnp.concatenate([-values[..., middle:], values[..., :middle]], axis=-1)


def rotary_tables(span, columns):
    middle = columns // 2
    places = jnp.arange(span, dtype=jnp.int32).astype(jnp.float32)
    spectrum = 10000.0 ** (-jnp.arange(middle, dtype=jnp.int32).astype(jnp.float32) / middle)
    angles = places[:, None] * spectrum[None, :]
    angles = jnp.concatenate([angles, angles], axis=1)
    return (jnp.cos(angles)[None], jnp.sin(angles)[None])


def decay_table(span, head_id):
    log_rate = jnp.log(1.0 - jnp.exp2(-5.0 - head_id.astype(jnp.float32)))
    places = jnp.arange(span, dtype=jnp.int32)
    offsets = places[:, None] - places[None, :]
    decayed = jnp.exp(jnp.maximum(offsets, 0).astype(jnp.float32) * log_rate)
    return jnp.where(offsets >= 0, decayed, 0.0)


def gelu_tanh(values):
    return jax.nn.gelu(values, approximate=True)


def matmul(left, right):
    return jnp.dot(left, right, preferred_element_type=jnp.float32)


class Place:
    def __init__(self):
        d, t = lax.axis_index("dp"), lax.axis_index("tensor")
        self.x, self.y, self.c = lax.rem(d, 2), t // 2, lax.rem(t, 2)
        dx, ty = d + 1 - 2 * self.x, (1 - self.y) * 2 + self.c
        self.sib = (d, t + 1 - 2 * self.c)
        self.xn = (dx, t)
        self.yn = (d, ty)

    def block(self, j, other_core=0):
        x = 1 - self.x if j in (1, 3) else self.x
        y = 1 - self.y if j in (2, 3) else self.y
        c = 1 - self.c if other_core else self.c
        return x * 4 + y * 2 + c


def greet(place):
    barrier = pltpu.get_barrier_semaphore()
    for partner in (place.sib, place.xn, place.yn):
        pl.semaphore_signal(barrier, inc=1, device_id=partner, device_id_type=MESH)
    pl.semaphore_wait(barrier, 3)


def rows_of(index, rows):
    return pl.ds(pl.multiple_of(index * rows, rows), rows)


class Gather:
    @staticmethod
    def scratch():
        return [pltpu.SemaphoreType.DMA((13,)), pltpu.SemaphoreType.DMA((13,))]

    def __init__(self, place, src, out, send, recv):
        rows = src.shape[0]
        half = rows // 2
        p = place

        def remote(k, source, j, lo, n, target, core=0):
            where = pl.ds(pl.multiple_of(p.block(j, core) * rows + lo, 8), n)
            source = source.at[pl.ds(lo, n)] if source is src else source.at[where]
            return pltpu.make_async_remote_copy(
                src_ref=source,
                dst_ref=out.at[where],
                send_sem=send.at[k],
                recv_sem=recv.at[k],
                device_id=target,
                device_id_type=MESH,
            )

        self.p, self.rows, self.half = p, rows, half
        self.local = pltpu.make_async_copy(src, out.at[rows_of(p.block(0), rows)], send.at[12])
        h = half
        self.xa = remote(0, src, 0, 0, h, p.xn)
        self.xb = remote(1, src, 0, h, h, p.xn)
        self.ya = remote(2, src, 0, 0, h, p.yn)
        self.yb = remote(3, src, 0, h, h, p.yn)
        self.s0 = remote(4, src, 0, 0, rows, p.sib)
        self.da = remote(5, out, 1, 0, h, p.yn)
        self.db = remote(6, out, 2, h, h, p.xn)
        self.s1 = remote(7, out, 1, 0, rows, p.sib)
        self.s2 = remote(8, out, 2, 0, rows, p.sib)
        self.s3a = remote(9, out, 3, 0, h, p.sib)
        self.s3b = remote(10, out, 3, h, h, p.sib)

    def start(self):
        for copy in (self.xa, self.yb, self.xb, self.ya, self.s0, self.local):
            copy.start()

    def start_first_half(self):
        self.xa.start()
        self.ya.start()

    def start_second_half(self):
        for copy in (self.yb, self.xb, self.s0, self.local):
            copy.start()

    def forward(self):
        self.forward_across()
        self.forward_beside()

    def forward_across(self):
        self.xa.wait_recv()
        self.da.start()
        self.yb.wait_recv()
        self.db.start()

    def forward_beside(self):
        self.xb.wait_recv()
        self.s1.start()
        self.ya.wait_recv()
        self.s2.start()

    def own_arrived(self):
        self.local.wait()
        self.s0.wait_recv()

    def across_arrived(self):
        self.da.wait_recv()
        self.s3a.start()
        self.db.wait_recv()
        self.s3b.start()
        self.s3a.wait_recv()
        self.s3b.wait_recv()

    def drain(self):
        for copy in (self.s0, self.s1, self.s2, self.s3a, self.s3b):
            copy.wait_send()
        for copy in (self.xa, self.xb, self.ya, self.yb, self.da, self.db):
            copy.wait_send()

    def finish(self):
        self.da.wait_recv()
        self.s3a.start()
        self.db.wait_recv()
        self.s3b.start()
        self.local.wait()
        for copy in (self.s0, self.s1, self.s2, self.s3a, self.s3b):
            copy.wait()
        for copy in (self.xa, self.xb, self.ya, self.yb, self.da, self.db):
            copy.wait_send()


class Reduce:
    @staticmethod
    def scratch(rows, columns):
        return [
            pltpu.VMEM((4, rows, columns), BF16),
            pltpu.VMEM((4, rows, columns), BF16),
            pltpu.VMEM((2, rows, columns), BF16),
            pltpu.VMEM((2, rows // 2, columns), BF16),
            pltpu.SemaphoreType.DMA((14,)),
            pltpu.SemaphoreType.DMA((10,)),
        ]

    def __init__(self, place, part, mine, theirs, got, across, send, recv):
        p = place
        rows = mine.shape[1]
        h = rows // 2
        self.rows, self.half = rows, h
        self.mine, self.theirs, self.got, self.across = mine, theirs, got, across

        def remote(k, source, target_ref, target):
            return pltpu.make_async_remote_copy(
                src_ref=source,
                dst_ref=target_ref,
                send_sem=send.at[k],
                recv_sem=recv.at[k],
                device_id=target,
                device_id_type=MESH,
            )

        a, b = pl.ds(0, h), pl.ds(h, h)
        self.load = [
            pltpu.make_async_copy(part.at[rows_of(p.block(j), rows)], mine.at[j], send.at[10 + j])
            for j in range(4)
        ]
        self.swap = [
            remote(j, part.at[rows_of(p.block(j, 1), rows)], theirs.at[j], p.sib) for j in range(4)
        ]
        self.da = remote(4, mine.at[3, a], across.at[0], p.xn)
        self.db = remote(5, mine.at[3, b], across.at[1], p.yn)
        self.xa = remote(6, mine.at[1, a], got.at[0, a], p.xn)
        self.xb = remote(7, mine.at[1, b], got.at[0, b], p.xn)
        self.ya = remote(8, mine.at[2, a], got.at[1, a], p.yn)
        self.yb = remote(9, mine.at[2, b], got.at[1, b], p.yn)

    def add(self, j, lo, n, other, other_lo):
        def body(i, carry):
            r = pl.ds(pl.multiple_of(lo + i * CHUNK, CHUNK), CHUNK)
            q = pl.ds(pl.multiple_of(other_lo + i * CHUNK, CHUNK), CHUNK)
            self.mine[j, r] = (self.mine[j, r].astype(F32) + other[q].astype(F32)).astype(BF16)
            return carry

        lax.fori_loop(0, n // CHUNK, body, 0)

    def start(self):
        for j in (3, 1, 2, 0):
            self.swap[j].start()
            self.load[j].start()

    def run(self):
        rows, h = self.rows, self.half
        for j, copies in ((3, (self.da, self.db)), (1, (self.xa,)), (2, (self.yb,))):
            self.load[j].wait()
            self.swap[j].wait_recv()
            self.add(j, 0, rows, self.theirs.at[j], 0)
            for copy in copies:
                copy.start()
        self.db.wait_recv()
        self.add(1, h, h, self.across.at[1], 0)
        self.xb.start()
        self.da.wait_recv()
        self.add(2, 0, h, self.across.at[0], 0)
        self.ya.start()
        self.load[0].wait()
        self.swap[0].wait_recv()
        for copy in (self.xa, self.yb, self.xb, self.ya):
            copy.wait_recv()

    def total(self, r):
        pieces = (self.mine[0, r], self.theirs[0, r], self.got[0, r], self.got[1, r])
        one, two, three, four = (piece.astype(F32) for piece in pieces)
        return (one + two) + (three + four)

    def finish(self):
        for copy in (*self.swap, self.da, self.db, self.xa, self.xb, self.ya, self.yb):
            copy.wait_send()


def chunks(rows, body):
    def step(i, carry):
        body(pl.ds(pl.multiple_of(i * CHUNK, CHUNK), CHUNK))
        return carry

    lax.fori_loop(0, rows // CHUNK, step, 0)


def first_kernel(x_ref, cot_ref, gains_ref, out_x, out_cot, normed, *sems):
    place = Place()
    greet(place)
    gain, shift = gains_ref[0:1, :], gains_ref[1:2, :]

    def body(r):
        hat, _ = normalize(x_ref[r].astype(F32), EPSILON)
        normed[r] = (hat * gain + shift).astype(BF16)

    chunks(x_ref.shape[0], body)
    one = Gather(place, normed, out_x, *sems[:2])
    two = Gather(place, cot_ref, out_cot, *sems[2:])
    one.start()
    two.start()
    one.forward()
    two.forward()
    one.finish()
    two.finish()


def second_kernel(part_ref, x_ref, gains_ref, out_all, middle_ref, normed, *scratch):
    place = Place()
    greet(place)
    reduce = Reduce(place, part_ref, *scratch[:6])
    reduce.start()
    reduce.run()
    gain, shift = gains_ref[2:3, :], gains_ref[3:4, :]

    def body(r):
        middle = x_ref[r].astype(F32) + reduce.total(r)
        middle_ref[r] = middle
        hat, _ = normalize(middle, EPSILON)
        normed[r] = (hat * gain + shift).astype(BF16)

    chunks(x_ref.shape[0], body)
    gather = Gather(place, normed, out_all, *scratch[6:])
    gather.start()
    gather.forward()
    gather.finish()
    reduce.finish()


def third_kernel(
    part_ref, middle_ref, cot_ref, gains_ref, out_all, back_ref, pieces_ref, low, *scratch
):
    place = Place()
    greet(place)
    reduce = Reduce(place, part_ref, *scratch[:6])
    reduce.start()
    pieces_ref[...] = jnp.zeros_like(pieces_ref)
    reduce.run()
    gain = gains_ref[2:3, :]

    def body(r):
        upstream = reduce.total(r)
        hat, inverse = normalize(middle_ref[r], EPSILON)
        scaled = upstream * hat
        pieces_ref[0] += scaled[0:8] + scaled[8:16]
        pieces_ref[1] += upstream[0:8] + upstream[8:16]
        back = cot_ref[r].astype(F32) + normalize_back(upstream * gain, hat, inverse)
        back_ref[r] = back
        low[r] = back.astype(BF16)

    chunks(middle_ref.shape[0], body)
    gather = Gather(place, low, out_all, *scratch[6:])
    gather.start()
    gather.forward()
    gather.finish()
    reduce.finish()


def fourth_kernel(
    first_ref, mixer_ref, x_ref, middle_ref, gains_ref, delta_ref, final_ref, pieces_ref, *scratch
):
    place = Place()
    greet(place)
    one = Reduce(place, first_ref, *scratch[:6])
    two = Reduce(place, mixer_ref, *scratch[6:])
    one.start()
    two.start()
    pieces_ref[...] = jnp.zeros_like(pieces_ref)
    one.run()
    two.run()
    gain = gains_ref[0:1, :]

    def body(r):
        upstream = one.total(r)
        hat, inverse = normalize(x_ref[r].astype(F32), EPSILON)
        scaled = upstream * hat
        pieces_ref[0] += scaled[0:8] + scaled[8:16]
        pieces_ref[1] += upstream[0:8] + upstream[8:16]
        delta_ref[r] = normalize_back(upstream * gain, hat, inverse)
        final_ref[r] = middle_ref[r] + two.total(r)

    chunks(x_ref.shape[0], body)
    one.finish()
    two.finish()


ANY = pl.BlockSpec(memory_space=pl.ANY)
VM = pl.BlockSpec(memory_space=pltpu.VMEM)


def call(kernel, ident, args, specs, outs, out_specs, scratch, nbytes):
    return pl.pallas_call(
        kernel,
        out_shape=outs,
        in_specs=specs,
        out_specs=out_specs,
        scratch_shapes=scratch,
        compiler_params=pltpu.CompilerParams(
            collective_id=ident, has_side_effects=True, vmem_limit_bytes=32 << 20
        ),
        cost_estimate=pl.CostEstimate(flops=0, bytes_accessed=nbytes, transcendentals=0),
        name=kernel.__name__,
    )(*args)


def per_device(
    groups,
    swap,
    incoming_signals,
    loss_sensitivity,
    token_counts_per_slot,
    leading_norm_multiplier,
    leading_norm_offset,
    question_projection,
    lookup_projection,
    content_projection,
    silu_switch_projection,
    retention_result_projection,
    trailing_norm_multiplier,
    trailing_norm_offset,
    feedforward_switch_projection,
    expanding_projection,
    contracting_projection,
):
    local_rows, hidden_size = incoming_signals.shape
    total_rows = 8 * local_rows
    slots_here = token_counts_per_slot.shape[0]
    dp_rank, tensor_rank = lax.axis_index("dp"), lax.axis_index("tensor")
    side = lax.rem(dp_rank, 2)
    row_ids = tensor_rank * local_rows + jnp.arange(local_rows, dtype=jnp.int32)
    slot_match = (row_ids // SEQ_LEN)[:, None] == jnp.arange(slots_here, dtype=jnp.int32)[None, :]
    row_lengths = jnp.sum(jnp.where(slot_match, token_counts_per_slot[None, :], 0), axis=1)
    valid_rows = (row_ids % SEQ_LEN < row_lengths)[:, None]

    def exchange(weight, axis, join):
        half = weight.shape[axis] // 2
        keep = lax.dynamic_slice_in_dim(weight, side * half, half, axis)
        give = lax.dynamic_slice_in_dim(weight, (1 - side) * half, half, axis)
        take = lax.ppermute(give, "dp", swap)
        return jnp.where(
            side == 0,
            jnp.concatenate([keep, take], axis=join),
            jnp.concatenate([take, keep], axis=join),
        )

    def spread(block, axis):
        return lax.all_gather(block, "dp", axis=axis, tiled=True, axis_index_groups=groups)

    query_half = exchange(question_projection, 1, 0)
    key_half = exchange(lookup_projection, 1, 0)
    query_key = spread(jnp.concatenate([query_half, key_half], axis=1), 0)
    value_full = spread(exchange(content_projection, 1, 0), 0)
    swish_full = spread(exchange(silu_switch_projection, 1, 0), 0)
    output_full = spread(exchange(retention_result_projection, 0, 1), 1)
    gate_full = spread(exchange(feedforward_switch_projection, 1, 0), 0)
    up_full = spread(exchange(expanding_projection, 1, 0), 0)
    down_full = spread(exchange(contracting_projection, 0, 1), 1)

    gains = jnp.stack(
        [leading_norm_multiplier, leading_norm_offset, trailing_norm_multiplier, trailing_norm_offset]
    )
    gains = lax.all_gather(gains, "dp", axis=1, tiled=True).astype(F32)
    gains = jnp.concatenate([gains, gains], axis=0)

    all_rows = jax.ShapeDtypeStruct((total_rows, hidden_size), BF16)
    own_rows = jax.ShapeDtypeStruct((local_rows, hidden_size), F32)
    pieces = jax.ShapeDtypeStruct((2, 8, hidden_size), F32)
    row_low = pltpu.VMEM((local_rows, hidden_size), BF16)
    reduce_scratch = Reduce.scratch(local_rows, hidden_size)
    moved = total_rows * hidden_size * 2

    out_low = jnp.where(valid_rows, loss_sensitivity, 0)
    normed_all, out_all = call(
        first_kernel,
        0,
        (incoming_signals, out_low, gains),
        [VM, VM, VM],
        (all_rows, all_rows),
        (ANY, ANY),
        [row_low, *Gather.scratch(), *Gather.scratch()],
        24 * moved,
    )

    slot_count = total_rows // SEQ_LEN
    shape_key = (slot_count, SEQ_LEN, KEY_DIM)
    shape_value = (slot_count, SEQ_LEN, VAL_DIM)
    query_key_proj = matmul(normed_all, query_key)
    query_proj = query_key_proj[:, :KEY_DIM].reshape(shape_key)
    key_proj = query_key_proj[:, KEY_DIM:].reshape(shape_key)
    value_heads = matmul(normed_all, value_full).reshape(shape_value).astype(BF16)
    swish_heads = matmul(normed_all, swish_full).reshape(shape_value)
    cosines, sines = rotary_tables(SEQ_LEN, KEY_DIM)
    decays = decay_table(SEQ_LEN, tensor_rank * 2 + side)
    query_rot = (query_proj * cosines + rotate_half(query_proj) * sines).astype(BF16)
    key_rot = ((key_proj * cosines + rotate_half(key_proj) * sines) * KEY_DIM ** (-0.5)).astype(BF16)
    scores = (
        jnp.einsum("snk,smk->snm", query_rot, key_rot, preferred_element_type=F32) * decays[None]
    ).astype(BF16)
    retained = jnp.einsum("snm,smv->snv", scores, value_heads, preferred_element_type=F32)
    group_hat, group_inverse = normalize(retained, GROUP_EPSILON)
    sigmoid_gate = jax.nn.sigmoid(swish_heads)
    gated = (swish_heads * sigmoid_gate * group_hat).reshape(total_rows, VAL_DIM).astype(BF16)
    retention_part = matmul(gated, output_full).astype(BF16)

    mixer_all, middle_rows = call(
        second_kernel,
        1,
        (retention_part, incoming_signals, gains),
        [ANY, VM, VM],
        (all_rows, own_rows),
        (ANY, VM),
        [row_low, *reduce_scratch, *Gather.scratch()],
        24 * moved,
    )

    gate_proj = matmul(mixer_all, gate_full)
    up_proj = matmul(mixer_all, up_full)
    gelu_gate, gelu_back = jax.vjp(gelu_tanh, gate_proj)
    hidden = (gelu_gate * up_proj).astype(BF16)
    down_gradient = matmul(hidden.T, out_all).astype(BF16)
    hidden_back = matmul(out_all, down_full.T)
    gate_back = gelu_back(hidden_back * up_proj)[0].astype(BF16)
    up_back = (hidden_back * gelu_gate).astype(BF16)
    gate_gradient = matmul(mixer_all.T, gate_back).astype(BF16)
    up_gradient = matmul(mixer_all.T, up_back).astype(BF16)
    mixer_input_part = (matmul(gate_back, gate_full.T) + matmul(up_back, up_full.T)).astype(BF16)
    mixer_part = matmul(hidden, down_full).astype(BF16)

    middle_all, middle_back, after_pieces = call(
        third_kernel,
        2,
        (mixer_input_part, middle_rows, out_low, gains),
        [ANY, VM, VM, VM],
        (all_rows, own_rows, pieces),
        (ANY, VM, VM),
        [row_low, *reduce_scratch, *Gather.scratch()],
        24 * moved,
    )

    output_gradient = matmul(gated.T, middle_all).astype(BF16)
    gated_back = matmul(middle_all, output_full.T).reshape(shape_value)
    swish_back = (
        (gated_back * group_hat * sigmoid_gate * (1.0 + swish_heads * (1.0 - sigmoid_gate)))
        .reshape(total_rows, VAL_DIM)
        .astype(BF16)
    )
    retained_back = normalize_back(
        gated_back * swish_heads * sigmoid_gate, group_hat, group_inverse
    ).astype(BF16)
    score_back = (
        jnp.einsum("snv,smv->snm", retained_back, value_heads, preferred_element_type=F32)
        * decays[None]
    ).astype(BF16)
    query_rot_back = jnp.einsum("snm,smk->snk", score_back, key_rot, preferred_element_type=F32)
    key_rot_back = jnp.einsum("snm,snk->smk", score_back, query_rot, preferred_element_type=F32)
    value_back = jnp.einsum("snm,snv->smv", scores, retained_back, preferred_element_type=F32)
    query_back = (
        (query_rot_back * cosines - rotate_half(query_rot_back) * sines)
        .reshape(total_rows, KEY_DIM)
        .astype(BF16)
    )
    key_back = (
        ((key_rot_back * cosines - rotate_half(key_rot_back) * sines) * KEY_DIM ** (-0.5))
        .reshape(total_rows, KEY_DIM)
        .astype(BF16)
    )
    value_low = value_back.reshape(total_rows, VAL_DIM).astype(BF16)
    swish_gradient = matmul(normed_all.T, swish_back).astype(BF16)
    value_gradient = matmul(normed_all.T, value_low).astype(BF16)
    query_key_back = jnp.concatenate([query_back, key_back], axis=1)
    query_key_gradient = matmul(normed_all.T, query_key_back).astype(BF16)
    first_part = (
        matmul(query_key_back, query_key.T)
        + matmul(value_low, value_full.T)
        + matmul(swish_back, swish_full.T)
    ).astype(BF16)

    delta, final_rows, before_pieces = call(
        fourth_kernel,
        3,
        (first_part, mixer_part, incoming_signals, middle_rows, gains),
        [ANY, ANY, VM, VM, VM],
        (own_rows, own_rows, pieces),
        (VM, VM, VM),
        [*reduce_scratch, *reduce_scratch],
        24 * moved,
    )
    layer_output = jnp.where(valid_rows, final_rows, 0.0).astype(BF16)
    input_delta = middle_back + delta

    gain_pieces = jnp.concatenate(
        [jnp.sum(before_pieces, axis=1), jnp.sum(after_pieces, axis=1)], axis=0
    )
    gain_sums = lax.psum(gain_pieces, ("dp", "tensor"))
    width = leading_norm_multiplier.shape[0]
    gain_sums = lax.dynamic_slice_in_dim(gain_sums, dp_rank * width, width, 1)

    def collect(gradient, axis):
        return lax.psum_scatter(
            gradient, "dp", scatter_dimension=axis, tiled=True, axis_index_groups=groups
        )

    def restore(block, axis, join):
        half = block.shape[axis] // 2
        keep = lax.dynamic_slice_in_dim(block, side * half, half, axis)
        give = lax.dynamic_slice_in_dim(block, (1 - side) * half, half, axis)
        take = lax.ppermute(give, "dp", swap)
        return jnp.where(
            side == 0,
            jnp.concatenate([keep, take], axis=join),
            jnp.concatenate([take, keep], axis=join),
        ).astype(F32)

    down_owned = restore(collect(down_gradient, 1), 1, 0)
    gate_owned = restore(collect(gate_gradient, 0), 0, 1)
    up_owned = restore(collect(up_gradient, 0), 0, 1)
    output_owned = restore(collect(output_gradient, 1), 1, 0)
    swish_owned = restore(collect(swish_gradient, 0), 0, 1)
    value_owned = restore(collect(value_gradient, 0), 0, 1)
    query_key_owned = collect(query_key_gradient, 0)
    query_owned = restore(query_key_owned[:, :KEY_DIM], 0, 1)
    key_owned = restore(query_key_owned[:, KEY_DIM:], 0, 1)
    return (
        layer_output,
        input_delta,
        gain_sums[0],
        gain_sums[1],
        query_owned,
        key_owned,
        value_owned,
        swish_owned,
        output_owned,
        gain_sums[2],
        gain_sums[3],
        gate_owned,
        up_owned,
        down_owned,
    )


PLANES = 4
QK, VALUE, SWISH, OUTPUT, GATE, UP, DOWN = range(7)
WIDE = 512
QUERY, KEY = 7, 8
FEED_FORWARD = (DOWN, GATE, UP)
INNER_SUMS = (*FEED_FORWARD, OUTPUT)
GRADIENTS = (*FEED_FORWARD, OUTPUT, SWISH, VALUE, QUERY, KEY)
TILE = 256


def nt(left, right):
    return lax.dot_general(left, right, (((1,), (1,)), ((), ())), preferred_element_type=F32)


def loop(count, body):
    def step(i, carry):
        body(i)
        return carry

    lax.fori_loop(0, count, step, 0)


def together(*steps):
    for step in steps:
        step()


def at(index, size):
    return pl.ds(pl.multiple_of(index * size, size), size)


def mega_scratch(rows, hidden):
    total = 8 * rows
    dma = pltpu.SemaphoreType.DMA
    return dict(
        w=pltpu.VMEM((7, hidden, WIDE), BF16),
        xs=pltpu.VMEM((total, hidden), BF16),
        xt=pltpu.VMEM((total, hidden), BF16),
        outs=pltpu.VMEM((total, hidden), BF16),
        part=pltpu.VMEM((total, hidden), BF16),
        theirs=pltpu.VMEM((4, rows, hidden), BF16),
        got=pltpu.VMEM((2, rows, hidden), BF16),
        across=pltpu.VMEM((2, rows // 2, hidden), BF16),
        q=pltpu.VMEM((total, KEY_DIM), BF16),
        k=pltpu.VMEM((total, KEY_DIM), BF16),
        v=pltpu.VMEM((total, VAL_DIM), BF16),
        sc=pltpu.VMEM((total, SEQ_LEN), BF16),
        swish=pltpu.VMEM((total, VAL_DIM), F32),
        ghat=pltpu.VMEM((total, VAL_DIM), F32),
        ginv=pltpu.VMEM((total, 128), F32),
        gated=pltpu.VMEM((total, VAL_DIM), BF16),
        hid=pltpu.VMEM((total, WIDE), BF16),
        gate=pltpu.VMEM((TILE, WIDE), F32),
        up=pltpu.VMEM((TILE, WIDE), F32),
        gb=pltpu.VMEM((total, WIDE), BF16),
        ub=pltpu.VMEM((total, WIDE), BF16),
        sb=pltpu.VMEM((total, SEQ_LEN), BF16),
        qkb=pltpu.VMEM((total, 2 * KEY_DIM), BF16),
        turned=pltpu.VMEM((WIDE, total), BF16),
        st=pltpu.VMEM((4, WIDE, WIDE), BF16),
        decay=pltpu.VMEM((SEQ_LEN, SEQ_LEN), F32),
        low=pltpu.VMEM((rows, hidden), BF16),
        middle=pltpu.VMEM((rows, hidden), F32),
        back=pltpu.VMEM((rows, hidden), F32),
        pieces=pltpu.VMEM((4, 8, hidden), F32),
        gparts=pltpu.VMEM((8, 8, 256), F32),
        gain=pltpu.VMEM((8, hidden), F32),
        gsend=pltpu.VMEM((8, 8, 256), F32),
        gsum=pltpu.VMEM((4, 8, 256), F32),
        xr=pltpu.VMEM((rows, hidden), BF16),
        cr=pltpu.VMEM((rows, hidden), BF16),
        rows2=pltpu.VMEM((rows, hidden), BF16),
        cot2=pltpu.VMEM((rows, hidden), BF16),
        ub2=pltpu.VMEM((total, WIDE), BF16),
        gated2=pltpu.VMEM((total, VAL_DIM), BF16),
        hop_s=dma((9,)),
        hop_r=dma((9,)),
        gd_s=dma((13,)),
        gd_r=dma((13,)),
        gown=pltpu.VMEM((8, 256), F32),
        ex_s=dma((8,)),
        ex_r=dma((8,)),
        ex_l=dma((8,)),
        zs=dma((7, 2, 4)),
        zr=dma((7, 2, 4)),
        rs=dma((8, 3)),
        rr=dma((8, 4)),
        ra=dma((8, 3)),
        stl=dma((4,)),
        fl=dma((4,)),
        fe_s=dma((8,)),
        fe_r=dma((8,)),
        gg_s=dma((8,)),
        gg_r=dma((8,)),
        gt_s=dma((4,)),
        gt_r=dma((4,)),
        ga_s=dma((13,)),
        ga_r=dma((13,)),
        gc_s=dma((13,)),
        gc_r=dma((13,)),
        re_s=dma((10,)),
        re_r=dma((10,)),
        ol=dma((6,)),
        free=pltpu.SemaphoreType.REGULAR,
    )


class PlaneSum(Reduce):
    def __init__(self, place, part, theirs, got, across, send, recv):
        p = place
        rows = theirs.shape[1]
        h = rows // 2
        self.rows, self.half, self.part = rows, h, part
        self.theirs, self.got, self.across = theirs, got, across
        self.base = [p.block(j) * rows for j in range(4)]

        def remote(k, source, target_ref, target):
            return pltpu.make_async_remote_copy(
                src_ref=source,
                dst_ref=target_ref,
                send_sem=send.at[k],
                recv_sem=recv.at[k],
                device_id=target,
                device_id_type=MESH,
            )

        def piece(j, lo):
            return part.at[pl.ds(pl.multiple_of(self.base[j] + lo, 8), h)]

        self.place, self.remote = p, remote
        a, b = pl.ds(0, h), pl.ds(h, h)
        self.swap = [
            remote(j, part.at[rows_of(p.block(j, 1), rows)], theirs.at[j], p.sib) for j in range(4)
        ]
        self.da = remote(4, piece(3, 0), across.at[0], p.xn)
        self.db = remote(5, piece(3, h), across.at[1], p.yn)
        self.xa = remote(6, piece(1, 0), got.at[0, a], p.xn)
        self.xb = remote(7, piece(1, h), got.at[0, b], p.xn)
        self.ya = remote(8, piece(2, 0), got.at[1, a], p.yn)
        self.yb = remote(9, piece(2, h), got.at[1, b], p.yn)

    def add(self, j, lo, n, other, other_lo):
        def body(i):
            r = pl.ds(pl.multiple_of(self.base[j] + lo + i * CHUNK, CHUNK), CHUNK)
            q = pl.ds(pl.multiple_of(other_lo + i * CHUNK, CHUNK), CHUNK)
            self.part[r] = (self.part[r].astype(F32) + other[q].astype(F32)).astype(BF16)

        loop(n // CHUNK, body)

    def start(self):
        for j in (3, 1, 2, 0):
            self.swap[j].start()

    def fill(self, tile_value, sending=None):
        def body(i):
            self.fill_chip(jnp.where(i == 0, 3, jnp.where(i == 3, 0, i)), tile_value, sending)

        loop(4, body)

    def chip(self, j):
        p = self.place
        chip_x = jnp.where(lax.rem(j, 2) == 1, 1 - p.x, p.x)
        chip_y = jnp.where(j >= 2, 1 - p.y, p.y)
        return chip_x * 2 + chip_y

    def fill_chip(self, j, tile_value, sending=None):
        chip = self.chip(j)
        r = at(chip, 2 * self.rows)

        def inner(n):
            c = at(n, WIDE)
            self.part[r, c] = tile_value(r, c).astype(BF16)

        loop(self.part.shape[1] // WIDE, inner)
        source = self.part.at[rows_of(chip * 2 + 1 - self.place.c, self.rows)]
        send = self.remote(j, source, self.theirs.at[j], self.place.sib)
        if sending is None:
            send.start()
        else:
            pl.when(sending)(send.start)

    def take(self, j):
        copies = {3: (self.da, self.db), 1: (self.xa,), 2: (self.yb,)}[j]
        self.swap[j].wait_recv()
        self.add(j, 0, self.rows, self.theirs.at[j], 0)
        for copy in copies:
            copy.start()

    def run1(self):
        for j in (3, 1, 2):
            self.take(j)

    def run2(self):
        h = self.half
        self.db.wait_recv()
        self.add(1, h, h, self.across.at[1], 0)
        self.xb.start()
        self.da.wait_recv()
        self.add(2, 0, h, self.across.at[0], 0)
        self.ya.start()

    def run3(self):
        self.swap[0].wait_recv()
        for copy in (self.xa, self.yb, self.xb, self.ya):
            copy.wait_recv()

    def run(self):
        self.run1()
        self.run2()
        self.run3()

    def total(self, i):
        r = pl.ds(pl.multiple_of(i * CHUNK, CHUNK), CHUNK)
        mine = pl.ds(pl.multiple_of(self.base[0] + i * CHUNK, CHUNK), CHUNK)
        pieces = (self.part[mine], self.theirs[0, r], self.got[0, r], self.got[1, r])
        one, two, three, four = (piece.astype(F32) for piece in pieces)
        return (one + two) + (three + four)


def mega_kernel(names, count_in, count_out, *refs):
    x_hbm, cot_hbm, counts_ref, cos_ref, sin_ref = refs[:5]
    gain_refs = refs[5:9]
    q_w, k_w, v_w, s_w, o_w, g_w, u_w, d_w = refs[9:count_in]
    outs = refs[count_in : count_in + count_out]
    final_out, delta_out, gains_out, q_g, k_g, v_g, s_g, o_g, g_g, u_g, d_g, stage, heard, added, parked = outs
    b = {name: ref for name, ref in zip(names, refs[count_in + count_out :], strict=True)}
    w, xs, xt, st, part, turned = b["w"], b["xs"], b["xt"], b["st"], b["part"], b["turned"]
    x_ref, cot_ref = b["xr"], b["cr"]
    rows, hidden = x_ref.shape
    width = hidden // 8

    dp, tensor = lax.axis_index("dp"), lax.axis_index("tensor")
    place = Place()
    x, z = place.x, dp // 2
    first_plane, inner = z == 0, (z == 1) | (z == 2)
    outer = jnp.logical_not(inner)

    barrier = pltpu.get_barrier_semaphore()
    for i in range(1, 8):
        other = (lax.rem(dp + i, 8), tensor)
        pl.semaphore_signal(barrier, inc=1, device_id=other, device_id_type=MESH)
    for i in range(1, 4):
        other = (dp, lax.rem(tensor + i, 4))
        pl.semaphore_signal(barrier, inc=1, device_id=other, device_id_type=MESH)

    def remote(source, target_ref, send, recv, target):
        return pltpu.make_async_remote_copy(
            src_ref=source,
            dst_ref=target_ref,
            send_sem=send,
            recv_sem=recv,
            device_id=target,
            device_id_type=MESH,
        )

    def plane(step):
        return ((z + step) * 2 + x, tensor)

    def column_exchange(n, weight, k, lane, half):
        where = w.at[k, pl.ds(pl.multiple_of(z * 512 + x * 256, 256), width), pl.ds(lane, half)]
        keep = pltpu.make_async_copy(weight.at[:, at(x, half)], where, b["ex_l"].at[n])
        give = remote(
            weight.at[:, at(1 - x, half)], where, b["ex_s"].at[n], b["ex_r"].at[n], place.xn
        )
        return keep, give

    def row_exchange(n, weight, k):
        where = w.at[k, at(z, 512), at(x, width)]
        keep = pltpu.make_async_copy(weight.at[at(x, 512)], where, b["ex_l"].at[n])
        give = remote(weight.at[at(1 - x, 512)], where, b["ex_s"].at[n], b["ex_r"].at[n], place.xn)
        return keep, give

    exchanges = [
        [column_exchange(0, q_w, QK, 0, 256), column_exchange(1, k_w, QK, 256, 256)],
        [column_exchange(2, v_w, VALUE, 0, 512)],
        [column_exchange(3, s_w, SWISH, 0, 512)],
        [row_exchange(4, o_w, OUTPUT)],
        [column_exchange(5, g_w, GATE, 0, 512)],
        [column_exchange(6, u_w, UP, 0, 512)],
        [row_exchange(7, d_w, DOWN)],
    ]

    def keep(k):
        for local, _ in exchanges[k]:
            local.start()

    def give(k):
        for _, send in exchanges[k]:
            send.start()

    towards = jnp.where(z == 1, -1, 1)
    near, far = jnp.where(z == 1, 2, 1), jnp.where(z == 1, 3, 0)
    own_steps = (
        jnp.where(first_plane, 2, jnp.where(inner, 1, -2)),
        jnp.where(first_plane, 1, -1),
    )
    beside = place.xn

    def parts(k):
        return (0, 1) if k == QK else (0,)

    def block_copy(k, block, half, slot, target):
        if k == QK:
            side = x if half == 0 else 1 - x
            ref = w.at[k, pl.ds(pl.multiple_of(block * 512 + side * 256, 256), 256)]
        else:
            ref = w.at[k, at(block, 512)]
        return remote(ref, ref, b["zs"].at[k, half, slot], b["zr"].at[k, half, block], target)

    def kept(k):
        for local, _ in exchanges[k]:
            local.wait()

    def swapped(k):
        for _, send in exchanges[k]:
            send.wait_recv()

    def spread_half(k, half):
        def both():
            for slot, step in enumerate(own_steps):
                block_copy(k, z, half, slot, plane(step)).start()

        if k in FEED_FORWARD:
            step = jnp.where(outer, jnp.where(first_plane, 1, -1), -towards)
            block_copy(k, z, half, 0, plane(step)).start()
        else:
            both()

    def spread(k):
        kept(k)
        swapped(k)
        spread_half(k, 0)

    def pass_on(k):
        @pl.when(inner)
        def _():
            for half in parts(k):
                for slot, block in ((2, near), (3, far)):
                    copy = block_copy(k, block, half, slot, plane(towards))
                    copy.wait_recv()
                    copy.start()

    def arrive(k):
        for half in parts(k):

            @pl.when(inner)
            def _(half=half):
                block_copy(k, jnp.where(z == 1, 0, 3), half, 0, beside).wait_recv()

            @pl.when(outer)
            def _(half=half):
                for i in range(3):
                    block = jnp.where(first_plane, i + 1, i)
                    block_copy(k, block, half, 0, beside).wait_recv()

    def pass_inner(k):
        copy = block_copy(k, jnp.where(z == 1, 0, 3), 0, 1, plane(-towards))
        copy.wait_recv()
        copy.start()

    def arrive_inner(k):
        for block in (near, far):
            block_copy(k, block, 0, 0, beside).wait_recv()

    def weights_sent():
        for k in range(7):
            for _, send in exchanges[k]:
                send.wait_send()
            for half in parts(k):
                block_copy(k, z, half, 0, beside).wait_send()
                if k in FEED_FORWARD:
                    pl.when(inner)(lambda k=k, half=half: block_copy(k, z, half, 1, beside).wait_send())
                else:
                    block_copy(k, z, half, 1, beside).wait_send()

                    @pl.when(inner)
                    def _(k=k, half=half):
                        for slot in (2, 3):
                            block_copy(k, z, half, slot, beside).wait_send()

    def lanes_of(c):
        if c in (QUERY, KEY):
            return QK, pl.ds(256 * (c - QUERY), 256)
        return c, pl.ds(0, 512)

    def share(ref, c, *index):
        chunk, lanes = lanes_of(c)
        return ref.at[(chunk, *index, slice(None), lanes)]

    def slot_of(c, slot):
        return st.at[slot, :, pl.ds(0, 256 if c in (QUERY, KEY) else 512)]

    def number(c):
        return c if c < QUERY else c - QUERY + (0 if c == QUERY else 6)

    def staged(c, block, slot):
        return pltpu.make_async_copy(slot_of(c, slot), share(stage, c, block), b["stl"].at[slot])

    def to_added(c, block, which, target, slot=None):
        n = number(c)
        return remote(
            share(stage, c, block),
            share(added, c, which),
            b["rs"].at[n, which if slot is None else slot],
            b["ra"].at[n, which],
            target,
        )

    def to_heard(c, block, slot, target):
        n = number(c)
        return remote(
            share(stage, c, block), share(heard, c, z), b["rs"].at[n, slot], b["rr"].at[n, z], target
        )

    def all_staged(c):
        for block in range(PLANES):
            staged(c, block, block).wait()

    def send_gradient(c):
        all_staged(c)
        step = jnp.where(first_plane, 1, -1)

        @pl.when(outer)
        def _():
            to_added(c, 3 - z, 0, plane(step)).start()
            to_added(c, z + 2 * step, 1, plane(step)).start()
            to_heard(c, z + step, 2, plane(step)).start()

    def send_inner(c):
        to_added(c, far, 2, plane(-towards), 0).start()
        to_heard(c, near, 1, plane(-towards)).start()

    def rounds(c, body):
        lanes = 256 if c in (QUERY, KEY) else 512

        def step(i):
            body(pl.ds(pl.multiple_of(i * 32, 32), 32), pl.ds(0, lanes))

        loop(WIDE // 32, step)

    def local(source, target, n):
        return pltpu.make_async_copy(source, target, b["fl"].at[n])

    def combine(c):
        @pl.when(inner)
        def _():
            blocks = (far, near)
            mine = [local(share(stage, c, blocks[i]), slot_of(c, i), i) for i in range(2)]
            for copy in mine:
                copy.start()
            theirs = [local(share(added, c, i), slot_of(c, 2 + i), 2 + i) for i in range(2)]
            for i in range(2):
                to_added(c, blocks[i], i, beside).wait_recv()
                theirs[i].start()
            for i in range(2):
                mine[i].wait()
                theirs[i].wait()

                def body(r, lanes, i=i):
                    st[i, r, lanes] = (
                        st[i, r, lanes].astype(F32) + st[2 + i, r, lanes].astype(F32)
                    ).astype(BF16)

                rounds(c, body)
                back = local(slot_of(c, i), share(stage, c, blocks[i]), i)
                back.start()
            for i in range(2):
                local(slot_of(c, i), share(stage, c, blocks[i]), i).wait()
            send_inner(c)

    def combine_inner(c):
        block = z + towards
        mine = local(share(stage, c, block), slot_of(c, 0), 0)
        theirs = local(share(added, c, 2), slot_of(c, 1), 1)
        mine.start()
        to_added(c, block, 2, beside, 0).wait_recv()
        theirs.start()
        mine.wait()
        theirs.wait()

        def body(r, lanes):
            st[0, r, lanes] = (
                st[0, r, lanes].astype(F32) + st[1, r, lanes].astype(F32)
            ).astype(BF16)

        rounds(c, body)
        back = local(slot_of(c, 0), share(stage, c, block), 0)
        back.start()
        back.wait()
        to_heard(c, block, 2, plane(towards)).start()

    homes = {
        QUERY: q_g, KEY: k_g, VALUE: v_g, SWISH: s_g, OUTPUT: o_g, GATE: g_g, UP: u_g, DOWN: d_g
    }

    def home_copies(c, source):
        home, (_, lanes) = homes[c], lanes_of(c)
        if c in (OUTPUT, DOWN):
            kept_half, given_half = (slice(None), at(x, 256)), (slice(None), at(1 - x, 256))
            slot = home.at[at(x, 512)]
        else:
            kept_half, given_half = (at(x, 256),), (at(1 - x, 256),)
            slot = home.at[:, at(x, home.shape[1] // 2)]
        n = number(c)
        return (
            local(slot_of(c, 0).at[kept_half], slot, 3),
            remote(source.at[given_half], slot, b["fe_s"].at[n], b["fe_r"].at[n], beside),
        )

    def finish_gradient(c, last=False):
        n = number(c)

        def own_load():
            return local(share(stage, c, z), slot_of(c, 0), 0)

        def arrival(i, source):
            remote(
                share(stage, c, 0), share(heard, c, source), b["rs"].at[n, 2], b["rr"].at[n, source], beside
            ).wait_recv()
            load = local(share(heard, c, source), slot_of(c, i), i)
            load.start()
            return load

        source = jnp.where((z == 0) | (z == 2), 1, 2)
        if c in INNER_SUMS:

            @pl.when(outer)
            def _():
                arrival(0, source).wait()

        else:

            @pl.when(outer)
            def _():
                own_load().start()
                arrival(1, source).wait()
                own_load().wait()

                def body(r, lanes):
                    st[0, r, lanes] = (
                        st[0, r, lanes].astype(F32) + st[1, r, lanes].astype(F32)
                    ).astype(BF16)

                rounds(c, body)

        @pl.when(inner)
        def _():
            own_load().start()
            loads = [arrival(1, source)]
            if c not in INNER_SUMS:
                loads.append(arrival(2, jnp.where(z == 1, 0, 3)))
            own_load().wait()
            for load in loads:
                load.wait()

            def body(r, lanes):
                acc = st[0, r, lanes].astype(F32) + st[1, r, lanes].astype(F32)
                if c not in INNER_SUMS:
                    acc = acc + st[2, r, lanes].astype(F32)
                st[0, r, lanes] = acc.astype(BF16)

            rounds(c, body)

        source = slot_of(c, 0) if last else share(stage, c, z)
        stay, send = home_copies(c, source)
        if not last:
            store = local(slot_of(c, 0), share(stage, c, z), 0)
            store.start()
            stay.start()
            store.wait()
            send.start()
            stay.wait()
        else:
            send.start()
            stay.start()
            stay.wait()

    def gradients_done():
        for c in GRADIENTS:
            n = number(c)
            source = slot_of(c, 0) if c == KEY else share(stage, c, z)
            _, send = home_copies(c, source)
            send.wait()

            def sent(c=c, n=n):
                for slot in range(3):
                    remote(
                        share(stage, c, 0), share(heard, c, 0), b["rs"].at[n, slot], b["rr"].at[n, 0], beside
                    ).wait_send()

            if c in INNER_SUMS:
                pl.when(inner)(sent)
            else:
                sent()

    across_step = jnp.where(outer, jnp.where(first_plane, 1, -1), towards)

    def hop(n, source, target, part_of=slice(None)):
        return remote(
            source.at[part_of], target.at[part_of], b["hop_s"].at[n], b["hop_r"].at[n], plane(across_step)
        )

    halves = (pl.ds(0, rows // 2), pl.ds(rows // 2, rows // 2))

    def neighbours_may_write():
        for partner in (place.sib, place.xn, place.yn):
            pl.semaphore_signal(b["free"], inc=1, device_id=partner, device_id_type=MESH)

    def may_write():
        pl.semaphore_wait(b["free"], 3)

    def gain_copy(i):
        target = lax.rem(dp + i, 8)
        return remote(
            b["gown"], b["gparts"].at[dp], b["gg_s"].at[i], b["gg_r"].at[dp], (target, tensor)
        )

    def gain_arrival(i):
        source = lax.rem(dp + i, 8)
        return remote(
            b["gown"], b["gparts"].at[source], b["gg_s"].at[i], b["gg_r"].at[source], (source, tensor)
        )

    gather_sems = (b["ga_s"], b["ga_r"])

    def plane_sum(ref):
        return PlaneSum(place, ref, b["theirs"], b["got"], b["across"], b["re_s"], b["re_r"])

    for k in range(7):
        keep(k)
    gown = b["gown"]
    for n in range(8):
        gown[n : n + 1, :] = gain_refs[n % 4][...].astype(F32).reshape(1, 256)
    load_x = pltpu.make_async_copy(x_hbm, x_ref, b["ol"].at[3])
    load_cot = pltpu.make_async_copy(cot_hbm, cot_ref, b["ol"].at[4])
    load_x.start()
    load_cot.start()
    mine = pltpu.make_async_copy(gown, b["gparts"].at[dp], b["ol"].at[0])
    mine.start()
    kept(QK)
    pl.semaphore_wait(barrier, 10)
    for i in range(1, 8):
        gain_copy(i).start()
    give(QK)
    spread_half(QK, 0)
    give(VALUE)
    head = (tensor * 2 + x).astype(F32)
    rate = jnp.log(1.0 - jnp.exp2(-5.0 - jnp.full((8, SEQ_LEN), head, F32)))[0:1]

    def body(i):
        r = at(i, 64)
        n = lax.broadcasted_iota(jnp.int32, (64, SEQ_LEN), 0) + i * 64
        m = lax.broadcasted_iota(jnp.int32, (64, SEQ_LEN), 1)
        gap = n - m
        b["decay"][r] = jnp.where(gap >= 0, jnp.exp(jnp.maximum(gap, 0).astype(F32) * rate), 0.0)

    loop(SEQ_LEN // 64, body)
    load_x.wait()
    swapped(QK)
    spread_half(QK, 1)
    mine.wait()
    for i in range(1, 8):
        gain_arrival(i).wait_recv()
    for i in range(8):
        b["gain"][:, i * 256 : (i + 1) * 256] = b["gparts"][i]
    gain = b["gain"]
    low = b["low"]

    def body(i):
        r = at(i, CHUNK)
        hat, _ = normalize(x_ref[r].astype(F32), EPSILON)
        low[r] = (hat * gain[0:1, :] + gain[1:2, :]).astype(BF16)

    loop(rows // CHUNK, body)
    first = Gather(place, low, xs, *gather_sems)
    first.start()
    spread(VALUE)
    load_cot.wait()
    count = counts_ref[0]

    def body(i):
        r = at(i, CHUNK)
        row = lax.broadcasted_iota(jnp.int32, (CHUNK, hidden), 0) + (tensor * rows + i * CHUNK)
        cot_ref[r] = jnp.where(row < count, cot_ref[r].astype(F32), 0.0).astype(BF16)

    loop(rows // CHUNK, body)
    pl.when(outer)(lambda: hop(2, cot_ref, b["cot2"]).start())
    first.forward()
    for k in range(SWISH, DOWN + 1):
        give(k)
    cotangent = Gather(place, cot_ref, b["outs"], b["gc_s"], b["gc_r"])
    pl.when(inner)(cotangent.start)
    pass_on(QK)
    spread(SWISH)
    first.finish()

    def turned_rows(i):
        return at(i // 2, 512), at(lax.rem(i, 2), 8 * rows)

    def body(i):
        r, lanes = turned_rows(i // 2)
        r = pl.ds(pl.multiple_of((i // 4) * 512 + lax.rem(i, 2) * 256, 256), 256)
        xt[r, lanes] = xs[:, at(i, 256)].T

    loop(hidden // 256, body)
    park = pltpu.make_async_copy(xt, parked, b["ol"].at[5])
    unpark = pltpu.make_async_copy(parked, xt, b["ol"].at[0])
    pl.when(inner)(park.start)
    spread(OUTPUT)

    arrive(QK)

    def turn(acc, tile, scale):
        spot = at(lax.rem(tile, SEQ_LEN // TILE), TILE)
        cos, sin = cos_ref[spot], sin_ref[spot]
        one, two = acc[:, :128], acc[:, 128:]
        return (((one * cos - two * sin) * scale).astype(BF16), ((two * cos + one * sin) * scale).astype(BF16))

    def body(i):
        r = at(i, TILE)
        acc = matmul(xs[r], w[QK])
        b["q"][r, :128], b["q"][r, 128:] = turn(acc[:, :KEY_DIM], i, 1.0)
        b["k"][r, :128], b["k"][r, 128:] = turn(acc[:, KEY_DIM:], i, KEY_DIM ** (-0.5))

    tiles = 8 * rows // TILE
    per_slot = SEQ_LEN // TILE
    loop(tiles, body)

    def slot_rows(i):
        return at(i // per_slot, SEQ_LEN)

    def body(i):
        r = at(i, TILE)
        decay = b["decay"][at(lax.rem(i, per_slot), TILE)]
        b["sc"][r] = (nt(b["q"][r], b["k"][slot_rows(i)]) * decay).astype(BF16)

    loop(tiles, body)

    for k in (GATE, UP, DOWN):
        spread(k)
    pass_on(VALUE)
    arrive(VALUE)

    def body(i):
        r = at(i, TILE)
        b["v"][r] = matmul(xs[r], w[VALUE]).astype(BF16)

    loop(tiles, body)

    def body(i):
        r = at(i, TILE)
        retained = matmul(b["sc"][r], b["v"][slot_rows(i)])
        hat, inverse = normalize(retained, GROUP_EPSILON)
        b["ghat"][r] = hat
        b["ginv"][r] = jnp.broadcast_to(inverse, (TILE, 128))

    loop(tiles, body)
    @pl.when(inner)
    def _():
        cotangent.forward()
        cotangent.finish()

    pass_on(SWISH)
    arrive(SWISH)

    def body(i):
        r = at(i, TILE)
        swish = matmul(xs[r], w[SWISH])
        b["swish"][r] = swish
        b["gated"][r] = (swish * jax.nn.sigmoid(swish) * b["ghat"][r]).astype(BF16)

    loop(tiles, body)

    pass_on(OUTPUT)
    arrive(OUTPUT)

    def grid_of(i):
        return at(i // PLANES, TILE), at(lax.rem(i, PLANES), 512)

    reduce = plane_sum(part)
    reduce.fill(lambda r, c: matmul(b["gated"][r], w[OUTPUT, c]))
    reduce.run()
    def body(i):
        r = at(i, CHUNK)
        middle = x_ref[r].astype(F32) + reduce.total(i)
        b["middle"][r] = middle
        hat, _ = normalize(middle, EPSILON)
        low[r] = (hat * gain[2:3, :] + gain[3:4, :]).astype(BF16)

    loop(rows // CHUNK, body)

    @pl.when(outer)
    def _():
        for n in range(2):
            hop(n, low, b["rows2"], halves[n]).start()
        hop(6, b["gated"], b["gated2"]).start()

    pl.when(inner)(lambda: pass_inner(GATE))

    def gelu_of(t):
        inner_value = 0.7978845608028654 * (t + 0.044715 * t * t * t)
        tanh = jnp.tanh(inner_value)
        return 0.5 * (1.0 + tanh), tanh

    def turned_of(ref):
        def body(i):
            turned[:, at(i, TILE)] = ref[at(i, TILE)].T

        loop(tiles, body)

    def stage_block(c, i, value):
        st[i] = value.astype(BF16)
        staged(c, i, i).start()

    def times_turned(left, r, k):
        acc = nt(left[r, 0:512], w[k, 0:512])
        for plane_at in range(1, PLANES):
            lanes = slice(plane_at * 512, plane_at * 512 + 512)
            acc = acc + nt(left[r, lanes], w[k, lanes])
        return acc

    def hidden_tile(mixer, hid, r):
        gate = matmul(mixer[r], w[GATE])
        b["gate"][...] = gate
        up = matmul(mixer[r], w[UP])
        b["up"][...] = up
        gate = b["gate"][...]
        share_of, _ = gelu_of(gate)
        hid[r] = (gate * share_of * up).astype(BF16)

    def back_tile(cots, gb, ub, r):
        back = times_turned(cots, r, DOWN)
        gate, up = b["gate"][...], b["up"][...]
        share_of, tanh = gelu_of(gate)
        slope = 0.5 * gate * (1.0 - tanh * tanh) * (0.7978845608028654 * (1.0 + 0.134145 * gate * gate))
        gb[r] = (back * up * (share_of + slope)).astype(BF16)
        ub[r] = (back * gate * share_of).astype(BF16)

    def refill(c):
        copies = [pltpu.make_async_copy(stage.at[c, i], st.at[i], b["fl"].at[i]) for i in range(PLANES)]
        for copy in copies:
            copy.start()
        for copy in copies:
            copy.wait()

    def product_of(c, i, value, more):
        stage_block(c, i, value + st[i].astype(F32) if more else value)

    def down_gradient(hid, cots, more):
        if more:
            refill(DOWN)
        turned_of(hid)

        def body(i):
            product_of(DOWN, i, matmul(turned[...], cots[:, at(i, 512)]), more)

        loop(PLANES, body)
        all_staged(DOWN)

    def weight_gradient(c, mixer, right, more):
        if more:
            refill(c)

        def body(i):
            def body_turn(j):
                turned[:, at(j, TILE)] = mixer[at(j, TILE), at(i, 512)].T

            loop(tiles, body_turn)
            product_of(c, i, matmul(turned[...], right[...]), more)

        loop(PLANES, body)
        all_staged(c)

    def mixer_input(gb, ub):
        return lambda r, c: nt(gb[r], w[GATE, c]) + nt(ub[r], w[UP, c])

    def mixer_output(hid, target):
        def body(i):
            r, c = grid_of(i)
            target[r, c] = matmul(hid[r], w[DOWN, c]).astype(BF16)

        loop(tiles * PLANES, body)

    b["pieces"][...] = jnp.zeros_like(b["pieces"])

    def second_norm_backward(r, upstream):
        hat, inverse = normalize(b["middle"][r], EPSILON)
        scaled = upstream * hat
        b["pieces"][2] += scaled[0:8] + scaled[8:16]
        b["pieces"][3] += upstream[0:8] + upstream[8:16]
        back = cot_ref[r].astype(F32) + normalize_back(upstream * gain[2:3, :], hat, inverse)
        b["back"][r] = back
        low[r] = back.astype(BF16)

    hid2, gb2, ub2 = b["sb"], b["qkb"], b["ub2"]
    outs_ref = b["outs"]

    @pl.when(inner)
    def _():
        second = Gather(place, low, xs, *gather_sems)
        second.start()
        hop(2, cot_ref, b["cot2"]).wait_recv()
        second.forward()
        pass_inner(UP)
        other_cot = Gather(place, b["cot2"], part, b["gc_s"], b["gc_r"])
        reduce.finish()
        neighbours_may_write()
        may_write()
        other_cot.start()
        pass_inner(DOWN)
        second.finish()
        arrive_inner(GATE)
        arrive_inner(UP)
        other_cot.forward()
        arrive_inner(DOWN)

        def body(i):
            r = at(i, TILE)
            hidden_tile(xs, b["hid"], r)
            back_tile(outs_ref, b["gb"], b["ub"], r)

        loop(tiles, body)
        down_gradient(b["hid"], outs_ref, False)
        neighbours_may_write()
        other_cot.finish()
        other = Gather(place, b["rows2"], outs_ref, b["gd_s"], b["gd_r"])
        may_write()
        hop(0, low, b["rows2"], halves[0]).wait_recv()
        other.start_first_half()
        hop(1, low, b["rows2"], halves[1]).wait_recv()
        other.start_second_half()
        weight_gradient(GATE, xs, b["gb"], False)
        other.forward_across()
        other.own_arrived()
        park.wait()
        reduce2 = plane_sum(xt)

        def body(i):
            pl.when(i == 1)(lambda: together(other.forward_beside, other.s1.wait_recv))
            pl.when(i == 2)(other.s2.wait_recv)
            pl.when(i == 3)(other.across_arrived)
            r = at(reduce2.chip(i), TILE)
            hidden_tile(outs_ref, hid2, r)
            back_tile(part, gb2, ub2, r)
            reduce2.fill_chip(i, mixer_input(gb2, ub2))
            pl.when(i == 2)(lambda: reduce2.take(1))
            pl.when(i == 3)(lambda: reduce2.take(2))

        loop(PLANES, body)
        reduce2.take(3)
        weight_gradient(UP, xs, b["ub"], False)
        reduce2.run2()
        down_gradient(hid2, part, True)
        send_inner(DOWN)
        reduce2.run3()
        for n in range(2):

            def body(i, n=n):
                i = n * (rows // 2 // CHUNK) + i
                b["rows2"][at(i, CHUNK)] = reduce2.total(i).astype(BF16)

            other.drain() if n == 0 else None
            loop(rows // 2 // CHUNK, body)
            hop(3 + n, b["rows2"], b["rows2"], halves[n]).start()
        reduce2.finish()
        unpark.start()
        neighbours_may_write()
        may_write()
        reduce3 = plane_sum(part)
        reduce3.fill(mixer_input(b["gb"], b["ub"]))
        reduce3.run1()
        weight_gradient(GATE, outs_ref, gb2, True)
        send_inner(GATE)
        reduce3.run2()
        weight_gradient(UP, outs_ref, ub2, True)
        send_inner(UP)
        combine_inner(DOWN)
        reduce3.run3()

        def body(i):
            second_norm_backward(at(i, CHUNK), reduce3.total(i))

        loop(rows // CHUNK, body)
        reduce3.finish()
        neighbours_may_write()
        may_write()
        hop(7, low, b["cot2"]).wait_recv()

    third = Gather(place, low, xs, *gather_sems)
    other_middle = Gather(place, b["cot2"], part, b["gd_s"], b["gd_r"])
    outs_ref = b["outs"]

    @pl.when(outer)
    def _():
        reduce.finish()
        for n in range(2):
            hop(n, low, b["rows2"], halves[n]).wait_send()
        for n in range(2):
            hop(3 + n, b["rows2"], b["rows2"], halves[n]).wait_recv()

            def body(i, n=n):
                r = pl.ds(pl.multiple_of(n * (rows // 2) + i * CHUNK, CHUNK), CHUNK)
                second_norm_backward(r, b["rows2"][r].astype(F32))

            loop(rows // 2 // CHUNK, body)
            if n == 0:
                third.start_first_half()
            else:
                third.start_second_half()
                hop(7, low, b["cot2"]).start()
        third.forward()
        third.finish()

    def output_gradient(rows_ref, cots, more):
        if more:
            refill(OUTPUT)
        turned_of(rows_ref)

        def body(i):
            product_of(OUTPUT, i, matmul(turned[...], cots[:, at(i, 512)]), more)

        loop(PLANES, body)
        all_staged(OUTPUT)

    reduce5 = plane_sum(outs_ref)

    @pl.when(inner)
    def _():
        third.start()
        mixer_output(hid2, outs_ref)
        third.forward_across()
        other_middle.start()
        finish_gradient(DOWN)
        combine_inner(GATE)
        third.forward_beside()
        third.finish()
        other_middle.forward_across()

    swb, rb, vlow = b["gb"], b["ub2"], b["ub"]

    def body(i):
        r = at(i, TILE)
        back = times_turned(xs, r, OUTPUT)
        swish, hat = b["swish"][r], b["ghat"][r]
        gate = jax.nn.sigmoid(swish)
        swb[r] = (back * hat * gate * (1.0 + swish * (1.0 - gate))).astype(BF16)
        rb[r] = normalize_back(back * swish * gate, hat, b["ginv"][r, 0:1]).astype(BF16)

    loop(tiles, body)

    def projection_gradient(c, right, lanes=slice(None)):
        def body(i):
            value = matmul(xt[turned_rows(i)], right[:, lanes]).astype(BF16)
            st[i, :, 0 : value.shape[1]] = value
            staged(c, i, i).start()

        loop(PLANES, body)
        send_gradient(c)

    pl.when(inner)(lambda: together(other_middle.forward_beside, unpark.wait))
    projection_gradient(SWISH, swb)

    @pl.when(inner)
    def _():
        output_gradient(b["gated"], xs, False)

    combine(SWISH)

    @pl.when(inner)
    def _():
        other_middle.finish()
        reduce5.start()
        hop(6, b["gated"], b["gated2"]).wait_recv()
        output_gradient(b["gated2"], part, True)
        send_inner(OUTPUT)
        combine_inner(UP)
        reduce5.run1()

    def body(i):
        r = at(i, TILE)
        decay = b["decay"][at(lax.rem(i, per_slot), TILE)]
        b["sb"][r] = (nt(rb[r], b["v"][slot_rows(i)]) * decay).astype(BF16)

    loop(tiles, body)
    turned_of(b["sc"])

    def body(i):
        vlow[at(i, TILE)] = matmul(
            turned[at(lax.rem(i, per_slot), TILE), slot_rows(i)], rb[slot_rows(i)]
        ).astype(BF16)

    loop(tiles, body)
    projection_gradient(VALUE, vlow)
    pl.when(inner)(reduce5.run2)
    pl.when(inner)(lambda: combine_inner(SWISH))
    turned_of(b["sb"])

    def turn_back(acc, tile, scale):
        spot = at(lax.rem(tile, per_slot), TILE)
        cos, sin = cos_ref[spot], sin_ref[spot]
        one, two = acc[:, :128], acc[:, 128:]
        return (((one * cos + two * sin) * scale).astype(BF16), ((two * cos - one * sin) * scale).astype(BF16))

    def body(i):
        r = at(i, TILE)
        qkb = b["qkb"]
        query = matmul(b["sb"][r], b["k"][slot_rows(i)])
        qkb[r, 0:128], qkb[r, 128:256] = turn_back(query, i, 1.0)
        key = matmul(turned[at(lax.rem(i, per_slot), TILE), slot_rows(i)], b["q"][slot_rows(i)])
        qkb[r, 256:384], qkb[r, 384:512] = turn_back(key, i, KEY_DIM ** (-0.5))

    loop(tiles, body)
    projection_gradient(QUERY, b["qkb"], slice(0, 256))
    projection_gradient(KEY, b["qkb"], slice(256, 512))
    reduce6 = plane_sum(outs_ref)

    @pl.when(inner)
    def _():
        reduce5.run3()

        def body(i):
            b["cot2"][at(i, CHUNK)] = reduce5.total(i).astype(BF16)

        loop(rows // CHUNK, body)
        hop(5, b["cot2"], b["cot2"]).start()
        reduce5.finish()
        neighbours_may_write()

    combine(VALUE)

    @pl.when(inner)
    def _():
        finish_gradient(GATE)
        may_write()
        reduce6.fill(lambda r, c: matmul(b["hid"][r], w[DOWN, c]))
        combine_inner(OUTPUT)
        reduce6.run1()

    reduce = plane_sum(part)
    reduce.fill(
        lambda r, c: nt(b["qkb"][r], w[QK, c]) + nt(vlow[r], w[VALUE, c]) + nt(swb[r], w[SWISH, c]),
        sending=outer,
    )
    pl.when(inner)(reduce6.run2)
    combine(QUERY)
    pl.when(inner)(lambda: combine_inner(VALUE))
    pl.when(outer)(lambda: finish_gradient(DOWN))

    @pl.when(inner)
    def _():
        reduce6.run3()

        def body(i):
            b["middle"][at(i, CHUNK)] += reduce6.total(i)

        loop(rows // CHUNK, body)
        reduce6.finish()
        neighbours_may_write()
        may_write()
        reduce.start()

    pl.when(outer)(lambda: finish_gradient(GATE))
    reduce.run1()
    combine(KEY)
    pl.when(inner)(lambda: combine_inner(QUERY))
    reduce.run2()
    finish_gradient(UP)
    pl.when(inner)(lambda: combine_inner(KEY))
    finish_gradient(SWISH)
    reduce.run3()

    def body(i):
        r = at(i, CHUNK)
        upstream = reduce.total(i)
        hat, inverse = normalize(x_ref[r].astype(F32), EPSILON)
        scaled = upstream * hat
        b["pieces"][0] += scaled[0:8] + scaled[8:16]
        b["pieces"][1] += upstream[0:8] + upstream[8:16]
        b["back"][r] += normalize_back(upstream * gain[0:1, :], hat, inverse)

    loop(rows // CHUNK, body)
    reduce.finish()
    delta_copy = pltpu.make_async_copy(b["back"], delta_out, b["ol"].at[2])
    delta_copy.start()

    for i in range(1, 8):
        gain_copy(i).wait_send()
    gsend, gparts, gsum = b["gsend"], b["gparts"], b["gsum"]
    for i in range(8):
        for n in range(4):
            lanes = slice(i * 256, i * 256 + 256)
            gsend[i, n : n + 1, :] = jnp.sum(b["pieces"][n, :, lanes], axis=0, keepdims=True)
            gsend[i, n + 4 : n + 5, :] = jnp.zeros((1, 256), F32)

    def share_copy(i):
        target = lax.rem(dp + i, 8)
        return remote(
            gsend.at[target], gparts.at[dp], b["gg_s"].at[i], b["gg_r"].at[dp], (target, tensor)
        )

    for i in range(1, 8):
        share_copy(i).start()
    @pl.when(outer)
    def _():
        hop(2, cot_ref, b["cot2"]).wait_send()
        hop(5, b["cot2"], b["cot2"]).wait_recv()

        def body(i):
            r = at(i, CHUNK)
            b["middle"][r] += b["cot2"][r].astype(F32)

        loop(rows // CHUNK, body)

    final_copy = pltpu.make_async_copy(b["middle"], final_out, b["ol"].at[1])
    final_copy.start()
    finish_gradient(OUTPUT)
    finish_gradient(VALUE)
    finish_gradient(QUERY)
    acc = gsend[dp]
    for i in range(1, 8):
        gain_arrival(i).wait_recv()
        acc = acc + gparts[lax.rem(dp + i, 8)]
    gsum[tensor] = acc

    def sum_copy(i, source):
        target = lax.rem(tensor + i, 4)
        return remote(
            gsum.at[source], gsum.at[source], b["gt_s"].at[i], b["gt_r"].at[source], (dp, target)
        )

    for i in range(1, 4):
        sum_copy(i, tensor).start()
    finish_gradient(KEY, last=True)
    for i in range(1, 4):
        sum_copy(i, lax.rem(tensor + i, 4)).wait_recv()
    for i in range(1, 4):
        sum_copy(i, tensor).wait_send()
    for i in range(1, 8):
        share_copy(i).wait_send()
    gains_out[...] = (gsum[0] + gsum[1]) + (gsum[2] + gsum[3])
    final_copy.wait()
    delta_copy.wait()
    weights_sent()

    @pl.when(inner)
    def _():
        for n in range(2):
            hop(3 + n, b["rows2"], b["rows2"], halves[n]).wait_send()
        hop(5, b["cot2"], b["cot2"]).wait_send()

    @pl.when(outer)
    def _():
        hop(6, b["gated"], b["gated2"]).wait_send()
        hop(7, low, b["cot2"]).wait_send()

    gradients_done()


def whole_layer(
    incoming_signals,
    loss_sensitivity,
    token_counts_per_slot,
    leading_norm_multiplier,
    leading_norm_offset,
    question_projection,
    lookup_projection,
    content_projection,
    silu_switch_projection,
    retention_result_projection,
    trailing_norm_multiplier,
    trailing_norm_offset,
    feedforward_switch_projection,
    expanding_projection,
    contracting_projection,
):
    rows, hidden = incoming_signals.shape
    places = np.arange(SEQ_LEN, dtype=np.float32)
    middle = KEY_DIM // 2
    spectrum = np.float32(10000.0) ** (-np.arange(middle, dtype=np.float32) / np.float32(middle))
    angles = places[:, None] * spectrum[None, :]
    weights = (
        question_projection,
        lookup_projection,
        content_projection,
        silu_switch_projection,
        retention_result_projection,
        feedforward_switch_projection,
        expanding_projection,
        contracting_projection,
    )
    gains = (
        leading_norm_multiplier, leading_norm_offset, trailing_norm_multiplier, trailing_norm_offset
    )
    tables = (jnp.asarray(np.cos(angles)), jnp.asarray(np.sin(angles)))
    args = (incoming_signals, loss_sensitivity, token_counts_per_slot, *tables, *gains, *weights)
    scratch = mega_scratch(rows, hidden)
    shape = jax.ShapeDtypeStruct
    outs = (
        shape((rows, hidden), F32),
        shape((rows, hidden), F32),
        shape((8, 256), F32),
        *(shape(weight.shape, BF16) for weight in weights),
        shape((7, PLANES, WIDE, WIDE), BF16),
        shape((7, PLANES, WIDE, WIDE), BF16),
        shape((7, 3, WIDE, WIDE), BF16),
        shape((8 * rows, hidden), BF16),
    )
    scalar = pl.BlockSpec(memory_space=pltpu.SMEM)
    results = pl.pallas_call(
        functools.partial(mega_kernel, tuple(scratch), len(args), len(outs)),
        out_shape=outs,
        in_specs=[ANY, ANY, scalar] + [VM] * 6 + [ANY] * 8,
        out_specs=tuple([ANY, ANY, VM] + [ANY] * 12),
        scratch_shapes=list(scratch.values()),
        compiler_params=pltpu.CompilerParams(
            collective_id=0, has_side_effects=True, vmem_limit_bytes=67043328
        ),
        name="whole_layer",
    )(*args)
    final_rows, delta, gain_sums = results[:3]
    owned = results[3:11]
    wide = pl.pallas_call(
        widen_kernel,
        out_shape=(
            shape((rows, hidden), BF16),
            shape((rows, hidden), F32),
            *(shape(weight.shape, F32) for weight in weights),
        ),
        in_specs=[scalar] + [ANY] * 10,
        out_specs=(ANY,) * 10,
        scratch_shapes=[
            pltpu.VMEM((rows, hidden), F32),
            pltpu.VMEM((rows, hidden), F32),
            pltpu.VMEM((rows, hidden), BF16),
            *(pltpu.VMEM(weight.shape, BF16) for weight in weights),
            *(pltpu.VMEM(weight.shape, F32) for weight in weights),
            pltpu.SemaphoreType.DMA((10,)),
            pltpu.SemaphoreType.DMA((10,)),
        ],
        compiler_params=pltpu.CompilerParams(vmem_limit_bytes=67043328),
        name="widen",
    )(token_counts_per_slot, final_rows, delta, *owned)
    query, key, value, swish, output, gate, up, down = wide[2:]
    return (
        wide[0],
        wide[1],
        gain_sums[0],
        gain_sums[1],
        query,
        key,
        value,
        swish,
        output,
        gain_sums[2],
        gain_sums[3],
        gate,
        up,
        down,
    )


def widen_kernel(counts_ref, *refs):
    sources, targets, scratch = refs[:10], refs[10:20], refs[20:]
    final, delta, low = scratch[:3]
    narrow, wide, (came, went) = scratch[3:11], scratch[11:19], scratch[19:]
    buffers = (final, delta, *narrow)
    loads = [
        pltpu.make_async_copy(source, buffer, came.at[i])
        for i, (source, buffer) in enumerate(zip(sources, buffers, strict=True))
    ]
    stores = [
        pltpu.make_async_copy(buffer, target, went.at[i])
        for i, (buffer, target) in enumerate(zip((low, delta, *wide), targets, strict=True))
    ]
    for load in loads:
        load.start()
    rows, hidden = final.shape
    tensor, count = lax.axis_index("tensor"), counts_ref[0]
    loads[0].wait()

    def body(i):
        r = at(i, CHUNK)
        row = lax.broadcasted_iota(jnp.int32, (CHUNK, hidden), 0) + (tensor * rows + i * CHUNK)
        low[r] = jnp.where(row < count, final[r], 0.0).astype(BF16)

    loop(rows // CHUNK, body)
    stores[0].start()
    loads[1].wait()
    stores[1].start()
    for n in range(8):
        loads[n + 2].wait()

        def body(i, n=n):
            r = at(i, 32)
            wide[n][r] = narrow[n][r].astype(F32)

        loop(narrow[n].shape[0] // 32, body)
        stores[n + 2].start()
    for store in stores:
        store.wait()


def solution(mesh):
    ranks = mesh.shape["dp"]
    groups = [[2 * k + side for k in range(ranks // 2)] for side in range(2)]
    swap = [(rank, rank + 1 - 2 * (rank % 2)) for rank in range(ranks)]
    rows, gain, column, row = P(("dp", "tensor"), None), P("dp"), P("dp", "tensor"), P("tensor", "dp")
    weights = (gain, gain, column, column, column, column, row, gain, gain, column, column, row)
    one_kernel = ranks == 8 and mesh.shape["tensor"] == 4
    return jax.shard_map(
        whole_layer if one_kernel else functools.partial(per_device, groups, swap),
        mesh=mesh,
        in_specs=(rows, rows, P("dp"), *weights),
        out_specs=(rows, rows, *weights),
        check_vma=False,
    )
```

```python
import functools

import jax
import jax.numpy as jnp
import numpy as np
from jax import lax
from jax.experimental import pallas as pl
from jax.experimental.pallas import tpu as pltpu
from jax.sharding import PartitionSpec as P

KEY_DIM = 256
VAL_DIM = 512
SEQ_LEN = 512

EPSILON = 1e-05
GROUP_EPSILON = 0.1

MESH = pl.DeviceIdType.MESH
F32 = jnp.float32
BF16 = jnp.bfloat16
CHUNK = 16


def normalize(values, epsilon):
    centre = values - jnp.mean(values, axis=-1, keepdims=True)
    inverse = lax.rsqrt(jnp.mean(centre * centre, axis=-1, keepdims=True) + epsilon)
    return (centre * inverse, inverse)


def normalize_back(upstream, normed, inverse):
    return inverse * (
        upstream
        - jnp.mean(upstream, axis=-1, keepdims=True)
        - normed * jnp.mean(upstream * normed, axis=-1, keepdims=True)
    )


def rotate_half(values):
    middle = values.shape[-1] // 2
    return jnp.concatenate([-values[..., middle:], values[..., :middle]], axis=-1)


def rotary_tables(span, columns):
    middle = columns // 2
    places = jnp.arange(span, dtype=jnp.int32).astype(jnp.float32)
    spectrum = 10000.0 ** (-jnp.arange(middle, dtype=jnp.int32).astype(jnp.float32) / middle)
    angles = places[:, None] * spectrum[None, :]
    angles = jnp.concatenate([angles, angles], axis=1)
    return (jnp.cos(angles)[None], jnp.sin(angles)[None])


def decay_table(span, head_id):
    log_rate = jnp.log(1.0 - jnp.exp2(-5.0 - head_id.astype(jnp.float32)))
    places = jnp.arange(span, dtype=jnp.int32)
    offsets = places[:, None] - places[None, :]
    decayed = jnp.exp(jnp.maximum(offsets, 0).astype(jnp.float32) * log_rate)
    return jnp.where(offsets >= 0, decayed, 0.0)


def gelu_tanh(values):
    return jax.nn.gelu(values, approximate=True)


def matmul(left, right):
    return jnp.dot(left, right, preferred_element_type=jnp.float32)


class Place:
    def __init__(self):
        d, t = lax.axis_index("dp"), lax.axis_index("tensor")
        self.x, self.y, self.c = lax.rem(d, 2), t // 2, lax.rem(t, 2)
        dx, ty = d + 1 - 2 * self.x, (1 - self.y) * 2 + self.c
        self.sib = (d, t + 1 - 2 * self.c)
        self.xn = (dx, t)
        self.yn = (d, ty)

    def block(self, j, other_core=0):
        x = 1 - self.x if j in (1, 3) else self.x
        y = 1 - self.y if j in (2, 3) else self.y
        c = 1 - self.c if other_core else self.c
        return x * 4 + y * 2 + c


def greet(place):
    barrier = pltpu.get_barrier_semaphore()
    for partner in (place.sib, place.xn, place.yn):
        pl.semaphore_signal(barrier, inc=1, device_id=partner, device_id_type=MESH)
    pl.semaphore_wait(barrier, 3)


def rows_of(index, rows):
    return pl.ds(pl.multiple_of(index * rows, rows), rows)


class Gather:
    @staticmethod
    def scratch():
        return [pltpu.SemaphoreType.DMA((13,)), pltpu.SemaphoreType.DMA((13,))]

    def __init__(self, place, src, out, send, recv):
        rows = src.shape[0]
        half = rows // 2
        p = place

        def remote(k, source, j, lo, n, target, core=0):
            where = pl.ds(pl.multiple_of(p.block(j, core) * rows + lo, 8), n)
            source = source.at[pl.ds(lo, n)] if source is src else source.at[where]
            return pltpu.make_async_remote_copy(
                src_ref=source,
                dst_ref=out.at[where],
                send_sem=send.at[k],
                recv_sem=recv.at[k],
                device_id=target,
                device_id_type=MESH,
            )

        self.p, self.rows, self.half = p, rows, half
        self.local = pltpu.make_async_copy(src, out.at[rows_of(p.block(0), rows)], send.at[12])
        h = half
        self.xa = remote(0, src, 0, 0, h, p.xn)
        self.xb = remote(1, src, 0, h, h, p.xn)
        self.ya = remote(2, src, 0, 0, h, p.yn)
        self.yb = remote(3, src, 0, h, h, p.yn)
        self.s0 = remote(4, src, 0, 0, rows, p.sib)
        self.da = remote(5, out, 1, 0, h, p.yn)
        self.db = remote(6, out, 2, h, h, p.xn)
        self.s1 = remote(7, out, 1, 0, rows, p.sib)
        self.s2 = remote(8, out, 2, 0, rows, p.sib)
        self.s3a = remote(9, out, 3, 0, h, p.sib)
        self.s3b = remote(10, out, 3, h, h, p.sib)

    def start(self):
        for copy in (self.xa, self.yb, self.xb, self.ya, self.s0, self.local):
            copy.start()

    def start_first_half(self):
        self.xa.start()
        self.ya.start()

    def start_second_half(self):
        for copy in (self.yb, self.xb, self.s0, self.local):
            copy.start()

    def forward(self):
        self.forward_across()
        self.forward_beside()

    def forward_across(self):
        self.xa.wait_recv()
        self.da.start()
        self.yb.wait_recv()
        self.db.start()

    def forward_beside(self):
        self.xb.wait_recv()
        self.s1.start()
        self.ya.wait_recv()
        self.s2.start()

    def own_arrived(self):
        self.local.wait()
        self.s0.wait_recv()

    def across_arrived(self):
        self.da.wait_recv()
        self.s3a.start()
        self.db.wait_recv()
        self.s3b.start()
        self.s3a.wait_recv()
        self.s3b.wait_recv()

    def drain(self):
        for copy in (self.s0, self.s1, self.s2, self.s3a, self.s3b):
            copy.wait_send()
        for copy in (self.xa, self.xb, self.ya, self.yb, self.da, self.db):
            copy.wait_send()

    def finish(self):
        self.da.wait_recv()
        self.s3a.start()
        self.db.wait_recv()
        self.s3b.start()
        self.local.wait()
        for copy in (self.s0, self.s1, self.s2, self.s3a, self.s3b):
            copy.wait()
        for copy in (self.xa, self.xb, self.ya, self.yb, self.da, self.db):
            copy.wait_send()


class Reduce:
    @staticmethod
    def scratch(rows, columns):
        return [
            pltpu.VMEM((4, rows, columns), BF16),
            pltpu.VMEM((4, rows, columns), BF16),
            pltpu.VMEM((2, rows, columns), BF16),
            pltpu.VMEM((2, rows // 2, columns), BF16),
            pltpu.SemaphoreType.DMA((14,)),
            pltpu.SemaphoreType.DMA((10,)),
        ]

    def __init__(self, place, part, mine, theirs, got, across, send, recv):
        p = place
        rows = mine.shape[1]
        h = rows // 2
        self.rows, self.half = rows, h
        self.mine, self.theirs, self.got, self.across = mine, theirs, got, across

        def remote(k, source, target_ref, target):
            return pltpu.make_async_remote_copy(
                src_ref=source,
                dst_ref=target_ref,
                send_sem=send.at[k],
                recv_sem=recv.at[k],
                device_id=target,
                device_id_type=MESH,
            )

        a, b = pl.ds(0, h), pl.ds(h, h)
        self.load = [
            pltpu.make_async_copy(part.at[rows_of(p.block(j), rows)], mine.at[j], send.at[10 + j])
            for j in range(4)
        ]
        self.swap = [
            remote(j, part.at[rows_of(p.block(j, 1), rows)], theirs.at[j], p.sib) for j in range(4)
        ]
        self.da = remote(4, mine.at[3, a], across.at[0], p.xn)
        self.db = remote(5, mine.at[3, b], across.at[1], p.yn)
        self.xa = remote(6, mine.at[1, a], got.at[0, a], p.xn)
        self.xb = remote(7, mine.at[1, b], got.at[0, b], p.xn)
        self.ya = remote(8, mine.at[2, a], got.at[1, a], p.yn)
        self.yb = remote(9, mine.at[2, b], got.at[1, b], p.yn)

    def add(self, j, lo, n, other, other_lo):
        def body(i, carry):
            r = pl.ds(pl.multiple_of(lo + i * CHUNK, CHUNK), CHUNK)
            q = pl.ds(pl.multiple_of(other_lo + i * CHUNK, CHUNK), CHUNK)
            self.mine[j, r] = (self.mine[j, r].astype(F32) + other[q].astype(F32)).astype(BF16)
            return carry

        lax.fori_loop(0, n // CHUNK, body, 0)

    def start(self):
        for j in (3, 1, 2, 0):
            self.swap[j].start()
            self.load[j].start()

    def run(self):
        rows, h = self.rows, self.half
        for j, copies in ((3, (self.da, self.db)), (1, (self.xa,)), (2, (self.yb,))):
            self.load[j].wait()
            self.swap[j].wait_recv()
            self.add(j, 0, rows, self.theirs.at[j], 0)
            for copy in copies:
                copy.start()
        self.db.wait_recv()
        self.add(1, h, h, self.across.at[1], 0)
        self.xb.start()
        self.da.wait_recv()
        self.add(2, 0, h, self.across.at[0], 0)
        self.ya.start()
        self.load[0].wait()
        self.swap[0].wait_recv()
        for copy in (self.xa, self.yb, self.xb, self.ya):
            copy.wait_recv()

    def total(self, r):
        pieces = (self.mine[0, r], self.theirs[0, r], self.got[0, r], self.got[1, r])
        one, two, three, four = (piece.astype(F32) for piece in pieces)
        return (one + two) + (three + four)

    def finish(self):
        for copy in (*self.swap, self.da, self.db, self.xa, self.xb, self.ya, self.yb):
            copy.wait_send()


def chunks(rows, body):
    def step(i, carry):
        body(pl.ds(pl.multiple_of(i * CHUNK, CHUNK), CHUNK))
        return carry

    lax.fori_loop(0, rows // CHUNK, step, 0)


def first_kernel(x_ref, cot_ref, gains_ref, out_x, out_cot, normed, *sems):
    place = Place()
    greet(place)
    gain, shift = gains_ref[0:1, :], gains_ref[1:2, :]

    def body(r):
        hat, _ = normalize(x_ref[r].astype(F32), EPSILON)
        normed[r] = (hat * gain + shift).astype(BF16)

    chunks(x_ref.shape[0], body)
    one = Gather(place, normed, out_x, *sems[:2])
    two = Gather(place, cot_ref, out_cot, *sems[2:])
    one.start()
    two.start()
    one.forward()
    two.forward()
    one.finish()
    two.finish()


def second_kernel(part_ref, x_ref, gains_ref, out_all, middle_ref, normed, *scratch):
    place = Place()
    greet(place)
    reduce = Reduce(place, part_ref, *scratch[:6])
    reduce.start()
    reduce.run()
    gain, shift = gains_ref[2:3, :], gains_ref[3:4, :]

    def body(r):
        middle = x_ref[r].astype(F32) + reduce.total(r)
        middle_ref[r] = middle
        hat, _ = normalize(middle, EPSILON)
        normed[r] = (hat * gain + shift).astype(BF16)

    chunks(x_ref.shape[0], body)
    gather = Gather(place, normed, out_all, *scratch[6:])
    gather.start()
    gather.forward()
    gather.finish()
    reduce.finish()


def third_kernel(
    part_ref, middle_ref, cot_ref, gains_ref, out_all, back_ref, pieces_ref, low, *scratch
):
    place = Place()
    greet(place)
    reduce = Reduce(place, part_ref, *scratch[:6])
    reduce.start()
    pieces_ref[...] = jnp.zeros_like(pieces_ref)
    reduce.run()
    gain = gains_ref[2:3, :]

    def body(r):
        upstream = reduce.total(r)
        hat, inverse = normalize(middle_ref[r], EPSILON)
        scaled = upstream * hat
        pieces_ref[0] += scaled[0:8] + scaled[8:16]
        pieces_ref[1] += upstream[0:8] + upstream[8:16]
        back = cot_ref[r].astype(F32) + normalize_back(upstream * gain, hat, inverse)
        back_ref[r] = back
        low[r] = back.astype(BF16)

    chunks(middle_ref.shape[0], body)
    gather = Gather(place, low, out_all, *scratch[6:])
    gather.start()
    gather.forward()
    gather.finish()
    reduce.finish()


def fourth_kernel(
    first_ref, mixer_ref, x_ref, middle_ref, gains_ref, delta_ref, final_ref, pieces_ref, *scratch
):
    place = Place()
    greet(place)
    one = Reduce(place, first_ref, *scratch[:6])
    two = Reduce(place, mixer_ref, *scratch[6:])
    one.start()
    two.start()
    pieces_ref[...] = jnp.zeros_like(pieces_ref)
    one.run()
    two.run()
    gain = gains_ref[0:1, :]

    def body(r):
        upstream = one.total(r)
        hat, inverse = normalize(x_ref[r].astype(F32), EPSILON)
        scaled = upstream * hat
        pieces_ref[0] += scaled[0:8] + scaled[8:16]
        pieces_ref[1] += upstream[0:8] + upstream[8:16]
        delta_ref[r] = normalize_back(upstream * gain, hat, inverse)
        final_ref[r] = middle_ref[r] + two.total(r)

    chunks(x_ref.shape[0], body)
    one.finish()
    two.finish()


ANY = pl.BlockSpec(memory_space=pl.ANY)
VM = pl.BlockSpec(memory_space=pltpu.VMEM)


def call(kernel, ident, args, specs, outs, out_specs, scratch, nbytes):
    return pl.pallas_call(
        kernel,
        out_shape=outs,
        in_specs=specs,
        out_specs=out_specs,
        scratch_shapes=scratch,
        compiler_params=pltpu.CompilerParams(
            collective_id=ident, has_side_effects=True, vmem_limit_bytes=32 << 20
        ),
        cost_estimate=pl.CostEstimate(flops=0, bytes_accessed=nbytes, transcendentals=0),
        name=kernel.__name__,
    )(*args)


def per_device(
    groups,
    swap,
    incoming_signals,
    loss_sensitivity,
    token_counts_per_slot,
    leading_norm_multiplier,
    leading_norm_offset,
    question_projection,
    lookup_projection,
    content_projection,
    silu_switch_projection,
    retention_result_projection,
    trailing_norm_multiplier,
    trailing_norm_offset,
    feedforward_switch_projection,
    expanding_projection,
    contracting_projection,
):
    local_rows, hidden_size = incoming_signals.shape
    total_rows = 8 * local_rows
    slots_here = token_counts_per_slot.shape[0]
    dp_rank, tensor_rank = lax.axis_index("dp"), lax.axis_index("tensor")
    side = lax.rem(dp_rank, 2)
    row_ids = tensor_rank * local_rows + jnp.arange(local_rows, dtype=jnp.int32)
    slot_match = (row_ids // SEQ_LEN)[:, None] == jnp.arange(slots_here, dtype=jnp.int32)[None, :]
    row_lengths = jnp.sum(jnp.where(slot_match, token_counts_per_slot[None, :], 0), axis=1)
    valid_rows = (row_ids % SEQ_LEN < row_lengths)[:, None]

    def exchange(weight, axis, join):
        half = weight.shape[axis] // 2
        keep = lax.dynamic_slice_in_dim(weight, side * half, half, axis)
        give = lax.dynamic_slice_in_dim(weight, (1 - side) * half, half, axis)
        take = lax.ppermute(give, "dp", swap)
        return jnp.where(
            side == 0,
            jnp.concatenate([keep, take], axis=join),
            jnp.concatenate([take, keep], axis=join),
        )

    def spread(block, axis):
        return lax.all_gather(block, "dp", axis=axis, tiled=True, axis_index_groups=groups)

    query_half = exchange(question_projection, 1, 0)
    key_half = exchange(lookup_projection, 1, 0)
    query_key = spread(jnp.concatenate([query_half, key_half], axis=1), 0)
    value_full = spread(exchange(content_projection, 1, 0), 0)
    swish_full = spread(exchange(silu_switch_projection, 1, 0), 0)
    output_full = spread(exchange(retention_result_projection, 0, 1), 1)
    gate_full = spread(exchange(feedforward_switch_projection, 1, 0), 0)
    up_full = spread(exchange(expanding_projection, 1, 0), 0)
    down_full = spread(exchange(contracting_projection, 0, 1), 1)

    gains = jnp.stack(
        [leading_norm_multiplier, leading_norm_offset, trailing_norm_multiplier, trailing_norm_offset]
    )
    gains = lax.all_gather(gains, "dp", axis=1, tiled=True).astype(F32)
    gains = jnp.concatenate([gains, gains], axis=0)

    all_rows = jax.ShapeDtypeStruct((total_rows, hidden_size), BF16)
    own_rows = jax.ShapeDtypeStruct((local_rows, hidden_size), F32)
    pieces = jax.ShapeDtypeStruct((2, 8, hidden_size), F32)
    row_low = pltpu.VMEM((local_rows, hidden_size), BF16)
    reduce_scratch = Reduce.scratch(local_rows, hidden_size)
    moved = total_rows * hidden_size * 2

    out_low = jnp.where(valid_rows, loss_sensitivity, 0)
    normed_all, out_all = call(
        first_kernel,
        0,
        (incoming_signals, out_low, gains),
        [VM, VM, VM],
        (all_rows, all_rows),
        (ANY, ANY),
        [row_low, *Gather.scratch(), *Gather.scratch()],
        24 * moved,
    )

    slot_count = total_rows // SEQ_LEN
    shape_key = (slot_count, SEQ_LEN, KEY_DIM)
    shape_value = (slot_count, SEQ_LEN, VAL_DIM)
    query_key_proj = matmul(normed_all, query_key)
    query_proj = query_key_proj[:, :KEY_DIM].reshape(shape_key)
    key_proj = query_key_proj[:, KEY_DIM:].reshape(shape_key)
    value_heads = matmul(normed_all, value_full).reshape(shape_value).astype(BF16)
    swish_heads = matmul(normed_all, swish_full).reshape(shape_value)
    cosines, sines = rotary_tables(SEQ_LEN, KEY_DIM)
    decays = decay_table(SEQ_LEN, tensor_rank * 2 + side)
    query_rot = (query_proj * cosines + rotate_half(query_proj) * sines).astype(BF16)
    key_rot = ((key_proj * cosines + rotate_half(key_proj) * sines) * KEY_DIM ** (-0.5)).astype(BF16)
    scores = (
        jnp.einsum("snk,smk->snm", query_rot, key_rot, preferred_element_type=F32) * decays[None]
    ).astype(BF16)
    retained = jnp.einsum("snm,smv->snv", scores, value_heads, preferred_element_type=F32)
    group_hat, group_inverse = normalize(retained, GROUP_EPSILON)
    sigmoid_gate = jax.nn.sigmoid(swish_heads)
    gated = (swish_heads * sigmoid_gate * group_hat).reshape(total_rows, VAL_DIM).astype(BF16)
    retention_part = matmul(gated, output_full).astype(BF16)

    mixer_all, middle_rows = call(
        second_kernel,
        1,
        (retention_part, incoming_signals, gains),
        [ANY, VM, VM],
        (all_rows, own_rows),
        (ANY, VM),
        [row_low, *reduce_scratch, *Gather.scratch()],
        24 * moved,
    )

    gate_proj = matmul(mixer_all, gate_full)
    up_proj = matmul(mixer_all, up_full)
    gelu_gate, gelu_back = jax.vjp(gelu_tanh, gate_proj)
    hidden = (gelu_gate * up_proj).astype(BF16)
    down_gradient = matmul(hidden.T, out_all).astype(BF16)
    hidden_back = matmul(out_all, down_full.T)
    gate_back = gelu_back(hidden_back * up_proj)[0].astype(BF16)
    up_back = (hidden_back * gelu_gate).astype(BF16)
    gate_gradient = matmul(mixer_all.T, gate_back).astype(BF16)
    up_gradient = matmul(mixer_all.T, up_back).astype(BF16)
    mixer_input_part = (matmul(gate_back, gate_full.T) + matmul(up_back, up_full.T)).astype(BF16)
    mixer_part = matmul(hidden, down_full).astype(BF16)

    middle_all, middle_back, after_pieces = call(
        third_kernel,
        2,
        (mixer_input_part, middle_rows, out_low, gains),
        [ANY, VM, VM, VM],
        (all_rows, own_rows, pieces),
        (ANY, VM, VM),
        [row_low, *reduce_scratch, *Gather.scratch()],
        24 * moved,
    )

    output_gradient = matmul(gated.T, middle_all).astype(BF16)
    gated_back = matmul(middle_all, output_full.T).reshape(shape_value)
    swish_back = (
        (gated_back * group_hat * sigmoid_gate * (1.0 + swish_heads * (1.0 - sigmoid_gate)))
        .reshape(total_rows, VAL_DIM)
        .astype(BF16)
    )
    retained_back = normalize_back(
        gated_back * swish_heads * sigmoid_gate, group_hat, group_inverse
    ).astype(BF16)
    score_back = (
        jnp.einsum("snv,smv->snm", retained_back, value_heads, preferred_element_type=F32)
        * decays[None]
    ).astype(BF16)
    query_rot_back = jnp.einsum("snm,smk->snk", score_back, key_rot, preferred_element_type=F32)
    key_rot_back = jnp.einsum("snm,snk->smk", score_back, query_rot, preferred_element_type=F32)
    value_back = jnp.einsum("snm,snv->smv", scores, retained_back, preferred_element_type=F32)
    query_back = (
        (query_rot_back * cosines - rotate_half(query_rot_back) * sines)
        .reshape(total_rows, KEY_DIM)
        .astype(BF16)
    )
    key_back = (
        ((key_rot_back * cosines - rotate_half(key_rot_back) * sines) * KEY_DIM ** (-0.5))
        .reshape(total_rows, KEY_DIM)
        .astype(BF16)
    )
    value_low = value_back.reshape(total_rows, VAL_DIM).astype(BF16)
    swish_gradient = matmul(normed_all.T, swish_back).astype(BF16)
    value_gradient = matmul(normed_all.T, value_low).astype(BF16)
    query_key_back = jnp.concatenate([query_back, key_back], axis=1)
    query_key_gradient = matmul(normed_all.T, query_key_back).astype(BF16)
    first_part = (
        matmul(query_key_back, query_key.T)
        + matmul(value_low, value_full.T)
        + matmul(swish_back, swish_full.T)
    ).astype(BF16)

    delta, final_rows, before_pieces = call(
        fourth_kernel,
        3,
        (first_part, mixer_part, incoming_signals, middle_rows, gains),
        [ANY, ANY, VM, VM, VM],
        (own_rows, own_rows, pieces),
        (VM, VM, VM),
        [*reduce_scratch, *reduce_scratch],
        24 * moved,
    )
    layer_output = jnp.where(valid_rows, final_rows, 0.0).astype(BF16)
    input_delta = middle_back + delta

    gain_pieces = jnp.concatenate(
        [jnp.sum(before_pieces, axis=1), jnp.sum(after_pieces, axis=1)], axis=0
    )
    gain_sums = lax.psum(gain_pieces, ("dp", "tensor"))
    width = leading_norm_multiplier.shape[0]
    gain_sums = lax.dynamic_slice_in_dim(gain_sums, dp_rank * width, width, 1)

    def collect(gradient, axis):
        return lax.psum_scatter(
            gradient, "dp", scatter_dimension=axis, tiled=True, axis_index_groups=groups
        )

    def restore(block, axis, join):
        half = block.shape[axis] // 2
        keep = lax.dynamic_slice_in_dim(block, side * half, half, axis)
        give = lax.dynamic_slice_in_dim(block, (1 - side) * half, half, axis)
        take = lax.ppermute(give, "dp", swap)
        return jnp.where(
            side == 0,
            jnp.concatenate([keep, take], axis=join),
            jnp.concatenate([take, keep], axis=join),
        ).astype(F32)

    down_owned = restore(collect(down_gradient, 1), 1, 0)
    gate_owned = restore(collect(gate_gradient, 0), 0, 1)
    up_owned = restore(collect(up_gradient, 0), 0, 1)
    output_owned = restore(collect(output_gradient, 1), 1, 0)
    swish_owned = restore(collect(swish_gradient, 0), 0, 1)
    value_owned = restore(collect(value_gradient, 0), 0, 1)
    query_key_owned = collect(query_key_gradient, 0)
    query_owned = restore(query_key_owned[:, :KEY_DIM], 0, 1)
    key_owned = restore(query_key_owned[:, KEY_DIM:], 0, 1)
    return (
        layer_output,
        input_delta,
        gain_sums[0],
        gain_sums[1],
        query_owned,
        key_owned,
        value_owned,
        swish_owned,
        output_owned,
        gain_sums[2],
        gain_sums[3],
        gate_owned,
        up_owned,
        down_owned,
    )


PLANES = 4
QK, VALUE, SWISH, OUTPUT, GATE, UP, DOWN = range(7)
WIDE = 512
QUERY, KEY = 7, 8
FEED_FORWARD = (DOWN, GATE, UP)
INNER_SUMS = (*FEED_FORWARD, OUTPUT)
GRADIENTS = (*FEED_FORWARD, OUTPUT, SWISH, VALUE, QUERY, KEY)
TILE = 256


def nt(left, right):
    return lax.dot_general(left, right, (((1,), (1,)), ((), ())), preferred_element_type=F32)


def loop(count, body):
    def step(i, carry):
        body(i)
        return carry

    lax.fori_loop(0, count, step, 0)


def together(*steps):
    for step in steps:
        step()


def at(index, size):
    return pl.ds(pl.multiple_of(index * size, size), size)


def mega_scratch(rows, hidden):
    total = 8 * rows
    dma = pltpu.SemaphoreType.DMA
    return dict(
        w=pltpu.VMEM((7, hidden, WIDE), BF16),
        xs=pltpu.VMEM((total, hidden), BF16),
        xt=pltpu.VMEM((total, hidden), BF16),
        outs=pltpu.VMEM((total, hidden), BF16),
        part=pltpu.VMEM((total, hidden), BF16),
        room=pltpu.VMEM((7 * rows, hidden), BF16),
        q=pltpu.VMEM((total, KEY_DIM), BF16),
        k=pltpu.VMEM((total, KEY_DIM), BF16),
        v=pltpu.VMEM((total, VAL_DIM), BF16),
        sc=pltpu.VMEM((total, SEQ_LEN), BF16),
        swish=pltpu.VMEM((total, VAL_DIM), F32),
        ghat=pltpu.VMEM((total, VAL_DIM), F32),
        ginv=pltpu.VMEM((total, 128), F32),
        gated=pltpu.VMEM((total, VAL_DIM), BF16),
        hid=pltpu.VMEM((total, WIDE), BF16),
        gate=pltpu.VMEM((TILE, WIDE), F32),
        up=pltpu.VMEM((TILE, WIDE), F32),
        gb=pltpu.VMEM((total, WIDE), BF16),
        ub=pltpu.VMEM((total, WIDE), BF16),
        sb=pltpu.VMEM((total, SEQ_LEN), BF16),
        qkb=pltpu.VMEM((total, 2 * KEY_DIM), BF16),
        turned=pltpu.VMEM((WIDE, total), BF16),
        st=pltpu.VMEM((4, WIDE, WIDE), BF16),
        decay=pltpu.VMEM((SEQ_LEN, SEQ_LEN), F32),
        low=pltpu.VMEM((rows, hidden), BF16),
        middle=pltpu.VMEM((rows, hidden), F32),
        back=pltpu.VMEM((rows, hidden), F32),
        pieces=pltpu.VMEM((4, 8, hidden), F32),
        gparts=pltpu.VMEM((8, 8, 256), F32),
        gain=pltpu.VMEM((8, hidden), F32),
        gsend=pltpu.VMEM((8, 8, 256), F32),
        gsum=pltpu.VMEM((4, 8, 256), F32),
        xr=pltpu.VMEM((rows, hidden), BF16),
        cr=pltpu.VMEM((rows, hidden), BF16),
        rows2=pltpu.VMEM((rows, hidden), BF16),
        cot2=pltpu.VMEM((rows, hidden), BF16),
        ub2=pltpu.VMEM((total, WIDE), BF16),
        gated2=pltpu.VMEM((total, VAL_DIM), BF16),
        hop_s=dma((9,)),
        hop_r=dma((9,)),
        gd_s=dma((13,)),
        gd_r=dma((13,)),
        gown=pltpu.VMEM((8, 256), F32),
        ex_s=dma((8,)),
        ex_r=dma((8,)),
        ex_l=dma((8,)),
        zs=dma((7, 2, 4)),
        zr=dma((7, 2, 4)),
        rs=dma((8, 3)),
        rr=dma((8, 4)),
        ra=dma((8, 3)),
        stl=dma((4,)),
        fl=dma((4,)),
        fe_s=dma((8,)),
        fe_r=dma((8,)),
        gg_s=dma((8,)),
        gg_r=dma((8,)),
        gt_s=dma((4,)),
        gt_r=dma((4,)),
        ga_s=dma((13,)),
        ga_r=dma((13,)),
        gc_s=dma((13,)),
        gc_r=dma((13,)),
        re_s=dma((10,)),
        re_r=dma((10,)),
        rf_s=dma((10,)),
        rf_r=dma((10,)),
        ol=dma((6,)),
        free=pltpu.SemaphoreType.REGULAR,
    )


class PlaneSum(Reduce):
    def __init__(self, place, part, room, rows, send, recv, y_first=False):
        p = place
        h = rows // 2
        self.rows, self.half, self.part, self.room, self.y_first = rows, h, part, room, y_first
        self.base = [p.block(j) * rows for j in range(4)]

        def remote(k, source, target_ref, target):
            return pltpu.make_async_remote_copy(
                src_ref=source,
                dst_ref=target_ref,
                send_sem=send.at[k],
                recv_sem=recv.at[k],
                device_id=target,
                device_id_type=MESH,
            )

        def piece(j, lo):
            return part.at[pl.ds(pl.multiple_of(self.base[j] + lo, 8), h)]

        def got(k, lo):
            return room.at[pl.ds((4 + k) * rows + lo, h)]

        def across(k):
            return room.at[pl.ds(6 * rows + k * h, h)]

        self.place, self.remote = p, remote
        self.swap = [
            remote(j, part.at[rows_of(p.block(j, 1), rows)], self.theirs(j), p.sib) for j in range(4)
        ]
        self.da = remote(4, piece(3, 0), across(0), p.yn if y_first else p.xn)
        self.db = remote(5, piece(3, h), across(1), p.yn)
        self.xa = remote(6, piece(1, 0), got(0, 0), p.xn)
        self.xb = remote(7, piece(1, h), got(0, h), p.xn)
        self.ya = remote(8, piece(2, 0), got(1, 0), p.yn)
        self.yb = remote(9, piece(2, h), got(1, h), p.yn)

    def theirs(self, j):
        return self.room.at[rows_of(j, self.rows)]

    def add(self, j, lo, n, first):
        def body(i):
            r = pl.ds(pl.multiple_of(self.base[j] + lo + i * CHUNK, CHUNK), CHUNK)
            q = pl.ds(pl.multiple_of(first + i * CHUNK, CHUNK), CHUNK)
            self.part[r] = (self.part[r].astype(F32) + self.room[q].astype(F32)).astype(BF16)

        loop(n // CHUNK, body)

    def start(self):
        for j in (3, 1, 2, 0):
            self.swap[j].start()

    def fill(self, tile_value, sending=None):
        def body(i):
            self.fill_chip(jnp.where(i == 0, 3, jnp.where(i == 3, 0, i)), tile_value, sending)

        loop(4, body)

    def chip(self, j):
        p = self.place
        chip_x = jnp.where(lax.rem(j, 2) == 1, 1 - p.x, p.x)
        chip_y = jnp.where(j >= 2, 1 - p.y, p.y)
        return chip_x * 2 + chip_y

    def fill_chip(self, j, tile_value, sending=None):
        chip = self.chip(j)
        r = at(chip, 2 * self.rows)

        def inner(n):
            c = at(n, WIDE)
            self.part[r, c] = tile_value(r, c).astype(BF16)

        loop(self.part.shape[1] // WIDE, inner)
        source = self.part.at[rows_of(chip * 2 + 1 - self.place.c, self.rows)]
        send = self.remote(j, source, self.theirs(j), self.place.sib)
        if sending is None:
            send.start()
        else:
            pl.when(sending)(send.start)

    def take(self, j):
        if self.y_first:
            copies = {3: (self.da, self.db), 1: (), 2: (self.ya, self.yb)}[j]
        else:
            copies = {3: (self.da, self.db), 1: (self.xa,), 2: (self.yb,)}[j]
        self.swap[j].wait_recv()
        self.add(j, 0, self.rows, j * self.rows)
        for copy in copies:
            copy.start()

    def run1(self):
        for j in (3, 1, 2):
            self.take(j)

    def run2(self):
        h, across = self.half, 6 * self.rows
        if self.y_first:
            self.da.wait_recv()
            self.add(1, 0, h, across)
            self.xa.start()
            self.db.wait_recv()
            self.add(1, h, h, across + h)
            self.xb.start()
            return
        self.db.wait_recv()
        self.add(1, h, h, across + h)
        self.xb.start()
        self.da.wait_recv()
        self.add(2, 0, h, across)
        self.ya.start()

    def run3(self):
        self.swap[0].wait_recv()
        for copy in (self.xa, self.yb, self.xb, self.ya):
            copy.wait_recv()

    def run(self):
        self.run1()
        self.run2()
        self.run3()

    def total(self, i):
        def at_row(first):
            return pl.ds(pl.multiple_of(first + i * CHUNK, CHUNK), CHUNK)

        n = self.rows
        pieces = (self.part[at_row(self.base[0])], *(self.room[at_row(k * n)] for k in (0, 4, 5)))
        one, two, three, four = (piece.astype(F32) for piece in pieces)
        return (one + two) + (three + four)


def mega_kernel(names, count_in, count_out, *refs):
    x_hbm, cot_hbm, counts_ref, cos_ref, sin_ref = refs[:5]
    gain_refs = refs[5:9]
    q_w, k_w, v_w, s_w, o_w, g_w, u_w, d_w = refs[9:count_in]
    outs = refs[count_in : count_in + count_out]
    final_out, delta_out, gains_out, q_g, k_g, v_g, s_g, o_g, g_g, u_g, d_g, stage, heard, added, parked = outs
    b = {name: ref for name, ref in zip(names, refs[count_in + count_out :], strict=True)}
    w, xs, xt, st, part, turned = b["w"], b["xs"], b["xt"], b["st"], b["part"], b["turned"]
    x_ref, cot_ref = b["xr"], b["cr"]
    rows, hidden = x_ref.shape
    width = hidden // 8

    dp, tensor = lax.axis_index("dp"), lax.axis_index("tensor")
    place = Place()
    x, z = place.x, dp // 2
    first_plane, inner = z == 0, (z == 1) | (z == 2)
    outer = jnp.logical_not(inner)

    barrier = pltpu.get_barrier_semaphore()
    for i in range(1, 8):
        other = (lax.rem(dp + i, 8), tensor)
        pl.semaphore_signal(barrier, inc=1, device_id=other, device_id_type=MESH)
    for i in range(1, 4):
        other = (dp, lax.rem(tensor + i, 4))
        pl.semaphore_signal(barrier, inc=1, device_id=other, device_id_type=MESH)

    def remote(source, target_ref, send, recv, target):
        return pltpu.make_async_remote_copy(
            src_ref=source,
            dst_ref=target_ref,
            send_sem=send,
            recv_sem=recv,
            device_id=target,
            device_id_type=MESH,
        )

    def plane(step):
        return ((z + step) * 2 + x, tensor)

    def column_exchange(n, weight, k, lane, half):
        where = w.at[k, pl.ds(pl.multiple_of(z * 512 + x * 256, 256), width), pl.ds(lane, half)]
        keep = pltpu.make_async_copy(weight.at[:, at(x, half)], where, b["ex_l"].at[n])
        give = remote(
            weight.at[:, at(1 - x, half)], where, b["ex_s"].at[n], b["ex_r"].at[n], place.xn
        )
        return keep, give

    def row_exchange(n, weight, k):
        where = w.at[k, at(z, 512), at(x, width)]
        keep = pltpu.make_async_copy(weight.at[at(x, 512)], where, b["ex_l"].at[n])
        give = remote(weight.at[at(1 - x, 512)], where, b["ex_s"].at[n], b["ex_r"].at[n], place.xn)
        return keep, give

    exchanges = [
        [column_exchange(0, q_w, QK, 0, 256), column_exchange(1, k_w, QK, 256, 256)],
        [column_exchange(2, v_w, VALUE, 0, 512)],
        [column_exchange(3, s_w, SWISH, 0, 512)],
        [row_exchange(4, o_w, OUTPUT)],
        [column_exchange(5, g_w, GATE, 0, 512)],
        [column_exchange(6, u_w, UP, 0, 512)],
        [row_exchange(7, d_w, DOWN)],
    ]

    def keep(k):
        for local, _ in exchanges[k]:
            local.start()

    def give(k):
        for _, send in exchanges[k]:
            send.start()

    towards = jnp.where(z == 1, -1, 1)
    near, far = jnp.where(z == 1, 2, 1), jnp.where(z == 1, 3, 0)
    own_steps = (
        jnp.where(first_plane, 2, jnp.where(inner, 1, -2)),
        jnp.where(first_plane, 1, -1),
    )
    beside = place.xn

    def parts(k):
        return (0, 1) if k == QK else (0,)

    def block_copy(k, block, half, slot, target):
        if k == QK:
            side = x if half == 0 else 1 - x
            ref = w.at[k, pl.ds(pl.multiple_of(block * 512 + side * 256, 256), 256)]
        else:
            ref = w.at[k, at(block, 512)]
        return remote(ref, ref, b["zs"].at[k, half, slot], b["zr"].at[k, half, block], target)

    def kept(k):
        for local, _ in exchanges[k]:
            local.wait()

    def swapped(k):
        for _, send in exchanges[k]:
            send.wait_recv()

    def spread_half(k, half):
        def both():
            for slot, step in enumerate(own_steps):
                block_copy(k, z, half, slot, plane(step)).start()

        if k in FEED_FORWARD:
            step = jnp.where(outer, jnp.where(first_plane, 1, -1), -towards)
            block_copy(k, z, half, 0, plane(step)).start()
        else:
            both()

    def spread(k):
        kept(k)
        swapped(k)
        spread_half(k, 0)

    def pass_on(k):
        @pl.when(inner)
        def _():
            for half in parts(k):
                for slot, block in ((2, near), (3, far)):
                    copy = block_copy(k, block, half, slot, plane(towards))
                    copy.wait_recv()
                    copy.start()

    def arrive(k):
        for half in parts(k):

            @pl.when(inner)
            def _(half=half):
                block_copy(k, jnp.where(z == 1, 0, 3), half, 0, beside).wait_recv()

            @pl.when(outer)
            def _(half=half):
                for i in range(3):
                    block = jnp.where(first_plane, i + 1, i)
                    block_copy(k, block, half, 0, beside).wait_recv()

    def pass_inner(k):
        copy = block_copy(k, jnp.where(z == 1, 0, 3), 0, 1, plane(-towards))
        copy.wait_recv()
        copy.start()

    def arrive_inner(k):
        for block in (near, far):
            block_copy(k, block, 0, 0, beside).wait_recv()

    def weights_sent():
        for k in range(7):
            for _, send in exchanges[k]:
                send.wait_send()
            for half in parts(k):
                block_copy(k, z, half, 0, beside).wait_send()
                if k in FEED_FORWARD:
                    pl.when(inner)(lambda k=k, half=half: block_copy(k, z, half, 1, beside).wait_send())
                else:
                    block_copy(k, z, half, 1, beside).wait_send()

                    @pl.when(inner)
                    def _(k=k, half=half):
                        for slot in (2, 3):
                            block_copy(k, z, half, slot, beside).wait_send()

    def lanes_of(c):
        if c in (QUERY, KEY):
            return QK, pl.ds(256 * (c - QUERY), 256)
        return c, pl.ds(0, 512)

    def share(ref, c, *index):
        chunk, lanes = lanes_of(c)
        return ref.at[(chunk, *index, slice(None), lanes)]

    def slot_of(c, slot):
        return st.at[slot, :, pl.ds(0, 256 if c in (QUERY, KEY) else 512)]

    def number(c):
        return c if c < QUERY else c - QUERY + (0 if c == QUERY else 6)

    def staged(c, block, slot):
        return pltpu.make_async_copy(slot_of(c, slot), share(stage, c, block), b["stl"].at[slot])

    def to_added(c, block, which, target, slot=None):
        n = number(c)
        return remote(
            share(stage, c, block),
            share(added, c, which),
            b["rs"].at[n, which if slot is None else slot],
            b["ra"].at[n, which],
            target,
        )

    def to_heard(c, block, slot, target):
        n = number(c)
        return remote(
            share(stage, c, block), share(heard, c, z), b["rs"].at[n, slot], b["rr"].at[n, z], target
        )

    def all_staged(c):
        for block in range(PLANES):
            staged(c, block, block).wait()

    def send_gradient(c):
        all_staged(c)
        step = jnp.where(first_plane, 1, -1)

        @pl.when(outer)
        def _():
            to_added(c, 3 - z, 0, plane(step)).start()
            to_added(c, z + 2 * step, 1, plane(step)).start()
            to_heard(c, z + step, 2, plane(step)).start()

    def send_inner(c):
        to_added(c, far, 2, plane(-towards), 0).start()
        to_heard(c, near, 1, plane(-towards)).start()

    def rounds(c, body):
        lanes = 256 if c in (QUERY, KEY) else 512

        def step(i):
            body(pl.ds(pl.multiple_of(i * 32, 32), 32), pl.ds(0, lanes))

        loop(WIDE // 32, step)

    def local(source, target, n):
        return pltpu.make_async_copy(source, target, b["fl"].at[n])

    def combine(c):
        @pl.when(inner)
        def _():
            blocks = (far, near)
            mine = [local(share(stage, c, blocks[i]), slot_of(c, i), i) for i in range(2)]
            for copy in mine:
                copy.start()
            theirs = [local(share(added, c, i), slot_of(c, 2 + i), 2 + i) for i in range(2)]
            for i in range(2):
                to_added(c, blocks[i], i, beside).wait_recv()
                theirs[i].start()
            for i in range(2):
                mine[i].wait()
                theirs[i].wait()

                def body(r, lanes, i=i):
                    st[i, r, lanes] = (
                        st[i, r, lanes].astype(F32) + st[2 + i, r, lanes].astype(F32)
                    ).astype(BF16)

                rounds(c, body)
                back = local(slot_of(c, i), share(stage, c, blocks[i]), i)
                back.start()
            for i in range(2):
                local(slot_of(c, i), share(stage, c, blocks[i]), i).wait()
            send_inner(c)

    def combine_inner(c):
        block = z + towards
        mine = local(share(stage, c, block), slot_of(c, 0), 0)
        theirs = local(share(added, c, 2), slot_of(c, 1), 1)
        mine.start()
        to_added(c, block, 2, beside, 0).wait_recv()
        theirs.start()
        mine.wait()
        theirs.wait()

        def body(r, lanes):
            st[0, r, lanes] = (
                st[0, r, lanes].astype(F32) + st[1, r, lanes].astype(F32)
            ).astype(BF16)

        rounds(c, body)
        back = local(slot_of(c, 0), share(stage, c, block), 0)
        back.start()
        back.wait()
        to_heard(c, block, 2, plane(towards)).start()

    homes = {
        QUERY: q_g, KEY: k_g, VALUE: v_g, SWISH: s_g, OUTPUT: o_g, GATE: g_g, UP: u_g, DOWN: d_g
    }

    def home_copies(c, source):
        home, (_, lanes) = homes[c], lanes_of(c)
        if c in (OUTPUT, DOWN):
            kept_half, given_half = (slice(None), at(x, 256)), (slice(None), at(1 - x, 256))
            slot = home.at[at(x, 512)]
        else:
            kept_half, given_half = (at(x, 256),), (at(1 - x, 256),)
            slot = home.at[:, at(x, home.shape[1] // 2)]
        n = number(c)
        return (
            local(slot_of(c, 0).at[kept_half], slot, 3),
            remote(source.at[given_half], slot, b["fe_s"].at[n], b["fe_r"].at[n], beside),
        )

    def finish_gradient(c, last=False):
        n = number(c)

        def own_load():
            return local(share(stage, c, z), slot_of(c, 0), 0)

        def arrival(i, source):
            remote(
                share(stage, c, 0), share(heard, c, source), b["rs"].at[n, 2], b["rr"].at[n, source], beside
            ).wait_recv()
            load = local(share(heard, c, source), slot_of(c, i), i)
            load.start()
            return load

        source = jnp.where((z == 0) | (z == 2), 1, 2)
        if c in INNER_SUMS:

            @pl.when(outer)
            def _():
                arrival(0, source).wait()

        else:

            @pl.when(outer)
            def _():
                own_load().start()
                arrival(1, source).wait()
                own_load().wait()

                def body(r, lanes):
                    st[0, r, lanes] = (
                        st[0, r, lanes].astype(F32) + st[1, r, lanes].astype(F32)
                    ).astype(BF16)

                rounds(c, body)

        @pl.when(inner)
        def _():
            own_load().start()
            loads = [arrival(1, source)]
            if c not in INNER_SUMS:
                loads.append(arrival(2, jnp.where(z == 1, 0, 3)))
            own_load().wait()
            for load in loads:
                load.wait()

            def body(r, lanes):
                acc = st[0, r, lanes].astype(F32) + st[1, r, lanes].astype(F32)
                if c not in INNER_SUMS:
                    acc = acc + st[2, r, lanes].astype(F32)
                st[0, r, lanes] = acc.astype(BF16)

            rounds(c, body)

        source = slot_of(c, 0) if last else share(stage, c, z)
        stay, send = home_copies(c, source)
        if not last:
            store = local(slot_of(c, 0), share(stage, c, z), 0)
            store.start()
            stay.start()
            store.wait()
            send.start()
            stay.wait()
        else:
            send.start()
            stay.start()
            stay.wait()

    def gradients_done():
        for c in GRADIENTS:
            n = number(c)
            source = slot_of(c, 0) if c == KEY else share(stage, c, z)
            _, send = home_copies(c, source)
            send.wait()

            def sent(c=c, n=n):
                for slot in range(3):
                    remote(
                        share(stage, c, 0), share(heard, c, 0), b["rs"].at[n, slot], b["rr"].at[n, 0], beside
                    ).wait_send()

            if c in INNER_SUMS:
                pl.when(inner)(sent)
            else:
                sent()

    across_step = jnp.where(outer, jnp.where(first_plane, 1, -1), towards)

    def hop(n, source, target, part_of=slice(None)):
        return remote(
            source.at[part_of], target.at[part_of], b["hop_s"].at[n], b["hop_r"].at[n], plane(across_step)
        )

    halves = (pl.ds(0, rows // 2), pl.ds(rows // 2, rows // 2))

    def neighbours_may_write():
        for partner in (place.sib, place.xn, place.yn):
            pl.semaphore_signal(b["free"], inc=1, device_id=partner, device_id_type=MESH)

    def may_write():
        pl.semaphore_wait(b["free"], 3)

    def gain_copy(i):
        target = lax.rem(dp + i, 8)
        return remote(
            b["gown"], b["gparts"].at[dp], b["gg_s"].at[i], b["gg_r"].at[dp], (target, tensor)
        )

    def gain_arrival(i):
        source = lax.rem(dp + i, 8)
        return remote(
            b["gown"], b["gparts"].at[source], b["gg_s"].at[i], b["gg_r"].at[source], (source, tensor)
        )

    gather_sems = (b["ga_s"], b["ga_r"])

    def plane_sum(ref, y_first=False):
        return PlaneSum(place, ref, b["room"], rows, b["re_s"], b["re_r"], y_first)

    for k in range(7):
        keep(k)
    gown = b["gown"]
    for n in range(8):
        gown[n : n + 1, :] = gain_refs[n % 4][...].astype(F32).reshape(1, 256)
    load_x = pltpu.make_async_copy(x_hbm, x_ref, b["ol"].at[3])
    load_cot = pltpu.make_async_copy(cot_hbm, cot_ref, b["ol"].at[4])
    load_x.start()
    load_cot.start()
    mine = pltpu.make_async_copy(gown, b["gparts"].at[dp], b["ol"].at[0])
    mine.start()
    kept(QK)
    pl.semaphore_wait(barrier, 10)
    for i in range(1, 8):
        gain_copy(i).start()
    give(QK)
    spread_half(QK, 0)
    give(VALUE)
    head = (tensor * 2 + x).astype(F32)
    rate = jnp.log(1.0 - jnp.exp2(-5.0 - jnp.full((8, SEQ_LEN), head, F32)))[0:1]

    def body(i):
        r = at(i, 64)
        n = lax.broadcasted_iota(jnp.int32, (64, SEQ_LEN), 0) + i * 64
        m = lax.broadcasted_iota(jnp.int32, (64, SEQ_LEN), 1)
        gap = n - m
        b["decay"][r] = jnp.where(gap >= 0, jnp.exp(jnp.maximum(gap, 0).astype(F32) * rate), 0.0)

    loop(SEQ_LEN // 64, body)
    load_x.wait()
    swapped(QK)
    spread_half(QK, 1)
    mine.wait()
    for i in range(1, 8):
        gain_arrival(i).wait_recv()
    for i in range(8):
        b["gain"][:, i * 256 : (i + 1) * 256] = b["gparts"][i]
    gain = b["gain"]
    low = b["low"]

    def body(i):
        r = at(i, CHUNK)
        hat, _ = normalize(x_ref[r].astype(F32), EPSILON)
        low[r] = (hat * gain[0:1, :] + gain[1:2, :]).astype(BF16)

    loop(rows // CHUNK, body)
    first = Gather(place, low, xs, *gather_sems)
    first.start()
    spread(VALUE)
    load_cot.wait()
    count = counts_ref[0]

    def body(i):
        r = at(i, CHUNK)
        row = lax.broadcasted_iota(jnp.int32, (CHUNK, hidden), 0) + (tensor * rows + i * CHUNK)
        cot_ref[r] = jnp.where(row < count, cot_ref[r].astype(F32), 0.0).astype(BF16)

    loop(rows // CHUNK, body)
    pl.when(outer)(lambda: hop(2, cot_ref, b["cot2"]).start())
    first.forward()
    for k in range(SWISH, DOWN + 1):
        give(k)
    cotangent = Gather(place, cot_ref, b["outs"], b["gc_s"], b["gc_r"])
    pl.when(inner)(cotangent.start)
    pass_on(QK)
    spread(SWISH)
    first.finish()

    def turned_rows(i):
        return at(i // 2, 512), at(lax.rem(i, 2), 8 * rows)

    def body(i):
        r, lanes = turned_rows(i // 2)
        r = pl.ds(pl.multiple_of((i // 4) * 512 + lax.rem(i, 2) * 256, 256), 256)
        xt[r, lanes] = xs[:, at(i, 256)].T

    loop(hidden // 256, body)
    park = pltpu.make_async_copy(xt, parked, b["ol"].at[5])
    unpark = pltpu.make_async_copy(parked, xt, b["ol"].at[0])
    pl.when(inner)(park.start)
    spread(OUTPUT)

    arrive(QK)

    def turn(acc, tile, scale):
        spot = at(lax.rem(tile, SEQ_LEN // TILE), TILE)
        cos, sin = cos_ref[spot], sin_ref[spot]
        one, two = acc[:, :128], acc[:, 128:]
        return (((one * cos - two * sin) * scale).astype(BF16), ((two * cos + one * sin) * scale).astype(BF16))

    def body(i):
        r = at(i, TILE)
        acc = matmul(xs[r], w[QK])
        b["q"][r, :128], b["q"][r, 128:] = turn(acc[:, :KEY_DIM], i, 1.0)
        b["k"][r, :128], b["k"][r, 128:] = turn(acc[:, KEY_DIM:], i, KEY_DIM ** (-0.5))

    tiles = 8 * rows // TILE
    per_slot = SEQ_LEN // TILE
    loop(tiles, body)

    def slot_rows(i):
        return at(i // per_slot, SEQ_LEN)

    def body(i):
        r = at(i, TILE)
        decay = b["decay"][at(lax.rem(i, per_slot), TILE)]
        b["sc"][r] = (nt(b["q"][r], b["k"][slot_rows(i)]) * decay).astype(BF16)

    loop(tiles, body)

    for k in (GATE, UP, DOWN):
        spread(k)
    pass_on(VALUE)
    arrive(VALUE)

    def body(i):
        r = at(i, TILE)
        b["v"][r] = matmul(xs[r], w[VALUE]).astype(BF16)

    loop(tiles, body)

    def body(i):
        r = at(i, TILE)
        retained = matmul(b["sc"][r], b["v"][slot_rows(i)])
        hat, inverse = normalize(retained, GROUP_EPSILON)
        b["ghat"][r] = hat
        b["ginv"][r] = jnp.broadcast_to(inverse, (TILE, 128))

    loop(tiles, body)
    @pl.when(inner)
    def _():
        cotangent.forward()
        cotangent.finish()

    pass_on(SWISH)
    arrive(SWISH)

    def body(i):
        r = at(i, TILE)
        swish = matmul(xs[r], w[SWISH])
        b["swish"][r] = swish
        b["gated"][r] = (swish * jax.nn.sigmoid(swish) * b["ghat"][r]).astype(BF16)

    loop(tiles, body)

    pass_on(OUTPUT)
    arrive(OUTPUT)

    def grid_of(i):
        return at(i // PLANES, TILE), at(lax.rem(i, PLANES), 512)

    reduce = plane_sum(part)
    reduce.fill(lambda r, c: matmul(b["gated"][r], w[OUTPUT, c]))
    reduce.run()
    def body(i):
        r = at(i, CHUNK)
        middle = x_ref[r].astype(F32) + reduce.total(i)
        b["middle"][r] = middle
        hat, _ = normalize(middle, EPSILON)
        low[r] = (hat * gain[2:3, :] + gain[3:4, :]).astype(BF16)

    loop(rows // CHUNK, body)

    @pl.when(outer)
    def _():
        for n in range(2):
            hop(n, low, b["rows2"], halves[n]).start()
        hop(6, b["gated"], b["gated2"]).start()

    pl.when(inner)(lambda: pass_inner(GATE))

    def gelu_of(t):
        inner_value = 0.7978845608028654 * (t + 0.044715 * t * t * t)
        tanh = jnp.tanh(inner_value)
        return 0.5 * (1.0 + tanh), tanh

    def turned_of(ref):
        def body(i):
            turned[:, at(i, TILE)] = ref[at(i, TILE)].T

        loop(tiles, body)

    def stage_block(c, i, value):
        st[i] = value.astype(BF16)
        staged(c, i, i).start()

    def times_turned(left, r, k):
        acc = nt(left[r, 0:512], w[k, 0:512])
        for plane_at in range(1, PLANES):
            lanes = slice(plane_at * 512, plane_at * 512 + 512)
            acc = acc + nt(left[r, lanes], w[k, lanes])
        return acc

    def hidden_tile(mixer, hid, r):
        gate = matmul(mixer[r], w[GATE])
        b["gate"][...] = gate
        up = matmul(mixer[r], w[UP])
        b["up"][...] = up
        gate = b["gate"][...]
        share_of, _ = gelu_of(gate)
        hid[r] = (gate * share_of * up).astype(BF16)

    def back_tile(cots, gb, ub, r):
        back = times_turned(cots, r, DOWN)
        gate, up = b["gate"][...], b["up"][...]
        share_of, tanh = gelu_of(gate)
        slope = 0.5 * gate * (1.0 - tanh * tanh) * (0.7978845608028654 * (1.0 + 0.134145 * gate * gate))
        gb[r] = (back * up * (share_of + slope)).astype(BF16)
        ub[r] = (back * gate * share_of).astype(BF16)

    def refill(c):
        copies = [pltpu.make_async_copy(stage.at[c, i], st.at[i], b["fl"].at[i]) for i in range(PLANES)]
        for copy in copies:
            copy.start()
        for copy in copies:
            copy.wait()

    def product_of(c, i, value, more):
        stage_block(c, i, value + st[i].astype(F32) if more else value)

    def down_gradient(hid, cots, more):
        if more:
            refill(DOWN)
        turned_of(hid)

        def body(i):
            product_of(DOWN, i, matmul(turned[...], cots[:, at(i, 512)]), more)

        loop(PLANES, body)
        all_staged(DOWN)

    def weight_gradient(c, mixer, right, more):
        if more:
            refill(c)

        def body(i):
            def body_turn(j):
                turned[:, at(j, TILE)] = mixer[at(j, TILE), at(i, 512)].T

            loop(tiles, body_turn)
            product_of(c, i, matmul(turned[...], right[...]), more)

        loop(PLANES, body)
        all_staged(c)

    def mixer_input(gb, ub):
        return lambda r, c: nt(gb[r], w[GATE, c]) + nt(ub[r], w[UP, c])

    def mixer_output(hid, target):
        def body(i):
            r, c = grid_of(i)
            target[r, c] = matmul(hid[r], w[DOWN, c]).astype(BF16)

        loop(tiles * PLANES, body)

    b["pieces"][...] = jnp.zeros_like(b["pieces"])

    def second_norm_backward(r, upstream):
        hat, inverse = normalize(b["middle"][r], EPSILON)
        scaled = upstream * hat
        b["pieces"][2] += scaled[0:8] + scaled[8:16]
        b["pieces"][3] += upstream[0:8] + upstream[8:16]
        back = cot_ref[r].astype(F32) + normalize_back(upstream * gain[2:3, :], hat, inverse)
        b["back"][r] = back
        low[r] = back.astype(BF16)

    hid2, gb2, ub2 = b["sb"], b["qkb"], b["ub2"]
    outs_ref = b["outs"]

    @pl.when(inner)
    def _():
        second = Gather(place, low, xs, *gather_sems)
        second.start()
        hop(2, cot_ref, b["cot2"]).wait_recv()
        second.forward()
        pass_inner(UP)
        other_cot = Gather(place, b["cot2"], part, b["gc_s"], b["gc_r"])
        reduce.finish()
        neighbours_may_write()
        may_write()
        other_cot.start()
        pass_inner(DOWN)
        second.finish()
        arrive_inner(GATE)
        arrive_inner(UP)
        other_cot.forward()
        arrive_inner(DOWN)

        def body(i):
            r = at(i, TILE)
            hidden_tile(xs, b["hid"], r)
            back_tile(outs_ref, b["gb"], b["ub"], r)

        loop(tiles, body)
        down_gradient(b["hid"], outs_ref, False)
        neighbours_may_write()
        other_cot.finish()
        other = Gather(place, b["rows2"], outs_ref, b["gd_s"], b["gd_r"])
        may_write()
        for n in range(2):
            hop(n, low, b["rows2"], halves[n]).wait_recv()
        other.start()
        weight_gradient(GATE, xs, b["gb"], False)
        other.forward_across()
        other.own_arrived()
        park.wait()
        reduce2 = plane_sum(xt)

        def body(i):
            pl.when(i == 1)(lambda: together(other.forward_beside, other.s1.wait_recv))
            pl.when(i == 2)(other.s2.wait_recv)
            pl.when(i == 3)(other.across_arrived)
            r = at(reduce2.chip(i), TILE)
            hidden_tile(outs_ref, hid2, r)
            back_tile(part, gb2, ub2, r)
            reduce2.fill_chip(i, mixer_input(gb2, ub2))
            pl.when(i == 2)(lambda: reduce2.take(1))
            pl.when(i == 3)(lambda: reduce2.take(2))

        loop(PLANES, body)
        reduce2.take(3)
        down_gradient(hid2, part, True)
        send_inner(DOWN)
        weight_gradient(UP, xs, b["ub"], False)
        reduce2.run2()
        weight_gradient(GATE, outs_ref, gb2, True)
        send_inner(GATE)
        reduce2.run3()
        for n in range(2):

            def body(i, n=n):
                i = n * (rows // 2 // CHUNK) + i
                b["rows2"][at(i, CHUNK)] = reduce2.total(i).astype(BF16)

            other.drain() if n == 0 else None
            loop(rows // 2 // CHUNK, body)
            hop(3 + n, b["rows2"], b["rows2"], halves[n]).start()
        reduce2.finish()
        unpark.start()
        neighbours_may_write()
        may_write()
        reduce3 = plane_sum(part)
        reduce3.fill(mixer_input(b["gb"], b["ub"]))
        reduce3.run1()
        weight_gradient(UP, outs_ref, ub2, True)
        send_inner(UP)
        reduce3.run2()
        combine_inner(DOWN)
        reduce3.run3()

        def body(i):
            second_norm_backward(at(i, CHUNK), reduce3.total(i))

        loop(rows // CHUNK, body)
        reduce3.finish()
        neighbours_may_write()
        may_write()
        hop(7, low, b["cot2"]).wait_recv()

    third = Gather(place, low, xs, *gather_sems)
    other_middle = Gather(place, b["cot2"], part, b["gd_s"], b["gd_r"])
    outs_ref = b["outs"]

    @pl.when(outer)
    def _():
        reduce.finish()
        for n in range(2):
            hop(n, low, b["rows2"], halves[n]).wait_send()
        for n in range(2):
            hop(3 + n, b["rows2"], b["rows2"], halves[n]).wait_recv()

            def body(i, n=n):
                r = pl.ds(pl.multiple_of(n * (rows // 2) + i * CHUNK, CHUNK), CHUNK)
                second_norm_backward(r, b["rows2"][r].astype(F32))

            loop(rows // 2 // CHUNK, body)
            if n == 0:
                third.start_first_half()
            else:
                third.start_second_half()
                hop(7, low, b["cot2"]).start()
        third.forward()
        third.finish()

    def output_gradient(rows_ref, cots, more):
        if more:
            refill(OUTPUT)
        turned_of(rows_ref)

        def body(i):
            product_of(OUTPUT, i, matmul(turned[...], cots[:, at(i, 512)]), more)

        loop(PLANES, body)
        all_staged(OUTPUT)

    reduce5 = plane_sum(outs_ref, y_first=True)

    @pl.when(inner)
    def _():
        third.start()
        mixer_output(hid2, outs_ref)
        third.forward_across()
        combine_inner(GATE)
        third.forward_beside()
        third.finish()
        other_middle.start()

    swb, rb, vlow = b["gb"], b["ub2"], b["ub"]

    def body(i):
        r = at(i, TILE)
        back = times_turned(xs, r, OUTPUT)
        swish, hat = b["swish"][r], b["ghat"][r]
        gate = jax.nn.sigmoid(swish)
        swb[r] = (back * hat * gate * (1.0 + swish * (1.0 - gate))).astype(BF16)
        rb[r] = normalize_back(back * swish * gate, hat, b["ginv"][r, 0:1]).astype(BF16)

    loop(tiles, body)

    def projection_gradient(c, right, lanes=slice(None)):
        def body(i):
            value = matmul(xt[turned_rows(i)], right[:, lanes]).astype(BF16)
            st[i, :, 0 : value.shape[1]] = value
            staged(c, i, i).start()

        loop(PLANES, body)
        send_gradient(c)

    pl.when(inner)(unpark.wait)
    projection_gradient(SWISH, swb)
    pl.when(inner)(other_middle.forward_across)
    combine(SWISH)

    @pl.when(inner)
    def _():
        other_middle.forward_beside()
        finish_gradient(DOWN)
        finish_gradient(GATE)
        output_gradient(b["gated"], xs, False)
        other_middle.finish()
        reduce5.start()
        hop(6, b["gated"], b["gated2"]).wait_recv()
        output_gradient(b["gated2"], part, True)
        send_inner(OUTPUT)
        combine_inner(UP)
        reduce5.run1()

    def body(i):
        r = at(i, TILE)
        decay = b["decay"][at(lax.rem(i, per_slot), TILE)]
        b["sb"][r] = (nt(rb[r], b["v"][slot_rows(i)]) * decay).astype(BF16)

    loop(tiles, body)
    turned_of(b["sc"])

    def body(i):
        vlow[at(i, TILE)] = matmul(
            turned[at(lax.rem(i, per_slot), TILE), slot_rows(i)], rb[slot_rows(i)]
        ).astype(BF16)

    loop(tiles, body)
    projection_gradient(VALUE, vlow)
    pl.when(inner)(lambda: combine_inner(SWISH))
    turned_of(b["sb"])

    def turn_back(acc, tile, scale):
        spot = at(lax.rem(tile, per_slot), TILE)
        cos, sin = cos_ref[spot], sin_ref[spot]
        one, two = acc[:, :128], acc[:, 128:]
        return (((one * cos + two * sin) * scale).astype(BF16), ((two * cos - one * sin) * scale).astype(BF16))

    def body(i):
        r = at(i, TILE)
        qkb = b["qkb"]
        query = matmul(b["sb"][r], b["k"][slot_rows(i)])
        qkb[r, 0:128], qkb[r, 128:256] = turn_back(query, i, 1.0)
        key = matmul(turned[at(lax.rem(i, per_slot), TILE), slot_rows(i)], b["q"][slot_rows(i)])
        qkb[r, 256:384], qkb[r, 384:512] = turn_back(key, i, KEY_DIM ** (-0.5))

    loop(tiles, body)
    projection_gradient(QUERY, b["qkb"], slice(0, 256))
    projection_gradient(KEY, b["qkb"], slice(256, 512))
    pl.when(inner)(reduce5.run2)
    combine(VALUE)
    reduce6 = PlaneSum(place, outs_ref, xt, rows, b["rf_s"], b["rf_r"], y_first=True)
    pl.when(inner)(lambda: finish_gradient(UP))

    reduce = plane_sum(part)
    reduce.fill(
        lambda r, c: nt(b["qkb"][r], w[QK, c]) + nt(vlow[r], w[VALUE, c]) + nt(swb[r], w[SWISH, c]),
        sending=outer,
    )

    @pl.when(inner)
    def _():
        reduce5.run3()

        def body(i):
            b["cot2"][at(i, CHUNK)] = reduce5.total(i).astype(BF16)

        loop(rows // CHUNK, body)
        hop(5, b["cot2"], b["cot2"]).start()
        reduce5.finish()
        neighbours_may_write()
        may_write()
        reduce.start()

    def delta_rows():
        reduce.run3()

        def body(i):
            r = at(i, CHUNK)
            upstream = reduce.total(i)
            hat, inverse = normalize(x_ref[r].astype(F32), EPSILON)
            scaled = upstream * hat
            b["pieces"][0] += scaled[0:8] + scaled[8:16]
            b["pieces"][1] += upstream[0:8] + upstream[8:16]
            b["back"][r] += normalize_back(upstream * gain[0:1, :], hat, inverse)

        loop(rows // CHUNK, body)
        reduce.finish()
        delta_copy().start()
        share_gains()

    def delta_copy():
        return pltpu.make_async_copy(b["back"], delta_out, b["ol"].at[2])

    def final_copy():
        return pltpu.make_async_copy(b["middle"], final_out, b["ol"].at[1])

    gsend, gparts, gsum = b["gsend"], b["gparts"], b["gsum"]

    def share_copy(i):
        target = lax.rem(dp + i, 8)
        return remote(
            gsend.at[target], gparts.at[dp], b["gg_s"].at[i], b["gg_r"].at[dp], (target, tensor)
        )

    def share_gains():
        for i in range(1, 8):
            gain_copy(i).wait_send()
        for i in range(8):
            for n in range(4):
                lanes = slice(i * 256, i * 256 + 256)
                gsend[i, n : n + 1, :] = jnp.sum(b["pieces"][n, :, lanes], axis=0, keepdims=True)
                gsend[i, n + 4 : n + 5, :] = jnp.zeros((1, 256), F32)
        for i in range(1, 8):
            share_copy(i).start()

    @pl.when(outer)
    def _():
        finish_gradient(DOWN)
        reduce.run1()
        finish_gradient(GATE)
        reduce.run2()
        delta_rows()
        finish_gradient(UP)
        finish_gradient(SWISH)
        hop(2, cot_ref, b["cot2"]).wait_send()
        hop(5, b["cot2"], b["cot2"]).wait_recv()

        def body(i):
            r = at(i, CHUNK)
            b["middle"][r] += b["cot2"][r].astype(F32)

        loop(rows // CHUNK, body)
        final_copy().start()
        finish_gradient(OUTPUT)
        finish_gradient(VALUE)

    @pl.when(inner)
    def _():
        combine_inner(OUTPUT)
        reduce.run1()
        combine(QUERY)
        reduce6.fill(lambda r, c: matmul(b["hid"][r], w[DOWN, c]))
        reduce.run2()
        reduce6.run1()
        combine_inner(VALUE)
        finish_gradient(SWISH)
        combine(KEY)
        delta_rows()
        reduce6.run2()
        combine_inner(QUERY)
        finish_gradient(OUTPUT)
        combine_inner(KEY)
        finish_gradient(VALUE)
        reduce6.run3()

        def body(i):
            b["middle"][at(i, CHUNK)] += reduce6.total(i)

        loop(rows // CHUNK, body)
        reduce6.finish()
        final_copy().start()

    finish_gradient(QUERY)
    acc = gsend[dp]
    for i in range(1, 8):
        gain_arrival(i).wait_recv()
        acc = acc + gparts[lax.rem(dp + i, 8)]
    gsum[tensor] = acc

    def sum_copy(i, source):
        target = lax.rem(tensor + i, 4)
        return remote(
            gsum.at[source], gsum.at[source], b["gt_s"].at[i], b["gt_r"].at[source], (dp, target)
        )

    for i in range(1, 4):
        sum_copy(i, tensor).start()
    finish_gradient(KEY, last=True)
    for i in range(1, 4):
        sum_copy(i, lax.rem(tensor + i, 4)).wait_recv()
    for i in range(1, 4):
        sum_copy(i, tensor).wait_send()
    for i in range(1, 8):
        share_copy(i).wait_send()
    gains_out[...] = (gsum[0] + gsum[1]) + (gsum[2] + gsum[3])
    final_copy().wait()
    delta_copy().wait()
    weights_sent()

    @pl.when(inner)
    def _():
        for n in range(2):
            hop(3 + n, b["rows2"], b["rows2"], halves[n]).wait_send()
        hop(5, b["cot2"], b["cot2"]).wait_send()

    @pl.when(outer)
    def _():
        hop(6, b["gated"], b["gated2"]).wait_send()
        hop(7, low, b["cot2"]).wait_send()

    gradients_done()


def whole_layer(
    incoming_signals,
    loss_sensitivity,
    token_counts_per_slot,
    leading_norm_multiplier,
    leading_norm_offset,
    question_projection,
    lookup_projection,
    content_projection,
    silu_switch_projection,
    retention_result_projection,
    trailing_norm_multiplier,
    trailing_norm_offset,
    feedforward_switch_projection,
    expanding_projection,
    contracting_projection,
):
    rows, hidden = incoming_signals.shape
    places = np.arange(SEQ_LEN, dtype=np.float32)
    middle = KEY_DIM // 2
    spectrum = np.float32(10000.0) ** (-np.arange(middle, dtype=np.float32) / np.float32(middle))
    angles = places[:, None] * spectrum[None, :]
    weights = (
        question_projection,
        lookup_projection,
        content_projection,
        silu_switch_projection,
        retention_result_projection,
        feedforward_switch_projection,
        expanding_projection,
        contracting_projection,
    )
    gains = (
        leading_norm_multiplier, leading_norm_offset, trailing_norm_multiplier, trailing_norm_offset
    )
    tables = (jnp.asarray(np.cos(angles)), jnp.asarray(np.sin(angles)))
    args = (incoming_signals, loss_sensitivity, token_counts_per_slot, *tables, *gains, *weights)
    scratch = mega_scratch(rows, hidden)
    shape = jax.ShapeDtypeStruct
    outs = (
        shape((rows, hidden), F32),
        shape((rows, hidden), F32),
        shape((8, 256), F32),
        *(shape(weight.shape, BF16) for weight in weights),
        shape((7, PLANES, WIDE, WIDE), BF16),
        shape((7, PLANES, WIDE, WIDE), BF16),
        shape((7, 3, WIDE, WIDE), BF16),
        shape((8 * rows, hidden), BF16),
    )
    scalar = pl.BlockSpec(memory_space=pltpu.SMEM)
    results = pl.pallas_call(
        functools.partial(mega_kernel, tuple(scratch), len(args), len(outs)),
        out_shape=outs,
        in_specs=[ANY, ANY, scalar] + [VM] * 6 + [ANY] * 8,
        out_specs=tuple([ANY, ANY, VM] + [ANY] * 12),
        scratch_shapes=list(scratch.values()),
        compiler_params=pltpu.CompilerParams(
            collective_id=0, has_side_effects=True, vmem_limit_bytes=67043328
        ),
        name="whole_layer",
    )(*args)
    final_rows, delta, gain_sums = results[:3]
    owned = results[3:11]
    wide = pl.pallas_call(
        widen_kernel,
        out_shape=(
            shape((rows, hidden), BF16),
            shape((rows, hidden), F32),
            *(shape(weight.shape, F32) for weight in weights),
        ),
        in_specs=[scalar] + [ANY] * 10,
        out_specs=(ANY,) * 10,
        scratch_shapes=[
            pltpu.VMEM((rows, hidden), F32),
            pltpu.VMEM((rows, hidden), F32),
            pltpu.VMEM((rows, hidden), BF16),
            *(pltpu.VMEM(weight.shape, BF16) for weight in weights),
            *(pltpu.VMEM(weight.shape, F32) for weight in weights),
            pltpu.SemaphoreType.DMA((10,)),
            pltpu.SemaphoreType.DMA((10,)),
        ],
        compiler_params=pltpu.CompilerParams(vmem_limit_bytes=67043328),
        name="widen",
    )(token_counts_per_slot, final_rows, delta, *owned)
    query, key, value, swish, output, gate, up, down = wide[2:]
    return (
        wide[0],
        wide[1],
        gain_sums[0],
        gain_sums[1],
        query,
        key,
        value,
        swish,
        output,
        gain_sums[2],
        gain_sums[3],
        gate,
        up,
        down,
    )


def widen_kernel(counts_ref, *refs):
    sources, targets, scratch = refs[:10], refs[10:20], refs[20:]
    final, delta, low = scratch[:3]
    narrow, wide, (came, went) = scratch[3:11], scratch[11:19], scratch[19:]
    buffers = (final, delta, *narrow)
    loads = [
        pltpu.make_async_copy(source, buffer, came.at[i])
        for i, (source, buffer) in enumerate(zip(sources, buffers, strict=True))
    ]
    stores = [
        pltpu.make_async_copy(buffer, target, went.at[i])
        for i, (buffer, target) in enumerate(zip((low, delta, *wide), targets, strict=True))
    ]
    for load in loads:
        load.start()
    rows, hidden = final.shape
    tensor, count = lax.axis_index("tensor"), counts_ref[0]
    loads[0].wait()

    def body(i):
        r = at(i, CHUNK)
        row = lax.broadcasted_iota(jnp.int32, (CHUNK, hidden), 0) + (tensor * rows + i * CHUNK)
        low[r] = jnp.where(row < count, final[r], 0.0).astype(BF16)

    loop(rows // CHUNK, body)
    stores[0].start()
    loads[1].wait()
    stores[1].start()
    for n in range(8):
        loads[n + 2].wait()

        def body(i, n=n):
            r = at(i, 32)
            wide[n][r] = narrow[n][r].astype(F32)

        loop(narrow[n].shape[0] // 32, body)
        stores[n + 2].start()
    for store in stores:
        store.wait()


def solution(mesh):
    ranks = mesh.shape["dp"]
    groups = [[2 * k + side for k in range(ranks // 2)] for side in range(2)]
    swap = [(rank, rank + 1 - 2 * (rank % 2)) for rank in range(ranks)]
    rows, gain, column, row = P(("dp", "tensor"), None), P("dp"), P("dp", "tensor"), P("tensor", "dp")
    weights = (gain, gain, column, column, column, column, row, gain, gain, column, column, row)
    one_kernel = ranks == 8 and mesh.shape["tensor"] == 4
    return jax.shard_map(
        whole_layer if one_kernel else functools.partial(per_device, groups, swap),
        mesh=mesh,
        in_specs=(rows, rows, P("dp"), *weights),
        out_specs=(rows, rows, *weights),
        check_vma=False,
    )
```

```python
import functools

import jax
import jax.numpy as jnp
import numpy as np
from jax import lax
from jax.experimental import pallas as pl
from jax.experimental.pallas import tpu as pltpu
from jax.sharding import PartitionSpec as P

KEY_DIM = 256
VAL_DIM = 512
SEQ_LEN = 512

EPSILON = 1e-05
GROUP_EPSILON = 0.1

MESH = pl.DeviceIdType.MESH
F32 = jnp.float32
BF16 = jnp.bfloat16
CHUNK = 16


def normalize(values, epsilon):
    centre = values - jnp.mean(values, axis=-1, keepdims=True)
    inverse = lax.rsqrt(jnp.mean(centre * centre, axis=-1, keepdims=True) + epsilon)
    return (centre * inverse, inverse)


def normalize_back(upstream, normed, inverse):
    return inverse * (
        upstream
        - jnp.mean(upstream, axis=-1, keepdims=True)
        - normed * jnp.mean(upstream * normed, axis=-1, keepdims=True)
    )


def rotate_half(values):
    middle = values.shape[-1] // 2
    return jnp.concatenate([-values[..., middle:], values[..., :middle]], axis=-1)


def rotary_tables(span, columns):
    middle = columns // 2
    places = jnp.arange(span, dtype=jnp.int32).astype(jnp.float32)
    spectrum = 10000.0 ** (-jnp.arange(middle, dtype=jnp.int32).astype(jnp.float32) / middle)
    angles = places[:, None] * spectrum[None, :]
    angles = jnp.concatenate([angles, angles], axis=1)
    return (jnp.cos(angles)[None], jnp.sin(angles)[None])


def decay_table(span, head_id):
    log_rate = jnp.log(1.0 - jnp.exp2(-5.0 - head_id.astype(jnp.float32)))
    places = jnp.arange(span, dtype=jnp.int32)
    offsets = places[:, None] - places[None, :]
    decayed = jnp.exp(jnp.maximum(offsets, 0).astype(jnp.float32) * log_rate)
    return jnp.where(offsets >= 0, decayed, 0.0)


def gelu_tanh(values):
    return jax.nn.gelu(values, approximate=True)


def matmul(left, right):
    return jnp.dot(left, right, preferred_element_type=jnp.float32)


class Place:
    def __init__(self):
        d, t = lax.axis_index("dp"), lax.axis_index("tensor")
        self.x, self.y, self.c = lax.rem(d, 2), t // 2, lax.rem(t, 2)
        dx, ty = d + 1 - 2 * self.x, (1 - self.y) * 2 + self.c
        self.sib = (d, t + 1 - 2 * self.c)
        self.xn = (dx, t)
        self.yn = (d, ty)

    def block(self, j, other_core=0):
        x = 1 - self.x if j in (1, 3) else self.x
        y = 1 - self.y if j in (2, 3) else self.y
        c = 1 - self.c if other_core else self.c
        return x * 4 + y * 2 + c


def greet(place):
    barrier = pltpu.get_barrier_semaphore()
    for partner in (place.sib, place.xn, place.yn):
        pl.semaphore_signal(barrier, inc=1, device_id=partner, device_id_type=MESH)
    pl.semaphore_wait(barrier, 3)


def rows_of(index, rows):
    return pl.ds(pl.multiple_of(index * rows, rows), rows)


class Gather:
    @staticmethod
    def scratch():
        return [pltpu.SemaphoreType.DMA((13,)), pltpu.SemaphoreType.DMA((13,))]

    def __init__(self, place, src, out, send, recv):
        rows = src.shape[0]
        half = rows // 2
        p = place

        def remote(k, source, j, lo, n, target, core=0):
            where = pl.ds(pl.multiple_of(p.block(j, core) * rows + lo, 8), n)
            source = source.at[pl.ds(lo, n)] if source is src else source.at[where]
            return pltpu.make_async_remote_copy(
                src_ref=source,
                dst_ref=out.at[where],
                send_sem=send.at[k],
                recv_sem=recv.at[k],
                device_id=target,
                device_id_type=MESH,
            )

        self.p, self.rows, self.half = p, rows, half
        self.local = pltpu.make_async_copy(src, out.at[rows_of(p.block(0), rows)], send.at[12])
        h = half
        self.xa = remote(0, src, 0, 0, h, p.xn)
        self.xb = remote(1, src, 0, h, h, p.xn)
        self.ya = remote(2, src, 0, 0, h, p.yn)
        self.yb = remote(3, src, 0, h, h, p.yn)
        self.s0 = remote(4, src, 0, 0, rows, p.sib)
        self.da = remote(5, out, 1, 0, h, p.yn)
        self.db = remote(6, out, 2, h, h, p.xn)
        self.s1 = remote(7, out, 1, 0, rows, p.sib)
        self.s2 = remote(8, out, 2, 0, rows, p.sib)
        self.s3a = remote(9, out, 3, 0, h, p.sib)
        self.s3b = remote(10, out, 3, h, h, p.sib)

    def start(self):
        for copy in (self.xa, self.yb, self.xb, self.ya, self.s0, self.local):
            copy.start()

    def start_first_half(self):
        self.xa.start()
        self.ya.start()

    def start_second_half(self):
        for copy in (self.yb, self.xb, self.s0, self.local):
            copy.start()

    def forward(self):
        self.forward_across()
        self.forward_beside()

    def forward_across(self):
        self.xa.wait_recv()
        self.da.start()
        self.yb.wait_recv()
        self.db.start()

    def forward_beside(self):
        self.xb.wait_recv()
        self.s1.start()
        self.ya.wait_recv()
        self.s2.start()

    def own_arrived(self):
        self.local.wait()
        self.s0.wait_recv()

    def across_arrived(self):
        self.da.wait_recv()
        self.s3a.start()
        self.db.wait_recv()
        self.s3b.start()
        self.s3a.wait_recv()
        self.s3b.wait_recv()

    def drain(self):
        for copy in (self.s0, self.s1, self.s2, self.s3a, self.s3b):
            copy.wait_send()
        for copy in (self.xa, self.xb, self.ya, self.yb, self.da, self.db):
            copy.wait_send()

    def finish(self):
        self.da.wait_recv()
        self.s3a.start()
        self.db.wait_recv()
        self.s3b.start()
        self.local.wait()
        for copy in (self.s0, self.s1, self.s2, self.s3a, self.s3b):
            copy.wait()
        for copy in (self.xa, self.xb, self.ya, self.yb, self.da, self.db):
            copy.wait_send()


class Reduce:
    @staticmethod
    def scratch(rows, columns):
        return [
            pltpu.VMEM((4, rows, columns), BF16),
            pltpu.VMEM((4, rows, columns), BF16),
            pltpu.VMEM((2, rows, columns), BF16),
            pltpu.VMEM((2, rows // 2, columns), BF16),
            pltpu.SemaphoreType.DMA((14,)),
            pltpu.SemaphoreType.DMA((10,)),
        ]

    def __init__(self, place, part, mine, theirs, got, across, send, recv):
        p = place
        rows = mine.shape[1]
        h = rows // 2
        self.rows, self.half = rows, h
        self.mine, self.theirs, self.got, self.across = mine, theirs, got, across

        def remote(k, source, target_ref, target):
            return pltpu.make_async_remote_copy(
                src_ref=source,
                dst_ref=target_ref,
                send_sem=send.at[k],
                recv_sem=recv.at[k],
                device_id=target,
                device_id_type=MESH,
            )

        a, b = pl.ds(0, h), pl.ds(h, h)
        self.load = [
            pltpu.make_async_copy(part.at[rows_of(p.block(j), rows)], mine.at[j], send.at[10 + j])
            for j in range(4)
        ]
        self.swap = [
            remote(j, part.at[rows_of(p.block(j, 1), rows)], theirs.at[j], p.sib) for j in range(4)
        ]
        self.da = remote(4, mine.at[3, a], across.at[0], p.xn)
        self.db = remote(5, mine.at[3, b], across.at[1], p.yn)
        self.xa = remote(6, mine.at[1, a], got.at[0, a], p.xn)
        self.xb = remote(7, mine.at[1, b], got.at[0, b], p.xn)
        self.ya = remote(8, mine.at[2, a], got.at[1, a], p.yn)
        self.yb = remote(9, mine.at[2, b], got.at[1, b], p.yn)

    def add(self, j, lo, n, other, other_lo):
        def body(i, carry):
            r = pl.ds(pl.multiple_of(lo + i * CHUNK, CHUNK), CHUNK)
            q = pl.ds(pl.multiple_of(other_lo + i * CHUNK, CHUNK), CHUNK)
            self.mine[j, r] = (self.mine[j, r].astype(F32) + other[q].astype(F32)).astype(BF16)
            return carry

        lax.fori_loop(0, n // CHUNK, body, 0)

    def start(self):
        for j in (3, 1, 2, 0):
            self.swap[j].start()
            self.load[j].start()

    def run(self):
        rows, h = self.rows, self.half
        for j, copies in ((3, (self.da, self.db)), (1, (self.xa,)), (2, (self.yb,))):
            self.load[j].wait()
            self.swap[j].wait_recv()
            self.add(j, 0, rows, self.theirs.at[j], 0)
            for copy in copies:
                copy.start()
        self.db.wait_recv()
        self.add(1, h, h, self.across.at[1], 0)
        self.xb.start()
        self.da.wait_recv()
        self.add(2, 0, h, self.across.at[0], 0)
        self.ya.start()
        self.load[0].wait()
        self.swap[0].wait_recv()
        for copy in (self.xa, self.yb, self.xb, self.ya):
            copy.wait_recv()

    def total(self, r):
        pieces = (self.mine[0, r], self.theirs[0, r], self.got[0, r], self.got[1, r])
        one, two, three, four = (piece.astype(F32) for piece in pieces)
        return (one + two) + (three + four)

    def finish(self):
        for copy in (*self.swap, self.da, self.db, self.xa, self.xb, self.ya, self.yb):
            copy.wait_send()


def chunks(rows, body):
    def step(i, carry):
        body(pl.ds(pl.multiple_of(i * CHUNK, CHUNK), CHUNK))
        return carry

    lax.fori_loop(0, rows // CHUNK, step, 0)


def first_kernel(x_ref, cot_ref, gains_ref, out_x, out_cot, normed, *sems):
    place = Place()
    greet(place)
    gain, shift = gains_ref[0:1, :], gains_ref[1:2, :]

    def body(r):
        hat, _ = normalize(x_ref[r].astype(F32), EPSILON)
        normed[r] = (hat * gain + shift).astype(BF16)

    chunks(x_ref.shape[0], body)
    one = Gather(place, normed, out_x, *sems[:2])
    two = Gather(place, cot_ref, out_cot, *sems[2:])
    one.start()
    two.start()
    one.forward()
    two.forward()
    one.finish()
    two.finish()


def second_kernel(part_ref, x_ref, gains_ref, out_all, middle_ref, normed, *scratch):
    place = Place()
    greet(place)
    reduce = Reduce(place, part_ref, *scratch[:6])
    reduce.start()
    reduce.run()
    gain, shift = gains_ref[2:3, :], gains_ref[3:4, :]

    def body(r):
        middle = x_ref[r].astype(F32) + reduce.total(r)
        middle_ref[r] = middle
        hat, _ = normalize(middle, EPSILON)
        normed[r] = (hat * gain + shift).astype(BF16)

    chunks(x_ref.shape[0], body)
    gather = Gather(place, normed, out_all, *scratch[6:])
    gather.start()
    gather.forward()
    gather.finish()
    reduce.finish()


def third_kernel(
    part_ref, middle_ref, cot_ref, gains_ref, out_all, back_ref, pieces_ref, low, *scratch
):
    place = Place()
    greet(place)
    reduce = Reduce(place, part_ref, *scratch[:6])
    reduce.start()
    pieces_ref[...] = jnp.zeros_like(pieces_ref)
    reduce.run()
    gain = gains_ref[2:3, :]

    def body(r):
        upstream = reduce.total(r)
        hat, inverse = normalize(middle_ref[r], EPSILON)
        scaled = upstream * hat
        pieces_ref[0] += scaled[0:8] + scaled[8:16]
        pieces_ref[1] += upstream[0:8] + upstream[8:16]
        back = cot_ref[r].astype(F32) + normalize_back(upstream * gain, hat, inverse)
        back_ref[r] = back
        low[r] = back.astype(BF16)

    chunks(middle_ref.shape[0], body)
    gather = Gather(place, low, out_all, *scratch[6:])
    gather.start()
    gather.forward()
    gather.finish()
    reduce.finish()


def fourth_kernel(
    first_ref, mixer_ref, x_ref, middle_ref, gains_ref, delta_ref, final_ref, pieces_ref, *scratch
):
    place = Place()
    greet(place)
    one = Reduce(place, first_ref, *scratch[:6])
    two = Reduce(place, mixer_ref, *scratch[6:])
    one.start()
    two.start()
    pieces_ref[...] = jnp.zeros_like(pieces_ref)
    one.run()
    two.run()
    gain = gains_ref[0:1, :]

    def body(r):
        upstream = one.total(r)
        hat, inverse = normalize(x_ref[r].astype(F32), EPSILON)
        scaled = upstream * hat
        pieces_ref[0] += scaled[0:8] + scaled[8:16]
        pieces_ref[1] += upstream[0:8] + upstream[8:16]
        delta_ref[r] = normalize_back(upstream * gain, hat, inverse)
        final_ref[r] = middle_ref[r] + two.total(r)

    chunks(x_ref.shape[0], body)
    one.finish()
    two.finish()


ANY = pl.BlockSpec(memory_space=pl.ANY)
VM = pl.BlockSpec(memory_space=pltpu.VMEM)


def call(kernel, ident, args, specs, outs, out_specs, scratch, nbytes):
    return pl.pallas_call(
        kernel,
        out_shape=outs,
        in_specs=specs,
        out_specs=out_specs,
        scratch_shapes=scratch,
        compiler_params=pltpu.CompilerParams(
            collective_id=ident, has_side_effects=True, vmem_limit_bytes=32 << 20
        ),
        cost_estimate=pl.CostEstimate(flops=0, bytes_accessed=nbytes, transcendentals=0),
        name=kernel.__name__,
    )(*args)


def per_device(
    groups,
    swap,
    incoming_signals,
    loss_sensitivity,
    token_counts_per_slot,
    leading_norm_multiplier,
    leading_norm_offset,
    question_projection,
    lookup_projection,
    content_projection,
    silu_switch_projection,
    retention_result_projection,
    trailing_norm_multiplier,
    trailing_norm_offset,
    feedforward_switch_projection,
    expanding_projection,
    contracting_projection,
):
    local_rows, hidden_size = incoming_signals.shape
    total_rows = 8 * local_rows
    slots_here = token_counts_per_slot.shape[0]
    dp_rank, tensor_rank = lax.axis_index("dp"), lax.axis_index("tensor")
    side = lax.rem(dp_rank, 2)
    row_ids = tensor_rank * local_rows + jnp.arange(local_rows, dtype=jnp.int32)
    slot_match = (row_ids // SEQ_LEN)[:, None] == jnp.arange(slots_here, dtype=jnp.int32)[None, :]
    row_lengths = jnp.sum(jnp.where(slot_match, token_counts_per_slot[None, :], 0), axis=1)
    valid_rows = (row_ids % SEQ_LEN < row_lengths)[:, None]

    def exchange(weight, axis, join):
        half = weight.shape[axis] // 2
        keep = lax.dynamic_slice_in_dim(weight, side * half, half, axis)
        give = lax.dynamic_slice_in_dim(weight, (1 - side) * half, half, axis)
        take = lax.ppermute(give, "dp", swap)
        return jnp.where(
            side == 0,
            jnp.concatenate([keep, take], axis=join),
            jnp.concatenate([take, keep], axis=join),
        )

    def spread(block, axis):
        return lax.all_gather(block, "dp", axis=axis, tiled=True, axis_index_groups=groups)

    query_half = exchange(question_projection, 1, 0)
    key_half = exchange(lookup_projection, 1, 0)
    query_key = spread(jnp.concatenate([query_half, key_half], axis=1), 0)
    value_full = spread(exchange(content_projection, 1, 0), 0)
    swish_full = spread(exchange(silu_switch_projection, 1, 0), 0)
    output_full = spread(exchange(retention_result_projection, 0, 1), 1)
    gate_full = spread(exchange(feedforward_switch_projection, 1, 0), 0)
    up_full = spread(exchange(expanding_projection, 1, 0), 0)
    down_full = spread(exchange(contracting_projection, 0, 1), 1)

    gains = jnp.stack(
        [leading_norm_multiplier, leading_norm_offset, trailing_norm_multiplier, trailing_norm_offset]
    )
    gains = lax.all_gather(gains, "dp", axis=1, tiled=True).astype(F32)
    gains = jnp.concatenate([gains, gains], axis=0)

    all_rows = jax.ShapeDtypeStruct((total_rows, hidden_size), BF16)
    own_rows = jax.ShapeDtypeStruct((local_rows, hidden_size), F32)
    pieces = jax.ShapeDtypeStruct((2, 8, hidden_size), F32)
    row_low = pltpu.VMEM((local_rows, hidden_size), BF16)
    reduce_scratch = Reduce.scratch(local_rows, hidden_size)
    moved = total_rows * hidden_size * 2

    out_low = jnp.where(valid_rows, loss_sensitivity, 0)
    normed_all, out_all = call(
        first_kernel,
        0,
        (incoming_signals, out_low, gains),
        [VM, VM, VM],
        (all_rows, all_rows),
        (ANY, ANY),
        [row_low, *Gather.scratch(), *Gather.scratch()],
        24 * moved,
    )

    slot_count = total_rows // SEQ_LEN
    shape_key = (slot_count, SEQ_LEN, KEY_DIM)
    shape_value = (slot_count, SEQ_LEN, VAL_DIM)
    query_key_proj = matmul(normed_all, query_key)
    query_proj = query_key_proj[:, :KEY_DIM].reshape(shape_key)
    key_proj = query_key_proj[:, KEY_DIM:].reshape(shape_key)
    value_heads = matmul(normed_all, value_full).reshape(shape_value).astype(BF16)
    swish_heads = matmul(normed_all, swish_full).reshape(shape_value)
    cosines, sines = rotary_tables(SEQ_LEN, KEY_DIM)
    decays = decay_table(SEQ_LEN, tensor_rank * 2 + side)
    query_rot = (query_proj * cosines + rotate_half(query_proj) * sines).astype(BF16)
    key_rot = ((key_proj * cosines + rotate_half(key_proj) * sines) * KEY_DIM ** (-0.5)).astype(BF16)
    scores = (
        jnp.einsum("snk,smk->snm", query_rot, key_rot, preferred_element_type=F32) * decays[None]
    ).astype(BF16)
    retained = jnp.einsum("snm,smv->snv", scores, value_heads, preferred_element_type=F32)
    group_hat, group_inverse = normalize(retained, GROUP_EPSILON)
    sigmoid_gate = jax.nn.sigmoid(swish_heads)
    gated = (swish_heads * sigmoid_gate * group_hat).reshape(total_rows, VAL_DIM).astype(BF16)
    retention_part = matmul(gated, output_full).astype(BF16)

    mixer_all, middle_rows = call(
        second_kernel,
        1,
        (retention_part, incoming_signals, gains),
        [ANY, VM, VM],
        (all_rows, own_rows),
        (ANY, VM),
        [row_low, *reduce_scratch, *Gather.scratch()],
        24 * moved,
    )

    gate_proj = matmul(mixer_all, gate_full)
    up_proj = matmul(mixer_all, up_full)
    gelu_gate, gelu_back = jax.vjp(gelu_tanh, gate_proj)
    hidden = (gelu_gate * up_proj).astype(BF16)
    down_gradient = matmul(hidden.T, out_all).astype(BF16)
    hidden_back = matmul(out_all, down_full.T)
    gate_back = gelu_back(hidden_back * up_proj)[0].astype(BF16)
    up_back = (hidden_back * gelu_gate).astype(BF16)
    gate_gradient = matmul(mixer_all.T, gate_back).astype(BF16)
    up_gradient = matmul(mixer_all.T, up_back).astype(BF16)
    mixer_input_part = (matmul(gate_back, gate_full.T) + matmul(up_back, up_full.T)).astype(BF16)
    mixer_part = matmul(hidden, down_full).astype(BF16)

    middle_all, middle_back, after_pieces = call(
        third_kernel,
        2,
        (mixer_input_part, middle_rows, out_low, gains),
        [ANY, VM, VM, VM],
        (all_rows, own_rows, pieces),
        (ANY, VM, VM),
        [row_low, *reduce_scratch, *Gather.scratch()],
        24 * moved,
    )

    output_gradient = matmul(gated.T, middle_all).astype(BF16)
    gated_back = matmul(middle_all, output_full.T).reshape(shape_value)
    swish_back = (
        (gated_back * group_hat * sigmoid_gate * (1.0 + swish_heads * (1.0 - sigmoid_gate)))
        .reshape(total_rows, VAL_DIM)
        .astype(BF16)
    )
    retained_back = normalize_back(
        gated_back * swish_heads * sigmoid_gate, group_hat, group_inverse
    ).astype(BF16)
    score_back = (
        jnp.einsum("snv,smv->snm", retained_back, value_heads, preferred_element_type=F32)
        * decays[None]
    ).astype(BF16)
    query_rot_back = jnp.einsum("snm,smk->snk", score_back, key_rot, preferred_element_type=F32)
    key_rot_back = jnp.einsum("snm,snk->smk", score_back, query_rot, preferred_element_type=F32)
    value_back = jnp.einsum("snm,snv->smv", scores, retained_back, preferred_element_type=F32)
    query_back = (
        (query_rot_back * cosines - rotate_half(query_rot_back) * sines)
        .reshape(total_rows, KEY_DIM)
        .astype(BF16)
    )
    key_back = (
        ((key_rot_back * cosines - rotate_half(key_rot_back) * sines) * KEY_DIM ** (-0.5))
        .reshape(total_rows, KEY_DIM)
        .astype(BF16)
    )
    value_low = value_back.reshape(total_rows, VAL_DIM).astype(BF16)
    swish_gradient = matmul(normed_all.T, swish_back).astype(BF16)
    value_gradient = matmul(normed_all.T, value_low).astype(BF16)
    query_key_back = jnp.concatenate([query_back, key_back], axis=1)
    query_key_gradient = matmul(normed_all.T, query_key_back).astype(BF16)
    first_part = (
        matmul(query_key_back, query_key.T)
        + matmul(value_low, value_full.T)
        + matmul(swish_back, swish_full.T)
    ).astype(BF16)

    delta, final_rows, before_pieces = call(
        fourth_kernel,
        3,
        (first_part, mixer_part, incoming_signals, middle_rows, gains),
        [ANY, ANY, VM, VM, VM],
        (own_rows, own_rows, pieces),
        (VM, VM, VM),
        [*reduce_scratch, *reduce_scratch],
        24 * moved,
    )
    layer_output = jnp.where(valid_rows, final_rows, 0.0).astype(BF16)
    input_delta = middle_back + delta

    gain_pieces = jnp.concatenate(
        [jnp.sum(before_pieces, axis=1), jnp.sum(after_pieces, axis=1)], axis=0
    )
    gain_sums = lax.psum(gain_pieces, ("dp", "tensor"))
    width = leading_norm_multiplier.shape[0]
    gain_sums = lax.dynamic_slice_in_dim(gain_sums, dp_rank * width, width, 1)

    def collect(gradient, axis):
        return lax.psum_scatter(
            gradient, "dp", scatter_dimension=axis, tiled=True, axis_index_groups=groups
        )

    def restore(block, axis, join):
        half = block.shape[axis] // 2
        keep = lax.dynamic_slice_in_dim(block, side * half, half, axis)
        give = lax.dynamic_slice_in_dim(block, (1 - side) * half, half, axis)
        take = lax.ppermute(give, "dp", swap)
        return jnp.where(
            side == 0,
            jnp.concatenate([keep, take], axis=join),
            jnp.concatenate([take, keep], axis=join),
        ).astype(F32)

    down_owned = restore(collect(down_gradient, 1), 1, 0)
    gate_owned = restore(collect(gate_gradient, 0), 0, 1)
    up_owned = restore(collect(up_gradient, 0), 0, 1)
    output_owned = restore(collect(output_gradient, 1), 1, 0)
    swish_owned = restore(collect(swish_gradient, 0), 0, 1)
    value_owned = restore(collect(value_gradient, 0), 0, 1)
    query_key_owned = collect(query_key_gradient, 0)
    query_owned = restore(query_key_owned[:, :KEY_DIM], 0, 1)
    key_owned = restore(query_key_owned[:, KEY_DIM:], 0, 1)
    return (
        layer_output,
        input_delta,
        gain_sums[0],
        gain_sums[1],
        query_owned,
        key_owned,
        value_owned,
        swish_owned,
        output_owned,
        gain_sums[2],
        gain_sums[3],
        gate_owned,
        up_owned,
        down_owned,
    )


PLANES = 4
QK, VALUE, SWISH, OUTPUT, GATE, UP, DOWN = range(7)
WIDE = 512
QUERY, KEY = 7, 8
FEED_FORWARD = (DOWN, GATE, UP)
INNER_SUMS = (*FEED_FORWARD, OUTPUT)
GRADIENTS = (*FEED_FORWARD, OUTPUT, SWISH, VALUE, QUERY, KEY)
TILE = 256


def nt(left, right):
    return lax.dot_general(left, right, (((1,), (1,)), ((), ())), preferred_element_type=F32)


def loop(count, body):
    def step(i, carry):
        body(i)
        return carry

    lax.fori_loop(0, count, step, 0)


def together(*steps):
    for step in steps:
        step()


def at(index, size):
    return pl.ds(pl.multiple_of(index * size, size), size)


def mega_scratch(rows, hidden):
    total = 8 * rows
    dma = pltpu.SemaphoreType.DMA
    return dict(
        w=pltpu.VMEM((7, hidden, WIDE), BF16),
        xs=pltpu.VMEM((total, hidden), BF16),
        xt=pltpu.VMEM((total, hidden), BF16),
        outs=pltpu.VMEM((total, hidden), BF16),
        part=pltpu.VMEM((total, hidden), BF16),
        room=pltpu.VMEM((7 * rows, hidden), BF16),
        q=pltpu.VMEM((total, KEY_DIM), BF16),
        k=pltpu.VMEM((total, KEY_DIM), BF16),
        v=pltpu.VMEM((total, VAL_DIM), BF16),
        sc=pltpu.VMEM((total, SEQ_LEN), BF16),
        swish=pltpu.VMEM((total, VAL_DIM), F32),
        ghat=pltpu.VMEM((total, VAL_DIM), F32),
        ginv=pltpu.VMEM((total, 128), F32),
        gated=pltpu.VMEM((total, VAL_DIM), BF16),
        hid=pltpu.VMEM((total, WIDE), BF16),
        gate=pltpu.VMEM((TILE, WIDE), F32),
        up=pltpu.VMEM((TILE, WIDE), F32),
        gb=pltpu.VMEM((total, WIDE), BF16),
        ub=pltpu.VMEM((total, WIDE), BF16),
        sb=pltpu.VMEM((total, SEQ_LEN), BF16),
        qkb=pltpu.VMEM((total, 2 * KEY_DIM), BF16),
        turned=pltpu.VMEM((WIDE, total), BF16),
        st=pltpu.VMEM((4, WIDE, WIDE), BF16),
        decay=pltpu.VMEM((SEQ_LEN, SEQ_LEN), F32),
        low=pltpu.VMEM((rows, hidden), BF16),
        middle=pltpu.VMEM((rows, hidden), F32),
        back=pltpu.VMEM((rows, hidden), F32),
        pieces=pltpu.VMEM((4, 8, hidden), F32),
        gparts=pltpu.VMEM((8, 8, 256), F32),
        gain=pltpu.VMEM((8, hidden), F32),
        gsend=pltpu.VMEM((8, 8, 256), F32),
        gsum=pltpu.VMEM((4, 8, 256), F32),
        xr=pltpu.VMEM((rows, hidden), BF16),
        cr=pltpu.VMEM((rows, hidden), BF16),
        rows2=pltpu.VMEM((rows, hidden), BF16),
        cot2=pltpu.VMEM((rows, hidden), BF16),
        ub2=pltpu.VMEM((total, WIDE), BF16),
        gated2=pltpu.VMEM((total, VAL_DIM), BF16),
        hop_s=dma((9,)),
        hop_r=dma((9,)),
        gd_s=dma((13,)),
        gd_r=dma((13,)),
        gown=pltpu.VMEM((8, 256), F32),
        ex_s=dma((8,)),
        ex_r=dma((8,)),
        ex_l=dma((8,)),
        zs=dma((7, 2, 4)),
        zr=dma((7, 2, 4)),
        rs=dma((8, 3)),
        rr=dma((8, 4)),
        ra=dma((8, 3)),
        stl=dma((4,)),
        fl=dma((4,)),
        fe_s=dma((8,)),
        fe_r=dma((8,)),
        gg_s=dma((8,)),
        gg_r=dma((8,)),
        gt_s=dma((4,)),
        gt_r=dma((4,)),
        ga_s=dma((13,)),
        ga_r=dma((13,)),
        gc_s=dma((13,)),
        gc_r=dma((13,)),
        re_s=dma((10,)),
        re_r=dma((10,)),
        rf_s=dma((10,)),
        rf_r=dma((10,)),
        ol=dma((6,)),
        free=pltpu.SemaphoreType.REGULAR,
    )


class PlaneSum(Reduce):
    def __init__(self, place, part, room, rows, send, recv, y_first=False):
        p = place
        h = rows // 2
        self.rows, self.half, self.part, self.room, self.y_first = rows, h, part, room, y_first
        self.base = [p.block(j) * rows for j in range(4)]

        def remote(k, source, target_ref, target):
            return pltpu.make_async_remote_copy(
                src_ref=source,
                dst_ref=target_ref,
                send_sem=send.at[k],
                recv_sem=recv.at[k],
                device_id=target,
                device_id_type=MESH,
            )

        def piece(j, lo):
            return part.at[pl.ds(pl.multiple_of(self.base[j] + lo, 8), h)]

        def got(k, lo):
            return room.at[pl.ds((4 + k) * rows + lo, h)]

        def across(k):
            return room.at[pl.ds(6 * rows + k * h, h)]

        self.place, self.remote = p, remote
        self.swap = [
            remote(j, part.at[rows_of(p.block(j, 1), rows)], self.theirs(j), p.sib) for j in range(4)
        ]
        self.da = remote(4, piece(3, 0), across(0), p.yn if y_first else p.xn)
        self.db = remote(5, piece(3, h), across(1), p.yn)
        self.xa = remote(6, piece(1, 0), got(0, 0), p.xn)
        self.xb = remote(7, piece(1, h), got(0, h), p.xn)
        self.ya = remote(8, piece(2, 0), got(1, 0), p.yn)
        self.yb = remote(9, piece(2, h), got(1, h), p.yn)

    def theirs(self, j):
        return self.room.at[rows_of(j, self.rows)]

    def add(self, j, lo, n, first):
        def body(i):
            r = pl.ds(pl.multiple_of(self.base[j] + lo + i * CHUNK, CHUNK), CHUNK)
            q = pl.ds(pl.multiple_of(first + i * CHUNK, CHUNK), CHUNK)
            self.part[r] = (self.part[r].astype(F32) + self.room[q].astype(F32)).astype(BF16)

        loop(n // CHUNK, body)

    def start(self):
        for j in (3, 1, 2, 0):
            self.swap[j].start()

    def fill(self, tile_value, sending=None):
        def body(i):
            self.fill_chip(jnp.where(i == 0, 3, jnp.where(i == 3, 0, i)), tile_value, sending)

        loop(4, body)

    def chip(self, j):
        p = self.place
        chip_x = jnp.where(lax.rem(j, 2) == 1, 1 - p.x, p.x)
        chip_y = jnp.where(j >= 2, 1 - p.y, p.y)
        return chip_x * 2 + chip_y

    def fill_chip(self, j, tile_value, sending=None):
        chip = self.chip(j)
        r = at(chip, 2 * self.rows)

        def inner(n):
            c = at(n, WIDE)
            self.part[r, c] = tile_value(r, c).astype(BF16)

        loop(self.part.shape[1] // WIDE, inner)
        source = self.part.at[rows_of(chip * 2 + 1 - self.place.c, self.rows)]
        send = self.remote(j, source, self.theirs(j), self.place.sib)
        if sending is None:
            send.start()
        else:
            pl.when(sending)(send.start)

    def take(self, j):
        if self.y_first:
            copies = {3: (self.da, self.db), 1: (), 2: (self.ya, self.yb)}[j]
        else:
            copies = {3: (self.da, self.db), 1: (self.xa,), 2: (self.yb,)}[j]
        self.swap[j].wait_recv()
        self.add(j, 0, self.rows, j * self.rows)
        for copy in copies:
            copy.start()

    def run1(self):
        for j in (3, 1, 2):
            self.take(j)

    def run2(self):
        h, across = self.half, 6 * self.rows
        if self.y_first:
            self.da.wait_recv()
            self.add(1, 0, h, across)
            self.xa.start()
            self.db.wait_recv()
            self.add(1, h, h, across + h)
            self.xb.start()
            return
        self.db.wait_recv()
        self.add(1, h, h, across + h)
        self.xb.start()
        self.da.wait_recv()
        self.add(2, 0, h, across)
        self.ya.start()

    def run3(self):
        self.swap[0].wait_recv()
        for copy in (self.xa, self.yb, self.xb, self.ya):
            copy.wait_recv()

    def run(self):
        self.run1()
        self.run2()
        self.run3()

    def total(self, i):
        def at_row(first):
            return pl.ds(pl.multiple_of(first + i * CHUNK, CHUNK), CHUNK)

        n = self.rows
        pieces = (self.part[at_row(self.base[0])], *(self.room[at_row(k * n)] for k in (0, 4, 5)))
        one, two, three, four = (piece.astype(F32) for piece in pieces)
        return (one + two) + (three + four)


def mega_kernel(names, count_in, count_out, *refs):
    x_hbm, cot_hbm, counts_ref, cos_ref, sin_ref = refs[:5]
    gain_refs = refs[5:9]
    q_w, k_w, v_w, s_w, o_w, g_w, u_w, d_w = refs[9:count_in]
    outs = refs[count_in : count_in + count_out]
    final_out, delta_out, gains_out, q_g, k_g, v_g, s_g, o_g, g_g, u_g, d_g, stage, heard, added, parked = outs
    b = {name: ref for name, ref in zip(names, refs[count_in + count_out :], strict=True)}
    w, xs, xt, st, part, turned = b["w"], b["xs"], b["xt"], b["st"], b["part"], b["turned"]
    x_ref, cot_ref = b["xr"], b["cr"]
    rows, hidden = x_ref.shape
    width = hidden // 8

    dp, tensor = lax.axis_index("dp"), lax.axis_index("tensor")
    place = Place()
    x, z = place.x, dp // 2
    first_plane, inner = z == 0, (z == 1) | (z == 2)
    outer = jnp.logical_not(inner)

    barrier = pltpu.get_barrier_semaphore()
    for i in range(1, 8):
        other = (lax.rem(dp + i, 8), tensor)
        pl.semaphore_signal(barrier, inc=1, device_id=other, device_id_type=MESH)
    for i in range(1, 4):
        other = (dp, lax.rem(tensor + i, 4))
        pl.semaphore_signal(barrier, inc=1, device_id=other, device_id_type=MESH)

    def remote(source, target_ref, send, recv, target):
        return pltpu.make_async_remote_copy(
            src_ref=source,
            dst_ref=target_ref,
            send_sem=send,
            recv_sem=recv,
            device_id=target,
            device_id_type=MESH,
        )

    def plane(step):
        return ((z + step) * 2 + x, tensor)

    def column_exchange(n, weight, k, lane, half):
        where = w.at[k, pl.ds(pl.multiple_of(z * 512 + x * 256, 256), width), pl.ds(lane, half)]
        keep = pltpu.make_async_copy(weight.at[:, at(x, half)], where, b["ex_l"].at[n])
        give = remote(
            weight.at[:, at(1 - x, half)], where, b["ex_s"].at[n], b["ex_r"].at[n], place.xn
        )
        return keep, give

    def row_exchange(n, weight, k):
        where = w.at[k, at(z, 512), at(x, width)]
        keep = pltpu.make_async_copy(weight.at[at(x, 512)], where, b["ex_l"].at[n])
        give = remote(weight.at[at(1 - x, 512)], where, b["ex_s"].at[n], b["ex_r"].at[n], place.xn)
        return keep, give

    exchanges = [
        [column_exchange(0, q_w, QK, 0, 256), column_exchange(1, k_w, QK, 256, 256)],
        [column_exchange(2, v_w, VALUE, 0, 512)],
        [column_exchange(3, s_w, SWISH, 0, 512)],
        [row_exchange(4, o_w, OUTPUT)],
        [column_exchange(5, g_w, GATE, 0, 512)],
        [column_exchange(6, u_w, UP, 0, 512)],
        [row_exchange(7, d_w, DOWN)],
    ]

    def keep(k):
        for local, _ in exchanges[k]:
            local.start()

    def give(k):
        for _, send in exchanges[k]:
            send.start()

    towards = jnp.where(z == 1, -1, 1)
    near, far = jnp.where(z == 1, 2, 1), jnp.where(z == 1, 3, 0)
    own_steps = (
        jnp.where(first_plane, 2, jnp.where(inner, 1, -2)),
        jnp.where(first_plane, 1, -1),
    )
    beside = place.xn

    def parts(k):
        return (0, 1) if k == QK else (0,)

    def block_copy(k, block, half, slot, target):
        if k == QK:
            side = x if half == 0 else 1 - x
            ref = w.at[k, pl.ds(pl.multiple_of(block * 512 + side * 256, 256), 256)]
        else:
            ref = w.at[k, at(block, 512)]
        return remote(ref, ref, b["zs"].at[k, half, slot], b["zr"].at[k, half, block], target)

    def kept(k):
        for local, _ in exchanges[k]:
            local.wait()

    def swapped(k):
        for _, send in exchanges[k]:
            send.wait_recv()

    def spread_half(k, half):
        def both():
            for slot, step in enumerate(own_steps):
                block_copy(k, z, half, slot, plane(step)).start()

        if k in FEED_FORWARD:
            step = jnp.where(outer, jnp.where(first_plane, 1, -1), -towards)
            block_copy(k, z, half, 0, plane(step)).start()
        else:
            both()

    def spread(k):
        kept(k)
        swapped(k)
        spread_half(k, 0)

    def pass_on(k):
        @pl.when(inner)
        def _():
            for half in parts(k):
                for slot, block in ((2, near), (3, far)):
                    copy = block_copy(k, block, half, slot, plane(towards))
                    copy.wait_recv()
                    copy.start()

    def arrive(k):
        for half in parts(k):

            @pl.when(inner)
            def _(half=half):
                block_copy(k, jnp.where(z == 1, 0, 3), half, 0, beside).wait_recv()

            @pl.when(outer)
            def _(half=half):
                for i in range(3):
                    block = jnp.where(first_plane, i + 1, i)
                    block_copy(k, block, half, 0, beside).wait_recv()

    def pass_inner(k):
        copy = block_copy(k, jnp.where(z == 1, 0, 3), 0, 1, plane(-towards))
        copy.wait_recv()
        copy.start()

    def arrive_inner(k):
        for block in (near, far):
            block_copy(k, block, 0, 0, beside).wait_recv()

    def weights_sent():
        for k in range(7):
            for _, send in exchanges[k]:
                send.wait_send()
            for half in parts(k):
                block_copy(k, z, half, 0, beside).wait_send()
                if k in FEED_FORWARD:
                    pl.when(inner)(lambda k=k, half=half: block_copy(k, z, half, 1, beside).wait_send())
                else:
                    block_copy(k, z, half, 1, beside).wait_send()

                    @pl.when(inner)
                    def _(k=k, half=half):
                        for slot in (2, 3):
                            block_copy(k, z, half, slot, beside).wait_send()

    def lanes_of(c):
        if c in (QUERY, KEY):
            return QK, pl.ds(256 * (c - QUERY), 256)
        return c, pl.ds(0, 512)

    def share(ref, c, *index):
        chunk, lanes = lanes_of(c)
        return ref.at[(chunk, *index, slice(None), lanes)]

    def slot_of(c, slot):
        return st.at[slot, :, pl.ds(0, 256 if c in (QUERY, KEY) else 512)]

    def number(c):
        return c if c < QUERY else c - QUERY + (0 if c == QUERY else 6)

    def staged(c, block, slot):
        return pltpu.make_async_copy(slot_of(c, slot), share(stage, c, block), b["stl"].at[slot])

    def to_added(c, block, which, target, slot=None):
        n = number(c)
        return remote(
            share(stage, c, block),
            share(added, c, which),
            b["rs"].at[n, which if slot is None else slot],
            b["ra"].at[n, which],
            target,
        )

    def to_heard(c, block, slot, target):
        n = number(c)
        return remote(
            share(stage, c, block), share(heard, c, z), b["rs"].at[n, slot], b["rr"].at[n, z], target
        )

    def all_staged(c):
        for block in range(PLANES):
            staged(c, block, block).wait()

    def send_gradient(c):
        all_staged(c)
        step = jnp.where(first_plane, 1, -1)

        @pl.when(outer)
        def _():
            to_added(c, 3 - z, 0, plane(step)).start()
            to_added(c, z + 2 * step, 1, plane(step)).start()
            to_heard(c, z + step, 2, plane(step)).start()

    def send_inner(c):
        to_added(c, far, 2, plane(-towards), 0).start()
        to_heard(c, near, 1, plane(-towards)).start()

    def rounds(c, body):
        lanes = 256 if c in (QUERY, KEY) else 512

        def step(i):
            body(pl.ds(pl.multiple_of(i * 32, 32), 32), pl.ds(0, lanes))

        loop(WIDE // 32, step)

    def local(source, target, n):
        return pltpu.make_async_copy(source, target, b["fl"].at[n])

    def combine(c):
        @pl.when(inner)
        def _():
            blocks = (far, near)
            mine = [local(share(stage, c, blocks[i]), slot_of(c, i), i) for i in range(2)]
            for copy in mine:
                copy.start()
            theirs = [local(share(added, c, i), slot_of(c, 2 + i), 2 + i) for i in range(2)]
            for i in range(2):
                to_added(c, blocks[i], i, beside).wait_recv()
                theirs[i].start()
            for i in range(2):
                mine[i].wait()
                theirs[i].wait()

                def body(r, lanes, i=i):
                    st[i, r, lanes] = (
                        st[i, r, lanes].astype(F32) + st[2 + i, r, lanes].astype(F32)
                    ).astype(BF16)

                rounds(c, body)
                back = local(slot_of(c, i), share(stage, c, blocks[i]), i)
                back.start()
            for i in range(2):
                local(slot_of(c, i), share(stage, c, blocks[i]), i).wait()
            send_inner(c)

    def combine_inner(c):
        block = z + towards
        mine = local(share(stage, c, block), slot_of(c, 0), 0)
        theirs = local(share(added, c, 2), slot_of(c, 1), 1)
        mine.start()
        to_added(c, block, 2, beside, 0).wait_recv()
        theirs.start()
        mine.wait()
        theirs.wait()

        def body(r, lanes):
            st[0, r, lanes] = (
                st[0, r, lanes].astype(F32) + st[1, r, lanes].astype(F32)
            ).astype(BF16)

        rounds(c, body)
        back = local(slot_of(c, 0), share(stage, c, block), 0)
        back.start()
        back.wait()
        to_heard(c, block, 2, plane(towards)).start()

    homes = {
        QUERY: q_g, KEY: k_g, VALUE: v_g, SWISH: s_g, OUTPUT: o_g, GATE: g_g, UP: u_g, DOWN: d_g
    }

    def home_copies(c, source):
        home, (_, lanes) = homes[c], lanes_of(c)
        if c in (OUTPUT, DOWN):
            kept_half, given_half = (slice(None), at(x, 256)), (slice(None), at(1 - x, 256))
            slot = home.at[at(x, 512)]
        else:
            kept_half, given_half = (at(x, 256),), (at(1 - x, 256),)
            slot = home.at[:, at(x, home.shape[1] // 2)]
        n = number(c)
        return (
            local(slot_of(c, 0).at[kept_half], slot, 3),
            remote(source.at[given_half], slot, b["fe_s"].at[n], b["fe_r"].at[n], beside),
        )

    def finish_gradient(c, last=False):
        n = number(c)

        def own_load():
            return local(share(stage, c, z), slot_of(c, 0), 0)

        def arrival(i, source):
            remote(
                share(stage, c, 0), share(heard, c, source), b["rs"].at[n, 2], b["rr"].at[n, source], beside
            ).wait_recv()
            load = local(share(heard, c, source), slot_of(c, i), i)
            load.start()
            return load

        source = jnp.where((z == 0) | (z == 2), 1, 2)
        if c in INNER_SUMS:

            @pl.when(outer)
            def _():
                arrival(0, source).wait()

        else:

            @pl.when(outer)
            def _():
                own_load().start()
                arrival(1, source).wait()
                own_load().wait()

                def body(r, lanes):
                    st[0, r, lanes] = (
                        st[0, r, lanes].astype(F32) + st[1, r, lanes].astype(F32)
                    ).astype(BF16)

                rounds(c, body)

        @pl.when(inner)
        def _():
            own_load().start()
            loads = [arrival(1, source)]
            if c not in INNER_SUMS:
                loads.append(arrival(2, jnp.where(z == 1, 0, 3)))
            own_load().wait()
            for load in loads:
                load.wait()

            def body(r, lanes):
                acc = st[0, r, lanes].astype(F32) + st[1, r, lanes].astype(F32)
                if c not in INNER_SUMS:
                    acc = acc + st[2, r, lanes].astype(F32)
                st[0, r, lanes] = acc.astype(BF16)

            rounds(c, body)

        source = slot_of(c, 0) if last else share(stage, c, z)
        stay, send = home_copies(c, source)
        if not last:
            store = local(slot_of(c, 0), share(stage, c, z), 0)
            store.start()
            stay.start()
            store.wait()
            send.start()
            stay.wait()
        else:
            send.start()
            stay.start()
            stay.wait()

    def gradients_done():
        for c in GRADIENTS:
            n = number(c)
            source = slot_of(c, 0) if c == KEY else share(stage, c, z)
            _, send = home_copies(c, source)
            send.wait()

            def sent(c=c, n=n):
                for slot in range(3):
                    remote(
                        share(stage, c, 0), share(heard, c, 0), b["rs"].at[n, slot], b["rr"].at[n, 0], beside
                    ).wait_send()

            if c in INNER_SUMS:
                pl.when(inner)(sent)
            else:
                sent()

    across_step = jnp.where(outer, jnp.where(first_plane, 1, -1), towards)

    def hop(n, source, target, part_of=slice(None)):
        return remote(
            source.at[part_of], target.at[part_of], b["hop_s"].at[n], b["hop_r"].at[n], plane(across_step)
        )

    halves = (pl.ds(0, rows // 2), pl.ds(rows // 2, rows // 2))

    def neighbours_may_write():
        for partner in (place.sib, place.xn, place.yn):
            pl.semaphore_signal(b["free"], inc=1, device_id=partner, device_id_type=MESH)

    def may_write():
        pl.semaphore_wait(b["free"], 3)

    def gain_copy(i):
        target = lax.rem(dp + i, 8)
        return remote(
            b["gown"], b["gparts"].at[dp], b["gg_s"].at[i], b["gg_r"].at[dp], (target, tensor)
        )

    def gain_arrival(i):
        source = lax.rem(dp + i, 8)
        return remote(
            b["gown"], b["gparts"].at[source], b["gg_s"].at[i], b["gg_r"].at[source], (source, tensor)
        )

    gather_sems = (b["ga_s"], b["ga_r"])

    def plane_sum(ref, y_first=False):
        return PlaneSum(place, ref, b["room"], rows, b["re_s"], b["re_r"], y_first)

    for k in range(7):
        keep(k)
    gown = b["gown"]
    for n in range(8):
        gown[n : n + 1, :] = gain_refs[n % 4][...].astype(F32).reshape(1, 256)
    load_x = pltpu.make_async_copy(x_hbm, x_ref, b["ol"].at[3])
    load_cot = pltpu.make_async_copy(cot_hbm, cot_ref, b["ol"].at[4])
    load_x.start()
    load_cot.start()
    mine = pltpu.make_async_copy(gown, b["gparts"].at[dp], b["ol"].at[0])
    mine.start()
    kept(QK)
    pl.semaphore_wait(barrier, 10)
    for i in range(1, 8):
        gain_copy(i).start()
    give(QK)
    spread_half(QK, 0)
    give(VALUE)
    head = (tensor * 2 + x).astype(F32)
    rate = jnp.log(1.0 - jnp.exp2(-5.0 - jnp.full((8, SEQ_LEN), head, F32)))[0:1]

    def body(i):
        r = at(i, 64)
        n = lax.broadcasted_iota(jnp.int32, (64, SEQ_LEN), 0) + i * 64
        m = lax.broadcasted_iota(jnp.int32, (64, SEQ_LEN), 1)
        gap = n - m
        b["decay"][r] = jnp.where(gap >= 0, jnp.exp(jnp.maximum(gap, 0).astype(F32) * rate), 0.0)

    loop(SEQ_LEN // 64, body)
    load_x.wait()
    swapped(QK)
    spread_half(QK, 1)
    mine.wait()
    for i in range(1, 8):
        gain_arrival(i).wait_recv()
    for i in range(8):
        b["gain"][:, i * 256 : (i + 1) * 256] = b["gparts"][i]
    gain = b["gain"]
    low = b["low"]

    def body(i):
        r = at(i, CHUNK)
        hat, _ = normalize(x_ref[r].astype(F32), EPSILON)
        low[r] = (hat * gain[0:1, :] + gain[1:2, :]).astype(BF16)

    loop(rows // CHUNK, body)
    first = Gather(place, low, xs, *gather_sems)
    first.start()
    spread(VALUE)
    load_cot.wait()
    count = counts_ref[0]

    def body(i):
        r = at(i, CHUNK)
        row = lax.broadcasted_iota(jnp.int32, (CHUNK, hidden), 0) + (tensor * rows + i * CHUNK)
        cot_ref[r] = jnp.where(row < count, cot_ref[r].astype(F32), 0.0).astype(BF16)

    loop(rows // CHUNK, body)
    pl.when(outer)(lambda: hop(2, cot_ref, b["cot2"]).start())
    first.forward()
    for k in range(SWISH, DOWN + 1):
        give(k)
    cotangent = Gather(place, cot_ref, b["outs"], b["gc_s"], b["gc_r"])
    pl.when(inner)(cotangent.start)
    pass_on(QK)
    spread(SWISH)
    first.finish()

    def turned_rows(i):
        return at(i // 2, 512), at(lax.rem(i, 2), 8 * rows)

    def body(i):
        r, lanes = turned_rows(i // 2)
        r = pl.ds(pl.multiple_of((i // 4) * 512 + lax.rem(i, 2) * 256, 256), 256)
        xt[r, lanes] = xs[:, at(i, 256)].T

    loop(hidden // 256, body)
    park = pltpu.make_async_copy(xt, parked, b["ol"].at[5])
    unpark = pltpu.make_async_copy(parked, xt, b["ol"].at[0])
    pl.when(inner)(park.start)
    spread(OUTPUT)

    arrive(QK)

    def turn(acc, tile, scale):
        spot = at(lax.rem(tile, SEQ_LEN // TILE), TILE)
        cos, sin = cos_ref[spot], sin_ref[spot]
        one, two = acc[:, :128], acc[:, 128:]
        return (((one * cos - two * sin) * scale).astype(BF16), ((two * cos + one * sin) * scale).astype(BF16))

    def body(i):
        r = at(i, TILE)
        acc = matmul(xs[r], w[QK])
        b["q"][r, :128], b["q"][r, 128:] = turn(acc[:, :KEY_DIM], i, 1.0)
        b["k"][r, :128], b["k"][r, 128:] = turn(acc[:, KEY_DIM:], i, KEY_DIM ** (-0.5))

    tiles = 8 * rows // TILE
    per_slot = SEQ_LEN // TILE
    loop(tiles, body)

    def slot_rows(i):
        return at(i // per_slot, SEQ_LEN)

    def body(i):
        r = at(i, TILE)
        decay = b["decay"][at(lax.rem(i, per_slot), TILE)]
        b["sc"][r] = (nt(b["q"][r], b["k"][slot_rows(i)]) * decay).astype(BF16)

    loop(tiles, body)

    for k in (GATE, UP, DOWN):
        spread(k)
    pass_on(VALUE)
    arrive(VALUE)

    def body(i):
        r = at(i, TILE)
        b["v"][r] = matmul(xs[r], w[VALUE]).astype(BF16)

    loop(tiles, body)

    def body(i):
        r = at(i, TILE)
        retained = matmul(b["sc"][r], b["v"][slot_rows(i)])
        hat, inverse = normalize(retained, GROUP_EPSILON)
        b["ghat"][r] = hat
        b["ginv"][r] = jnp.broadcast_to(inverse, (TILE, 128))

    loop(tiles, body)
    @pl.when(inner)
    def _():
        cotangent.forward()
        cotangent.finish()

    pass_on(SWISH)
    arrive(SWISH)

    def body(i):
        r = at(i, TILE)
        swish = matmul(xs[r], w[SWISH])
        b["swish"][r] = swish
        b["gated"][r] = (swish * jax.nn.sigmoid(swish) * b["ghat"][r]).astype(BF16)

    loop(tiles, body)

    pass_on(OUTPUT)
    arrive(OUTPUT)

    def grid_of(i):
        return at(i // PLANES, TILE), at(lax.rem(i, PLANES), 512)

    reduce = plane_sum(part)
    reduce.fill(lambda r, c: matmul(b["gated"][r], w[OUTPUT, c]))
    reduce.run()
    def body(i):
        r = at(i, CHUNK)
        middle = x_ref[r].astype(F32) + reduce.total(i)
        b["middle"][r] = middle
        hat, _ = normalize(middle, EPSILON)
        low[r] = (hat * gain[2:3, :] + gain[3:4, :]).astype(BF16)

    loop(rows // CHUNK, body)

    @pl.when(outer)
    def _():
        for n in range(2):
            hop(n, low, b["rows2"], halves[n]).start()
        hop(6, b["gated"], b["gated2"]).start()

    pl.when(inner)(lambda: pass_inner(GATE))

    def gelu_of(t):
        inner_value = 0.7978845608028654 * (t + 0.044715 * t * t * t)
        tanh = jnp.tanh(inner_value)
        return 0.5 * (1.0 + tanh), tanh

    def turned_of(ref):
        def body(i):
            turned[:, at(i, TILE)] = ref[at(i, TILE)].T

        loop(tiles, body)

    def stage_block(c, i, value):
        st[i] = value.astype(BF16)
        staged(c, i, i).start()

    def times_turned(left, r, k):
        acc = nt(left[r, 0:512], w[k, 0:512])
        for plane_at in range(1, PLANES):
            lanes = slice(plane_at * 512, plane_at * 512 + 512)
            acc = acc + nt(left[r, lanes], w[k, lanes])
        return acc

    def hidden_tile(mixer, hid, r):
        gate = matmul(mixer[r], w[GATE])
        b["gate"][...] = gate
        up = matmul(mixer[r], w[UP])
        b["up"][...] = up
        gate = b["gate"][...]
        share_of, _ = gelu_of(gate)
        hid[r] = (gate * share_of * up).astype(BF16)

    def back_tile(cots, gb, ub, r):
        back = times_turned(cots, r, DOWN)
        gate, up = b["gate"][...], b["up"][...]
        share_of, tanh = gelu_of(gate)
        slope = 0.5 * gate * (1.0 - tanh * tanh) * (0.7978845608028654 * (1.0 + 0.134145 * gate * gate))
        gb[r] = (back * up * (share_of + slope)).astype(BF16)
        ub[r] = (back * gate * share_of).astype(BF16)

    def refill(c):
        copies = [pltpu.make_async_copy(stage.at[c, i], st.at[i], b["fl"].at[i]) for i in range(PLANES)]
        for copy in copies:
            copy.start()
        for copy in copies:
            copy.wait()

    def product_of(c, i, value, more):
        stage_block(c, i, value + st[i].astype(F32) if more else value)

    def down_gradient(hid, cots, more):
        if more:
            refill(DOWN)
        turned_of(hid)

        def body(i):
            product_of(DOWN, i, matmul(turned[...], cots[:, at(i, 512)]), more)

        loop(PLANES, body)
        all_staged(DOWN)

    def weight_gradient(c, mixer, right, more):
        if more:
            refill(c)

        def body(i):
            def body_turn(j):
                turned[:, at(j, TILE)] = mixer[at(j, TILE), at(i, 512)].T

            loop(tiles, body_turn)
            product_of(c, i, matmul(turned[...], right[...]), more)

        loop(PLANES, body)
        all_staged(c)

    def mixer_input(gb, ub):
        return lambda r, c: nt(gb[r], w[GATE, c]) + nt(ub[r], w[UP, c])

    def mixer_output(hid, target):
        def body(i):
            r, c = grid_of(i)
            target[r, c] = matmul(hid[r], w[DOWN, c]).astype(BF16)

        loop(tiles * PLANES, body)

    b["pieces"][...] = jnp.zeros_like(b["pieces"])

    def second_norm_backward(r, upstream):
        hat, inverse = normalize(b["middle"][r], EPSILON)
        scaled = upstream * hat
        b["pieces"][2] += scaled[0:8] + scaled[8:16]
        b["pieces"][3] += upstream[0:8] + upstream[8:16]
        back = cot_ref[r].astype(F32) + normalize_back(upstream * gain[2:3, :], hat, inverse)
        b["back"][r] = back
        low[r] = back.astype(BF16)

    hid2, gb2, ub2 = b["sb"], b["qkb"], b["ub2"]
    outs_ref = b["outs"]

    @pl.when(inner)
    def _():
        second = Gather(place, low, xs, *gather_sems)
        second.start()
        hop(2, cot_ref, b["cot2"]).wait_recv()
        second.forward()
        pass_inner(UP)
        other_cot = Gather(place, b["cot2"], part, b["gc_s"], b["gc_r"])
        reduce.finish()
        neighbours_may_write()
        may_write()
        other_cot.start()
        pass_inner(DOWN)
        second.finish()
        arrive_inner(GATE)
        arrive_inner(UP)
        other_cot.forward()
        arrive_inner(DOWN)

        def body(i):
            r = at(i, TILE)
            hidden_tile(xs, b["hid"], r)
            back_tile(outs_ref, b["gb"], b["ub"], r)

        loop(tiles, body)
        down_gradient(b["hid"], outs_ref, False)
        neighbours_may_write()
        other_cot.finish()
        other = Gather(place, b["rows2"], outs_ref, b["gd_s"], b["gd_r"])
        may_write()
        for n in range(2):
            hop(n, low, b["rows2"], halves[n]).wait_recv()
        other.start()
        weight_gradient(GATE, xs, b["gb"], False)
        other.forward_across()
        other.own_arrived()
        park.wait()
        reduce2 = plane_sum(xt)

        def body(i):
            pl.when(i == 1)(lambda: together(other.forward_beside, other.s1.wait_recv))
            pl.when(i == 2)(other.s2.wait_recv)
            pl.when(i == 3)(other.across_arrived)
            r = at(reduce2.chip(i), TILE)
            hidden_tile(outs_ref, hid2, r)
            back_tile(part, gb2, ub2, r)
            reduce2.fill_chip(i, mixer_input(gb2, ub2))
            pl.when(i == 2)(lambda: reduce2.take(1))
            pl.when(i == 3)(lambda: reduce2.take(2))

        loop(PLANES, body)
        reduce2.take(3)
        down_gradient(hid2, part, True)
        send_inner(DOWN)
        reduce2.run2()
        weight_gradient(UP, xs, b["ub"], False)
        reduce2.run3()
        for n in range(2):

            def body(i, n=n):
                i = n * (rows // 2 // CHUNK) + i
                b["rows2"][at(i, CHUNK)] = reduce2.total(i).astype(BF16)

            other.drain() if n == 0 else None
            loop(rows // 2 // CHUNK, body)
            hop(3 + n, b["rows2"], b["rows2"], halves[n]).start()
        reduce2.finish()
        unpark.start()
        neighbours_may_write()
        may_write()
        reduce3 = plane_sum(part)
        reduce3.fill(mixer_input(b["gb"], b["ub"]))
        reduce3.run1()
        weight_gradient(GATE, outs_ref, gb2, True)
        send_inner(GATE)
        reduce3.run2()
        weight_gradient(UP, outs_ref, ub2, True)
        send_inner(UP)
        combine_inner(DOWN)
        reduce3.run3()

        def body(i):
            second_norm_backward(at(i, CHUNK), reduce3.total(i))

        loop(rows // CHUNK, body)
        reduce3.finish()
        neighbours_may_write()
        may_write()
        hop(7, low, b["cot2"]).wait_recv()

    third = Gather(place, low, xs, *gather_sems)
    other_middle = Gather(place, b["cot2"], part, b["gd_s"], b["gd_r"])
    outs_ref = b["outs"]

    @pl.when(outer)
    def _():
        reduce.finish()
        for n in range(2):
            hop(n, low, b["rows2"], halves[n]).wait_send()
        for n in range(2):
            hop(3 + n, b["rows2"], b["rows2"], halves[n]).wait_recv()

            def body(i, n=n):
                r = pl.ds(pl.multiple_of(n * (rows // 2) + i * CHUNK, CHUNK), CHUNK)
                second_norm_backward(r, b["rows2"][r].astype(F32))

            loop(rows // 2 // CHUNK, body)
            if n == 0:
                third.start_first_half()
            else:
                third.start_second_half()
                hop(7, low, b["cot2"]).start()
        third.forward()
        third.finish()

    def output_gradient(rows_ref, cots, more):
        if more:
            refill(OUTPUT)
        turned_of(rows_ref)

        def body(i):
            product_of(OUTPUT, i, matmul(turned[...], cots[:, at(i, 512)]), more)

        loop(PLANES, body)
        all_staged(OUTPUT)

    reduce5 = plane_sum(outs_ref, y_first=True)

    @pl.when(inner)
    def _():
        third.start()
        mixer_output(hid2, outs_ref)
        third.forward_across()
        combine_inner(GATE)
        third.forward_beside()
        third.finish()
        other_middle.start()

    swb, rb, vlow = b["gb"], b["ub2"], b["ub"]

    def body(i):
        r = at(i, TILE)
        back = times_turned(xs, r, OUTPUT)
        swish, hat = b["swish"][r], b["ghat"][r]
        gate = jax.nn.sigmoid(swish)
        swb[r] = (back * hat * gate * (1.0 + swish * (1.0 - gate))).astype(BF16)
        rb[r] = normalize_back(back * swish * gate, hat, b["ginv"][r, 0:1]).astype(BF16)

    loop(tiles, body)

    def projection_gradient(c, right, lanes=slice(None)):
        def body(i):
            value = matmul(xt[turned_rows(i)], right[:, lanes]).astype(BF16)
            st[i, :, 0 : value.shape[1]] = value
            staged(c, i, i).start()

        loop(PLANES, body)
        send_gradient(c)

    pl.when(inner)(unpark.wait)
    projection_gradient(SWISH, swb)
    pl.when(inner)(other_middle.forward_across)
    combine(SWISH)

    @pl.when(inner)
    def _():
        other_middle.forward_beside()
        finish_gradient(DOWN)
        finish_gradient(GATE)
        output_gradient(b["gated"], xs, False)
        other_middle.finish()
        reduce5.start()
        hop(6, b["gated"], b["gated2"]).wait_recv()
        output_gradient(b["gated2"], part, True)
        send_inner(OUTPUT)
        combine_inner(UP)
        reduce5.run1()

    def body(i):
        r = at(i, TILE)
        decay = b["decay"][at(lax.rem(i, per_slot), TILE)]
        b["sb"][r] = (nt(rb[r], b["v"][slot_rows(i)]) * decay).astype(BF16)

    loop(tiles, body)
    turned_of(b["sc"])

    def body(i):
        vlow[at(i, TILE)] = matmul(
            turned[at(lax.rem(i, per_slot), TILE), slot_rows(i)], rb[slot_rows(i)]
        ).astype(BF16)

    loop(tiles, body)
    projection_gradient(VALUE, vlow)
    pl.when(inner)(lambda: combine_inner(SWISH))
    turned_of(b["sb"])

    def turn_back(acc, tile, scale):
        spot = at(lax.rem(tile, per_slot), TILE)
        cos, sin = cos_ref[spot], sin_ref[spot]
        one, two = acc[:, :128], acc[:, 128:]
        return (((one * cos + two * sin) * scale).astype(BF16), ((two * cos - one * sin) * scale).astype(BF16))

    def body(i):
        r = at(i, TILE)
        qkb = b["qkb"]
        query = matmul(b["sb"][r], b["k"][slot_rows(i)])
        qkb[r, 0:128], qkb[r, 128:256] = turn_back(query, i, 1.0)
        key = matmul(turned[at(lax.rem(i, per_slot), TILE), slot_rows(i)], b["q"][slot_rows(i)])
        qkb[r, 256:384], qkb[r, 384:512] = turn_back(key, i, KEY_DIM ** (-0.5))

    loop(tiles, body)
    projection_gradient(QUERY, b["qkb"], slice(0, 256))
    projection_gradient(KEY, b["qkb"], slice(256, 512))
    pl.when(inner)(reduce5.run2)
    combine(VALUE)
    reduce6 = PlaneSum(place, outs_ref, xt, rows, b["rf_s"], b["rf_r"], y_first=True)
    pl.when(inner)(lambda: finish_gradient(UP))

    reduce = plane_sum(part)
    reduce.fill(
        lambda r, c: nt(b["qkb"][r], w[QK, c]) + nt(vlow[r], w[VALUE, c]) + nt(swb[r], w[SWISH, c]),
        sending=outer,
    )

    @pl.when(inner)
    def _():
        reduce5.run3()

        def body(i):
            b["cot2"][at(i, CHUNK)] = reduce5.total(i).astype(BF16)

        loop(rows // CHUNK, body)
        hop(5, b["cot2"], b["cot2"]).start()
        reduce5.finish()
        neighbours_may_write()
        may_write()
        reduce.start()

    def delta_rows():
        reduce.run3()

        def body(i):
            r = at(i, CHUNK)
            upstream = reduce.total(i)
            hat, inverse = normalize(x_ref[r].astype(F32), EPSILON)
            scaled = upstream * hat
            b["pieces"][0] += scaled[0:8] + scaled[8:16]
            b["pieces"][1] += upstream[0:8] + upstream[8:16]
            b["back"][r] += normalize_back(upstream * gain[0:1, :], hat, inverse)

        loop(rows // CHUNK, body)
        reduce.finish()
        delta_copy().start()
        share_gains()

    def delta_copy():
        return pltpu.make_async_copy(b["back"], delta_out, b["ol"].at[2])

    def final_copy():
        return pltpu.make_async_copy(b["middle"], final_out, b["ol"].at[1])

    gsend, gparts, gsum = b["gsend"], b["gparts"], b["gsum"]

    def share_copy(i):
        target = lax.rem(dp + i, 8)
        return remote(
            gsend.at[target], gparts.at[dp], b["gg_s"].at[i], b["gg_r"].at[dp], (target, tensor)
        )

    def share_gains():
        for i in range(1, 8):
            gain_copy(i).wait_send()
        for i in range(8):
            for n in range(4):
                lanes = slice(i * 256, i * 256 + 256)
                gsend[i, n : n + 1, :] = jnp.sum(b["pieces"][n, :, lanes], axis=0, keepdims=True)
                gsend[i, n + 4 : n + 5, :] = jnp.zeros((1, 256), F32)
        for i in range(1, 8):
            share_copy(i).start()

    @pl.when(outer)
    def _():
        finish_gradient(DOWN)
        reduce.run1()
        finish_gradient(GATE)
        reduce.run2()
        delta_rows()
        finish_gradient(UP)
        finish_gradient(SWISH)
        hop(2, cot_ref, b["cot2"]).wait_send()
        hop(5, b["cot2"], b["cot2"]).wait_recv()

        def body(i):
            r = at(i, CHUNK)
            b["middle"][r] += b["cot2"][r].astype(F32)

        loop(rows // CHUNK, body)
        final_copy().start()
        finish_gradient(OUTPUT)
        finish_gradient(VALUE)

    @pl.when(inner)
    def _():
        combine_inner(OUTPUT)
        reduce.run1()
        combine(QUERY)
        reduce6.fill(lambda r, c: matmul(b["hid"][r], w[DOWN, c]))
        reduce.run2()
        reduce6.run1()
        combine_inner(VALUE)
        finish_gradient(SWISH)
        combine(KEY)
        delta_rows()
        combine_inner(QUERY)
        reduce6.run2()
        finish_gradient(OUTPUT)
        combine_inner(KEY)
        finish_gradient(VALUE)
        reduce6.run3()

        def body(i):
            b["middle"][at(i, CHUNK)] += reduce6.total(i)

        loop(rows // CHUNK, body)
        reduce6.finish()
        final_copy().start()

    finish_gradient(QUERY)
    acc = gsend[dp]
    for i in range(1, 8):
        gain_arrival(i).wait_recv()
        acc = acc + gparts[lax.rem(dp + i, 8)]
    gsum[tensor] = acc

    def sum_copy(i, source):
        target = lax.rem(tensor + i, 4)
        return remote(
            gsum.at[source], gsum.at[source], b["gt_s"].at[i], b["gt_r"].at[source], (dp, target)
        )

    for i in range(1, 4):
        sum_copy(i, tensor).start()
    finish_gradient(KEY, last=True)
    for i in range(1, 4):
        sum_copy(i, lax.rem(tensor + i, 4)).wait_recv()
    for i in range(1, 4):
        sum_copy(i, tensor).wait_send()
    for i in range(1, 8):
        share_copy(i).wait_send()
    gains_out[...] = (gsum[0] + gsum[1]) + (gsum[2] + gsum[3])
    final_copy().wait()
    delta_copy().wait()
    weights_sent()

    @pl.when(inner)
    def _():
        for n in range(2):
            hop(3 + n, b["rows2"], b["rows2"], halves[n]).wait_send()
        hop(5, b["cot2"], b["cot2"]).wait_send()

    @pl.when(outer)
    def _():
        hop(6, b["gated"], b["gated2"]).wait_send()
        hop(7, low, b["cot2"]).wait_send()

    gradients_done()


def whole_layer(
    incoming_signals,
    loss_sensitivity,
    token_counts_per_slot,
    leading_norm_multiplier,
    leading_norm_offset,
    question_projection,
    lookup_projection,
    content_projection,
    silu_switch_projection,
    retention_result_projection,
    trailing_norm_multiplier,
    trailing_norm_offset,
    feedforward_switch_projection,
    expanding_projection,
    contracting_projection,
):
    rows, hidden = incoming_signals.shape
    places = np.arange(SEQ_LEN, dtype=np.float32)
    middle = KEY_DIM // 2
    spectrum = np.float32(10000.0) ** (-np.arange(middle, dtype=np.float32) / np.float32(middle))
    angles = places[:, None] * spectrum[None, :]
    weights = (
        question_projection,
        lookup_projection,
        content_projection,
        silu_switch_projection,
        retention_result_projection,
        feedforward_switch_projection,
        expanding_projection,
        contracting_projection,
    )
    gains = (
        leading_norm_multiplier, leading_norm_offset, trailing_norm_multiplier, trailing_norm_offset
    )
    tables = (jnp.asarray(np.cos(angles)), jnp.asarray(np.sin(angles)))
    args = (incoming_signals, loss_sensitivity, token_counts_per_slot, *tables, *gains, *weights)
    scratch = mega_scratch(rows, hidden)
    shape = jax.ShapeDtypeStruct
    outs = (
        shape((rows, hidden), F32),
        shape((rows, hidden), F32),
        shape((8, 256), F32),
        *(shape(weight.shape, BF16) for weight in weights),
        shape((7, PLANES, WIDE, WIDE), BF16),
        shape((7, PLANES, WIDE, WIDE), BF16),
        shape((7, 3, WIDE, WIDE), BF16),
        shape((8 * rows, hidden), BF16),
    )
    scalar = pl.BlockSpec(memory_space=pltpu.SMEM)
    results = pl.pallas_call(
        functools.partial(mega_kernel, tuple(scratch), len(args), len(outs)),
        out_shape=outs,
        in_specs=[ANY, ANY, scalar] + [VM] * 6 + [ANY] * 8,
        out_specs=tuple([ANY, ANY, VM] + [ANY] * 12),
        scratch_shapes=list(scratch.values()),
        compiler_params=pltpu.CompilerParams(
            collective_id=0, has_side_effects=True, vmem_limit_bytes=67043328
        ),
        name="whole_layer",
    )(*args)
    final_rows, delta, gain_sums = results[:3]
    gain = shape((256,), F32)
    owned = results[3:11]
    wide = pl.pallas_call(
        widen_kernel,
        out_shape=(
            shape((rows, hidden), BF16),
            shape((rows, hidden), F32),
            *(shape(weight.shape, F32) for weight in weights),
            *[gain] * 4,
        ),
        in_specs=[scalar, VM] + [ANY] * 10,
        out_specs=(ANY,) * 10 + (VM,) * 4,
        scratch_shapes=[
            pltpu.VMEM((rows, hidden), F32),
            pltpu.VMEM((rows, hidden), F32),
            pltpu.VMEM((rows, hidden), BF16),
            *(pltpu.VMEM(weight.shape, BF16) for weight in weights),
            *(pltpu.VMEM(weight.shape, F32) for weight in weights),
            pltpu.SemaphoreType.DMA((10,)),
            pltpu.SemaphoreType.DMA((10,)),
        ],
        compiler_params=pltpu.CompilerParams(vmem_limit_bytes=67043328),
        name="widen",
    )(token_counts_per_slot, gain_sums, final_rows, delta, *owned)
    query, key, value, swish, output, gate, up, down = wide[2:10]
    gain_sums = wide[10:]
    return (
        wide[0],
        wide[1],
        gain_sums[0],
        gain_sums[1],
        query,
        key,
        value,
        swish,
        output,
        gain_sums[2],
        gain_sums[3],
        gate,
        up,
        down,
    )


def widen_kernel(counts_ref, gains_ref, *refs):
    sources, targets, gain_refs, scratch = refs[:10], refs[10:20], refs[20:24], refs[24:]
    for n, gain_ref in enumerate(gain_refs):
        gain_ref[...] = gains_ref[n, :]
    final, delta, low = scratch[:3]
    narrow, wide, (came, went) = scratch[3:11], scratch[11:19], scratch[19:]
    buffers = (final, delta, *narrow)
    loads = [
        pltpu.make_async_copy(source, buffer, came.at[i])
        for i, (source, buffer) in enumerate(zip(sources, buffers, strict=True))
    ]
    stores = [
        pltpu.make_async_copy(buffer, target, went.at[i])
        for i, (buffer, target) in enumerate(zip((low, delta, *wide), targets, strict=True))
    ]
    for load in loads:
        load.start()
    rows, hidden = final.shape
    tensor, count = lax.axis_index("tensor"), counts_ref[0]
    loads[0].wait()

    def body(i):
        r = at(i, CHUNK)
        row = lax.broadcasted_iota(jnp.int32, (CHUNK, hidden), 0) + (tensor * rows + i * CHUNK)
        low[r] = jnp.where(row < count, final[r], 0.0).astype(BF16)

    loop(rows // CHUNK, body)
    stores[0].start()
    loads[1].wait()
    stores[1].start()
    for n in range(8):
        loads[n + 2].wait()

        def body(i, n=n):
            r = at(i, 32)
            wide[n][r] = narrow[n][r].astype(F32)

        loop(narrow[n].shape[0] // 32, body)
        stores[n + 2].start()
    for store in stores:
        store.wait()


def solution(mesh):
    ranks = mesh.shape["dp"]
    groups = [[2 * k + side for k in range(ranks // 2)] for side in range(2)]
    swap = [(rank, rank + 1 - 2 * (rank % 2)) for rank in range(ranks)]
    rows, gain, column, row = P(("dp", "tensor"), None), P("dp"), P("dp", "tensor"), P("tensor", "dp")
    weights = (gain, gain, column, column, column, column, row, gain, gain, column, column, row)
    one_kernel = ranks == 8 and mesh.shape["tensor"] == 4
    return jax.shard_map(
        whole_layer if one_kernel else functools.partial(per_device, groups, swap),
        mesh=mesh,
        in_specs=(rows, rows, P("dp"), *weights),
        out_specs=(rows, rows, *weights),
        check_vma=False,
    )
```
